32 devices in a mesh: dp: 8 (over z, x), seq: 4 (over y, core).
Axes of the slice: x: 2, y: 2, z: 4, core: 2. Of those that a mesh axis runs over, the one named last changes fastest.
Arguments:
- tokens: bfloat16 [16, 1024, 1024], P('dp', 'seq'), may hold values from -6 to 6
- cotangent: bfloat16 [16, 1024, 1024], P('dp', 'seq'), may hold values from -6 to 6
- doc_ids: int32 [16, 1024], P('dp', 'seq'), may hold values from 0 to 7, never falling along the last dimension, each value on 1 to 512 neighbouring positions
- master_blocks: float32 [768, 128, 128], P('dp'), may hold values from -1.5 to 1.5
- block_of_slot: int32 [768], replicated, may hold values from 0 to 767, as said below
- left_stats: float32 [768, 128, 128], P('dp'), may hold values from -0.3 to 4, as said below
- right_stats: float32 [768, 128, 128], P('dp'), may hold values from -0.3 to 4, as said below
- left_roots: float32 [768, 128, 128], P('dp'), may hold values from -0.25 to 4, as said below
- right_roots: float32 [768, 128, 128], P('dp'), may hold values from -0.25 to 4, as said below
- vector_params: float32 [37192], replicated, may hold values from -7.7 to 2.1
- first_moment: float32 [37192], replicated, may hold values from -0.6 to 0.6
- second_moment: float32 [37192], replicated, may hold values from 0.0005 to 0.002
- adam_step: int32 [1], replicated, may hold values from 1 to 4
Outputs:
- layer_out: bfloat16 [16, 1024, 1024], P('dp', 'seq')
- grad_tokens: float32 [16, 1024, 1024], P('dp', 'seq')
- grad_blocks: float32 [768, 128, 128], P('dp')
- new_left: float32 [768, 128, 128], P('dp')
- new_right: float32 [768, 128, 128], P('dp')
- new_master: float32 [768, 128, 128], P('dp')
- master_copy: bfloat16 [768, 128, 128], P('dp')
- grad_vectors: float32 [37192], replicated
- new_vectors: float32 [37192], replicated
- new_first: float32 [37192], replicated
- new_second: float32 [37192], replicated
The draws below stay inside these ranges and needn't reach their ends.
Inputs may be any that keep to these rules, and one draw needn't show every extreme that they name: `doc_ids`: within each sequence the ids never fall; every document holds 1 to 512 tokens, and one document of each sequence holds exactly 512. `block_of_slot`: each of the 768 blocks stands in exactly one slot. `left_stats`: each block is symmetric. `right_stats`: each block is symmetric. `left_roots`: each block is symmetric. `right_roots`: each block is symmetric.
All inputs are finite; a program needn't handle non-finite values.
Results may differ from the reference program's by a relative error of at most 0.019.
Values may be sent and summed in bfloat16 or wider, within the bound.
A program may use at most 384 MiB of HBM per device.

```python
import math
import jax
import jax.numpy as jnp
import numpy as np
from jax import lax

D = 1024
HEADS_SSM = 24
HEAD = 64
NSTATE = 128
HEADS = 8
KV_HEADS = 2
FF = 2048
KERNEL = 4
SSD_BLOCK = 256
BS = 128
LEN = 1024
DOCS = 8
DOC_MOST = 512
SEQS = 16
TOKENS = 16384
NBLK = 768
NVEC = 37192


def matrix_scales():
    inner = HEADS_SSM * HEAD
    shapes = [(D, inner, 1.0), (D, inner, 1.0), (D, 2 * NSTATE, 1.0), (D, HEADS * HEAD, 1.0), (D, KV_HEADS * HEAD, 1.0), (D, KV_HEADS * HEAD, 1.0), (inner, D, 1.0), (HEADS * HEAD, D, math.sqrt(max(LEN // 16, 1))), (D, FF, 1.0), (D, FF, 1.0), (FF, D, 1.0)]
    pieces = [np.full((rows // BS * (cols // BS),), factor / math.sqrt(rows), np.float32) for rows, cols, factor in shapes]
    return np.concatenate(pieces)


def slot_order(key):
    return jax.random.permutation(jax.random.fold_in(key, 17), NBLK).astype(jnp.int32)


def draw_block_of_slot(key, part):
    return slot_order(key)


def draw_master_blocks(key, part):
    table = jnp.asarray(matrix_scales())
    noise = jax.random.truncated_normal(jax.random.fold_in(key, 3), -4.0, 4.0, (NBLK, BS, BS), jnp.float32)
    return noise * table[slot_order(key)][:, None, None]


def symmetric_blocks(key, diag_low, diag_high, off_scale):
    base = jax.random.truncated_normal(jax.random.fold_in(key, 1), -4.0, 4.0, (NBLK, BS, BS), jnp.float32)
    off_part = (base + jnp.swapaxes(base, 1, 2)) * (off_scale / math.sqrt(2.0))
    diagonal = jnp.exp(jax.random.uniform(jax.random.fold_in(key, 2), (NBLK, BS, 1), jnp.float32, math.log(diag_low), math.log(diag_high)))
    places = jnp.arange(BS)
    identity = (places[:, None] == places[None, :]).astype(jnp.float32)[None]
    return off_part * (1.0 - identity) + diagonal * identity


def draw_left_stats(key, part):
    return symmetric_blocks(jax.random.fold_in(key, 101), 0.5, 2.0, 0.05)


def draw_right_stats(key, part):
    return symmetric_blocks(jax.random.fold_in(key, 102), 0.5, 2.0, 0.05)


def draw_left_roots(key, part):
    return symmetric_blocks(jax.random.fold_in(key, 103), 0.5, 2.0, 0.04)


def draw_right_roots(key, part):
    return symmetric_blocks(jax.random.fold_in(key, 104), 0.5, 2.0, 0.04)


def draw_vector_params(key, part):
    inner = HEADS_SSM * HEAD
    channels = inner + 2 * NSTATE

    def normal_piece(index, count, scale):
        return scale * jax.random.truncated_normal(jax.random.fold_in(key, index), -4.0, 4.0, (count,), jnp.float32)

    def uniform_piece(index, count, lower, upper):
        return jax.random.uniform(jax.random.fold_in(key, index), (count,), jnp.float32, lower, upper)
    gains = [1.0 + normal_piece(201, D, 0.1), 1.0 + normal_piece(202, D, 0.1), 1.0 + normal_piece(203, inner, 0.1)]
    rates = uniform_piece(207, HEADS_SSM, math.log(0.0015), math.log(0.04))
    pieces = gains + [normal_piece(204, KERNEL * channels, 0.5), normal_piece(205, channels, 0.2), uniform_piece(206, HEADS_SSM, -1.0, 1.0), rates, uniform_piece(208, HEADS_SSM, 0.5, 1.5), normal_piece(209, D * HEADS_SSM, 1.0 / math.sqrt(D))]
    return jnp.concatenate(pieces)


def steps_of(own_key, shape, shards, smallest, high):
    factor_of = 1.0
    for axis_at, blocks in shards:
        heights = jax.random.uniform(jax.random.fold_in(jax.random.fold_in(own_key, 6), axis_at), (blocks,), jnp.float32, smallest / len(shards), high / len(shards))
        factor_of = factor_of * jnp.repeat(jnp.exp(heights), shape[axis_at] // blocks).reshape((-1,) + (1,) * (len(shape) - 1 - axis_at))
    return factor_of


def length_profile(number_of, total, limit, skew):
    portions = [(1 << 20) // math.isqrt(grade ** skew) + 1 for grade in range(2, number_of + 1)]
    rest, counts = total - limit - (number_of - 1), [1] * (number_of - 1)
    while rest > 0:
        candidates = [i for i in range(number_of - 1) if counts[i] < limit]
        mass, remaining = sum([portions[i] for i in candidates]), rest
        for i in candidates:
            more = min(limit - counts[i], max(1, remaining * portions[i] // mass), rest)
            counts[i] = counts[i] + more
            rest = rest - more
    return np.array([limit] + counts)


def uneven(rng, count, total, limit, slope):
    if count == 2:
        one = jax.random.randint(rng, (), max(1, total - limit), min(limit, total - 1) + 1)
        return jnp.stack([one, total - one])
    sizes = jnp.asarray(length_profile(count, total, limit, slope), jnp.int32)
    pairs = (count - 1) // 2
    donor, receiver = sizes[1:1 + 2 * pairs:2], sizes[2:2 + 2 * pairs:2]
    margin = jnp.minimum(donor - 1, limit - receiver)
    moved = jax.random.randint(jax.random.fold_in(rng, 1), (pairs,), 0, 1 << 20) % (margin + 1)
    sizes = sizes.at[1:1 + 2 * pairs:2].set(donor - moved).at[2:2 + 2 * pairs:2].set(receiver + moved)
    return sizes[jax.random.permutation(jax.random.fold_in(rng, 2), count)]


def scatter_about(stream_key, dims, width, most, cuts=(), held_as=jnp.bfloat16):
    level = steps_of(stream_key, dims, cuts, -0.22, 0.18) if cuts else 1.0
    drawn = jax.random.normal(stream_key, dims, jnp.float32) * width * level
    return jnp.minimum(jnp.maximum(drawn, -most), most).astype(held_as)


def setup_inputs(seed: int = 0) -> dict:
    key_of = jax.random.split(jax.random.key(seed), 14)
    return {
        "tokens": scatter_about(key_of[0], (SEQS, LEN, D), 1.0, 6.0, ((0, 8), (1, 4))),
        "cotangent": scatter_about(key_of[1], (SEQS, LEN, D), 1.0, 6.0, ((0, 8), (1, 4))),
        "doc_ids": jax.vmap(lambda own: jnp.searchsorted(jnp.cumsum(uneven(own, DOCS, LEN, DOC_MOST, 2)), jnp.arange(LEN), side="right"))(jax.random.split(key_of[2], SEQS)).reshape((SEQS, LEN)).astype(jnp.int32),
        "master_blocks": draw_master_blocks(jax.random.fold_in(key_of[13], 71), 0),
        "block_of_slot": draw_block_of_slot(jax.random.fold_in(key_of[13], 71), 0),
        "left_stats": draw_left_stats(jax.random.fold_in(key_of[13], 71), 0),
        "right_stats": draw_right_stats(jax.random.fold_in(key_of[13], 71), 0),
        "left_roots": draw_left_roots(jax.random.fold_in(key_of[13], 71), 0),
        "right_roots": draw_right_roots(jax.random.fold_in(key_of[13], 71), 0),
        "vector_params": draw_vector_params(jax.random.fold_in(key_of[13], 71), 0),
        "first_moment": scatter_about(key_of[10], (NVEC,), 0.1, 0.6, (), jnp.float32),
        "second_moment": jnp.clip(jax.random.uniform(key_of[11], (NVEC,), jnp.float32, 0.0005, 0.002), 0.0005, 0.002),
        "adam_step": jax.random.randint(key_of[12], (1,), 1, 5).astype(jnp.int32),
    }


EPS = 1e-05
THETA = 100000000000.0
LR_MATRIX = 0.02
LR_VECTOR = 0.08
BETA_ONE = 0.9
BETA_TWO = 0.999
ADAM_EPS = 1e-08
NEG_BIG = -1e+30

@jax.custom_vjp
def low(v):
    return lax.optimization_barrier(v.astype(jnp.bfloat16)).astype(jnp.float32)

@jax.custom_vjp
def low_back(v):
    return v

def low_keep(v):
    return (low(v), None)

def low_pass(kept, grad):
    return (grad,)

def back_keep(v):
    return (v, None)

def back_low(kept, grad):
    return (low(grad),)
low.defvjp(low_keep, low_pass)
low_back.defvjp(back_keep, back_low)

def matrix_table():
    inner = HEADS_SSM * HEAD
    return [('w_z', D, inner), ('w_x', D, inner), ('w_bc', D, 2 * NSTATE), ('w_query', D, HEADS * HEAD), ('w_key', D, KV_HEADS * HEAD), ('w_value', D, KV_HEADS * HEAD), ('w_mixer_out', inner, D), ('w_attn_out', HEADS * HEAD, D), ('w_gate', D, FF), ('w_up', D, FF), ('w_down', FF, D)]

def vector_shapes():
    inner = HEADS_SSM * HEAD
    channels = inner + 2 * NSTATE
    return [('gain_attn_in', (D,)), ('gain_mlp_in', (D,)), ('gain_mixer', (inner,)), ('conv_weight', (KERNEL, channels)), ('conv_bias', (channels,)), ('dt_bias', (HEADS_SSM,)), ('a_log', (HEADS_SSM,)), ('skip', (HEADS_SSM,)), ('w_dt', (D, HEADS_SSM))]

def unpack_vectors(flat):
    result = {}
    offset = 0
    for name, shape in vector_shapes():
        count = math.prod(shape)
        result[name] = flat[offset:offset + count].reshape(shape)
        offset += count
    return result

def pack_vectors(parts):
    return jnp.concatenate([parts[name].reshape(-1) for name, shape in vector_shapes()])

def assemble(blocks):
    mats = {}
    offset = 0
    for name, rows, cols in matrix_table():
        count = rows // BS * (cols // BS)
        piece = blocks[offset:offset + count].reshape(rows // BS, cols // BS, BS, BS)
        mats[name] = piece.transpose(0, 2, 1, 3).reshape(rows, cols)
        offset += count
    return mats

def disassemble(mats):
    pieces = []
    for name, rows, cols in matrix_table():
        piece = mats[name].reshape(rows // BS, BS, cols // BS, BS).transpose(0, 2, 1, 3)
        pieces.append(piece.reshape(-1, BS, BS))
    return jnp.concatenate(pieces, axis=0)

def highest(left, right):
    return jnp.dot(left, right, precision=lax.Precision.HIGHEST, preferred_element_type=jnp.float32)

def rms_scale(values):
    return lax.rsqrt(lax.optimization_barrier(jnp.mean(values * values, axis=-1, keepdims=True)) + EPS)

def gate_norm(values, gate_z, gain):
    gated = values * jax.nn.silu(gate_z)
    return gated * rms_scale(gated) * gain

def rope_tables(positions):
    half = HEAD // 2
    frequency = jnp.exp(jnp.arange(half, dtype=jnp.float32) * (-2.0 * math.log(THETA) / HEAD))
    angles = positions[:, None] * frequency[None, :]
    return (jnp.cos(angles), jnp.sin(angles))

def rotate(values, cosine, sine):
    half = values.shape[-1] // 2
    front = values[..., :half]
    back = values[..., half:]
    cosine = cosine[:, None, :]
    sine = sine[:, None, :]
    return jnp.concatenate([front * cosine - back * sine, back * cosine + front * sine], axis=-1)

def decay_terms(delta_raw, dt_bias, a_log):
    delta = jax.nn.softplus(delta_raw + dt_bias)
    return (delta, delta * -jnp.exp(a_log))

def state_terms(ssm_in, b_proj, delta_raw, dt_bias, a_log, labels, link_last):
    delta, decay_log = decay_terms(delta_raw, dt_bias, a_log)
    cumulative = jnp.cumsum(decay_log, axis=0)
    same_end = (labels == labels[-1]).astype(jnp.float32)
    weights = jnp.exp(cumulative[-1][None, :] - cumulative) * same_end[:, None] * delta
    local_state = jnp.einsum('sh,shp,sn->hpn', weights, ssm_in, b_proj, precision=lax.Precision.HIGHEST)
    factor = jnp.exp(cumulative[-1]) * link_last
    return (factor, local_state)

def output_terms(ssm_in, b_proj, c_proj, delta_raw, dt_bias, a_log, skip, incoming, labels, link):
    delta, decay_log = decay_terms(delta_raw, dt_bias, a_log)
    cumulative = jnp.cumsum(decay_log, axis=0)
    places = jnp.arange(labels.shape[0])
    same = (labels[:, None] == labels[None, :]) & (places[:, None] >= places[None, :])
    gaps = jnp.where(same[:, :, None], cumulative[:, None, :] - cumulative[None, :, :], 0.0)
    decay_matrix = jnp.where(same[:, :, None], jnp.exp(gaps), 0.0)
    affinity = jnp.dot(c_proj, b_proj.T, precision=lax.Precision.HIGHEST, preferred_element_type=jnp.float32)
    weights = affinity[:, :, None] * decay_matrix * delta[None, :, :]
    within = jnp.einsum('tsh,shp->thp', weights, ssm_in, precision=lax.Precision.HIGHEST)
    carried = jnp.einsum('hpn,tn->thp', incoming, c_proj, precision=lax.Precision.HIGHEST)
    carried = carried * (jnp.exp(cumulative) * link[:, None])[:, :, None]
    return within + carried + skip[None, :, None] * ssm_in

def mixer_scan(ssm_in, b_proj, c_proj, delta_raw, dt_bias, a_log, skip, labels):
    length = labels.shape[0]
    count = length // SSD_BLOCK

    def one_block(carry, pieces):
        state, previous = carry
        part_in, part_b, part_c, part_delta, part_labels = pieces
        link = (part_labels == previous).astype(jnp.float32)
        output = output_terms(part_in, part_b, part_c, part_delta, dt_bias, a_log, skip, state, part_labels, link)
        factor, local_state = state_terms(part_in, part_b, part_delta, dt_bias, a_log, part_labels, link[-1])
        return ((factor[:, None, None] * state + local_state, part_labels[-1]), output)
    start = (jnp.zeros((HEADS_SSM, HEAD, NSTATE), jnp.float32), jnp.full((), -1, jnp.int32))
    pieces = (ssm_in.reshape(count, SSD_BLOCK, HEADS_SSM, HEAD), b_proj.reshape(count, SSD_BLOCK, NSTATE), c_proj.reshape(count, SSD_BLOCK, NSTATE), delta_raw.reshape(count, SSD_BLOCK, HEADS_SSM), labels.reshape(count, SSD_BLOCK))
    final, outputs = lax.scan(jax.checkpoint(one_block), start, pieces)
    return outputs.reshape(length, HEADS_SSM, HEAD)

def layer_forward(inputs, mats, vectors, labels):
    length = inputs.shape[0]
    inner = HEADS_SSM * HEAD
    groups = HEADS // KV_HEADS
    reach = KERNEL - 1
    normed_in = low(inputs * rms_scale(inputs) * vectors['gain_attn_in'])
    gate_z = low_back(highest(normed_in, mats['w_z']))
    conv_in = low(low_back(highest(normed_in, jnp.concatenate([mats['w_x'], mats['w_bc']], axis=1))))
    delta_raw = low_back(highest(normed_in, low(vectors['w_dt'])))
    padded = jnp.concatenate([jnp.zeros((reach, conv_in.shape[1]), jnp.float32), conv_in], axis=0)
    padded_labels = jnp.concatenate([jnp.full((reach,), -1, jnp.int32), labels])
    conv_acc = vectors['conv_bias'][None, :]
    for tap in range(KERNEL):
        mask = (padded_labels[tap:tap + length] == labels).astype(jnp.float32)[:, None]
        conv_acc = conv_acc + vectors['conv_weight'][tap][None, :] * padded[tap:tap + length] * mask
    activated = jax.nn.silu(conv_acc)
    ssm_in = low(activated[:, :inner]).reshape(length, HEADS_SSM, HEAD)
    b_proj = low(activated[:, inner:inner + NSTATE])
    c_proj = low(activated[:, inner + NSTATE:])
    mixed_ssm = mixer_scan(ssm_in, b_proj, c_proj, delta_raw, vectors['dt_bias'], vectors['a_log'], vectors['skip'], labels)
    normed_ssm = low(gate_norm(mixed_ssm.reshape(length, inner), gate_z, vectors['gain_mixer']))
    mixer_out = low_back(highest(normed_ssm, mats['w_mixer_out']))
    places = jnp.arange(length)
    before = lax.optimization_barrier(jnp.sum((labels[None, :] < labels[:, None]).astype(jnp.int32), axis=1))
    positions = (places - before).astype(jnp.float32)
    cosine, sine = rope_tables(positions)
    query = low(rotate(low_back(highest(normed_in, mats['w_query'])).reshape(length, HEADS, HEAD), cosine, sine))
    key_heads = low(rotate(low_back(highest(normed_in, mats['w_key'])).reshape(length, KV_HEADS, HEAD), cosine, sine))
    value_heads = low(low_back(highest(normed_in, mats['w_value']))).reshape(length, KV_HEADS, HEAD)
    query_heads = query.reshape(length, KV_HEADS, groups, HEAD)
    scores = low_back(jnp.einsum('tkgd,jkd->kgtj', query_heads, key_heads, precision=lax.Precision.HIGHEST) * (1.0 / math.sqrt(HEAD)))
    valid = (labels[:, None] == labels[None, :]) & (places[:, None] >= places[None, :])
    probs = jax.nn.softmax(jnp.where(valid, scores, NEG_BIG), axis=-1)
    context = jnp.einsum('kgtj,jkd->tkgd', low(probs), value_heads, precision=lax.Precision.HIGHEST).reshape(length, HEADS * HEAD)
    attn_out = low_back(highest(low(low_back(context)), mats['w_attn_out']))
    hidden = inputs + mixer_out + attn_out
    normed_mid = low(hidden * rms_scale(hidden) * vectors['gain_mlp_in'])
    gate = low_back(highest(normed_mid, mats['w_gate']))
    upper = low_back(highest(normed_mid, mats['w_up']))
    mixed = low(jax.nn.silu(gate) * upper)
    return hidden + low_back(highest(mixed, mats['w_down']))

def reference(tokens, cotangent, doc_ids, master_blocks, block_of_slot, left_stats, right_stats, left_roots, right_roots, vector_params, first_moment, second_moment, adam_step):
    inverse = jnp.argsort(block_of_slot).astype(jnp.int32)
    mats = assemble(jnp.take(master_blocks, inverse, axis=0))
    vectors = unpack_vectors(vector_params)

    def sequence_step(totals, item):
        row, cotan_row, label_row = item

        def run(inputs, weights, vector_dict):
            lowered = {name: low(value) for name, value in weights.items()}
            return layer_forward(inputs, lowered, vector_dict, label_row)
        result, pull = jax.vjp(run, row.astype(jnp.float32), mats, vectors)
        grad_in, grad_mats, grad_vecs = pull(cotan_row.astype(jnp.float32))
        totals = jax.tree.map(jnp.add, totals, (grad_mats, grad_vecs))
        return (totals, (result.astype(jnp.bfloat16), grad_in))
    zeros = jax.tree.map(jnp.zeros_like, (mats, vectors))
    totals, outputs = lax.scan(sequence_step, zeros, (tokens, cotangent, doc_ids))
    grad_mats, grad_vecs = totals
    layer_out, grad_tokens = outputs
    norm = 1.0 / math.sqrt(TOKENS)
    grad_blocks = jnp.take(disassemble(grad_mats), block_of_slot, axis=0) * norm
    new_left = 0.5 * left_stats + 0.5 * jnp.einsum('bij,bkj->bik', grad_blocks, grad_blocks, precision=lax.Precision.HIGHEST) / BS
    new_right = 0.5 * right_stats + 0.5 * jnp.einsum('bji,bjk->bik', grad_blocks, grad_blocks, precision=lax.Precision.HIGHEST) / BS
    inner_product = jnp.einsum('bij,bjk->bik', grad_blocks, right_roots, precision=lax.Precision.HIGHEST)
    direction = jnp.einsum('bij,bjk->bik', left_roots, inner_product, precision=lax.Precision.HIGHEST)
    new_master = master_blocks - LR_MATRIX * direction
    grad_vectors = pack_vectors(grad_vecs) * norm
    step_value = adam_step[0].astype(jnp.float32)
    new_first = BETA_ONE * first_moment + (1.0 - BETA_ONE) * grad_vectors
    new_second = BETA_TWO * second_moment + (1.0 - BETA_TWO) * grad_vectors * grad_vectors
    first_hat = new_first / (1.0 - jnp.power(BETA_ONE, step_value))
    second_hat = new_second / (1.0 - jnp.power(BETA_TWO, step_value))
    new_vectors = vector_params - LR_VECTOR * first_hat / (jnp.sqrt(second_hat) + ADAM_EPS)
    return (layer_out, grad_tokens, grad_blocks, new_left, new_right, new_master, new_master.astype(jnp.bfloat16), grad_vectors, new_vectors, new_first, new_second)
```

```python
import functools
import math

import jax
import jax.numpy as jnp
from jax import lax
from jax.experimental import pallas as pl
from jax.experimental.pallas import tpu as pltpu
from jax.sharding import PartitionSpec as P

D = 1024
HEADS_SSM = 24
HEAD = 64
NSTATE = 128
HEADS = 8
KV_HEADS = 2
FF = 2048
KERNEL = 4
BS = 128
DOC_MOST = 512
INNER = HEADS_SSM * HEAD
CHANNELS = INNER + 2 * NSTATE
REACH = KERNEL - 1
QDIM = HEADS * HEAD
KDIM = KV_HEADS * HEAD
LANES = 128
PAIRS = INNER // LANES

EPS = 1e-05
THETA = 100000000000.0
LR_MATRIX = 0.02
LR_VECTOR = 0.08
BETA_ONE = 0.9
BETA_TWO = 0.999
ADAM_EPS = 1e-08
NEG_BIG = -1e30
F32 = jnp.float32
BF16 = jnp.bfloat16
HIGHEST = lax.Precision.HIGHEST
VMEM_MOST = 60 << 20

SHAPES = (
    (D, INNER), (D, INNER), (D, 2 * NSTATE), (D, QDIM), (D, KDIM), (D, KDIM),
    (INNER, D), (QDIM, D), (D, FF), (D, FF), (FF, D),
)
WIDE_IN, TALL_OUT, WIDE_FF, TALL_FF = (0, 1, 2, 3, 4, 5), (6, 7), (8, 9), (10,)
SIZES = (D, D, INNER, KERNEL * CHANNELS, CHANNELS, HEADS_SSM, HEADS_SSM, HEADS_SSM, D * HEADS_SSM)


def block_offsets():
    starts, total = [], 0
    for rows, cols in SHAPES:
        starts.append(total)
        total += rows // BS * (cols // BS)
    return starts


def wide_order(members):
    starts = block_offsets()
    rows = SHAPES[members[0]][0] // BS
    return [starts[m] + r * (SHAPES[m][1] // BS) + q for r in range(rows) for m in members for q in range(SHAPES[m][1] // BS)]


def tall_order(members):
    starts = block_offsets()
    return [starts[m] + i for m in members for i in range(SHAPES[m][0] // BS * (SHAPES[m][1] // BS))]


def all_orders():
    return [wide_order(WIDE_IN), tall_order(TALL_OUT), wide_order(WIDE_FF), tall_order(TALL_FF)]


def unpack_vectors(flat):
    result, offset = [], 0
    for count in SIZES:
        result.append(flat[offset : offset + count])
        offset += count
    return result


def dot(left, right, precision=None):
    return jnp.dot(left, right, preferred_element_type=F32, precision=precision)


def dot_nt(left, right):
    return lax.dot_general(left, right, (((1,), (1,)), ((), ())), preferred_element_type=F32)


def dot_tn(left, right):
    return lax.dot_general(left, right, (((0,), (0,)), ((), ())), preferred_element_type=F32)


def sigmoid(v):
    return 1.0 / (1.0 + jnp.exp(-v))


def rms_scale(values):
    return lax.rsqrt(jnp.mean(values * values, axis=-1, keepdims=True) + EPS)


def kernel_params(**more):
    return pltpu.CompilerParams(vmem_limit_bytes=VMEM_MOST, **more)


def whole(shape):
    return pl.BlockSpec(shape, lambda *_: (0,) * len(shape))


MESH = pl.DeviceIdType.MESH
CORES = 2


def grid_of(mesh):
    try:
        wide = len({device.coords[0] for device in mesh.devices.flat})
    except AttributeError:
        wide = mesh.shape["seq"] // CORES
    return wide, mesh.shape["seq"] // CORES, mesh.shape["dp"] // wide


def parts_of(slots, tall):
    half = slots // CORES
    lone = half * 17 // 48 if tall == 2 and half >= 16 else 0
    return half, lone, half - lone


def place(grid):
    wide, tall, deep = grid
    dp, seq = lax.axis_index("dp"), lax.axis_index("seq")
    return dp % wide, seq // CORES, dp // wide, seq % CORES


def gather_kernel(grid, slots, src, out, kept, sem_own, sz, rz, sx, rx, sy, ry, sc, rc):
    wide, tall, deep = grid
    x, y, z, c = place(grid)
    half, lone, bulk = parts_of(slots, tall)
    me = z * wide + x
    seq = y * CORES + c
    base = c * half
    bulk_at = base + y * (half - bulk)
    lone_at = base + y * bulk
    other_at = base + (1 - y) * bulk if lone else base
    mate = y * CORES + (1 - c)
    over = (tall - 1 - y) * CORES + c

    barrier = pltpu.get_barrier_semaphore()
    count = jnp.int32(0)
    for axis, at, size in (("z", z, deep), ("x", x, wide)):
        for step in (1, -1):
            ok = (at + step >= 0) & (at + step < size)
            there = me + step * (wide if axis == "z" else 1)

            @pl.when(ok)
            def _(there=there):
                pl.semaphore_signal(barrier, inc=1, device_id=(there, seq), device_id_type=MESH)

            count = count + ok.astype(jnp.int32)
    pl.semaphore_signal(barrier, inc=1, device_id=(me, mate), device_id_type=MESH)
    count = count + 1
    if lone:
        pl.semaphore_signal(barrier, inc=1, device_id=(me, over), device_id_type=MESH)
        count = count + 1
    pl.semaphore_wait(barrier, count)

    take = pltpu.make_async_copy(src, kept, sem_own.at[0])
    take.start()
    sent = []

    def send(ok, source, target, send_sem, recv_sem, device):
        copy = pltpu.make_async_remote_copy(
            src_ref=source, dst_ref=target, send_sem=send_sem, recv_sem=recv_sem,
            device_id=device, device_id_type=MESH,
        )

        @pl.when(ok)
        def _():
            copy.start()

        sent.append((ok, copy))

    def arrived(ok, target, recv_sem):
        copy = pltpu.make_async_remote_copy(
            src_ref=target, dst_ref=target, send_sem=sem_own.at[0], recv_sem=recv_sem,
            device_id=(me, seq), device_id_type=MESH,
        )

        @pl.when(ok)
        def _():
            copy.wait_recv()

    yes = jnp.bool_(True)

    def piece(shard, at, size):
        return out.at[shard, pl.ds(at, size)]

    def pass_on(ok, shard):
        send(ok, piece(shard, bulk_at, bulk), piece(shard, bulk_at, bulk), sc.at[0, shard], rc.at[0, shard], (me, mate))
        if lone:
            send(ok, piece(shard, lone_at, lone), piece(shard, lone_at, lone), sy.at[shard], ry.at[shard], (me, over))

    def along_x(ok, zs, dirs, hop, own):
        for d, step in dirs:
            shard = zs * wide + x - step * hop
            go = ok & (x + step >= 0) & (x + step < wide)
            source = src.at[pl.ds(bulk_at, bulk)] if own else piece(shard, bulk_at, bulk)
            send(go, source, piece(shard, bulk_at, bulk), sx.at[d, hop, zs], rx.at[d, hop + 1, zs], (me + step, seq))

    both = ((0, 1), (1, -1))

    def columns(s):
        return [(yes, z)] if s == 0 else [((z - step * s >= 0) & (z - step * s < deep), z - step * s) for _, step in both]

    def x_in(s, hop):
        for ok, zs in columns(s):
            for d, step in both:
                from_x = x - step * hop
                come = ok & (from_x >= 0) & (from_x < wide)
                shard = zs * wide + from_x
                arrived(come, piece(shard, bulk_at, bulk), rx.at[d, hop, zs])
                along_x(come, zs, ((d, step),), hop, False)
                pass_on(come, shard)

    def y_in(ok, shard):
        if lone:
            arrived(ok, piece(shard, other_at, lone), ry.at[shard])
            send(ok, piece(shard, other_at, lone), piece(shard, other_at, lone), sc.at[1, shard], rc.at[1, shard], (me, mate))

    def y_all(s):
        for ok, zs in columns(s):
            if s > 0:
                y_in(ok, zs * wide + x)
            for hop in range(1, wide):
                for _, step in both:
                    from_x = x - step * hop
                    y_in(ok & (from_x >= 0) & (from_x < wide), zs * wide + from_x)

    for s in range(deep):
        for d, step in both:
            zs = z - step * s
            ok = (zs >= 0) & (zs < deep)
            shard = zs * wide + x
            if s:
                arrived(ok, piece(shard, bulk_at, bulk), rz.at[d, s])
            go = ok & (z + step >= 0) & (z + step < deep)
            source = piece(shard, bulk_at, bulk) if s else src.at[pl.ds(bulk_at, bulk)]
            if s + 1 < deep:
                send(go, source, piece(shard, bulk_at, bulk), sz.at[d, s], rz.at[d, s + 1], (me + step * wide, seq))
            if s:
                along_x(ok, zs, both, 0, False)
                pass_on(ok, shard)
        if s == 0:
            along_x(yes, z, both, 0, True)
            take.wait()
            put = pltpu.make_async_copy(kept, out.at[me], sem_own.at[1])
            put.start()
        else:
            for hop in range(1, wide):
                x_in(s - 1, hop)
        if s >= 2:
            y_all(s - 2)
    for hop in range(1, wide):
        x_in(deep - 1, hop)
    for s in range(max(deep - 2, 0), deep):
        y_all(s)
    put.wait()

    mate_base = (1 - c) * half
    mate_bulk = mate_base + y * (half - bulk)
    mate_other = mate_base + (1 - y) * bulk if lone else mate_base

    def last(shard, _):
        ok = shard != me
        arrived(ok, piece(shard, mate_bulk, bulk), rc.at[0, shard])
        if lone:
            arrived(ok, piece(shard, mate_other, lone), rc.at[1, shard])
        return 0

    lax.fori_loop(0, wide * deep, last, 0)
    for ok, copy in sent:
        @pl.when(ok)
        def _(copy=copy):
            copy.wait_send()


def gather_blocks(grid, own):
    wide, tall, deep = grid
    slots = own.shape[0]
    n = wide * deep
    sem = pltpu.SemaphoreType.DMA
    return pl.pallas_call(
        functools.partial(gather_kernel, grid, slots),
        out_shape=jax.ShapeDtypeStruct((n,) + own.shape, own.dtype),
        in_specs=[pl.BlockSpec(memory_space=pl.ANY)],
        out_specs=pl.BlockSpec(memory_space=pl.ANY),
        scratch_shapes=[
            pltpu.VMEM(own.shape, own.dtype),
            sem((2,)),
            sem((2, deep)), sem((2, deep + 1)),
            sem((2, wide, deep)), sem((2, wide + 1, deep)),
            sem((n,)), sem((n,)),
            sem((2, n)), sem((2, n)),
        ],
        compiler_params=pltpu.CompilerParams(collective_id=0, has_side_effects=True),
        name="gather_blocks",
    )(own)

def far_first(at, size, i):
    above, below = size - 1 - at, at
    less, more = jnp.minimum(above, below), jnp.maximum(above, below)
    long_side = jnp.where(above >= below, 1, -1)
    j = i - (more - less)
    near = at + jnp.where(j % 2 == 0, 1, -1) * (less - j // 2)
    return jnp.where(j < 0, at + long_side * (more - i), near)


def entry(at, size, source_below, target):
    lower = jnp.where(at > 0, size - at, 0) if size > 2 else 0
    return target - at if source_below else lower + at - target


def entries(size):
    return size + 1 if size > 2 else 1

SUBS = 2
LAG = 2
LONE = 1 / 3


def split_of(slots, tall):
    half = slots // CORES
    piece = half // SUBS
    lone = round(piece * LONE) if tall == 2 and piece >= 8 else 0
    return half, piece, lone, piece - lone


def reduce_kernel(grid, slots, part, vec, out, vec_out, acc, land_c, land_y, land_x, land_z, fin, vbuf, vland,
                  s_load, s_c, r_c, s_y, r_y, s_x, r_x, s_z, r_z, s_f, r_f, s_m, r_m, s_v, r_v):
    wide, tall, deep = grid
    n = wide * deep
    x, y, z, c = place(grid)
    half, size, lone, bulk = split_of(slots, tall)
    me = z * wide + x
    seq = y * CORES + c
    mate = y * CORES + (1 - c)
    bulk_at = y * lone
    lone_at = y * bulk
    other_at = (1 - y) * bulk
    bits = lambda size: [1 << b for b in range(size.bit_length() - 1)]
    partners = [(me, mate)]
    partners += [(me, (y ^ b) * CORES + c) for b in bits(tall)]
    partners += [(z * wide + (x ^ b), seq) for b in bits(wide)]
    partners += [((z ^ b) * wide + x, seq) for b in bits(deep)]

    barrier = pltpu.get_barrier_semaphore()
    count = jnp.int32(0)
    for step_by, at, length in ((wide, z, deep), (1, x, wide)):
        for step in (1, -1):
            ok = (at + step >= 0) & (at + step < length)

            @pl.when(ok)
            def _(there=me + step * step_by):
                pl.semaphore_signal(barrier, inc=1, device_id=(there, seq), device_id_type=MESH)

            count = count + ok.astype(jnp.int32)
    for device in partners:
        pl.semaphore_signal(barrier, inc=1, device_id=device, device_id_type=MESH)
    pl.semaphore_wait(barrier, count + len(partners))

    def remote(source, target, send_sem, recv_sem, device):
        return pltpu.make_async_remote_copy(
            src_ref=source, dst_ref=target, send_sem=send_sem, recv_sem=recv_sem,
            device_id=device, device_id_type=MESH,
        )

    def landed(target, recv_sem):
        remote(target, target, s_load.at[0], recv_sem, (me, seq)).wait_recv()

    group = wide * SUBS
    total = n * SUBS

    def item_of(k):
        xs, zs = far_first(x, wide, k % wide), far_first(z, deep, k // group)
        sub = (k // wide) % SUBS
        return xs, zs, sub, (zs * wide + xs) * SUBS + sub

    def own(k):
        xs, zs, sub, item = item_of(k)
        return pltpu.make_async_copy(part.at[zs * wide + xs, pl.ds(c * half + sub * size, size)], acc.at[item], s_load.at[item])

    def swap(k):
        xs, zs, sub, item = item_of(k)
        source = part.at[zs * wide + xs, pl.ds((1 - c) * half + sub * size, size)]
        return remote(source, land_c.at[item], s_c.at[item], r_c.at[item], (me, mate))

    def cross(item):
        return remote(acc.at[item, pl.ds(other_at, lone)], land_y.at[item], s_y.at[item], r_y.at[item], (me, (tall - 1 - y) * CORES + c))

    def begin(k, _):
        own(k).start()
        swap(k).start()
        return 0

    rounds = len(partners)

    def vec_copy(t):
        return remote(vbuf.at[t], vland.at[t], s_v.at[t], r_v.at[t], partners[t])

    vbuf[0] = vec[...]
    vec_copy(0).start()
    lax.fori_loop(0, total, begin, 0)
    for t in range(rounds):
        landed(vland.at[t], r_v.at[t])
        vbuf[t + 1] = vbuf[t] + vland[t]
        if t + 1 < rounds:
            vec_copy(t + 1).start()
    vec_out[...] = vbuf[rounds]

    def add(item, at, count, ref, first):
        def one(i, _):
            acc[item, at + i] = acc[item, at + i] + ref[first + (i,)]
            return 0

        lax.fori_loop(0, count, one, 0, unroll=4)

    def step_x(k, begin_it):
        xs, zs, sub, item = item_of(k)
        for below, step in ((True, 1), (False, -1)):
            to = entry(x + step, wide, below, xs)
            sent = remote(acc.at[item, pl.ds(bulk_at, bulk)], land_x.at[to, zs * SUBS + sub], s_x.at[item],
                          r_x.at[to, zs * SUBS + sub], (me + step, seq))

            @pl.when((xs - x) * step > 0)
            def _():
                if begin_it:
                    sent.start()
                else:
                    sent.wait_send()

    def take_x(k):
        xs, zs, sub, item = item_of(k)
        for below, step in ((True, 1), (False, -1)):
            comes = ((xs - x) * step >= 0) & (x - step >= 0) & (x - step < wide)
            at = entry(x, wide, below, xs)

            @pl.when(comes)
            def _():
                landed(land_x.at[at, zs * SUBS + sub], r_x.at[at, zs * SUBS + sub])
                add(item, bulk_at, bulk, land_x, (at, zs * SUBS + sub))

    def step_z(k, begin_it):
        xs, zs, sub, item = item_of(k)
        for below, step in ((True, 1), (False, -1)):
            to = entry(z + step, deep, below, zs)
            sent = remote(acc.at[item, pl.ds(bulk_at, bulk)], land_z.at[to, sub], s_z.at[zs * SUBS + sub], r_z.at[to, sub],
                          (me + step * wide, seq))

            @pl.when((zs - z) * step > 0)
            def _():
                if begin_it:
                    sent.start()
                else:
                    sent.wait_send()

    def take_z(k):
        xs, zs, sub, item = item_of(k)
        for below, step in ((True, 1), (False, -1)):
            comes = ((zs - z) * step >= 0) & (z - step >= 0) & (z - step < deep)
            at = entry(z, deep, below, zs)

            @pl.when(comes)
            def _():
                landed(land_z.at[at, sub], r_z.at[at, sub])
                add(item, bulk_at, bulk, land_z, (at, sub))

    planes = bits(tall)

    def swap_plane(t, sub):
        mine = pl.ds(bulk_at, bulk)
        return remote(acc.at[me * SUBS + sub, mine], fin.at[t, sub, mine], s_f.at[t, sub], r_f.at[t, sub], (me, (y ^ planes[t]) * CORES + c))

    def take_plane(t, sub):
        item = me * SUBS + sub
        theirs = pl.ds((1 - y) * lone if lone else 0, bulk)
        landed(fin.at[t, sub, theirs], r_f.at[t, sub])
        swap_plane(t, sub).wait_send()
        add(item, lone, size - 2 * lone, fin.at[t, sub, pl.ds(lone, size - 2 * lone)], ())
        if lone:
            cross(item).wait_send()
            acc[item, pl.ds(other_at, lone)] = fin[t, sub, pl.ds(other_at, lone)]

    def swap_core(sub):
        return remote(acc.at[me * SUBS + sub], out.at[pl.ds(c * half + sub * size, size)], s_m.at[sub], r_m.at[sub], (me, mate))

    def first(k, _):
        item = item_of(k)[3]
        own(k).wait()
        landed(land_c.at[item], r_c.at[item])
        add(item, 0, size, land_c, (item,))
        if lone:
            cross(item).start()
        return 0

    def second(k, _):
        @pl.when(k < total)
        def _():
            item = item_of(k)[3]
            if lone:
                landed(land_y.at[item], r_y.at[item])
                add(item, lone_at, lone, land_y, (item,))
            if wide > 2:
                @pl.when(item_of(k)[0] != x)
                def _():
                    take_x(k)
            step_x(k, True)

        late = k - LAG * wide

        @pl.when((late >= 0) & (late % wide == wide - 1))
        def _():
            take_x(late)
            take_z(late)
            step_z(late, True)

        return 0

    lax.fori_loop(0, total, first, 0)
    lax.fori_loop(0, total + (LAG - 1) * wide, second, 0)
    def finish(k, _):
        swap(k).wait_send()
        if lone:
            item = item_of(k)[3]

            @pl.when(item // SUBS != me)
            def _():
                cross(item).wait_send()

        step_x(k, False)

        @pl.when(k % wide == wide - 1)
        def _():
            step_z(k, False)

        return 0

    tail = [total + (LAG - 1) * wide + i for i in range(wide)]
    for k in tail:
        second(jnp.int32(k), 0)
    for t in range(len(planes)):
        for sub in range(SUBS):
            swap_plane(t, sub).start()
        for sub in range(SUBS):
            take_plane(t, sub)
            if t == len(planes) - 1:
                swap_core(sub).start()
    for sub in range(SUBS):
        out[pl.ds(c * half + sub * size, size)] = acc[me * SUBS + sub]
    lax.fori_loop(0, total, finish, 0)
    for t in range(rounds):
        vec_copy(t).wait_send()
    for sub in range(SUBS):
        swap_core(sub).wait_send()
        landed(out.at[pl.ds((1 - c) * half + sub * size, size)], r_m.at[sub])


def reduce_blocks(grid, part, vec):
    wide, tall, deep = grid
    n, slots = part.shape[:2]
    half, size, lone, bulk = split_of(slots, tall)
    tile = part.shape[2:]
    sem = pltpu.SemaphoreType.DMA
    rounds = sum(length.bit_length() - 1 for length in (CORES, wide, tall, deep))
    planes = max(tall.bit_length() - 1, 1)
    items = n * SUBS
    buf = lambda *lead: pltpu.VMEM(lead + tile, part.dtype)
    return pl.pallas_call(
        functools.partial(reduce_kernel, grid, slots),
        out_shape=(jax.ShapeDtypeStruct((slots,) + tile, part.dtype), jax.ShapeDtypeStruct(vec.shape, vec.dtype)),
        in_specs=[pl.BlockSpec(memory_space=pl.ANY), pl.BlockSpec(memory_space=pltpu.VMEM)],
        out_specs=(pl.BlockSpec(memory_space=pltpu.VMEM), pl.BlockSpec(memory_space=pltpu.VMEM)),
        scratch_shapes=[
            buf(items, size), buf(items, size), buf(items, max(lone, 1)), buf(entries(wide), deep * SUBS, bulk),
            buf(entries(deep), SUBS, bulk), buf(planes, SUBS, size),
            pltpu.VMEM((rounds + 1,) + vec.shape, vec.dtype), pltpu.VMEM((rounds,) + vec.shape, vec.dtype),
            sem((items,)), sem((items,)), sem((items,)), sem((items,)), sem((items,)), sem((items,)),
            sem((entries(wide), deep * SUBS)), sem((deep * SUBS,)), sem((entries(deep), SUBS)),
            sem((planes, SUBS)), sem((planes, SUBS)), sem((SUBS,)), sem((SUBS,)), sem((rounds,)), sem((rounds,)),
        ],
        compiler_params=pltpu.CompilerParams(collective_id=1, has_side_effects=True, vmem_limit_bytes=63 << 20),
        name="reduce_blocks",
    )(part, vec)


STEP_BLOCKS = 32
DEPTH = 4


def assemble_kernel(table, blocks, w_in, w_out, w_ff, w_down, wide, tall, s_in, s_out):
    outs = []
    for ref in (w_in, w_out, w_ff, w_down):
        rows, cols = ref.shape
        per_row = cols // BS
        deep = STEP_BLOCKS // per_row
        for r in range(rows // (BS * deep)):
            outs.append((ref, r * BS * deep, deep, per_row))

    def target(step):
        ref, at, deep, per_row = outs[step]
        slot = step % DEPTH
        return (wide.at[slot] if deep == 1 else tall.at[slot]), ref.at[pl.ds(at, BS * deep)], deep, per_row

    def fetch(step):
        buffer, _, deep, per_row = target(step)

        def one(i, _):
            rows = pl.ds(pl.multiple_of(i // per_row * BS, BS), BS)
            cols = pl.ds(pl.multiple_of(i % per_row * BS, BS), BS)
            pltpu.make_async_copy(blocks.at[table[step * STEP_BLOCKS + i]], buffer.at[rows, cols], s_in.at[step % DEPTH]).start()
            return 0

        lax.fori_loop(0, STEP_BLOCKS, one, 0)

    def put(step):
        buffer, place_to, _, _ = target(step)
        return pltpu.make_async_copy(buffer, place_to, s_out.at[step % DEPTH])

    steps = len(outs)
    for step in range(min(DEPTH - 1, steps)):
        fetch(step)
    for step in range(steps):
        buffer, place_to, _, _ = target(step)
        pltpu.make_async_copy(place_to, buffer, s_in.at[step % DEPTH]).wait()
        put(step).start()
        ahead = step + DEPTH - 1
        if ahead < steps:
            if step >= 1:
                put(step - 1).wait()
            fetch(ahead)
    for step in range(max(steps - DEPTH, 0), steps):
        put(step).wait()


def assemble(blocks, inverse):
    table = jnp.take(inverse, jnp.array(sum(all_orders(), []), jnp.int32))
    shapes = [(D, sum(SHAPES[m][1] for m in WIDE_IN)), (sum(SHAPES[m][0] for m in TALL_OUT), D), (D, 2 * FF), (FF, D)]
    hbm = pl.BlockSpec(memory_space=pl.ANY)
    return pl.pallas_call(
        assemble_kernel,
        out_shape=tuple(jax.ShapeDtypeStruct(shape, BF16) for shape in shapes),
        grid_spec=pltpu.PrefetchScalarGridSpec(
            num_scalar_prefetch=1, grid=(1,), in_specs=[hbm], out_specs=(hbm,) * 4,
            scratch_shapes=[
                pltpu.VMEM((DEPTH, BS, STEP_BLOCKS * BS), BF16),
                pltpu.VMEM((DEPTH, STEP_BLOCKS // (D // BS) * BS, D), BF16),
                pltpu.SemaphoreType.DMA((DEPTH,)), pltpu.SemaphoreType.DMA((DEPTH,)),
            ],
        ),
        compiler_params=kernel_params(),
        name="assemble",
    )(table, blocks)


GROUP = 32


def slot_grads_kernel(left_at, right_at, ins, mids, downs, outs, g_in, g_hidden, g_ff, cot, out, left, right):
    at = 0

    @pl.when(pl.program_id(0) == 0)
    def _():
        at = 0
        for ref in (ins, outs, mids, downs):
            for q in range(ref.shape[1] // BS):
                left[at : at + BS, :] = ref[:, q * BS : (q + 1) * BS].T
                at += BS
        at = 0
        for ref in (g_in, g_hidden, g_ff, cot):
            cols = ref.shape[1]
            right[:, at : at + cols] = ref[...]
            at += cols

    base = pl.program_id(0) * GROUP

    def one(i, _):
        rows = pl.ds(pl.multiple_of(left_at[base + i] * BS, BS), BS)
        cols = pl.ds(pl.multiple_of(right_at[base + i] * BS, BS), BS)
        out[i] = dot(left[rows, :], right[:, cols]).astype(BF16)
        return 0

    lax.fori_loop(0, GROUP, one, 0, unroll=4)


def grad_tables():
    lefts, rights = [], []
    left_base = {0: 0, 1: D, 2: D + INNER + QDIM, 3: 2 * D + INNER + QDIM}
    right_base = {0: 0, 1: 2 * INNER + 2 * NSTATE + QDIM + 2 * KDIM}
    right_base[2] = right_base[1] + D
    right_base[3] = right_base[2] + 2 * FF
    for kind, members in enumerate((WIDE_IN, TALL_OUT, WIDE_FF, TALL_FF)):
        row_at, col_at = left_base[kind] // BS, right_base[kind] // BS
        for m in members:
            rows, cols = SHAPES[m][0] // BS, SHAPES[m][1] // BS
            for r in range(rows):
                for q in range(cols):
                    lefts.append(row_at + r)
                    rights.append(col_at + q)
            if kind in (0, 2):
                col_at += cols
            else:
                row_at += rows
    return lefts, rights


def slot_grads(block_of_slot, ins, mids, downs, outs, g_in, g_hidden, g_ff, cot):
    lefts, rights = grad_tables()
    left_at = jnp.take(jnp.array(lefts, jnp.int32), block_of_slot)
    right_at = jnp.take(jnp.array(rights, jnp.int32), block_of_slot)
    count = block_of_slot.shape[0]
    arrays = (ins, mids, downs, outs, g_in, g_hidden, g_ff, cot)
    tokens = ins.shape[0]
    return pl.pallas_call(
        slot_grads_kernel,
        out_shape=jax.ShapeDtypeStruct((count, BS, BS), BF16),
        grid_spec=pltpu.PrefetchScalarGridSpec(
            num_scalar_prefetch=2, grid=(count // GROUP,),
            in_specs=[pl.BlockSpec(a.shape, lambda *_: (0, 0), pipeline_mode=pl.Buffered(1)) for a in arrays],
            out_specs=pl.BlockSpec((GROUP, BS, BS), lambda i, *_: (i, 0, 0)),
            scratch_shapes=[
                pltpu.VMEM((sum(a.shape[1] for a in arrays[:4]), tokens), BF16),
                pltpu.VMEM((tokens, sum(a.shape[1] for a in arrays[4:])), BF16),
            ],
        ),
        compiler_params=kernel_params(),
        name="slot_grads",
    )(left_at, right_at, *arrays)


SHAMPOO = 8


def shampoo_kernel(norm, total, master, left, right, left_root, right_root, grad, new_left, new_right, new_master, low):
    for i in range(SHAMPOO):
        g = total[i]
        value = g.astype(F32) * norm
        grad[i] = value
        new_left[i] = 0.5 * left[i] + dot_nt(g, g) * (0.5 * norm * norm / BS)
        new_right[i] = 0.5 * right[i] + dot_tn(g, g) * (0.5 * norm * norm / BS)
        inner = dot(g, right_root[i].astype(BF16))
        moved = dot(left_root[i].astype(BF16), inner.astype(BF16)) * (LR_MATRIX * norm)
        fresh = master[i] - moved
        new_master[i] = fresh
        low[i] = fresh.astype(BF16)


def shampoo(norm, total, master, left, right, left_root, right_root):
    slots = total.shape[0]
    spec = pl.BlockSpec((SHAMPOO, BS, BS), lambda i: (i, 0, 0))
    full = jax.ShapeDtypeStruct(master.shape, F32)
    return pl.pallas_call(
        functools.partial(shampoo_kernel, norm),
        out_shape=(full, full, full, full, jax.ShapeDtypeStruct(master.shape, BF16)),
        grid=(slots // SHAMPOO,),
        in_specs=[spec] * 6,
        out_specs=(spec,) * 5,
        compiler_params=kernel_params(),
        name="shampoo",
    )(total, master, left, right, left_root, right_root)


BLOCK = 256
HALO = 8


def lane_index(shape):
    return lax.broadcasted_iota(jnp.int32, shape, len(shape) - 1)


def conv_tile(extended, taps, marks, count):
    total = jnp.broadcast_to(taps[KERNEL : KERNEL + 1, :], (count, extended.shape[1]))
    for tap in range(KERNEL):
        total = total + taps[tap : tap + 1, :] * near_rows(extended, tap, count) * marks[:, tap : tap + 1]
    return total


def near_rows(extended, tap, count):
    back = REACH - tap
    moved = pltpu.roll(extended, back, 0) if back else extended
    return moved[HALO : HALO + count, :]


def softplus(v):
    return jnp.maximum(v, 0.0) + jnp.log(1.0 + jnp.exp(-jnp.abs(v)))


def chunk_decays(raw, params):
    delta = softplus(raw + params[0:1, :])
    decay = -delta * jnp.exp(params[1:2, :])
    block = raw.shape[0] if raw.shape[0] < BLOCK else BLOCK
    rows = lax.broadcasted_iota(jnp.int32, (block, block), 0)
    lower = (rows >= lane_index((block, block))).astype(F32)
    sums = [dot(lower, decay[i : i + block, :], HIGHEST) for i in range(0, raw.shape[0], block)]
    return delta, decay, jnp.concatenate(sums, axis=0)


def end_weights(delta, sums, marks):
    last = sums[-1:, :]
    return jnp.exp(last - sums) * delta * marks[:, 5:6], jnp.exp(last) * marks[-1:, 4:5]


def spread_matrix():
    rows = lax.broadcasted_iota(jnp.int32, (LANES, INNER), 0)
    return (rows == lane_index((LANES, INNER)) // HEAD).astype(F32)


def mix_first_kernel(proj_x, proj_bc, halo, taps, params, raw, marks, xbc, decays, decays_t, state, factor):
    tokens = raw.shape[0]
    mark = marks[...]
    for ref, at in ((proj_x, 0), (proj_bc, INNER)):
        step = 256
        for q in range(0, ref.shape[1], step):
            cols = slice(at + q, at + q + step)
            own = ref[:, q : q + step].astype(BF16).astype(F32)
            extended = jnp.concatenate([halo[:, cols].astype(F32), own], axis=0)
            value = conv_tile(extended, taps[:, cols], mark, tokens)
            xbc[:, cols] = (value * sigmoid(value)).astype(BF16)
    delta, decay, sums = chunk_decays(raw[...], params[...])
    decays[0] = delta
    decays[1] = sums
    decays_t[...] = sums.T
    spread = spread_matrix()
    total = jnp.zeros((NSTATE, INNER), F32)
    product = jnp.ones((1, LANES), F32)
    for i in range(0, tokens, BLOCK):
        rows = slice(i, i + BLOCK)
        weight, own = end_weights(delta[rows], sums[rows], mark[rows])
        weighted = (xbc[rows, :INNER].astype(F32) * dot(weight.astype(BF16), spread.astype(BF16))).astype(BF16)
        keep = dot(jnp.broadcast_to(own, (8, LANES)), spread, HIGHEST)[0:1]
        total = keep * total + dot_tn(xbc[rows, INNER : INNER + NSTATE], weighted)
        product = product * own
    state[...] = total.astype(BF16)
    factor[...] = jnp.broadcast_to(product, factor.shape)


def mix_first(proj, halo, taps, params, raw, marks):
    tokens = raw.shape[0]
    vmem = pl.BlockSpec(memory_space=pltpu.VMEM)
    return pl.pallas_call(
        mix_first_kernel,
        out_shape=(
            jax.ShapeDtypeStruct((tokens, CHANNELS), BF16),
            jax.ShapeDtypeStruct((2, tokens, LANES), F32),
            jax.ShapeDtypeStruct((LANES, tokens), F32),
            jax.ShapeDtypeStruct((NSTATE, INNER), BF16),
            jax.ShapeDtypeStruct((8, LANES), F32),
        ),
        grid=(1,),
        in_specs=[
            pl.BlockSpec((tokens, INNER), lambda i: (0, 1)),
            pl.BlockSpec((tokens, 2 * NSTATE), lambda i: (0, 2 * INNER // (2 * NSTATE))),
            vmem, vmem, vmem, vmem, vmem,
        ],
        out_specs=(vmem,) * 5,
        compiler_params=kernel_params(),
        name="mix_first",
    )(proj, proj, halo, taps, params, raw, marks)


def attend(left, right, mark_rows, mark_cols):
    return jnp.where(mark_rows & mark_cols, dot_nt(left, right), 0.0)


def halves(tile):
    low = lane_index(tile.shape) < HEAD
    zero = jnp.zeros_like(tile)
    return jnp.where(low, tile, zero), jnp.where(low, zero, tile)


def pair_column(values, a):
    return values[:, a * HEAD : a * HEAD + 1]


def mix_second_kernel(x, b, c, z, decays, decays_t, marks, labels, incoming, skip, gain, y, normed, states,
                      wide_sums, wide_delta, wide_end, keep, near, b_t, state, gated, squares):
    j = pl.program_id(0)
    tokens = x.shape[0]
    blocks = tokens // BLOCK
    cols = pl.ds(pl.multiple_of(j * LANES, LANES), LANES)

    @pl.when(j == 0)
    def _():
        spread = spread_matrix()
        rows = lax.broadcasted_iota(jnp.int32, (BLOCK, BLOCK), 0)
        ordered = rows >= lane_index((BLOCK, BLOCK))
        for i in range(blocks):
            at = slice(i * BLOCK, (i + 1) * BLOCK)
            mark = marks[at]
            same = mark[:, 6:7] == labels[0:1, at]
            near[i] = jnp.where(ordered & same, dot_nt(c[at], b[at]), 0.0)
            b_t[i] = b[at].T
            weight, own = end_weights(decays[0, at], decays[1, at], mark)
            wide_end[at] = dot(weight.astype(BF16), spread.astype(BF16)).astype(BF16)
            wide_sums[at] = dot(decays[1, at], spread, HIGHEST)
            wide_delta[at] = dot(decays[0, at].astype(BF16), spread.astype(BF16)).astype(BF16)
            keep[i] = dot(jnp.broadcast_to(own, (8, LANES)), spread, HIGHEST)
        squares[...] = jnp.zeros_like(squares)

    state[...] = incoming[...].astype(F32)
    for i in range(blocks):
        at = slice(i * BLOCK, (i + 1) * BLOCK)
        states[i] = state[...]
        tile = x[at].astype(F32)
        scaled = (tile * wide_delta[at, cols].astype(F32)).astype(BF16)
        sums = wide_sums[at, cols]
        total = jnp.zeros((BLOCK, LANES), F32)
        for a, part in enumerate(halves(scaled)):
            row = decays_t[pl.ds(2 * j + a, 1), at]
            weight = near[i] * jnp.exp(jnp.minimum(pair_column(sums, a) - row, 0.0))
            total = total + dot(weight.astype(BF16), part)
        carried = dot(c[at], state[...].astype(BF16))
        total = total + carried * jnp.exp(sums) * marks[at, 4:5] + skip[0:1, cols] * tile
        y[at] = total
        gate = z[at]
        gate = total * gate * sigmoid(gate)
        gated[at, cols] = gate
        squares[at] += gate * gate
        weighted = (tile * wide_end[at, cols].astype(F32)).astype(BF16)
        state[...] = keep[i, 0:1, cols] * state[...] + dot(b_t[i], weighted)
    states[blocks] = state[...]

    @pl.when(j == PAIRS - 1)
    def _():
        for i in range(blocks):
            at = slice(i * BLOCK, (i + 1) * BLOCK)
            scale = lax.rsqrt(jnp.sum(squares[at], axis=1, keepdims=True) / INNER + EPS)
            normed[at] = (gated[at] * scale * gain[0:1, :]).astype(BF16)


def mix_second(xbc, proj, decays, decays_t, marks, labels, incoming, skip, gain):
    tokens = xbc.shape[0]
    blocks = tokens // BLOCK
    tile = pl.BlockSpec((tokens, LANES), lambda j: (0, j))
    return pl.pallas_call(
        mix_second_kernel,
        out_shape=(
            jax.ShapeDtypeStruct((tokens, INNER), F32),
            jax.ShapeDtypeStruct((tokens, INNER), BF16),
            jax.ShapeDtypeStruct((blocks + 1, NSTATE, INNER), F32),
        ),
        grid=(PAIRS,),
        in_specs=[
            tile,
            pl.BlockSpec((tokens, NSTATE), lambda j: (0, INNER // NSTATE)),
            pl.BlockSpec((tokens, NSTATE), lambda j: (0, INNER // NSTATE + 1)),
            tile,
            whole(decays.shape), whole(decays_t.shape), whole(marks.shape), whole(labels.shape),
            pl.BlockSpec((NSTATE, LANES), lambda j: (0, j)),
            whole(skip.shape), whole(gain.shape),
        ],
        out_specs=(tile, whole((tokens, INNER)), pl.BlockSpec((blocks + 1, NSTATE, LANES), lambda j: (0, 0, j))),
        scratch_shapes=[
            pltpu.VMEM((tokens, INNER), F32), pltpu.VMEM((tokens, INNER), BF16), pltpu.VMEM((tokens, INNER), BF16),
            pltpu.VMEM((blocks, 8, INNER), F32), pltpu.VMEM((blocks, BLOCK, BLOCK), F32),
            pltpu.VMEM((blocks, NSTATE, BLOCK), BF16), pltpu.VMEM((NSTATE, LANES), F32),
            pltpu.VMEM((tokens, INNER), F32), pltpu.VMEM((tokens, LANES), F32),
        ],
        compiler_params=kernel_params(),
        name="mix_second",
    )(xbc, xbc, xbc, proj, decays, decays_t, marks, labels, incoming, skip, gain)


def gate_back_kernel(grad, y, z, gain, c, decays, marks, g_y, g_z, g_gain, g_state):
    step = pl.program_id(0)
    value, gate = y[...], z[...]
    opened = sigmoid(gate)
    swish = gate * opened
    gated = value * swish
    scale = lax.rsqrt(jnp.mean(gated * gated, axis=1, keepdims=True) + EPS)
    unit = gated * scale
    given = grad[...]
    scaled = given * gain[0:1, :]
    g_gated = scale * (scaled - unit * jnp.mean(scaled * unit, axis=1, keepdims=True))
    fresh = g_gated * swish
    g_y[...] = fresh.astype(BF16)
    g_z[...] = (g_gated * value * (opened + swish * (1.0 - opened))).astype(BF16)
    spread = spread_matrix()
    sums = decays[1]
    mark = marks[...]
    entry_weight = jnp.exp(sums) * mark[:, 4:5]
    own = jnp.exp(sums[-1:, :]) * mark[-1:, 4:5]
    keep = dot(jnp.broadcast_to(own, (8, LANES)), spread, HIGHEST)[0:1]
    weighted = (fresh * dot(entry_weight.astype(BF16), spread.astype(BF16))).astype(BF16)
    local = dot_tn(c[...], weighted)
    gains = jnp.broadcast_to(jnp.sum(given * unit, axis=0, keepdims=True), g_gain.shape)

    @pl.when(step == 0)
    def _():
        g_state[...] = local
        g_gain[...] = gains

    @pl.when(step > 0)
    def _():
        g_state[...] = keep * g_state[...] + local
        g_gain[...] += gains


def gate_back(grad, y, proj, gain, xbc, decays, marks):
    tokens = y.shape[0]
    blocks = tokens // BLOCK
    rows = lambda width, col: pl.BlockSpec((BLOCK, width), lambda i: (blocks - 1 - i, col))
    return pl.pallas_call(
        gate_back_kernel,
        out_shape=(
            jax.ShapeDtypeStruct((tokens, INNER), BF16),
            jax.ShapeDtypeStruct((tokens, INNER), BF16),
            jax.ShapeDtypeStruct((8, INNER), F32),
            jax.ShapeDtypeStruct((NSTATE, INNER), F32),
        ),
        grid=(blocks,),
        in_specs=[
            rows(INNER, 0), rows(INNER, 0), rows(INNER, 0), whole(gain.shape), rows(NSTATE, INNER // NSTATE + 1),
            pl.BlockSpec((2, BLOCK, LANES), lambda i: (0, blocks - 1 - i, 0)), rows(LANES, 0),
        ],
        out_specs=(rows(INNER, 0), rows(INNER, 0), whole((8, INNER)), whole((NSTATE, INNER))),
        compiler_params=kernel_params(),
        name="gate_back",
    )(grad, y, proj, gain, xbc, decays, marks)


def conv_back(grad, extended, taps, marks, count):
    acc = conv_tile(extended, taps, marks, count)
    opened = sigmoid(acc)
    g_acc = grad * (opened + acc * opened * (1.0 - opened))
    width = g_acc.shape[1]
    weights, result = [], jnp.zeros((HALO + count, width), F32)
    for tap in range(KERNEL):
        marked = g_acc * marks[:, tap : tap + 1]
        weights.append(jnp.sum(marked * near_rows(extended, tap, count), axis=0, keepdims=True))
        spread = jnp.concatenate([jnp.zeros((HALO, width), F32), marked * taps[tap : tap + 1, :]], axis=0)
        back = REACH - tap
        result = result + (pltpu.roll(spread, HALO + count - back, 0) if back else spread)
    weights.append(jnp.sum(g_acc, axis=0, keepdims=True))
    weights.append(jnp.zeros((8 - KERNEL - 1, width), F32))
    return result, jnp.concatenate(weights, axis=0)


def mix_back_kernel(x, b, c, proj_x, proj_bc, halo, taps, y, g_y, decays, decays_t, raw, params, marks, labels, states, leaving, skip,
                    g_conv, g_rim, g_taps, g_raw, g_params,
                    wide_sums, wide_delta, wide_end, wide_skip, keep, near, c_t, state, g_near, g_b, g_c, g_cum, g_delta, g_skip, ends):
    j = pl.program_id(0)
    tokens = x.shape[0]
    blocks = tokens // BLOCK
    cols = pl.ds(pl.multiple_of(j * LANES, LANES), LANES)
    lane = lane_index((LANES, LANES))
    gather = ((lax.broadcasted_iota(jnp.int32, (LANES, LANES), 0) // HEAD + 2 * j) == lane).astype(BF16)

    def collect(values):
        high = values.astype(BF16)
        return dot(high, gather) + dot((values - high.astype(F32)).astype(BF16), gather)

    @pl.when(j == 0)
    def _():
        spread = spread_matrix()
        rows = lax.broadcasted_iota(jnp.int32, (BLOCK, BLOCK), 0)
        ordered = rows <= lane_index((BLOCK, BLOCK))
        for i in range(blocks):
            at = slice(i * BLOCK, (i + 1) * BLOCK)
            mark = marks[at]
            same = mark[:, 6:7] == labels[0:1, at]
            near[i] = jnp.where(ordered & same, dot_nt(b[at], c[at]), 0.0)
            c_t[i] = c[at].T
            weight, own = end_weights(decays[0, at], decays[1, at], mark)
            end_only = jnp.exp(decays[1, at][-1:, :] - decays[1, at]) * mark[:, 5:6]
            wide_end[at] = dot(end_only.astype(BF16), spread.astype(BF16)).astype(BF16)
            wide_sums[at] = dot(decays[1, at], spread, HIGHEST)
            wide_delta[at] = dot(decays[0, at].astype(BF16), spread.astype(BF16)).astype(BF16)
            keep[i] = dot(jnp.broadcast_to(own, (8, LANES)), spread, HIGHEST)
        for ref in (g_near, g_b, g_c, g_cum, g_delta, g_skip, ends):
            ref[...] = jnp.zeros_like(ref)

    state[...] = leaving[...].astype(F32)
    g_x = []
    for i in range(blocks - 1, -1, -1):
        at = slice(i * BLOCK, (i + 1) * BLOCK)
        tile = x[at].astype(F32)
        step = wide_delta[at, cols].astype(F32)
        scaled = tile * step
        low_scaled = scaled.astype(BF16)
        sums = wide_sums[at, cols]
        end = wide_end[at, cols].astype(F32)
        given = g_y[at]
        low_state = state[...].astype(BF16)
        ends[i] += collect(jnp.broadcast_to(jnp.sum(states[i + 1] * state[...], axis=0, keepdims=True), (8, LANES)))
        total = end * dot(b[at], low_state)
        for a, (part, grad) in enumerate(zip(halves(low_scaled), halves(given))):
            row = decays_t[pl.ds(2 * j + a, 1), at]
            decay = jnp.exp(jnp.minimum(row - pair_column(sums, a), 0.0))
            total = total + dot((near[i] * decay).astype(BF16), grad)
            g_near[i] += decay * dot_nt(part, given)
        given = given.astype(F32)
        entry = jnp.exp(sums) * marks[at, 4:5]
        reached = (given * entry).astype(BF16)
        g_b[at] += dot_nt((scaled * end).astype(BF16), low_state)
        g_c[at] += dot_nt(reached, states[i].astype(BF16))
        own_skip = skip[0:1, cols]
        g_cum[at] += collect(given * (y[at] - own_skip * tile) - scaled * total)
        g_delta[at] += collect(total * tile)
        g_skip[...] += collect(jnp.broadcast_to(jnp.sum(given * tile, axis=0, keepdims=True), (8, LANES)))
        g_x.append(step * total + own_skip * given)
        state[...] = keep[i, 0:1, cols] * state[...] + dot(c_t[i], reached)

    mark = marks[...]
    own = proj_x[...].astype(BF16).astype(F32)
    extended = jnp.concatenate([halo[:, cols].astype(F32), own], axis=0)
    result, weights = conv_back(jnp.concatenate(g_x[::-1], axis=0), extended, taps[:, cols], mark, tokens)
    g_rim[:HALO, cols] = result[:HALO]
    g_rim[HALO:, cols] = result[tokens:]
    g_conv[:, cols] = result[HALO:].astype(BF16)
    g_taps[:, cols] = weights

    @pl.when(j == PAIRS - 1)
    def _():
        for i in range(blocks):
            at = slice(i * BLOCK, (i + 1) * BLOCK)
            rows = lax.broadcasted_iota(jnp.int32, (BLOCK, BLOCK), 0)
            seen = (rows <= lane_index((BLOCK, BLOCK))) & (marks[at, 6:7] == labels[0:1, at])
            grad = jnp.where(seen, g_near[i], 0.0)
            g_b[at] += dot(grad.astype(BF16), c[at])
            g_c[at] += dot(grad.T.astype(BF16), b[at])
        for k, ref in enumerate((g_b, g_c)):
            at = slice(INNER + k * NSTATE, INNER + (k + 1) * NSTATE)
            own = proj_bc[:, k * NSTATE : (k + 1) * NSTATE].astype(BF16).astype(F32)
            extended = jnp.concatenate([halo[:, at].astype(F32), own], axis=0)
            result, weights = conv_back(ref[...], extended, taps[:, at], mark, tokens)
            g_rim[:HALO, at] = result[:HALO]
            g_rim[HALO:, at] = result[tokens:]
            g_conv[:, at] = result[HALO:].astype(BF16)
            g_taps[:, at] = weights
        rate = -jnp.exp(params[1:2, :])
        bias_sum = jnp.zeros((1, LANES), F32)
        rate_sum = jnp.zeros((1, LANES), F32)
        rows = lax.broadcasted_iota(jnp.int32, (BLOCK, BLOCK), 0)
        upper = (rows <= lane_index((BLOCK, BLOCK))).astype(F32)
        for i in range(blocks):
            at = slice(i * BLOCK, (i + 1) * BLOCK)
            g_decay = dot(upper, g_cum[at], HIGHEST) + ends[i, 0:1, :]
            delta = decays[0, at]
            full = g_delta[at] + g_decay * rate
            full = full * sigmoid(raw[at] + params[0:1, :])
            g_raw[at] = full.astype(BF16)
            bias_sum = bias_sum + jnp.sum(full, axis=0, keepdims=True)
            rate_sum = rate_sum + jnp.sum(g_decay * delta * rate, axis=0, keepdims=True)
        g_params[...] = jnp.concatenate([bias_sum, rate_sum, g_skip[0:1, :], jnp.zeros((5, LANES), F32)], axis=0)


def mix_back(xbc, proj, halo, taps, y, g_y, decays, decays_t, raw, params, marks, labels, states, leaving, skip):
    tokens = xbc.shape[0]
    blocks = tokens // BLOCK
    tile = pl.BlockSpec((tokens, LANES), lambda j: (0, j))
    acc = lambda *shape: pltpu.VMEM(shape, F32)
    return pl.pallas_call(
        mix_back_kernel,
        out_shape=(
            jax.ShapeDtypeStruct((tokens, CHANNELS), BF16),
            jax.ShapeDtypeStruct((2 * HALO, CHANNELS), F32),
            jax.ShapeDtypeStruct((8, CHANNELS), F32),
            jax.ShapeDtypeStruct((tokens, LANES), BF16),
            jax.ShapeDtypeStruct((8, LANES), F32),
        ),
        grid=(PAIRS,),
        in_specs=[
            tile,
            pl.BlockSpec((tokens, NSTATE), lambda j: (0, INNER // NSTATE)),
            pl.BlockSpec((tokens, NSTATE), lambda j: (0, INNER // NSTATE + 1)),
            pl.BlockSpec((tokens, LANES), lambda j: (0, PAIRS + j)),
            pl.BlockSpec((tokens, 2 * NSTATE), lambda j: (0, 2 * INNER // (2 * NSTATE))),
            whole(halo.shape), whole(taps.shape), tile, tile,
            whole(decays.shape), whole(decays_t.shape), whole(raw.shape), whole(params.shape), whole(marks.shape), whole(labels.shape),
            pl.BlockSpec((blocks + 1, NSTATE, LANES), lambda j: (0, 0, j)),
            pl.BlockSpec((NSTATE, LANES), lambda j: (0, j)),
            whole(skip.shape),
        ],
        out_specs=(
            whole((tokens, CHANNELS)), whole((2 * HALO, CHANNELS)), whole((8, CHANNELS)), whole((tokens, LANES)), whole((8, LANES)),
        ),
        scratch_shapes=[
            acc(tokens, INNER), pltpu.VMEM((tokens, INNER), BF16), pltpu.VMEM((tokens, INNER), BF16), acc(8, LANES),
            acc(blocks, 8, INNER), acc(blocks, BLOCK, BLOCK), pltpu.VMEM((blocks, NSTATE, BLOCK), BF16), acc(NSTATE, LANES),
            acc(blocks, BLOCK, BLOCK), acc(tokens, NSTATE), acc(tokens, NSTATE), acc(tokens, LANES), acc(tokens, LANES),
            acc(8, LANES), acc(blocks, 8, LANES),
        ],
        compiler_params=kernel_params(),
        name="mix_back",
    )(xbc, xbc, xbc, proj, proj, halo, taps, y, g_y, decays, decays_t, raw, params, marks, labels, states, leaving, skip)


QBLOCK = 256
GROUPS = HEADS // KV_HEADS
QPAIRS = QDIM // LANES
SCALE = 1.0 / math.sqrt(HEAD)


def swap_halves(values):
    half = HEAD // 2
    front = lane_index(values.shape) % HEAD < half
    width = values.shape[-1]
    return jnp.where(front, pltpu.roll(values, width - half, 1), pltpu.roll(values, half, 1))


def turn(values, cosine, sine):
    return values * cosine + swap_halves(values) * sine


def rope_kernel(*refs):
    queries, (k, v, cosine, sine, q_out, kv_out) = refs[:QPAIRS], refs[QPAIRS:]
    cos, sin = cosine[...], sine[...]
    for p, q in enumerate(queries):
        q_out[:, p * LANES : (p + 1) * LANES] = turn(q[...], cos, sin).astype(BF16)
    kv_out[:, :KDIM] = turn(k[...], cos, sin).astype(BF16)
    kv_out[:, KDIM:] = v[...].astype(BF16)


def rope_all(proj, cosine, sine):
    tokens = proj.shape[0]
    start = 2 * INNER + 2 * NSTATE
    return pl.pallas_call(
        rope_kernel,
        out_shape=(jax.ShapeDtypeStruct((tokens, QDIM), BF16), jax.ShapeDtypeStruct((tokens, 2 * KDIM), BF16)),
        grid=(1,),
        in_specs=[
            pl.BlockSpec((tokens, LANES), lambda i, p=p: (0, start // LANES + p)) for p in range(QPAIRS + 2)
        ] + [whole(cosine.shape), whole(sine.shape)],
        out_specs=(whole((tokens, QDIM)), whole((tokens, 2 * KDIM))),
        compiler_params=kernel_params(),
        name="rope",
    )(*[proj] * (QPAIRS + 2), cosine, sine)


def both_sides(tile, both):
    low = lane_index(tile.shape) < HEAD
    zero = jnp.zeros_like(tile)
    moved = pltpu.roll(tile.astype(F32), HEAD, 1).astype(tile.dtype)
    both[0, 0] = jnp.where(low, tile, zero)
    both[0, 1] = jnp.where(low, zero, moved)
    both[1, 0] = jnp.where(low, moved, zero)
    both[1, 1] = jnp.where(low, zero, tile)


def attend_kernel(q, kv, key_labels, marks, context, stats, keys, values):
    block, pair = pl.program_id(0), pl.program_id(1)
    window = DOC_MOST + QBLOCK
    start = pl.multiple_of(block * QBLOCK, QBLOCK)

    @pl.when((block == 0) & (pair == 0))
    def _():
        both_sides(kv[:, :KDIM], keys)
        both_sides(kv[:, KDIM:], values)

    group = pair // (GROUPS // 2)
    rows = lax.broadcasted_iota(jnp.int32, (QBLOCK, window), 0)
    cols = lane_index((QBLOCK, window))
    seen = (cols <= rows + DOC_MOST) & (marks[:, 6:7] == key_labels[0, 0:1, :])
    total = jnp.zeros((QBLOCK, LANES), F32)
    found = jnp.zeros((QBLOCK, LANES), F32)
    for a in range(2):
        scores = dot_nt(q[...], keys[group, a, pl.ds(start, window), :]) * SCALE
        scores = jnp.where(seen, scores, NEG_BIG)
        most = jnp.max(scores, axis=1, keepdims=True)
        probs = jnp.exp(scores - most)
        mass = jnp.sum(probs, axis=1, keepdims=True)
        probs = probs * (1.0 / mass)
        total = total + dot(probs.astype(BF16), values[group, a, pl.ds(start, window), :])
        found = jnp.where(lane_index(found.shape) == a, most + jnp.log(mass), found)
    context[...] = total.astype(BF16)
    stats[0] = found.T[0:8, :]


def attend(q, kv, key_labels, marks):
    tokens = q.shape[0]
    blocks = tokens // QBLOCK
    tile = pl.BlockSpec((QBLOCK, LANES), lambda i, p: (i, p))
    return pl.pallas_call(
        attend_kernel,
        out_shape=(jax.ShapeDtypeStruct((tokens, QDIM), BF16), jax.ShapeDtypeStruct((QPAIRS, 8, tokens), F32)),
        grid=(blocks, QPAIRS),
        in_specs=[
            tile, whole(kv.shape), pl.BlockSpec((1,) + key_labels.shape[1:], lambda i, p: (i, 0, 0)),
            pl.BlockSpec((QBLOCK, LANES), lambda i, p: (i, 0)),
        ],
        out_specs=(tile, pl.BlockSpec((1, 8, QBLOCK), lambda i, p: (p, 0, i))),
        scratch_shapes=[pltpu.VMEM((2, 2) + (kv.shape[0], LANES), BF16)] * 2,
        compiler_params=kernel_params(),
        name="attend",
    )(q, kv, key_labels, marks)


def attend_back_kernel(q, kv, given, key_marks, query_labels, stats, cosine, sine, g_q, g_kv, keys, values, g_key, g_value):
    block, pair = pl.program_id(0), pl.program_id(1)
    window = DOC_MOST + QBLOCK
    start = pl.multiple_of(block * QBLOCK, QBLOCK)

    @pl.when((block == 0) & (pair == 0))
    def _():
        both_sides(kv[:, :KDIM], keys)
        both_sides(kv[:, KDIM:], values)
        g_key[...] = jnp.zeros_like(g_key)
        g_value[...] = jnp.zeros_like(g_value)

    group = pair // (GROUPS // 2)
    rows = lax.broadcasted_iota(jnp.int32, (window, QBLOCK), 0)
    cols = lane_index((window, QBLOCK))
    seen = (rows <= cols + DOC_MOST) & (key_marks[0, :, 0:1] == query_labels[0:1, :])
    at = pl.ds(start, window)
    query, grad = q[...], given[...].astype(BF16)
    total = jnp.zeros((QBLOCK, LANES), F32)
    for a, (query_part, grad_part) in enumerate(zip(halves(query), halves(grad))):
        key = keys[group, a, at, :]
        scores = jnp.where(seen, dot_nt(key, query) * SCALE, NEG_BIG)
        probs = jnp.exp(scores - stats[0, a : a + 1, :])
        g_probs = dot_nt(values[group, a, at, :], grad)
        mean = jnp.sum(probs * g_probs, axis=0, keepdims=True)
        g_scores = (probs * (g_probs - mean)).astype(BF16)
        g_key[group, at] += dot(g_scores, query_part) * SCALE
        g_value[group, at] += dot(probs.astype(BF16), grad_part)
        total = total + dot_tn(g_scores, key)
    g_q[...] = turn(total * SCALE, cosine[...], -sine[...]).astype(BF16)

    @pl.when((block == pl.num_programs(0) - 1) & (pair == QPAIRS - 1))
    def _():
        for k, ref in enumerate((g_key, g_value)):
            first = ref[0] + pltpu.roll(ref[0], HEAD, 1)
            second = ref[1] + pltpu.roll(ref[1], HEAD, 1)
            g_kv[:, k * KDIM : (k + 1) * KDIM] = jnp.where(lane_index(first.shape) < HEAD, first, second).astype(BF16)


def attend_back(q, kv, given, key_marks, query_labels, stats, cosine, sine):
    tokens = q.shape[0]
    blocks = tokens // QBLOCK
    tile = pl.BlockSpec((QBLOCK, LANES), lambda i, p: (i, p))
    row = pl.BlockSpec((QBLOCK, LANES), lambda i, p: (i, 0))
    return pl.pallas_call(
        attend_back_kernel,
        out_shape=(jax.ShapeDtypeStruct((tokens, QDIM), BF16), jax.ShapeDtypeStruct(kv.shape, BF16)),
        grid=(blocks, QPAIRS),
        in_specs=[
            tile, whole(kv.shape), pl.BlockSpec((QBLOCK, LANES), lambda i, p: (i, PAIRS + p)),
            pl.BlockSpec((1,) + key_marks.shape[1:], lambda i, p: (i, 0, 0)),
            pl.BlockSpec((8, QBLOCK), lambda i, p: (0, i)),
            pl.BlockSpec((1, 8, QBLOCK), lambda i, p: (p, 0, i)), row, row,
        ],
        out_specs=(tile, whole(kv.shape)),
        scratch_shapes=[pltpu.VMEM((2, 2) + (kv.shape[0], LANES), BF16)] * 2 + [pltpu.VMEM((2, kv.shape[0], LANES), F32)] * 2,
        compiler_params=kernel_params(),
        name="attend_back",
    )(q, kv, given, key_marks, query_labels, stats, cosine, sine)


def turn_back_kernel(g_kv, cosine, sine, out):
    out[:, :KDIM] = turn(g_kv[:, :KDIM], cosine[...], -sine[...]).astype(BF16)
    out[:, KDIM:] = g_kv[:, KDIM:].astype(BF16)


def turn_back(g_kv, cosine, sine):
    return pl.pallas_call(
        turn_back_kernel, out_shape=jax.ShapeDtypeStruct(g_kv.shape, BF16), compiler_params=kernel_params(), name="turn_back",
    )(g_kv, cosine, sine)


def spans(seq, micro):
    return seq // micro, micro


def regroup(rows, micro):
    seq = lax.axis_size("seq")
    each = seq // micro
    here = lax.axis_index("seq")
    pieces = []
    for t in range(micro):
        pairs = [(j, ((j + t) % micro) * each + j // micro) for j in range(seq)]
        pieces.append(lax.ppermute(lax.dynamic_index_in_dim(rows, (here + t) % micro, 0, False), "seq", pairs))
    order = here // each
    stacked = jnp.stack(pieces)
    return jnp.concatenate([lax.dynamic_index_in_dim(stacked, (order - q) % micro, 0, False) for q in range(micro)], axis=0)


def ungroup(rows, micro):
    seq = lax.axis_size("seq")
    each = seq // micro
    here = lax.axis_index("seq")
    order = here // each
    cut = rows.reshape((micro, rows.shape[0] // micro) + rows.shape[1:])
    pieces = []
    for t in range(micro):
        pairs = [(((j + t) % micro) * each + j // micro, j) for j in range(seq)]
        pieces.append(lax.ppermute(lax.dynamic_index_in_dim(cut, (order - t) % micro, 0, False), "seq", pairs))
    stacked = jnp.stack(pieces)
    return jnp.stack([lax.dynamic_index_in_dim(stacked, (m - here) % micro, 0, False) for m in range(micro)])


def along(value, steps, micro):
    seq = lax.axis_size("seq")
    each = seq // micro
    pairs = [(s, s + steps) for s in range(seq) if 0 <= s % each + steps < each]
    return lax.ppermute(value, "seq", pairs)


def pad_rows(*rows):
    width = rows[0].shape[-1]
    return jnp.concatenate([r.reshape(-1, width) for r in rows] + [jnp.zeros((8 - sum(r.size // width for r in rows), width), F32)], axis=0)


def shards(grid, tokens, cotangent, doc_ids, master_blocks, block_of_slot, left_stats, right_stats, left_roots, right_roots,
           vector_params, first_moment, second_moment, adam_step):
    micro, piece = tokens.shape[:2]
    seq = lax.axis_size("seq")
    each = seq // micro
    count = micro * piece
    here = lax.axis_index("seq")
    rank = here % each
    start = rank * count
    slots = master_blocks.shape[0]

    inverse = jnp.zeros_like(block_of_slot).at[block_of_slot].set(jnp.arange(block_of_slot.shape[0], dtype=jnp.int32), unique_indices=True)
    gathered = gather_blocks(grid, master_blocks.astype(BF16)).reshape(-1, BS, BS)
    w_in, w_out, w_ff, w_down = assemble(gathered, inverse)
    gain_in, gain_mid, gain_mix, conv_weight, conv_bias, dt_bias, a_log, skip, w_dt = unpack_vectors(vector_params)
    w_dt = jnp.pad(w_dt.reshape(D, HEADS_SSM), ((0, 0), (0, LANES - HEADS_SSM))).astype(BF16)
    taps = pad_rows(conv_weight.reshape(KERNEL, CHANNELS), conv_bias)
    lane_pad = lambda v: jnp.pad(v, (0, LANES - HEADS_SSM))
    params = pad_rows(lane_pad(dt_bias), lane_pad(a_log))
    wide_skip = pad_rows(jnp.repeat(skip, HEAD))
    wide_gain = pad_rows(gain_mix)

    labels_all = lax.all_gather(doc_ids, "seq", axis=1, tiled=True)
    row = lax.dynamic_index_in_dim(labels_all, here // each, 0, False)
    before = jnp.concatenate([jnp.full((DOC_MOST,), -1, jnp.int32), row])
    window = lax.dynamic_slice_in_dim(before, start, DOC_MOST + count)
    labels = window[DOC_MOST:]
    blocks = count // BLOCK
    columns = [(window[DOC_MOST - REACH + tap : DOC_MOST - REACH + tap + count] == labels).astype(F32) for tap in range(KERNEL)]
    by_block = labels.reshape(blocks, BLOCK)
    entries_at = window[DOC_MOST - 1 : DOC_MOST - 1 + count].reshape(blocks, BLOCK)[:, :1]
    columns.append((by_block == entries_at).astype(F32).reshape(-1))
    columns.append((by_block == by_block[:, -1:]).astype(F32).reshape(-1))
    columns.append(labels.astype(F32))
    marks = jnp.pad(jnp.stack(columns, axis=1), ((0, 0), (0, LANES - len(columns))))
    label_rows = jnp.broadcast_to(labels.astype(F32)[None], (8, count))
    far = jnp.stack([window[i : i + DOC_MOST + QBLOCK] for i in range(0, count, QBLOCK)]).astype(F32)
    key_labels = jnp.broadcast_to(far[:, None, :], (far.shape[0], 8, far.shape[1]))
    key_marks = jnp.broadcast_to(far[:, :, None], far.shape + (8,))
    first = jnp.sum((row[None, :] < labels[:, None]).astype(jnp.int32), axis=1)
    positions = (start + jnp.arange(count) - first).astype(F32)
    half = HEAD // 2
    frequency = jnp.exp(jnp.arange(half, dtype=F32) * (-2.0 * math.log(THETA) / HEAD))
    angles = positions[:, None] * frequency[None, :]
    cos, sin = jnp.cos(angles), jnp.sin(angles)
    cosine = jnp.concatenate([cos] * 4, axis=1)
    sine = jnp.concatenate([-sin, sin] * 2, axis=1)

    rows = regroup(tokens, micro)
    given = regroup(cotangent, micro)
    inputs = rows.astype(F32)
    normed_in = (inputs * rms_scale(inputs) * gain_in).astype(BF16)
    proj = dot(normed_in, w_in)
    raw = dot(normed_in, w_dt)
    halo = along(proj[count - HALO :, INNER : INNER + CHANNELS].astype(BF16), 1, micro)
    q, kv = rope_all(proj, cosine, sine)
    xbc, decays, decays_t, state, factor = mix_first(proj, halo, taps, params, raw, marks)
    past = min(each - 1, -(-DOC_MOST // count))
    earlier = [along(kv, back, micro) for back in range(past, 0, -1)]
    if past * count < DOC_MOST:
        earlier.insert(0, jnp.zeros((DOC_MOST - past * count, kv.shape[1]), BF16))
    reach = jnp.concatenate(earlier + [kv], axis=0)[-(DOC_MOST + count) :]
    wide = lambda f: jnp.repeat(f[0, :HEADS_SSM], HEAD)[None]
    incoming = along(state, each - 1, micro).astype(F32) if each > 1 else jnp.zeros(state.shape, F32)
    for back in range(each - 2, 0, -1):
        incoming = along(state, back, micro).astype(F32) + wide(along(factor, back, micro)) * incoming
    y, normed_ssm, states = mix_second(xbc, proj, decays, decays_t, marks, label_rows, incoming, wide_skip, wide_gain)
    context, stats = attend(q, reach, key_labels, marks)
    hidden = inputs + (dot(normed_ssm, w_out[:INNER]) + dot(context, w_out[INNER:]))
    normed_mid = (hidden * rms_scale(hidden) * gain_mid).astype(BF16)
    both = dot(normed_mid, w_ff)
    gate, upper = both[:, :FF], both[:, FF:]
    opened = sigmoid(gate)
    mixed = (gate * opened * upper).astype(BF16)
    layer_out = ungroup((hidden + dot(mixed, w_down)).astype(BF16), micro)

    g_mixed = dot_nt(given, w_down)
    g_gate = g_mixed * upper * (opened + gate * opened * (1.0 - opened))
    g_ff = jnp.concatenate([g_gate.astype(BF16), (g_mixed * gate * opened).astype(BF16)], axis=1)

    def norm_back(grad, values, gain):
        scale = rms_scale(values)
        unit = values * scale
        scaled = grad * gain
        return scale * (scaled - unit * jnp.mean(scaled * unit, axis=1, keepdims=True)), jnp.sum(grad * unit, axis=0)

    g_values, g_gain_mid = norm_back(dot_nt(g_ff, w_ff), hidden, gain_mid)
    g_hidden = given.astype(F32) + g_values
    hidden_low = g_hidden.astype(BF16)
    g_out = dot_nt(hidden_low, w_out)
    g_y, g_z, g_gain_mix, g_state = gate_back(g_out, y, proj, wide_gain, xbc, decays, marks)
    low_state = g_state.astype(BF16)
    leaving = along(low_state, 1 - each, micro).astype(F32) if each > 1 else jnp.zeros(state.shape, F32)
    for ahead in range(each - 2, 0, -1):
        leaving = along(low_state, -ahead, micro).astype(F32) + wide(along(factor, -ahead, micro)) * leaving
    g_q, g_reach = attend_back(q, reach, g_out, key_marks, label_rows, stats, cosine, sine)
    g_conv, g_rim, g_taps, g_raw, g_params = mix_back(
        xbc, proj, halo, taps, y, g_y, decays, decays_t, raw, params, marks, label_rows, states, leaving, wide_skip
    )
    g_kv = g_reach[-count:].astype(F32)
    for back in range(1, past + 1):
        low = max(0, DOC_MOST - back * count)
        part = g_reach[low : DOC_MOST - (back - 1) * count]
        moved = along(part, -back, micro).astype(F32)
        g_kv = g_kv + jnp.pad(moved, ((count - part.shape[0], 0), (0, 0)))
    g_kv = turn_back(g_kv, cosine, sine)
    rim = along(g_rim[:HALO], -1, micro)
    g_conv = lax.dynamic_update_slice(g_conv, (g_rim[HALO:] + rim).astype(BF16), (count - HALO, 0))
    g_in = jnp.concatenate([g_z, g_conv, g_q, g_kv], axis=1)
    g_values, g_gain_in = norm_back(dot_nt(g_in, w_in) + dot_nt(g_raw, w_dt), inputs, gain_in)
    grad_tokens = ungroup((g_values + g_hidden).astype(BF16), micro).astype(F32)
    g_w_dt = dot_tn(normed_in, g_raw)

    flat = slot_grads(block_of_slot, normed_in, normed_mid, mixed, jnp.concatenate([normed_ssm, context], axis=1),
                      g_in, hidden_low, g_ff, given)
    parts = [g_gain_in, g_gain_mid, g_gain_mix[0], g_taps[:KERNEL].reshape(-1), g_taps[KERNEL]]
    parts += [g_params[i, :HEADS_SSM] for i in range(3)] + [g_w_dt[:, :HEADS_SSM].reshape(-1)]
    width = vector_params.shape[0]
    height = -(-width // (8 * LANES)) * 8
    vector = jnp.concatenate(parts + [jnp.zeros((height * LANES - width,), F32)]).reshape(height, LANES)
    total, vector = reduce_blocks(grid, flat.reshape(-1, slots, BS, BS), vector)
    norm = 1.0 / math.sqrt(count * seq * lax.axis_size("dp"))
    updates = shampoo(norm, total, master_blocks, left_stats, right_stats, left_roots, right_roots)
    g_vector = vector.reshape(-1)[:width] * norm
    step = adam_step[0].astype(F32)
    new_first = BETA_ONE * first_moment + (1.0 - BETA_ONE) * g_vector
    new_second = BETA_TWO * second_moment + (1.0 - BETA_TWO) * g_vector * g_vector
    first_hat = new_first / (1.0 - jnp.power(BETA_ONE, step))
    second_hat = new_second / (1.0 - jnp.power(BETA_TWO, step))
    new_vector = vector_params - LR_VECTOR * first_hat / (jnp.sqrt(second_hat) + ADAM_EPS)
    return (layer_out, grad_tokens) + tuple(updates) + (g_vector, new_vector, new_first, new_second)


def solution(mesh):
    line, block, copied = P("dp", "seq", None), P("dp", None, None), P()
    return jax.shard_map(
        functools.partial(shards, grid_of(mesh)),
        mesh=mesh,
        in_specs=(line, line, P("dp", "seq"), block, copied, block, block, block, block, copied, copied, copied, copied),
        out_specs=(line, line) + (block,) * 5 + (copied,) * 4,
        check_vma=False,
    )
```

```python
import functools
import math

import jax
import jax.numpy as jnp
from jax import lax
from jax.experimental import pallas as pl
from jax.experimental.pallas import tpu as pltpu
from jax.sharding import PartitionSpec as P

D = 1024
HEADS_SSM = 24
HEAD = 64
NSTATE = 128
HEADS = 8
KV_HEADS = 2
FF = 2048
KERNEL = 4
BS = 128
DOC_MOST = 512
INNER = HEADS_SSM * HEAD
CHANNELS = INNER + 2 * NSTATE
REACH = KERNEL - 1
QDIM = HEADS * HEAD
KDIM = KV_HEADS * HEAD
LANES = 128
PAIRS = INNER // LANES

EPS = 1e-05
THETA = 100000000000.0
LR_MATRIX = 0.02
LR_VECTOR = 0.08
BETA_ONE = 0.9
BETA_TWO = 0.999
ADAM_EPS = 1e-08
NEG_BIG = -1e30
F32 = jnp.float32
BF16 = jnp.bfloat16
HIGHEST = lax.Precision.HIGHEST
VMEM_MOST = 60 << 20

SHAPES = (
    (D, INNER), (D, INNER), (D, 2 * NSTATE), (D, QDIM), (D, KDIM), (D, KDIM),
    (INNER, D), (QDIM, D), (D, FF), (D, FF), (FF, D),
)
WIDE_IN, TALL_OUT, WIDE_FF, TALL_FF = (0, 1, 2, 3, 4, 5), (6, 7), (8, 9), (10,)
SIZES = (D, D, INNER, KERNEL * CHANNELS, CHANNELS, HEADS_SSM, HEADS_SSM, HEADS_SSM, D * HEADS_SSM)


def block_offsets():
    starts, total = [], 0
    for rows, cols in SHAPES:
        starts.append(total)
        total += rows // BS * (cols // BS)
    return starts


def wide_order(members):
    starts = block_offsets()
    rows = SHAPES[members[0]][0] // BS
    return [starts[m] + r * (SHAPES[m][1] // BS) + q for r in range(rows) for m in members for q in range(SHAPES[m][1] // BS)]


def tall_order(members):
    starts = block_offsets()
    return [starts[m] + i for m in members for i in range(SHAPES[m][0] // BS * (SHAPES[m][1] // BS))]


def all_orders():
    return [wide_order(WIDE_IN), tall_order(TALL_OUT), wide_order(WIDE_FF), tall_order(TALL_FF)]


def unpack_vectors(flat):
    result, offset = [], 0
    for count in SIZES:
        result.append(flat[offset : offset + count])
        offset += count
    return result


def dot(left, right, precision=None):
    return jnp.dot(left, right, preferred_element_type=F32, precision=precision)


def dot_nt(left, right):
    return lax.dot_general(left, right, (((1,), (1,)), ((), ())), preferred_element_type=F32)


def dot_tn(left, right):
    return lax.dot_general(left, right, (((0,), (0,)), ((), ())), preferred_element_type=F32)


def sigmoid(v):
    return 1.0 / (1.0 + jnp.exp(-v))


def rms_scale(values):
    return lax.rsqrt(jnp.mean(values * values, axis=-1, keepdims=True) + EPS)


def kernel_params(**more):
    return pltpu.CompilerParams(vmem_limit_bytes=VMEM_MOST, **more)


def whole(shape):
    return pl.BlockSpec(shape, lambda *_: (0,) * len(shape))


MESH = pl.DeviceIdType.MESH
CORES = 2


def grid_of(mesh):
    try:
        wide = len({device.coords[0] for device in mesh.devices.flat})
    except AttributeError:
        wide = mesh.shape["seq"] // CORES
    return wide, mesh.shape["seq"] // CORES, mesh.shape["dp"] // wide


def parts_of(slots, tall):
    half = slots // CORES
    lone = half * 17 // 48 if tall == 2 and half >= 16 else 0
    return half, lone, half - lone


def place(grid):
    wide, tall, deep = grid
    dp, seq = lax.axis_index("dp"), lax.axis_index("seq")
    return dp % wide, seq // CORES, dp // wide, seq % CORES


def gather_kernel(grid, slots, master, tokens, cotangent, docs, out, rows, given, labels, wide_own, src, bounce,
                  sem_own, sem_load, sz, rz, sx, rx, sy, ry, sc, rc, s_rows, r_rows, s_docs, r_docs):
    wide, tall, deep = grid
    x, y, z, c = place(grid)
    half, lone, bulk = parts_of(slots, tall)
    me = z * wide + x
    seq = y * CORES + c
    base = c * half
    bulk_at = base + y * (half - bulk)
    lone_at = base + y * bulk
    other_at = base + (1 - y) * bulk if lone else base
    mate = y * CORES + (1 - c)
    over = (tall - 1 - y) * CORES + c
    peers = tall * CORES
    micro = tokens.shape[0]
    each = peers // micro

    loads = []
    for k in range(CORES):
        part = pl.ds(((c + k) % CORES) * half, half)
        loads.append((part, pltpu.make_async_copy(master.at[part], wide_own.at[part], sem_load.at[k])))
        loads[-1][1].start()

    barrier = pltpu.get_barrier_semaphore()
    count = jnp.int32(0)
    for axis, at, size in (("z", z, deep), ("x", x, wide)):
        for step in (1, -1):
            ok = (at + step >= 0) & (at + step < size)
            there = me + step * (wide if axis == "z" else 1)

            @pl.when(ok)
            def _(there=there):
                pl.semaphore_signal(barrier, inc=1, device_id=(there, seq), device_id_type=MESH)

            count = count + ok.astype(jnp.int32)
    for k in range(1, peers):
        pl.semaphore_signal(barrier, inc=1, device_id=(me, (seq + k) % peers), device_id_type=MESH)
    pl.semaphore_wait(barrier, count + (peers - 1))
    sent = []

    def send(ok, source, target, send_sem, recv_sem, device):
        copy = pltpu.make_async_remote_copy(
            src_ref=source, dst_ref=target, send_sem=send_sem, recv_sem=recv_sem,
            device_id=device, device_id_type=MESH,
        )

        @pl.when(ok)
        def _():
            copy.start()

        sent.append((ok, copy))

    def arrived(ok, target, recv_sem):
        copy = pltpu.make_async_remote_copy(
            src_ref=target, dst_ref=target, send_sem=sem_own.at[0], recv_sem=recv_sem,
            device_id=(me, seq), device_id_type=MESH,
        )

        @pl.when(ok)
        def _():
            copy.wait_recv()

    yes = jnp.bool_(True)

    at_home = []
    for t in range(micro):
        m = (seq + t) % micro
        there = m * each + seq // micro
        for k, (source, target) in enumerate(((tokens, rows), (cotangent, given))):
            place_to = target.at[seq % micro]
            send(there != seq, source.at[m], place_to, s_rows.at[k, t], r_rows.at[k, seq % micro], (me, there))
            take = pltpu.make_async_copy(source.at[m], bounce.at[k], sem_own.at[k])
            put = pltpu.make_async_copy(bounce.at[k], place_to, sem_own.at[k])
            at_home.append((there == seq, take, put))

            @pl.when(there == seq)
            def _(take=take):
                take.start()

    labels[seq] = docs[...]
    for k in range(1, peers):
        there = (seq + k) % peers
        send(yes, docs, labels.at[seq], s_docs.at[k], r_docs.at[seq], (me, there))

    def convert(k):
        part, copy = loads[k]
        copy.wait()
        base_at = ((c + k) % CORES) * half

        def one(i, _):
            src[base_at + i] = wide_own[base_at + i].astype(src.dtype)
            return 0

        lax.fori_loop(0, half, one, 0, unroll=2)

    convert(0)

    def piece(shard, at, size):
        return out.at[shard, pl.ds(at, size)]

    def pass_on(ok, shard):
        send(ok, piece(shard, bulk_at, bulk), piece(shard, bulk_at, bulk), sc.at[0, shard], rc.at[0, shard], (me, mate))
        if lone:
            send(ok, piece(shard, lone_at, lone), piece(shard, lone_at, lone), sy.at[shard], ry.at[shard], (me, over))

    def along_x(ok, zs, dirs, hop, own):
        for d, step in dirs:
            shard = zs * wide + x - step * hop
            go = ok & (x + step >= 0) & (x + step < wide)
            source = src.at[pl.ds(bulk_at, bulk)] if own else piece(shard, bulk_at, bulk)
            send(go, source, piece(shard, bulk_at, bulk), sx.at[d, hop, zs], rx.at[d, hop + 1, zs], (me + step, seq))

    both = ((0, 1), (1, -1))

    def columns(s):
        return [(yes, z)] if s == 0 else [((z - step * s >= 0) & (z - step * s < deep), z - step * s) for _, step in both]

    def x_in(s, hop):
        for ok, zs in columns(s):
            for d, step in both:
                from_x = x - step * hop
                come = ok & (from_x >= 0) & (from_x < wide)
                shard = zs * wide + from_x
                arrived(come, piece(shard, bulk_at, bulk), rx.at[d, hop, zs])
                along_x(come, zs, ((d, step),), hop, False)
                pass_on(come, shard)

    def y_in(ok, shard):
        if lone:
            arrived(ok, piece(shard, other_at, lone), ry.at[shard])
            send(ok, piece(shard, other_at, lone), piece(shard, other_at, lone), sc.at[1, shard], rc.at[1, shard], (me, mate))

    def y_all(s):
        for ok, zs in columns(s):
            if s > 0:
                y_in(ok, zs * wide + x)
            for hop in range(1, wide):
                for _, step in both:
                    from_x = x - step * hop
                    y_in(ok & (from_x >= 0) & (from_x < wide), zs * wide + from_x)

    for s in range(deep):
        for d, step in both:
            zs = z - step * s
            ok = (zs >= 0) & (zs < deep)
            shard = zs * wide + x
            if s:
                arrived(ok, piece(shard, bulk_at, bulk), rz.at[d, s])
            go = ok & (z + step >= 0) & (z + step < deep)
            source = piece(shard, bulk_at, bulk) if s else src.at[pl.ds(bulk_at, bulk)]
            if s + 1 < deep:
                send(go, source, piece(shard, bulk_at, bulk), sz.at[d, s], rz.at[d, s + 1], (me + step * wide, seq))
            if s:
                along_x(ok, zs, both, 0, False)
                pass_on(ok, shard)
        if s == 0:
            along_x(yes, z, both, 0, True)
            convert(1)
            keep = pltpu.make_async_copy(src, out.at[me], sem_load.at[0])
            keep.start()
            for ok, take, put in at_home:
                @pl.when(ok)
                def _(take=take, put=put):
                    take.wait()
                    put.start()
        else:
            for hop in range(1, wide):
                x_in(s - 1, hop)
        if s >= 2:
            y_all(s - 2)
    for hop in range(1, wide):
        x_in(deep - 1, hop)
    for s in range(max(deep - 2, 0), deep):
        y_all(s)
    keep.wait()
    for ok, take, put in at_home:
        @pl.when(ok)
        def _(put=put):
            put.wait()
    for q in range(micro):
        source = seq % each * micro + q
        for k, target in enumerate((rows, given)):
            arrived(source != seq, target.at[q], r_rows.at[k, q])
    for k in range(1, peers):
        source = (seq + k) % peers
        arrived(yes, labels.at[source], r_docs.at[source])

    mate_base = (1 - c) * half
    mate_bulk = mate_base + y * (half - bulk)
    mate_other = mate_base + (1 - y) * bulk if lone else mate_base

    def last(shard, _):
        ok = shard != me
        arrived(ok, piece(shard, mate_bulk, bulk), rc.at[0, shard])
        if lone:
            arrived(ok, piece(shard, mate_other, lone), rc.at[1, shard])
        return 0

    lax.fori_loop(0, wide * deep, last, 0)
    for ok, copy in sent:
        @pl.when(ok)
        def _(copy=copy):
            copy.wait_send()


def gather_blocks(grid, master, tokens, cotangent, docs):
    wide, tall, deep = grid
    slots = master.shape[0]
    n = wide * deep
    peers = tall * CORES
    micro = tokens.shape[0]
    low = tokens.dtype
    sem = pltpu.SemaphoreType.DMA
    hbm = pl.BlockSpec(memory_space=pl.ANY)
    vmem = pl.BlockSpec(memory_space=pltpu.VMEM)
    return pl.pallas_call(
        functools.partial(gather_kernel, grid, slots),
        out_shape=(
            jax.ShapeDtypeStruct((n,) + master.shape, low),
            jax.ShapeDtypeStruct(tokens.shape, low), jax.ShapeDtypeStruct(tokens.shape, low),
            jax.ShapeDtypeStruct((peers,) + docs.shape, docs.dtype),
        ),
        in_specs=[hbm, hbm, hbm, vmem],
        out_specs=(hbm, hbm, hbm, vmem),
        scratch_shapes=[
            pltpu.VMEM(master.shape, master.dtype), pltpu.VMEM(master.shape, low), pltpu.VMEM((2,) + tokens.shape[1:], low),
            sem((2,)), sem((CORES,)),
            sem((2, deep)), sem((2, deep + 1)),
            sem((2, wide, deep)), sem((2, wide + 1, deep)),
            sem((n,)), sem((n,)),
            sem((2, n)), sem((2, n)),
            sem((2, micro)), sem((2, micro)), sem((peers,)), sem((peers,)),
        ],
        compiler_params=pltpu.CompilerParams(collective_id=0, has_side_effects=True, vmem_limit_bytes=32 << 20),
        name="gather_blocks",
    )(master, tokens, cotangent, docs)

def far_first(at, size, i):
    above, below = size - 1 - at, at
    less, more = jnp.minimum(above, below), jnp.maximum(above, below)
    long_side = jnp.where(above >= below, 1, -1)
    j = i - (more - less)
    near = at + jnp.where(j % 2 == 0, 1, -1) * (less - j // 2)
    return jnp.where(j < 0, at + long_side * (more - i), near)


def entry(at, size, source_below, target):
    lower = jnp.where(at > 0, size - at, 0) if size > 2 else 0
    return target - at if source_below else lower + at - target


def entries(size):
    return size + 1 if size > 2 else 1

SUBS = 2
LAG = 2
LONE = 1 / 3


def split_of(slots, tall):
    half = slots // CORES
    piece = half // SUBS
    lone = round(piece * LONE) if tall == 2 and piece >= 8 else 0
    return half, piece, lone, piece - lone


def reduce_kernel(grid, slots, part, vec, out, vec_out, acc, land_c, land_y, land_x, land_z, fin, vbuf, vland,
                  s_load, s_c, r_c, s_y, r_y, s_x, r_x, s_z, r_z, s_f, r_f, s_m, r_m, s_v, r_v):
    wide, tall, deep = grid
    n = wide * deep
    x, y, z, c = place(grid)
    half, size, lone, bulk = split_of(slots, tall)
    me = z * wide + x
    seq = y * CORES + c
    mate = y * CORES + (1 - c)
    bulk_at = y * lone
    lone_at = y * bulk
    other_at = (1 - y) * bulk
    bits = lambda size: [1 << b for b in range(size.bit_length() - 1)]
    partners = [(me, mate)]
    partners += [(me, (y ^ b) * CORES + c) for b in bits(tall)]
    partners += [(z * wide + (x ^ b), seq) for b in bits(wide)]
    partners += [((z ^ b) * wide + x, seq) for b in bits(deep)]

    barrier = pltpu.get_barrier_semaphore()
    count = jnp.int32(0)
    for step_by, at, length in ((wide, z, deep), (1, x, wide)):
        for step in (1, -1):
            ok = (at + step >= 0) & (at + step < length)

            @pl.when(ok)
            def _(there=me + step * step_by):
                pl.semaphore_signal(barrier, inc=1, device_id=(there, seq), device_id_type=MESH)

            count = count + ok.astype(jnp.int32)
    for device in partners:
        pl.semaphore_signal(barrier, inc=1, device_id=device, device_id_type=MESH)
    pl.semaphore_wait(barrier, count + len(partners))

    def remote(source, target, send_sem, recv_sem, device):
        return pltpu.make_async_remote_copy(
            src_ref=source, dst_ref=target, send_sem=send_sem, recv_sem=recv_sem,
            device_id=device, device_id_type=MESH,
        )

    def landed(target, recv_sem):
        remote(target, target, s_load.at[0], recv_sem, (me, seq)).wait_recv()

    group = wide * SUBS
    total = n * SUBS

    def item_of(k):
        xs, zs = far_first(x, wide, k % wide), far_first(z, deep, k // group)
        sub = (k // wide) % SUBS
        return xs, zs, sub, (zs * wide + xs) * SUBS + sub

    def own(k):
        xs, zs, sub, item = item_of(k)
        return pltpu.make_async_copy(part.at[zs * wide + xs, pl.ds(c * half + sub * size, size)], acc.at[item], s_load.at[item])

    def swap(k):
        xs, zs, sub, item = item_of(k)
        source = part.at[zs * wide + xs, pl.ds((1 - c) * half + sub * size, size)]
        return remote(source, land_c.at[item], s_c.at[item], r_c.at[item], (me, mate))

    def cross(item):
        return remote(acc.at[item, pl.ds(other_at, lone)], land_y.at[item], s_y.at[item], r_y.at[item], (me, (tall - 1 - y) * CORES + c))

    def begin(k, _):
        own(k).start()
        swap(k).start()
        return 0

    rounds = len(partners)

    def vec_copy(t):
        return remote(vbuf.at[t], vland.at[t], s_v.at[t], r_v.at[t], partners[t])

    vbuf[0] = vec[...]
    vec_copy(0).start()
    lax.fori_loop(0, total, begin, 0)
    for t in range(rounds):
        landed(vland.at[t], r_v.at[t])
        vbuf[t + 1] = vbuf[t] + vland[t]
        if t + 1 < rounds:
            vec_copy(t + 1).start()
    vec_out[...] = vbuf[rounds]

    def add(item, at, count, ref, first):
        def one(i, _):
            acc[item, at + i] = acc[item, at + i] + ref[first + (i,)]
            return 0

        lax.fori_loop(0, count, one, 0, unroll=4)

    def step_x(k, begin_it):
        xs, zs, sub, item = item_of(k)
        for below, step in ((True, 1), (False, -1)):
            to = entry(x + step, wide, below, xs)
            sent = remote(acc.at[item, pl.ds(bulk_at, bulk)], land_x.at[to, zs * SUBS + sub], s_x.at[item],
                          r_x.at[to, zs * SUBS + sub], (me + step, seq))

            @pl.when((xs - x) * step > 0)
            def _():
                if begin_it:
                    sent.start()
                else:
                    sent.wait_send()

    def take_x(k):
        xs, zs, sub, item = item_of(k)
        for below, step in ((True, 1), (False, -1)):
            comes = ((xs - x) * step >= 0) & (x - step >= 0) & (x - step < wide)
            at = entry(x, wide, below, xs)

            @pl.when(comes)
            def _():
                landed(land_x.at[at, zs * SUBS + sub], r_x.at[at, zs * SUBS + sub])
                add(item, bulk_at, bulk, land_x, (at, zs * SUBS + sub))

    def step_z(k, begin_it):
        xs, zs, sub, item = item_of(k)
        for below, step in ((True, 1), (False, -1)):
            to = entry(z + step, deep, below, zs)
            sent = remote(acc.at[item, pl.ds(bulk_at, bulk)], land_z.at[to, sub], s_z.at[zs * SUBS + sub], r_z.at[to, sub],
                          (me + step * wide, seq))

            @pl.when((zs - z) * step > 0)
            def _():
                if begin_it:
                    sent.start()
                else:
                    sent.wait_send()

    def take_z(k):
        xs, zs, sub, item = item_of(k)
        for below, step in ((True, 1), (False, -1)):
            comes = ((zs - z) * step >= 0) & (z - step >= 0) & (z - step < deep)
            at = entry(z, deep, below, zs)

            @pl.when(comes)
            def _():
                landed(land_z.at[at, sub], r_z.at[at, sub])
                add(item, bulk_at, bulk, land_z, (at, sub))

    planes = bits(tall)

    def swap_plane(t, sub):
        mine = pl.ds(bulk_at, bulk)
        return remote(acc.at[me * SUBS + sub, mine], fin.at[t, sub, mine], s_f.at[t, sub], r_f.at[t, sub], (me, (y ^ planes[t]) * CORES + c))

    def take_plane(t, sub):
        item = me * SUBS + sub
        theirs = pl.ds((1 - y) * lone if lone else 0, bulk)
        landed(fin.at[t, sub, theirs], r_f.at[t, sub])
        swap_plane(t, sub).wait_send()
        add(item, lone, size - 2 * lone, fin.at[t, sub, pl.ds(lone, size - 2 * lone)], ())
        if lone:
            cross(item).wait_send()
            acc[item, pl.ds(other_at, lone)] = fin[t, sub, pl.ds(other_at, lone)]

    def swap_core(sub):
        return remote(acc.at[me * SUBS + sub], out.at[pl.ds(c * half + sub * size, size)], s_m.at[sub], r_m.at[sub], (me, mate))

    def first(k, _):
        item = item_of(k)[3]
        own(k).wait()
        landed(land_c.at[item], r_c.at[item])
        add(item, 0, size, land_c, (item,))
        if lone:
            cross(item).start()
        return 0

    def second(k, _):
        @pl.when(k < total)
        def _():
            item = item_of(k)[3]
            if lone:
                landed(land_y.at[item], r_y.at[item])
                add(item, lone_at, lone, land_y, (item,))
            if wide > 2:
                @pl.when(item_of(k)[0] != x)
                def _():
                    take_x(k)
            step_x(k, True)

        late = k - LAG * wide

        @pl.when((late >= 0) & (late % wide == wide - 1))
        def _():
            take_x(late)
            take_z(late)
            step_z(late, True)

        return 0

    lax.fori_loop(0, total, first, 0)
    lax.fori_loop(0, total + (LAG - 1) * wide, second, 0)
    def finish(k, _):
        swap(k).wait_send()
        if lone:
            item = item_of(k)[3]

            @pl.when(item // SUBS != me)
            def _():
                cross(item).wait_send()

        step_x(k, False)

        @pl.when(k % wide == wide - 1)
        def _():
            step_z(k, False)

        return 0

    tail = [total + (LAG - 1) * wide + i for i in range(wide)]
    for k in tail:
        second(jnp.int32(k), 0)
    for t in range(len(planes)):
        for sub in range(SUBS):
            swap_plane(t, sub).start()
        for sub in range(SUBS):
            take_plane(t, sub)
            if t == len(planes) - 1:
                swap_core(sub).start()
    for sub in range(SUBS):
        out[pl.ds(c * half + sub * size, size)] = acc[me * SUBS + sub]
    lax.fori_loop(0, total, finish, 0)
    for t in range(rounds):
        vec_copy(t).wait_send()
    for sub in range(SUBS):
        swap_core(sub).wait_send()
        landed(out.at[pl.ds((1 - c) * half + sub * size, size)], r_m.at[sub])


def reduce_blocks(grid, part, vec):
    wide, tall, deep = grid
    n, slots = part.shape[:2]
    half, size, lone, bulk = split_of(slots, tall)
    tile = part.shape[2:]
    sem = pltpu.SemaphoreType.DMA
    rounds = sum(length.bit_length() - 1 for length in (CORES, wide, tall, deep))
    planes = max(tall.bit_length() - 1, 1)
    items = n * SUBS
    buf = lambda *lead: pltpu.VMEM(lead + tile, part.dtype)
    return pl.pallas_call(
        functools.partial(reduce_kernel, grid, slots),
        out_shape=(jax.ShapeDtypeStruct((slots,) + tile, part.dtype), jax.ShapeDtypeStruct(vec.shape, vec.dtype)),
        in_specs=[pl.BlockSpec(memory_space=pl.ANY), pl.BlockSpec(memory_space=pltpu.VMEM)],
        out_specs=(pl.BlockSpec(memory_space=pltpu.VMEM), pl.BlockSpec(memory_space=pltpu.VMEM)),
        scratch_shapes=[
            buf(items, size), buf(items, size), buf(items, max(lone, 1)), buf(entries(wide), deep * SUBS, bulk),
            buf(entries(deep), SUBS, bulk), buf(planes, SUBS, size),
            pltpu.VMEM((rounds + 1,) + vec.shape, vec.dtype), pltpu.VMEM((rounds,) + vec.shape, vec.dtype),
            sem((items,)), sem((items,)), sem((items,)), sem((items,)), sem((items,)), sem((items,)),
            sem((entries(wide), deep * SUBS)), sem((deep * SUBS,)), sem((entries(deep), SUBS)),
            sem((planes, SUBS)), sem((planes, SUBS)), sem((SUBS,)), sem((SUBS,)), sem((rounds,)), sem((rounds,)),
        ],
        compiler_params=pltpu.CompilerParams(collective_id=1, has_side_effects=True, vmem_limit_bytes=63 << 20),
        name="reduce_blocks",
    )(part, vec)


STEP_BLOCKS = 32
DEPTH = 4


def assemble_kernel(table, blocks, w_in, w_out, w_ff, w_down, wide, tall, s_in, s_out):
    outs = []
    for ref in (w_in, w_out, w_ff, w_down):
        rows, cols = ref.shape
        per_row = cols // BS
        deep = STEP_BLOCKS // per_row
        for r in range(rows // (BS * deep)):
            outs.append((ref, r * BS * deep, deep, per_row))

    def target(step):
        ref, at, deep, per_row = outs[step]
        slot = step % DEPTH
        return (wide.at[slot] if deep == 1 else tall.at[slot]), ref.at[pl.ds(at, BS * deep)], deep, per_row

    def fetch(step):
        buffer, _, deep, per_row = target(step)

        def one(i, _):
            rows = pl.ds(pl.multiple_of(i // per_row * BS, BS), BS)
            cols = pl.ds(pl.multiple_of(i % per_row * BS, BS), BS)
            pltpu.make_async_copy(blocks.at[table[step * STEP_BLOCKS + i]], buffer.at[rows, cols], s_in.at[step % DEPTH]).start()
            return 0

        lax.fori_loop(0, STEP_BLOCKS, one, 0)

    def put(step):
        buffer, place_to, _, _ = target(step)
        return pltpu.make_async_copy(buffer, place_to, s_out.at[step % DEPTH])

    steps = len(outs)
    for step in range(min(DEPTH - 1, steps)):
        fetch(step)
    for step in range(steps):
        buffer, place_to, _, _ = target(step)
        pltpu.make_async_copy(place_to, buffer, s_in.at[step % DEPTH]).wait()
        put(step).start()
        ahead = step + DEPTH - 1
        if ahead < steps:
            if step >= 1:
                put(step - 1).wait()
            fetch(ahead)
    for step in range(max(steps - DEPTH, 0), steps):
        put(step).wait()


def slots_in_order(block_of_slot, order):
    match = jnp.array(order, jnp.int32)[:, None] == block_of_slot[None, :]
    return jnp.sum(jnp.where(match, jnp.arange(block_of_slot.shape[0], dtype=jnp.int32)[None, :], 0), axis=1)


def assemble(blocks, table):
    shapes = [(D, sum(SHAPES[m][1] for m in WIDE_IN)), (sum(SHAPES[m][0] for m in TALL_OUT), D), (D, 2 * FF), (FF, D)]
    hbm = pl.BlockSpec(memory_space=pl.ANY)
    return pl.pallas_call(
        assemble_kernel,
        out_shape=tuple(jax.ShapeDtypeStruct(shape, BF16) for shape in shapes),
        grid_spec=pltpu.PrefetchScalarGridSpec(
            num_scalar_prefetch=1, grid=(1,), in_specs=[hbm], out_specs=(hbm,) * 4,
            scratch_shapes=[
                pltpu.VMEM((DEPTH, BS, STEP_BLOCKS * BS), BF16),
                pltpu.VMEM((DEPTH, STEP_BLOCKS // (D // BS) * BS, D), BF16),
                pltpu.SemaphoreType.DMA((DEPTH,)), pltpu.SemaphoreType.DMA((DEPTH,)),
            ],
        ),
        compiler_params=kernel_params(),
        name="assemble",
    )(table, blocks)


UNIT_ROWS = 256
UNIT_COLS = 1024
STAGES = 3


def slot_grads_kernel(sizes, slot_of, *refs):
    count = sum(len(left) + len(right) for left, right in sizes)
    arrays, (out, left, right, turned, stage, s_in, s_out) = refs[:count], refs[count:]
    units = []
    groups, k, left_at, right_at, first = [], 0, 0, 0, 0
    for lefts, rights in sizes:
        copies, at = [], left_at
        for width in lefts:
            copies.append(pltpu.make_async_copy(arrays[k], left.at[:, pl.ds(at, width)], s_in.at[k]))
            at, k = at + width, k + 1
        rows, at = at - left_at, right_at
        for width in rights:
            copies.append(pltpu.make_async_copy(arrays[k], right.at[:, pl.ds(at, width)], s_in.at[k]))
            at, k = at + width, k + 1
        cols = at - right_at
        groups.append((copies, left_at, rows, right_at, cols, first))
        left_at, right_at = left_at + rows, right_at + cols
        first += rows // BS * (cols // BS)
    for copies, *_ in groups:
        for copy in copies:
            copy.start()

    def drain(slot):
        pltpu.make_async_copy(out.at[pl.ds(0, UNIT_ROWS // BS * (UNIT_COLS // BS))], out.at[pl.ds(0, UNIT_ROWS // BS * (UNIT_COLS // BS))],
                              s_out.at[slot]).wait()

    done = 0
    for copies, left_at, rows, right_at, cols, first in groups:
        for copy in copies:
            copy.wait()
        across = cols // UNIT_COLS

        def one(u, _, left_at=left_at, right_at=right_at, cols=cols, first=first, across=across, done=done):
            r, q = u // across, u % across
            slot = (done + u) % STAGES

            @pl.when(q == 0)
            def _():
                turned[...] = left[:, pl.ds(pl.multiple_of(left_at + r * UNIT_ROWS, BS), UNIT_ROWS)].T

            @pl.when(done + u >= STAGES)
            def _():
                drain(slot)

            column = pl.multiple_of(right_at + q * UNIT_COLS, BS)
            stage[slot] = dot(turned[...], right[:, pl.ds(column, UNIT_COLS)]).astype(BF16)
            for i in range(UNIT_ROWS // BS):
                for p in range(UNIT_COLS // BS):
                    block = first + (r * (UNIT_ROWS // BS) + i) * (cols // BS) + q * (UNIT_COLS // BS) + p
                    pltpu.make_async_copy(stage.at[slot, pl.ds(i * BS, BS), pl.ds(p * BS, BS)], out.at[slot_of[block]], s_out.at[slot]).start()
            return 0

        total = rows // UNIT_ROWS * across
        lax.fori_loop(0, total, one, 0)
        done += total
    for u in range(max(done - STAGES, 0), done):
        drain(u % STAGES)


def slot_grads(slot_of, groups):
    arrays = [a for lefts, rights in groups for a in lefts + rights]
    sizes = [([a.shape[1] for a in lefts], [a.shape[1] for a in rights]) for lefts, rights in groups]
    tokens = arrays[0].shape[0]
    hbm = pl.BlockSpec(memory_space=pl.ANY)
    return pl.pallas_call(
        functools.partial(slot_grads_kernel, sizes),
        out_shape=jax.ShapeDtypeStruct((slot_of.shape[0], BS, BS), BF16),
        grid_spec=pltpu.PrefetchScalarGridSpec(
            num_scalar_prefetch=1, grid=(1,), in_specs=[hbm] * len(arrays), out_specs=hbm,
            scratch_shapes=[
                pltpu.VMEM((tokens, sum(sum(left) for left, _ in sizes)), BF16),
                pltpu.VMEM((tokens, sum(sum(right) for _, right in sizes)), BF16),
                pltpu.VMEM((UNIT_ROWS, tokens), BF16),
                pltpu.VMEM((STAGES, UNIT_ROWS, UNIT_COLS), BF16),
                pltpu.SemaphoreType.DMA((len(arrays),)), pltpu.SemaphoreType.DMA((STAGES,)),
            ],
        ),
        compiler_params=kernel_params(),
        name="slot_grads",
    )(slot_of, *arrays)


SHAMPOO = 8


def shampoo_kernel(norm, total, master, left, right, left_root, right_root, grad, new_left, new_right, new_master, low):
    for i in range(SHAMPOO):
        g = total[i]
        value = g.astype(F32) * norm
        grad[i] = value
        new_left[i] = 0.5 * left[i] + dot_nt(g, g) * (0.5 * norm * norm / BS)
        new_right[i] = 0.5 * right[i] + dot_tn(g, g) * (0.5 * norm * norm / BS)
        inner = dot(g, right_root[i].astype(BF16))
        moved = dot(left_root[i].astype(BF16), inner.astype(BF16)) * (LR_MATRIX * norm)
        fresh = master[i] - moved
        new_master[i] = fresh
        low[i] = fresh.astype(BF16)


def shampoo(norm, total, master, left, right, left_root, right_root):
    slots = total.shape[0]
    spec = pl.BlockSpec((SHAMPOO, BS, BS), lambda i: (i, 0, 0))
    full = jax.ShapeDtypeStruct(master.shape, F32)
    return pl.pallas_call(
        functools.partial(shampoo_kernel, norm),
        out_shape=(full, full, full, full, jax.ShapeDtypeStruct(master.shape, BF16)),
        grid=(slots // SHAMPOO,),
        in_specs=[spec] * 6,
        out_specs=(spec,) * 5,
        compiler_params=kernel_params(),
        name="shampoo",
    )(total, master, left, right, left_root, right_root)


BLOCK = 256
HALO = 8


def lane_index(shape):
    return lax.broadcasted_iota(jnp.int32, shape, len(shape) - 1)


def conv_tile(extended, taps, marks, count):
    total = jnp.broadcast_to(taps[KERNEL : KERNEL + 1, :], (count, extended.shape[1]))
    for tap in range(KERNEL):
        total = total + taps[tap : tap + 1, :] * near_rows(extended, tap, count) * marks[:, tap : tap + 1]
    return total


def near_rows(extended, tap, count):
    back = REACH - tap
    moved = pltpu.roll(extended, back, 0) if back else extended
    return moved[HALO : HALO + count, :]


def softplus(v):
    return jnp.maximum(v, 0.0) + jnp.log(1.0 + jnp.exp(-jnp.abs(v)))


def chunk_decays(raw, params):
    delta = softplus(raw + params[0:1, :])
    decay = -delta * jnp.exp(params[1:2, :])
    block = raw.shape[0] if raw.shape[0] < BLOCK else BLOCK
    rows = lax.broadcasted_iota(jnp.int32, (block, block), 0)
    lower = (rows >= lane_index((block, block))).astype(F32)
    sums = [dot(lower, decay[i : i + block, :], HIGHEST) for i in range(0, raw.shape[0], block)]
    return delta, decay, jnp.concatenate(sums, axis=0)


def end_weights(delta, sums, marks):
    last = sums[-1:, :]
    return jnp.exp(last - sums) * delta * marks[:, 5:6], jnp.exp(last) * marks[-1:, 4:5]


def spread_matrix():
    rows = lax.broadcasted_iota(jnp.int32, (LANES, INNER), 0)
    return (rows == lane_index((LANES, INNER)) // HEAD).astype(F32)


def mix_first_kernel(proj_x, proj_bc, halo, taps, params, raw, marks, xbc, decays, decays_t, state, factor):
    tokens = raw.shape[0]
    mark = marks[...]
    for ref, at in ((proj_x, 0), (proj_bc, INNER)):
        step = 256
        for q in range(0, ref.shape[1], step):
            cols = slice(at + q, at + q + step)
            own = ref[:, q : q + step].astype(BF16).astype(F32)
            extended = jnp.concatenate([halo[:, cols].astype(F32), own], axis=0)
            value = conv_tile(extended, taps[:, cols], mark, tokens)
            xbc[:, cols] = (value * sigmoid(value)).astype(BF16)
    delta, decay, sums = chunk_decays(raw[...], params[...])
    decays[0] = delta
    decays[1] = sums
    decays_t[...] = sums.T
    spread = spread_matrix()
    total = jnp.zeros((NSTATE, INNER), F32)
    product = jnp.ones((1, LANES), F32)
    for i in range(0, tokens, BLOCK):
        rows = slice(i, i + BLOCK)
        weight, own = end_weights(delta[rows], sums[rows], mark[rows])
        weighted = (xbc[rows, :INNER].astype(F32) * dot(weight.astype(BF16), spread.astype(BF16))).astype(BF16)
        keep = dot(jnp.broadcast_to(own, (8, LANES)), spread, HIGHEST)[0:1]
        total = keep * total + dot_tn(xbc[rows, INNER : INNER + NSTATE], weighted)
        product = product * own
    state[...] = total.astype(BF16)
    factor[...] = jnp.broadcast_to(product, factor.shape)


def mix_first(proj, halo, taps, params, raw, marks):
    tokens = raw.shape[0]
    vmem = pl.BlockSpec(memory_space=pltpu.VMEM)
    return pl.pallas_call(
        mix_first_kernel,
        out_shape=(
            jax.ShapeDtypeStruct((tokens, CHANNELS), BF16),
            jax.ShapeDtypeStruct((2, tokens, LANES), F32),
            jax.ShapeDtypeStruct((LANES, tokens), F32),
            jax.ShapeDtypeStruct((NSTATE, INNER), BF16),
            jax.ShapeDtypeStruct((8, LANES), F32),
        ),
        grid=(1,),
        in_specs=[
            pl.BlockSpec((tokens, INNER), lambda i: (0, 1)),
            pl.BlockSpec((tokens, 2 * NSTATE), lambda i: (0, 2 * INNER // (2 * NSTATE))),
            vmem, vmem, vmem, vmem, vmem,
        ],
        out_specs=(vmem,) * 5,
        compiler_params=kernel_params(),
        name="mix_first",
    )(proj, proj, halo, taps, params, raw, marks)


def attend(left, right, mark_rows, mark_cols):
    return jnp.where(mark_rows & mark_cols, dot_nt(left, right), 0.0)


def halves(tile):
    low = lane_index(tile.shape) < HEAD
    zero = jnp.zeros_like(tile)
    return jnp.where(low, tile, zero), jnp.where(low, zero, tile)


def pair_column(values, a):
    return values[:, a * HEAD : a * HEAD + 1]


def mix_second_kernel(x, b, c, z, decays, decays_t, marks, labels, incoming, skip, gain, y, normed, states,
                      wide_sums, wide_delta, wide_end, keep, near, b_t, state, gated, squares):
    j = pl.program_id(0)
    tokens = x.shape[0]
    blocks = tokens // BLOCK
    cols = pl.ds(pl.multiple_of(j * LANES, LANES), LANES)

    @pl.when(j == 0)
    def _():
        spread = spread_matrix()
        rows = lax.broadcasted_iota(jnp.int32, (BLOCK, BLOCK), 0)
        ordered = rows >= lane_index((BLOCK, BLOCK))
        for i in range(blocks):
            at = slice(i * BLOCK, (i + 1) * BLOCK)
            mark = marks[at]
            same = mark[:, 6:7] == labels[0:1, at]
            near[i] = jnp.where(ordered & same, dot_nt(c[at], b[at]), 0.0)
            b_t[i] = b[at].T
            weight, own = end_weights(decays[0, at], decays[1, at], mark)
            wide_end[at] = dot(weight.astype(BF16), spread.astype(BF16)).astype(BF16)
            wide_sums[at] = dot(decays[1, at], spread, HIGHEST)
            wide_delta[at] = dot(decays[0, at].astype(BF16), spread.astype(BF16)).astype(BF16)
            keep[i] = dot(jnp.broadcast_to(own, (8, LANES)), spread, HIGHEST)
        squares[...] = jnp.zeros_like(squares)

    state[...] = incoming[...].astype(F32)
    for i in range(blocks):
        at = slice(i * BLOCK, (i + 1) * BLOCK)
        states[i] = state[...]
        tile = x[at].astype(F32)
        scaled = (tile * wide_delta[at, cols].astype(F32)).astype(BF16)
        sums = wide_sums[at, cols]
        total = jnp.zeros((BLOCK, LANES), F32)
        for a, part in enumerate(halves(scaled)):
            row = decays_t[pl.ds(2 * j + a, 1), at]
            weight = near[i] * jnp.exp(jnp.minimum(pair_column(sums, a) - row, 0.0))
            total = total + dot(weight.astype(BF16), part)
        carried = dot(c[at], state[...].astype(BF16))
        total = total + carried * jnp.exp(sums) * marks[at, 4:5] + skip[0:1, cols] * tile
        y[at] = total
        gate = z[at]
        gate = total * gate * sigmoid(gate)
        gated[at, cols] = gate
        squares[at] += gate * gate
        weighted = (tile * wide_end[at, cols].astype(F32)).astype(BF16)
        state[...] = keep[i, 0:1, cols] * state[...] + dot(b_t[i], weighted)
    states[blocks] = state[...]

    @pl.when(j == PAIRS - 1)
    def _():
        for i in range(blocks):
            at = slice(i * BLOCK, (i + 1) * BLOCK)
            scale = lax.rsqrt(jnp.sum(squares[at], axis=1, keepdims=True) / INNER + EPS)
            normed[at] = (gated[at] * scale * gain[0:1, :]).astype(BF16)


def mix_second(xbc, proj, decays, decays_t, marks, labels, incoming, skip, gain):
    tokens = xbc.shape[0]
    blocks = tokens // BLOCK
    tile = pl.BlockSpec((tokens, LANES), lambda j: (0, j))
    return pl.pallas_call(
        mix_second_kernel,
        out_shape=(
            jax.ShapeDtypeStruct((tokens, INNER), F32),
            jax.ShapeDtypeStruct((tokens, INNER), BF16),
            jax.ShapeDtypeStruct((blocks + 1, NSTATE, INNER), F32),
        ),
        grid=(PAIRS,),
        in_specs=[
            tile,
            pl.BlockSpec((tokens, NSTATE), lambda j: (0, INNER // NSTATE)),
            pl.BlockSpec((tokens, NSTATE), lambda j: (0, INNER // NSTATE + 1)),
            tile,
            whole(decays.shape), whole(decays_t.shape), whole(marks.shape), whole(labels.shape),
            pl.BlockSpec((NSTATE, LANES), lambda j: (0, j)),
            whole(skip.shape), whole(gain.shape),
        ],
        out_specs=(tile, whole((tokens, INNER)), pl.BlockSpec((blocks + 1, NSTATE, LANES), lambda j: (0, 0, j))),
        scratch_shapes=[
            pltpu.VMEM((tokens, INNER), F32), pltpu.VMEM((tokens, INNER), BF16), pltpu.VMEM((tokens, INNER), BF16),
            pltpu.VMEM((blocks, 8, INNER), F32), pltpu.VMEM((blocks, BLOCK, BLOCK), F32),
            pltpu.VMEM((blocks, NSTATE, BLOCK), BF16), pltpu.VMEM((NSTATE, LANES), F32),
            pltpu.VMEM((tokens, INNER), F32), pltpu.VMEM((tokens, LANES), F32),
        ],
        compiler_params=kernel_params(),
        name="mix_second",
    )(xbc, xbc, xbc, proj, decays, decays_t, marks, labels, incoming, skip, gain)


def gate_back_kernel(grad, y, z, gain, c, decays, marks, g_y, g_z, g_gain, g_state):
    step = pl.program_id(0)
    value, gate = y[...], z[...]
    opened = sigmoid(gate)
    swish = gate * opened
    gated = value * swish
    scale = lax.rsqrt(jnp.mean(gated * gated, axis=1, keepdims=True) + EPS)
    unit = gated * scale
    given = grad[...]
    scaled = given * gain[0:1, :]
    g_gated = scale * (scaled - unit * jnp.mean(scaled * unit, axis=1, keepdims=True))
    fresh = g_gated * swish
    g_y[...] = fresh.astype(BF16)
    g_z[...] = (g_gated * value * (opened + swish * (1.0 - opened))).astype(BF16)
    spread = spread_matrix()
    sums = decays[1]
    mark = marks[...]
    entry_weight = jnp.exp(sums) * mark[:, 4:5]
    own = jnp.exp(sums[-1:, :]) * mark[-1:, 4:5]
    keep = dot(jnp.broadcast_to(own, (8, LANES)), spread, HIGHEST)[0:1]
    weighted = (fresh * dot(entry_weight.astype(BF16), spread.astype(BF16))).astype(BF16)
    local = dot_tn(c[...], weighted)
    gains = jnp.broadcast_to(jnp.sum(given * unit, axis=0, keepdims=True), g_gain.shape)

    @pl.when(step == 0)
    def _():
        g_state[...] = local
        g_gain[...] = gains

    @pl.when(step > 0)
    def _():
        g_state[...] = keep * g_state[...] + local
        g_gain[...] += gains


def gate_back(grad, y, proj, gain, xbc, decays, marks):
    tokens = y.shape[0]
    blocks = tokens // BLOCK
    rows = lambda width, col: pl.BlockSpec((BLOCK, width), lambda i: (blocks - 1 - i, col))
    return pl.pallas_call(
        gate_back_kernel,
        out_shape=(
            jax.ShapeDtypeStruct((tokens, INNER), BF16),
            jax.ShapeDtypeStruct((tokens, INNER), BF16),
            jax.ShapeDtypeStruct((8, INNER), F32),
            jax.ShapeDtypeStruct((NSTATE, INNER), F32),
        ),
        grid=(blocks,),
        in_specs=[
            rows(INNER, 0), rows(INNER, 0), rows(INNER, 0), whole(gain.shape), rows(NSTATE, INNER // NSTATE + 1),
            pl.BlockSpec((2, BLOCK, LANES), lambda i: (0, blocks - 1 - i, 0)), rows(LANES, 0),
        ],
        out_specs=(rows(INNER, 0), rows(INNER, 0), whole((8, INNER)), whole((NSTATE, INNER))),
        compiler_params=kernel_params(),
        name="gate_back",
    )(grad, y, proj, gain, xbc, decays, marks)


def conv_back(grad, extended, taps, marks, count):
    acc = conv_tile(extended, taps, marks, count)
    opened = sigmoid(acc)
    g_acc = grad * (opened + acc * opened * (1.0 - opened))
    width = g_acc.shape[1]
    weights, result = [], jnp.zeros((HALO + count, width), F32)
    for tap in range(KERNEL):
        marked = g_acc * marks[:, tap : tap + 1]
        weights.append(jnp.sum(marked * near_rows(extended, tap, count), axis=0, keepdims=True))
        spread = jnp.concatenate([jnp.zeros((HALO, width), F32), marked * taps[tap : tap + 1, :]], axis=0)
        back = REACH - tap
        result = result + (pltpu.roll(spread, HALO + count - back, 0) if back else spread)
    weights.append(jnp.sum(g_acc, axis=0, keepdims=True))
    weights.append(jnp.zeros((8 - KERNEL - 1, width), F32))
    return result, jnp.concatenate(weights, axis=0)


def mix_back_kernel(x, b, c, proj_x, proj_bc, halo, taps, y, g_y, decays, decays_t, raw, params, marks, labels, states, leaving, skip,
                    g_conv, g_rim, g_taps, g_raw, g_params,
                    wide_sums, wide_delta, wide_end, wide_skip, keep, near, c_t, state, g_near, g_b, g_c, g_cum, g_delta, g_skip, ends):
    j = pl.program_id(0)
    tokens = x.shape[0]
    blocks = tokens // BLOCK
    cols = pl.ds(pl.multiple_of(j * LANES, LANES), LANES)
    lane = lane_index((LANES, LANES))
    gather = ((lax.broadcasted_iota(jnp.int32, (LANES, LANES), 0) // HEAD + 2 * j) == lane).astype(BF16)

    def collect(values):
        high = values.astype(BF16)
        return dot(high, gather) + dot((values - high.astype(F32)).astype(BF16), gather)

    @pl.when(j == 0)
    def _():
        spread = spread_matrix()
        rows = lax.broadcasted_iota(jnp.int32, (BLOCK, BLOCK), 0)
        ordered = rows <= lane_index((BLOCK, BLOCK))
        for i in range(blocks):
            at = slice(i * BLOCK, (i + 1) * BLOCK)
            mark = marks[at]
            same = mark[:, 6:7] == labels[0:1, at]
            near[i] = jnp.where(ordered & same, dot_nt(b[at], c[at]), 0.0)
            c_t[i] = c[at].T
            weight, own = end_weights(decays[0, at], decays[1, at], mark)
            end_only = jnp.exp(decays[1, at][-1:, :] - decays[1, at]) * mark[:, 5:6]
            wide_end[at] = dot(end_only.astype(BF16), spread.astype(BF16)).astype(BF16)
            wide_sums[at] = dot(decays[1, at], spread, HIGHEST)
            wide_delta[at] = dot(decays[0, at].astype(BF16), spread.astype(BF16)).astype(BF16)
            keep[i] = dot(jnp.broadcast_to(own, (8, LANES)), spread, HIGHEST)
        for ref in (g_near, g_b, g_c, g_cum, g_delta, g_skip, ends):
            ref[...] = jnp.zeros_like(ref)

    state[...] = leaving[...].astype(F32)
    g_x = []
    for i in range(blocks - 1, -1, -1):
        at = slice(i * BLOCK, (i + 1) * BLOCK)
        tile = x[at].astype(F32)
        step = wide_delta[at, cols].astype(F32)
        scaled = tile * step
        low_scaled = scaled.astype(BF16)
        sums = wide_sums[at, cols]
        end = wide_end[at, cols].astype(F32)
        given = g_y[at]
        low_state = state[...].astype(BF16)
        ends[i] += collect(jnp.broadcast_to(jnp.sum(states[i + 1] * state[...], axis=0, keepdims=True), (8, LANES)))
        total = end * dot(b[at], low_state)
        for a, (part, grad) in enumerate(zip(halves(low_scaled), halves(given))):
            row = decays_t[pl.ds(2 * j + a, 1), at]
            decay = jnp.exp(jnp.minimum(row - pair_column(sums, a), 0.0))
            total = total + dot((near[i] * decay).astype(BF16), grad)
            g_near[i] += decay * dot_nt(part, given)
        given = given.astype(F32)
        entry = jnp.exp(sums) * marks[at, 4:5]
        reached = (given * entry).astype(BF16)
        g_b[at] += dot_nt((scaled * end).astype(BF16), low_state)
        g_c[at] += dot_nt(reached, states[i].astype(BF16))
        own_skip = skip[0:1, cols]
        g_cum[at] += collect(given * (y[at] - own_skip * tile) - scaled * total)
        g_delta[at] += collect(total * tile)
        g_skip[...] += collect(jnp.broadcast_to(jnp.sum(given * tile, axis=0, keepdims=True), (8, LANES)))
        g_x.append(step * total + own_skip * given)
        state[...] = keep[i, 0:1, cols] * state[...] + dot(c_t[i], reached)

    mark = marks[...]
    own = proj_x[...].astype(BF16).astype(F32)
    extended = jnp.concatenate([halo[:, cols].astype(F32), own], axis=0)
    result, weights = conv_back(jnp.concatenate(g_x[::-1], axis=0), extended, taps[:, cols], mark, tokens)
    g_rim[:HALO, cols] = result[:HALO]
    g_rim[HALO:, cols] = result[tokens:]
    g_conv[:, cols] = result[HALO:].astype(BF16)
    g_taps[:, cols] = weights

    @pl.when(j == PAIRS - 1)
    def _():
        for i in range(blocks):
            at = slice(i * BLOCK, (i + 1) * BLOCK)
            rows = lax.broadcasted_iota(jnp.int32, (BLOCK, BLOCK), 0)
            seen = (rows <= lane_index((BLOCK, BLOCK))) & (marks[at, 6:7] == labels[0:1, at])
            grad = jnp.where(seen, g_near[i], 0.0)
            g_b[at] += dot(grad.astype(BF16), c[at])
            g_c[at] += dot(grad.T.astype(BF16), b[at])
        for k, ref in enumerate((g_b, g_c)):
            at = slice(INNER + k * NSTATE, INNER + (k + 1) * NSTATE)
            own = proj_bc[:, k * NSTATE : (k + 1) * NSTATE].astype(BF16).astype(F32)
            extended = jnp.concatenate([halo[:, at].astype(F32), own], axis=0)
            result, weights = conv_back(ref[...], extended, taps[:, at], mark, tokens)
            g_rim[:HALO, at] = result[:HALO]
            g_rim[HALO:, at] = result[tokens:]
            g_conv[:, at] = result[HALO:].astype(BF16)
            g_taps[:, at] = weights
        rate = -jnp.exp(params[1:2, :])
        bias_sum = jnp.zeros((1, LANES), F32)
        rate_sum = jnp.zeros((1, LANES), F32)
        rows = lax.broadcasted_iota(jnp.int32, (BLOCK, BLOCK), 0)
        upper = (rows <= lane_index((BLOCK, BLOCK))).astype(F32)
        for i in range(blocks):
            at = slice(i * BLOCK, (i + 1) * BLOCK)
            g_decay = dot(upper, g_cum[at], HIGHEST) + ends[i, 0:1, :]
            delta = decays[0, at]
            full = g_delta[at] + g_decay * rate
            full = full * sigmoid(raw[at] + params[0:1, :])
            g_raw[at] = full.astype(BF16)
            bias_sum = bias_sum + jnp.sum(full, axis=0, keepdims=True)
            rate_sum = rate_sum + jnp.sum(g_decay * delta * rate, axis=0, keepdims=True)
        g_params[...] = jnp.concatenate([bias_sum, rate_sum, g_skip[0:1, :], jnp.zeros((5, LANES), F32)], axis=0)


def mix_back(xbc, proj, halo, taps, y, g_y, decays, decays_t, raw, params, marks, labels, states, leaving, skip):
    tokens = xbc.shape[0]
    blocks = tokens // BLOCK
    tile = pl.BlockSpec((tokens, LANES), lambda j: (0, j))
    acc = lambda *shape: pltpu.VMEM(shape, F32)
    return pl.pallas_call(
        mix_back_kernel,
        out_shape=(
            jax.ShapeDtypeStruct((tokens, CHANNELS), BF16),
            jax.ShapeDtypeStruct((2 * HALO, CHANNELS), F32),
            jax.ShapeDtypeStruct((8, CHANNELS), F32),
            jax.ShapeDtypeStruct((tokens, LANES), BF16),
            jax.ShapeDtypeStruct((8, LANES), F32),
        ),
        grid=(PAIRS,),
        in_specs=[
            tile,
            pl.BlockSpec((tokens, NSTATE), lambda j: (0, INNER // NSTATE)),
            pl.BlockSpec((tokens, NSTATE), lambda j: (0, INNER // NSTATE + 1)),
            pl.BlockSpec((tokens, LANES), lambda j: (0, PAIRS + j)),
            pl.BlockSpec((tokens, 2 * NSTATE), lambda j: (0, 2 * INNER // (2 * NSTATE))),
            whole(halo.shape), whole(taps.shape), tile, tile,
            whole(decays.shape), whole(decays_t.shape), whole(raw.shape), whole(params.shape), whole(marks.shape), whole(labels.shape),
            pl.BlockSpec((blocks + 1, NSTATE, LANES), lambda j: (0, 0, j)),
            pl.BlockSpec((NSTATE, LANES), lambda j: (0, j)),
            whole(skip.shape),
        ],
        out_specs=(
            whole((tokens, CHANNELS)), whole((2 * HALO, CHANNELS)), whole((8, CHANNELS)), whole((tokens, LANES)), whole((8, LANES)),
        ),
        scratch_shapes=[
            acc(tokens, INNER), pltpu.VMEM((tokens, INNER), BF16), pltpu.VMEM((tokens, INNER), BF16), acc(8, LANES),
            acc(blocks, 8, INNER), acc(blocks, BLOCK, BLOCK), pltpu.VMEM((blocks, NSTATE, BLOCK), BF16), acc(NSTATE, LANES),
            acc(blocks, BLOCK, BLOCK), acc(tokens, NSTATE), acc(tokens, NSTATE), acc(tokens, LANES), acc(tokens, LANES),
            acc(8, LANES), acc(blocks, 8, LANES),
        ],
        compiler_params=kernel_params(),
        name="mix_back",
    )(xbc, xbc, xbc, proj, proj, halo, taps, y, g_y, decays, decays_t, raw, params, marks, labels, states, leaving, skip)


QBLOCK = 256
GROUPS = HEADS // KV_HEADS
QPAIRS = QDIM // LANES
SCALE = 1.0 / math.sqrt(HEAD)


def swap_halves(values):
    half = HEAD // 2
    front = lane_index(values.shape) % HEAD < half
    width = values.shape[-1]
    return jnp.where(front, pltpu.roll(values, width - half, 1), pltpu.roll(values, half, 1))


def turn(values, cosine, sine):
    return values * cosine + swap_halves(values) * sine


def rope_kernel(*refs):
    queries, (k, v, cosine, sine, q_out, kv_out) = refs[:QPAIRS], refs[QPAIRS:]
    cos, sin = cosine[...], sine[...]
    for p, q in enumerate(queries):
        q_out[:, p * LANES : (p + 1) * LANES] = turn(q[...], cos, sin).astype(BF16)
    kv_out[:, :KDIM] = turn(k[...], cos, sin).astype(BF16)
    kv_out[:, KDIM:] = v[...].astype(BF16)


def rope_all(proj, cosine, sine):
    tokens = proj.shape[0]
    start = 2 * INNER + 2 * NSTATE
    return pl.pallas_call(
        rope_kernel,
        out_shape=(jax.ShapeDtypeStruct((tokens, QDIM), BF16), jax.ShapeDtypeStruct((tokens, 2 * KDIM), BF16)),
        grid=(1,),
        in_specs=[
            pl.BlockSpec((tokens, LANES), lambda i, p=p: (0, start // LANES + p)) for p in range(QPAIRS + 2)
        ] + [whole(cosine.shape), whole(sine.shape)],
        out_specs=(whole((tokens, QDIM)), whole((tokens, 2 * KDIM))),
        compiler_params=kernel_params(),
        name="rope",
    )(*[proj] * (QPAIRS + 2), cosine, sine)


def both_sides(tile, both):
    low = lane_index(tile.shape) < HEAD
    zero = jnp.zeros_like(tile)
    moved = pltpu.roll(tile.astype(F32), HEAD, 1).astype(tile.dtype)
    both[0, 0] = jnp.where(low, tile, zero)
    both[0, 1] = jnp.where(low, zero, moved)
    both[1, 0] = jnp.where(low, moved, zero)
    both[1, 1] = jnp.where(low, zero, tile)


def attend_kernel(q, kv, key_labels, marks, context, stats, keys, values):
    block, pair = pl.program_id(0), pl.program_id(1)
    window = DOC_MOST + QBLOCK
    start = pl.multiple_of(block * QBLOCK, QBLOCK)

    @pl.when((block == 0) & (pair == 0))
    def _():
        both_sides(kv[:, :KDIM], keys)
        both_sides(kv[:, KDIM:], values)

    group = pair // (GROUPS // 2)
    rows = lax.broadcasted_iota(jnp.int32, (QBLOCK, window), 0)
    cols = lane_index((QBLOCK, window))
    seen = (cols <= rows + DOC_MOST) & (marks[:, 6:7] == key_labels[0, 0:1, :])
    total = jnp.zeros((QBLOCK, LANES), F32)
    found = jnp.zeros((QBLOCK, LANES), F32)
    for a in range(2):
        scores = dot_nt(q[...], keys[group, a, pl.ds(start, window), :]) * SCALE
        scores = jnp.where(seen, scores, NEG_BIG)
        most = jnp.max(scores, axis=1, keepdims=True)
        probs = jnp.exp(scores - most)
        mass = jnp.sum(probs, axis=1, keepdims=True)
        probs = probs * (1.0 / mass)
        total = total + dot(probs.astype(BF16), values[group, a, pl.ds(start, window), :])
        found = jnp.where(lane_index(found.shape) == a, most + jnp.log(mass), found)
    context[...] = total.astype(BF16)
    stats[0] = found.T[0:8, :]


def attend(q, kv, key_labels, marks):
    tokens = q.shape[0]
    blocks = tokens // QBLOCK
    tile = pl.BlockSpec((QBLOCK, LANES), lambda i, p: (i, p))
    return pl.pallas_call(
        attend_kernel,
        out_shape=(jax.ShapeDtypeStruct((tokens, QDIM), BF16), jax.ShapeDtypeStruct((QPAIRS, 8, tokens), F32)),
        grid=(blocks, QPAIRS),
        in_specs=[
            tile, whole(kv.shape), pl.BlockSpec((1,) + key_labels.shape[1:], lambda i, p: (i, 0, 0)),
            pl.BlockSpec((QBLOCK, LANES), lambda i, p: (i, 0)),
        ],
        out_specs=(tile, pl.BlockSpec((1, 8, QBLOCK), lambda i, p: (p, 0, i))),
        scratch_shapes=[pltpu.VMEM((2, 2) + (kv.shape[0], LANES), BF16)] * 2,
        compiler_params=kernel_params(),
        name="attend",
    )(q, kv, key_labels, marks)


def attend_back_kernel(q, kv, given, key_marks, query_labels, stats, cosine, sine, g_q, g_kv, keys, values, g_key, g_value):
    block, pair = pl.program_id(0), pl.program_id(1)
    window = DOC_MOST + QBLOCK
    start = pl.multiple_of(block * QBLOCK, QBLOCK)

    @pl.when((block == 0) & (pair == 0))
    def _():
        both_sides(kv[:, :KDIM], keys)
        both_sides(kv[:, KDIM:], values)
        g_key[...] = jnp.zeros_like(g_key)
        g_value[...] = jnp.zeros_like(g_value)

    group = pair // (GROUPS // 2)
    rows = lax.broadcasted_iota(jnp.int32, (window, QBLOCK), 0)
    cols = lane_index((window, QBLOCK))
    seen = (rows <= cols + DOC_MOST) & (key_marks[0, :, 0:1] == query_labels[0:1, :])
    at = pl.ds(start, window)
    query, grad = q[...], given[...].astype(BF16)
    total = jnp.zeros((QBLOCK, LANES), F32)
    for a, (query_part, grad_part) in enumerate(zip(halves(query), halves(grad))):
        key = keys[group, a, at, :]
        scores = jnp.where(seen, dot_nt(key, query) * SCALE, NEG_BIG)
        probs = jnp.exp(scores - stats[0, a : a + 1, :])
        g_probs = dot_nt(values[group, a, at, :], grad)
        mean = jnp.sum(probs * g_probs, axis=0, keepdims=True)
        g_scores = (probs * (g_probs - mean)).astype(BF16)
        g_key[group, at] += dot(g_scores, query_part) * SCALE
        g_value[group, at] += dot(probs.astype(BF16), grad_part)
        total = total + dot_tn(g_scores, key)
    g_q[...] = turn(total * SCALE, cosine[...], -sine[...]).astype(BF16)

    @pl.when((block == pl.num_programs(0) - 1) & (pair == QPAIRS - 1))
    def _():
        for k, ref in enumerate((g_key, g_value)):
            first = ref[0] + pltpu.roll(ref[0], HEAD, 1)
            second = ref[1] + pltpu.roll(ref[1], HEAD, 1)
            g_kv[:, k * KDIM : (k + 1) * KDIM] = jnp.where(lane_index(first.shape) < HEAD, first, second).astype(BF16)


def attend_back(q, kv, given, key_marks, query_labels, stats, cosine, sine):
    tokens = q.shape[0]
    blocks = tokens // QBLOCK
    tile = pl.BlockSpec((QBLOCK, LANES), lambda i, p: (i, p))
    row = pl.BlockSpec((QBLOCK, LANES), lambda i, p: (i, 0))
    return pl.pallas_call(
        attend_back_kernel,
        out_shape=(jax.ShapeDtypeStruct((tokens, QDIM), BF16), jax.ShapeDtypeStruct(kv.shape, BF16)),
        grid=(blocks, QPAIRS),
        in_specs=[
            tile, whole(kv.shape), pl.BlockSpec((QBLOCK, LANES), lambda i, p: (i, PAIRS + p)),
            pl.BlockSpec((1,) + key_marks.shape[1:], lambda i, p: (i, 0, 0)),
            pl.BlockSpec((8, QBLOCK), lambda i, p: (0, i)),
            pl.BlockSpec((1, 8, QBLOCK), lambda i, p: (p, 0, i)), row, row,
        ],
        out_specs=(tile, whole(kv.shape)),
        scratch_shapes=[pltpu.VMEM((2, 2) + (kv.shape[0], LANES), BF16)] * 2 + [pltpu.VMEM((2, kv.shape[0], LANES), F32)] * 2,
        compiler_params=kernel_params(),
        name="attend_back",
    )(q, kv, given, key_marks, query_labels, stats, cosine, sine)


def turn_back_kernel(g_kv, cosine, sine, out):
    out[:, :KDIM] = turn(g_kv[:, :KDIM], cosine[...], -sine[...]).astype(BF16)
    out[:, KDIM:] = g_kv[:, KDIM:].astype(BF16)


def turn_back(g_kv, cosine, sine):
    return pl.pallas_call(
        turn_back_kernel, out_shape=jax.ShapeDtypeStruct(g_kv.shape, BF16), compiler_params=kernel_params(), name="turn_back",
    )(g_kv, cosine, sine)


def ungroup(rows, micro):
    seq = lax.axis_size("seq")
    each = seq // micro
    here = lax.axis_index("seq")
    order = here // each
    cut = rows.reshape((micro, rows.shape[0] // micro) + rows.shape[1:])
    pieces = []
    for t in range(micro):
        pairs = [(((j + t) % micro) * each + j // micro, j) for j in range(seq)]
        pieces.append(lax.ppermute(lax.dynamic_index_in_dim(cut, (order - t) % micro, 0, False), "seq", pairs))
    stacked = jnp.stack(pieces)
    return jnp.stack([lax.dynamic_index_in_dim(stacked, (m - here) % micro, 0, False) for m in range(micro)])


def along(value, steps, micro):
    seq = lax.axis_size("seq")
    each = seq // micro
    pairs = [(s, s + steps) for s in range(seq) if 0 <= s % each + steps < each]
    return lax.ppermute(value, "seq", pairs)


def pad_rows(*rows):
    width = rows[0].shape[-1]
    return jnp.concatenate([r.reshape(-1, width) for r in rows] + [jnp.zeros((8 - sum(r.size // width for r in rows), width), F32)], axis=0)


def shards(grid, tokens, cotangent, doc_ids, master_blocks, block_of_slot, left_stats, right_stats, left_roots, right_roots,
           vector_params, first_moment, second_moment, adam_step):
    micro, piece = tokens.shape[:2]
    seq = lax.axis_size("seq")
    each = seq // micro
    count = micro * piece
    here = lax.axis_index("seq")
    rank = here % each
    start = rank * count
    slots = master_blocks.shape[0]

    orders = all_orders()
    table = slots_in_order(block_of_slot, sum(orders, []))
    gathered, rows, given, labels_all = gather_blocks(grid, master_blocks, tokens, cotangent, doc_ids)
    w_in, w_out, w_ff, w_down = assemble(gathered.reshape(-1, BS, BS), table)
    rows, given = rows.reshape(count, D), given.reshape(count, D)
    gain_in, gain_mid, gain_mix, conv_weight, conv_bias, dt_bias, a_log, skip, w_dt = unpack_vectors(vector_params)
    w_dt = jnp.pad(w_dt.reshape(D, HEADS_SSM), ((0, 0), (0, LANES - HEADS_SSM))).astype(BF16)
    taps = pad_rows(conv_weight.reshape(KERNEL, CHANNELS), conv_bias)
    lane_pad = lambda v: jnp.pad(v, (0, LANES - HEADS_SSM))
    params = pad_rows(lane_pad(dt_bias), lane_pad(a_log))
    wide_skip = pad_rows(jnp.repeat(skip, HEAD))
    wide_gain = pad_rows(gain_mix)

    row = lax.dynamic_index_in_dim(labels_all, here // each, 1, False).reshape(-1)
    before = jnp.concatenate([jnp.full((DOC_MOST,), -1, jnp.int32), row])
    window = lax.dynamic_slice_in_dim(before, start, DOC_MOST + count)
    labels = window[DOC_MOST:]
    blocks = count // BLOCK
    columns = [(window[DOC_MOST - REACH + tap : DOC_MOST - REACH + tap + count] == labels).astype(F32) for tap in range(KERNEL)]
    by_block = labels.reshape(blocks, BLOCK)
    entries_at = window[DOC_MOST - 1 : DOC_MOST - 1 + count].reshape(blocks, BLOCK)[:, :1]
    columns.append((by_block == entries_at).astype(F32).reshape(-1))
    columns.append((by_block == by_block[:, -1:]).astype(F32).reshape(-1))
    columns.append(labels.astype(F32))
    marks = jnp.pad(jnp.stack(columns, axis=1), ((0, 0), (0, LANES - len(columns))))
    label_rows = jnp.broadcast_to(labels.astype(F32)[None], (8, count))
    far = jnp.stack([window[i : i + DOC_MOST + QBLOCK] for i in range(0, count, QBLOCK)]).astype(F32)
    key_labels = jnp.broadcast_to(far[:, None, :], (far.shape[0], 8, far.shape[1]))
    key_marks = jnp.broadcast_to(far[:, :, None], far.shape + (8,))
    first = jnp.sum((row[None, :] < labels[:, None]).astype(jnp.int32), axis=1)
    positions = (start + jnp.arange(count) - first).astype(F32)
    half = HEAD // 2
    frequency = jnp.exp(jnp.arange(half, dtype=F32) * (-2.0 * math.log(THETA) / HEAD))
    angles = positions[:, None] * frequency[None, :]
    cos, sin = jnp.cos(angles), jnp.sin(angles)
    cosine = jnp.concatenate([cos] * 4, axis=1)
    sine = jnp.concatenate([-sin, sin] * 2, axis=1)

    inputs = rows.astype(F32)
    normed_in = (inputs * rms_scale(inputs) * gain_in).astype(BF16)
    proj = dot(normed_in, w_in)
    raw = dot(normed_in, w_dt)
    halo = along(proj[count - HALO :, INNER : INNER + CHANNELS].astype(BF16), 1, micro)
    q, kv = rope_all(proj, cosine, sine)
    xbc, decays, decays_t, state, factor = mix_first(proj, halo, taps, params, raw, marks)
    past = min(each - 1, -(-DOC_MOST // count))
    earlier = [along(kv, back, micro) for back in range(past, 0, -1)]
    if past * count < DOC_MOST:
        earlier.insert(0, jnp.zeros((DOC_MOST - past * count, kv.shape[1]), BF16))
    reach = jnp.concatenate(earlier + [kv], axis=0)[-(DOC_MOST + count) :]
    wide = lambda f: jnp.repeat(f[0, :HEADS_SSM], HEAD)[None]
    incoming = along(state, each - 1, micro).astype(F32) if each > 1 else jnp.zeros(state.shape, F32)
    for back in range(each - 2, 0, -1):
        incoming = along(state, back, micro).astype(F32) + wide(along(factor, back, micro)) * incoming
    y, normed_ssm, states = mix_second(xbc, proj, decays, decays_t, marks, label_rows, incoming, wide_skip, wide_gain)
    context, stats = attend(q, reach, key_labels, marks)
    hidden = inputs + (dot(normed_ssm, w_out[:INNER]) + dot(context, w_out[INNER:]))
    normed_mid = (hidden * rms_scale(hidden) * gain_mid).astype(BF16)
    both = dot(normed_mid, w_ff)
    gate, upper = both[:, :FF], both[:, FF:]
    opened = sigmoid(gate)
    mixed = (gate * opened * upper).astype(BF16)
    layer_out = ungroup((hidden + dot(mixed, w_down)).astype(BF16), micro)

    g_mixed = dot_nt(given, w_down)
    g_gate = g_mixed * upper * (opened + gate * opened * (1.0 - opened))
    g_ff = jnp.concatenate([g_gate.astype(BF16), (g_mixed * gate * opened).astype(BF16)], axis=1)

    def norm_back(grad, values, gain):
        scale = rms_scale(values)
        unit = values * scale
        scaled = grad * gain
        return scale * (scaled - unit * jnp.mean(scaled * unit, axis=1, keepdims=True)), jnp.sum(grad * unit, axis=0)

    g_values, g_gain_mid = norm_back(dot_nt(g_ff, w_ff), hidden, gain_mid)
    g_hidden = given.astype(F32) + g_values
    hidden_low = g_hidden.astype(BF16)
    g_out = dot_nt(hidden_low, w_out)
    g_y, g_z, g_gain_mix, g_state = gate_back(g_out, y, proj, wide_gain, xbc, decays, marks)
    low_state = g_state.astype(BF16)
    leaving = along(low_state, 1 - each, micro).astype(F32) if each > 1 else jnp.zeros(state.shape, F32)
    for ahead in range(each - 2, 0, -1):
        leaving = along(low_state, -ahead, micro).astype(F32) + wide(along(factor, -ahead, micro)) * leaving
    g_q, g_reach = attend_back(q, reach, g_out, key_marks, label_rows, stats, cosine, sine)
    g_conv, g_rim, g_taps, g_raw, g_params = mix_back(
        xbc, proj, halo, taps, y, g_y, decays, decays_t, raw, params, marks, label_rows, states, leaving, wide_skip
    )
    g_kv = g_reach[-count:].astype(F32)
    for back in range(1, past + 1):
        low = max(0, DOC_MOST - back * count)
        part = g_reach[low : DOC_MOST - (back - 1) * count]
        moved = along(part, -back, micro).astype(F32)
        g_kv = g_kv + jnp.pad(moved, ((count - part.shape[0], 0), (0, 0)))
    g_kv = turn_back(g_kv, cosine, sine)
    rim = along(g_rim[:HALO], -1, micro)
    g_conv = lax.dynamic_update_slice(g_conv, (g_rim[HALO:] + rim).astype(BF16), (count - HALO, 0))
    g_in = jnp.concatenate([g_z, g_conv, g_q, g_kv], axis=1)
    g_values, g_gain_in = norm_back(dot_nt(g_in, w_in) + dot_nt(g_raw, w_dt), inputs, gain_in)
    grad_tokens = ungroup((g_values + g_hidden).astype(BF16), micro).astype(F32)
    g_w_dt = dot_tn(normed_in, g_raw)

    flat = slot_grads(table, [
        ([normed_in], [g_z, g_conv, g_q, g_kv]), ([normed_ssm, context], [hidden_low]),
        ([normed_mid], [g_ff]), ([mixed], [given]),
    ])
    parts = [g_gain_in, g_gain_mid, g_gain_mix[0], g_taps[:KERNEL].reshape(-1), g_taps[KERNEL]]
    parts += [g_params[i, :HEADS_SSM] for i in range(3)] + [g_w_dt[:, :HEADS_SSM].reshape(-1)]
    width = vector_params.shape[0]
    height = -(-width // (8 * LANES)) * 8
    vector = jnp.concatenate(parts + [jnp.zeros((height * LANES - width,), F32)]).reshape(height, LANES)
    total, vector = reduce_blocks(grid, flat.reshape(-1, slots, BS, BS), vector)
    norm = 1.0 / math.sqrt(count * seq * lax.axis_size("dp"))
    updates = shampoo(norm, total, master_blocks, left_stats, right_stats, left_roots, right_roots)
    g_vector = vector.reshape(-1)[:width] * norm
    step = adam_step[0].astype(F32)
    new_first = BETA_ONE * first_moment + (1.0 - BETA_ONE) * g_vector
    new_second = BETA_TWO * second_moment + (1.0 - BETA_TWO) * g_vector * g_vector
    first_hat = new_first / (1.0 - jnp.power(BETA_ONE, step))
    second_hat = new_second / (1.0 - jnp.power(BETA_TWO, step))
    new_vector = vector_params - LR_VECTOR * first_hat / (jnp.sqrt(second_hat) + ADAM_EPS)
    return (layer_out, grad_tokens) + tuple(updates) + (g_vector, new_vector, new_first, new_second)


def solution(mesh):
    line, block, copied = P("dp", "seq", None), P("dp", None, None), P()
    return jax.shard_map(
        functools.partial(shards, grid_of(mesh)),
        mesh=mesh,
        in_specs=(line, line, P("dp", "seq"), block, copied, block, block, block, block, copied, copied, copied, copied),
        out_specs=(line, line) + (block,) * 5 + (copied,) * 4,
        check_vma=False,
    )
```

```python
import functools
import math

import jax
import jax.numpy as jnp
from jax import lax
from jax.experimental import pallas as pl
from jax.experimental.pallas import tpu as pltpu
from jax.sharding import PartitionSpec as P

D = 1024
HEADS_SSM = 24
HEAD = 64
NSTATE = 128
HEADS = 8
KV_HEADS = 2
FF = 2048
KERNEL = 4
BS = 128
DOC_MOST = 512
INNER = HEADS_SSM * HEAD
CHANNELS = INNER + 2 * NSTATE
REACH = KERNEL - 1
QDIM = HEADS * HEAD
KDIM = KV_HEADS * HEAD
LANES = 128
PAIRS = INNER // LANES

EPS = 1e-05
THETA = 100000000000.0
LR_MATRIX = 0.02
LR_VECTOR = 0.08
BETA_ONE = 0.9
BETA_TWO = 0.999
ADAM_EPS = 1e-08
NEG_BIG = -1e30
F32 = jnp.float32
BF16 = jnp.bfloat16
HIGHEST = lax.Precision.HIGHEST
VMEM_MOST = 60 << 20

SHAPES = (
    (D, INNER), (D, INNER), (D, 2 * NSTATE), (D, QDIM), (D, KDIM), (D, KDIM),
    (INNER, D), (QDIM, D), (D, FF), (D, FF), (FF, D),
)
WIDE_IN, TALL_OUT, WIDE_FF, TALL_FF = (0, 1, 2, 3, 4, 5), (6, 7), (8, 9), (10,)
SIZES = (D, D, INNER, KERNEL * CHANNELS, CHANNELS, HEADS_SSM, HEADS_SSM, HEADS_SSM, D * HEADS_SSM)


def block_offsets():
    starts, total = [], 0
    for rows, cols in SHAPES:
        starts.append(total)
        total += rows // BS * (cols // BS)
    return starts


def wide_order(members):
    starts = block_offsets()
    rows = SHAPES[members[0]][0] // BS
    return [starts[m] + r * (SHAPES[m][1] // BS) + q for r in range(rows) for m in members for q in range(SHAPES[m][1] // BS)]


def tall_order(members):
    starts = block_offsets()
    return [starts[m] + i for m in members for i in range(SHAPES[m][0] // BS * (SHAPES[m][1] // BS))]


def all_orders():
    return [wide_order(WIDE_IN), tall_order(TALL_OUT), wide_order(WIDE_FF), tall_order(TALL_FF)]


def unpack_vectors(flat):
    result, offset = [], 0
    for count in SIZES:
        result.append(flat[offset : offset + count])
        offset += count
    return result


def dot(left, right, precision=None):
    return jnp.dot(left, right, preferred_element_type=F32, precision=precision)


def dot_nt(left, right):
    return lax.dot_general(left, right, (((1,), (1,)), ((), ())), preferred_element_type=F32)


def dot_tn(left, right):
    return lax.dot_general(left, right, (((0,), (0,)), ((), ())), preferred_element_type=F32)


def sigmoid(v):
    return 1.0 / (1.0 + jnp.exp(-v))


def rms_scale(values):
    return lax.rsqrt(jnp.mean(values * values, axis=-1, keepdims=True) + EPS)


def kernel_params(**more):
    return pltpu.CompilerParams(vmem_limit_bytes=VMEM_MOST, **more)


def whole(shape):
    return pl.BlockSpec(shape, lambda *_: (0,) * len(shape))


MESH = pl.DeviceIdType.MESH
CORES = 2


def grid_of(mesh):
    try:
        wide = len({device.coords[0] for device in mesh.devices.flat})
    except AttributeError:
        wide = mesh.shape["seq"] // CORES
    return wide, mesh.shape["seq"] // CORES, mesh.shape["dp"] // wide


def parts_of(slots, tall):
    half = slots // CORES
    lone = half * 17 // 48 if tall == 2 and half >= 16 else 0
    return half, lone, half - lone


def place(grid):
    wide, tall, deep = grid
    dp, seq = lax.axis_index("dp"), lax.axis_index("seq")
    return dp % wide, seq // CORES, dp // wide, seq % CORES


def gather_kernel(grid, slots, master, tokens, cotangent, docs, out, rows, given, labels, wide_own, src, bounce,
                  sem_own, sem_load, sz, rz, sx, rx, sy, ry, sc, rc, s_rows, r_rows, s_docs, r_docs):
    wide, tall, deep = grid
    x, y, z, c = place(grid)
    half, lone, bulk = parts_of(slots, tall)
    me = z * wide + x
    seq = y * CORES + c
    base = c * half
    bulk_at = base + y * (half - bulk)
    lone_at = base + y * bulk
    other_at = base + (1 - y) * bulk if lone else base
    mate = y * CORES + (1 - c)
    over = (tall - 1 - y) * CORES + c
    peers = tall * CORES
    micro = tokens.shape[0]
    each = peers // micro

    loads = []
    for k in range(CORES):
        part = pl.ds(((c + k) % CORES) * half, half)
        loads.append((part, pltpu.make_async_copy(master.at[part], wide_own.at[part], sem_load.at[k])))
        loads[-1][1].start()

    barrier = pltpu.get_barrier_semaphore()
    count = jnp.int32(0)
    for axis, at, size in (("z", z, deep), ("x", x, wide)):
        for step in (1, -1):
            ok = (at + step >= 0) & (at + step < size)
            there = me + step * (wide if axis == "z" else 1)

            @pl.when(ok)
            def _(there=there):
                pl.semaphore_signal(barrier, inc=1, device_id=(there, seq), device_id_type=MESH)

            count = count + ok.astype(jnp.int32)
    for k in range(1, peers):
        pl.semaphore_signal(barrier, inc=1, device_id=(me, (seq + k) % peers), device_id_type=MESH)
    pl.semaphore_wait(barrier, count + (peers - 1))
    sent = []

    def send(ok, source, target, send_sem, recv_sem, device):
        copy = pltpu.make_async_remote_copy(
            src_ref=source, dst_ref=target, send_sem=send_sem, recv_sem=recv_sem,
            device_id=device, device_id_type=MESH,
        )

        @pl.when(ok)
        def _():
            copy.start()

        sent.append((ok, copy))

    def arrived(ok, target, recv_sem):
        copy = pltpu.make_async_remote_copy(
            src_ref=target, dst_ref=target, send_sem=sem_own.at[0], recv_sem=recv_sem,
            device_id=(me, seq), device_id_type=MESH,
        )

        @pl.when(ok)
        def _():
            copy.wait_recv()

    yes = jnp.bool_(True)

    at_home = []
    for t in range(micro):
        m = (seq + t) % micro
        there = m * each + seq // micro
        for k, (source, target) in enumerate(((tokens, rows), (cotangent, given))):
            place_to = target.at[seq % micro]
            send(there != seq, source.at[m], place_to, s_rows.at[k, t], r_rows.at[k, seq % micro], (me, there))
            take = pltpu.make_async_copy(source.at[m], bounce.at[k], sem_own.at[k])
            put = pltpu.make_async_copy(bounce.at[k], place_to, sem_own.at[k])
            at_home.append((there == seq, take, put))

            @pl.when(there == seq)
            def _(take=take):
                take.start()

    labels[seq] = docs[...]
    for k in range(1, peers):
        there = (seq + k) % peers
        send(yes, docs, labels.at[seq], s_docs.at[k], r_docs.at[seq], (me, there))

    def convert(k):
        part, copy = loads[k]
        copy.wait()
        base_at = ((c + k) % CORES) * half

        def one(i, _):
            src[base_at + i] = wide_own[base_at + i].astype(src.dtype)
            return 0

        lax.fori_loop(0, half, one, 0, unroll=2)

    convert(0)

    def piece(shard, at, size):
        return out.at[shard, pl.ds(at, size)]

    def pass_on(ok, shard):
        send(ok, piece(shard, bulk_at, bulk), piece(shard, bulk_at, bulk), sc.at[0, shard], rc.at[0, shard], (me, mate))
        if lone:
            send(ok, piece(shard, lone_at, lone), piece(shard, lone_at, lone), sy.at[shard], ry.at[shard], (me, over))

    def along_x(ok, zs, dirs, hop, own):
        for d, step in dirs:
            shard = zs * wide + x - step * hop
            go = ok & (x + step >= 0) & (x + step < wide)
            source = src.at[pl.ds(bulk_at, bulk)] if own else piece(shard, bulk_at, bulk)
            send(go, source, piece(shard, bulk_at, bulk), sx.at[d, hop, zs], rx.at[d, hop + 1, zs], (me + step, seq))

    both = ((0, 1), (1, -1))

    def columns(s):
        return [(yes, z)] if s == 0 else [((z - step * s >= 0) & (z - step * s < deep), z - step * s) for _, step in both]

    def x_in(s, hop):
        for ok, zs in columns(s):
            for d, step in both:
                from_x = x - step * hop
                come = ok & (from_x >= 0) & (from_x < wide)
                shard = zs * wide + from_x
                arrived(come, piece(shard, bulk_at, bulk), rx.at[d, hop, zs])
                along_x(come, zs, ((d, step),), hop, False)
                pass_on(come, shard)

    def y_in(ok, shard):
        if lone:
            arrived(ok, piece(shard, other_at, lone), ry.at[shard])
            send(ok, piece(shard, other_at, lone), piece(shard, other_at, lone), sc.at[1, shard], rc.at[1, shard], (me, mate))

    def y_all(s):
        for ok, zs in columns(s):
            if s > 0:
                y_in(ok, zs * wide + x)
            for hop in range(1, wide):
                for _, step in both:
                    from_x = x - step * hop
                    y_in(ok & (from_x >= 0) & (from_x < wide), zs * wide + from_x)

    for s in range(deep):
        for d, step in both:
            zs = z - step * s
            ok = (zs >= 0) & (zs < deep)
            shard = zs * wide + x
            if s:
                arrived(ok, piece(shard, bulk_at, bulk), rz.at[d, s])
            go = ok & (z + step >= 0) & (z + step < deep)
            source = piece(shard, bulk_at, bulk) if s else src.at[pl.ds(bulk_at, bulk)]
            if s + 1 < deep:
                send(go, source, piece(shard, bulk_at, bulk), sz.at[d, s], rz.at[d, s + 1], (me + step * wide, seq))
            if s:
                along_x(ok, zs, both, 0, False)
                pass_on(ok, shard)
        if s == 0:
            along_x(yes, z, both, 0, True)
            convert(1)
            keep = pltpu.make_async_copy(src, out.at[me], sem_load.at[0])
            keep.start()
            for ok, take, put in at_home:
                @pl.when(ok)
                def _(take=take, put=put):
                    take.wait()
                    put.start()
        else:
            for hop in range(1, wide):
                x_in(s - 1, hop)
        if s >= 2:
            y_all(s - 2)
    for hop in range(1, wide):
        x_in(deep - 1, hop)
    for s in range(max(deep - 2, 0), deep):
        y_all(s)
    keep.wait()
    for ok, take, put in at_home:
        @pl.when(ok)
        def _(put=put):
            put.wait()
    for q in range(micro):
        source = seq % each * micro + q
        for k, target in enumerate((rows, given)):
            arrived(source != seq, target.at[q], r_rows.at[k, q])
    for k in range(1, peers):
        source = (seq + k) % peers
        arrived(yes, labels.at[source], r_docs.at[source])

    mate_base = (1 - c) * half
    mate_bulk = mate_base + y * (half - bulk)
    mate_other = mate_base + (1 - y) * bulk if lone else mate_base

    def last(shard, _):
        ok = shard != me
        arrived(ok, piece(shard, mate_bulk, bulk), rc.at[0, shard])
        if lone:
            arrived(ok, piece(shard, mate_other, lone), rc.at[1, shard])
        return 0

    lax.fori_loop(0, wide * deep, last, 0)
    for ok, copy in sent:
        @pl.when(ok)
        def _(copy=copy):
            copy.wait_send()


def gather_blocks(grid, master, tokens, cotangent, docs):
    wide, tall, deep = grid
    slots = master.shape[0]
    n = wide * deep
    peers = tall * CORES
    micro = tokens.shape[0]
    low = tokens.dtype
    sem = pltpu.SemaphoreType.DMA
    hbm = pl.BlockSpec(memory_space=pl.ANY)
    vmem = pl.BlockSpec(memory_space=pltpu.VMEM)
    return pl.pallas_call(
        functools.partial(gather_kernel, grid, slots),
        out_shape=(
            jax.ShapeDtypeStruct((n,) + master.shape, low),
            jax.ShapeDtypeStruct(tokens.shape, low), jax.ShapeDtypeStruct(tokens.shape, low),
            jax.ShapeDtypeStruct((peers,) + docs.shape, docs.dtype),
        ),
        in_specs=[hbm, hbm, hbm, vmem],
        out_specs=(hbm, hbm, hbm, vmem),
        scratch_shapes=[
            pltpu.VMEM(master.shape, master.dtype), pltpu.VMEM(master.shape, low), pltpu.VMEM((2,) + tokens.shape[1:], low),
            sem((2,)), sem((CORES,)),
            sem((2, deep)), sem((2, deep + 1)),
            sem((2, wide, deep)), sem((2, wide + 1, deep)),
            sem((n,)), sem((n,)),
            sem((2, n)), sem((2, n)),
            sem((2, micro)), sem((2, micro)), sem((peers,)), sem((peers,)),
        ],
        compiler_params=pltpu.CompilerParams(collective_id=0, has_side_effects=True, vmem_limit_bytes=32 << 20),
        name="gather_blocks",
    )(master, tokens, cotangent, docs)

def far_first(at, size, i):
    above, below = size - 1 - at, at
    less, more = jnp.minimum(above, below), jnp.maximum(above, below)
    long_side = jnp.where(above >= below, 1, -1)
    j = i - (more - less)
    near = at + jnp.where(j % 2 == 0, 1, -1) * (less - j // 2)
    return jnp.where(j < 0, at + long_side * (more - i), near)


def entry(at, size, source_below, target):
    lower = jnp.where(at > 0, size - at, 0) if size > 2 else 0
    return target - at if source_below else lower + at - target


def entries(size):
    return size + 1 if size > 2 else 1

SUBS = 3
LONE = 5 / 16
RING = 6
STAGED = 3
LATE_ADD, LATE_X, LATE_Z, PER_HOP = 1, 3, 6, 3
CHUNK = 512
HELD = 12


def split_of(slots, tall):
    half = slots // CORES
    piece = half // SUBS
    lone = round(piece * LONE) if tall == 2 and piece >= 8 else 0
    return half, piece, lone, piece - lone


def reduce_kernel(grid, slots, widths, left_at, right_at, vec, *refs):
    wide, tall, deep = grid
    count = sum(len(w) for w in widths)
    arrays = refs[:count]
    (out, vec_out, turned, right, held, acc, stage, land_c, land_y, land_x, land_z, fin, vbuf, vland,
     s_left, s_right, s_c, r_c, s_y, r_y, s_x, r_x, s_z, r_z, s_f, r_f, s_m, r_m, s_v, r_v, free) = refs[count:]
    n = wide * deep
    x, y, z, c = place(grid)
    half, size, lone, bulk = split_of(slots, tall)
    me = z * wide + x
    seq = y * CORES + c
    mate = y * CORES + (1 - c)
    bulk_at = y * lone
    lone_at = y * bulk
    other_at = (1 - y) * bulk
    bits = lambda length: [1 << b for b in range(length.bit_length() - 1)]
    partners = [(me, mate)]
    partners += [(me, (y ^ b) * CORES + c) for b in bits(tall)]
    partners += [(z * wide + (x ^ b), seq) for b in bits(wide)]
    partners += [((z ^ b) * wide + x, seq) for b in bits(deep)]
    rounds = len(partners)

    chunks, k, at = [], 0, 0
    for width in widths[0]:
        for q in range(0, width, CHUNK):
            chunks.append((k, q, at + q))
        k, at = k + 1, at + width

    def chunk_copy(i):
        k, q, _ = chunks[i]
        return pltpu.make_async_copy(arrays[k].at[:, pl.ds(q, CHUNK)], held.at[i % HELD], s_left.at[i % HELD])

    ahead = min(HELD, len(chunks))
    for i in range(ahead):
        chunk_copy(i).start()
    copies, at = [], 0
    for width in widths[1]:
        def one(q, _, k=k, at=at):
            cols = pl.ds(pl.multiple_of(q * BS, BS), BS)
            pltpu.make_async_copy(arrays[k].at[:, cols], right.at[at + q], s_right.at[k - len(widths[0])]).start()
            return 0

        lax.fori_loop(0, width // BS, one, 0)
        part = right.at[pl.ds(at, width // BS)]
        copies.append(pltpu.make_async_copy(part, part, s_right.at[k - len(widths[0])]))
        k, at = k + 1, at + width // BS

    barrier = pltpu.get_barrier_semaphore()
    awaited = jnp.int32(0)
    for step_by, at, length in ((wide, z, deep), (1, x, wide)):
        for step in (1, -1):
            ok = (at + step >= 0) & (at + step < length)

            @pl.when(ok)
            def _(there=me + step * step_by):
                pl.semaphore_signal(barrier, inc=1, device_id=(there, seq), device_id_type=MESH)

            awaited = awaited + ok.astype(jnp.int32)
    for device in partners:
        pl.semaphore_signal(barrier, inc=1, device_id=device, device_id_type=MESH)
    pl.semaphore_wait(barrier, awaited + rounds)

    def remote(source, target, send_sem, recv_sem, device):
        return pltpu.make_async_remote_copy(
            src_ref=source, dst_ref=target, send_sem=send_sem, recv_sem=recv_sem,
            device_id=device, device_id_type=MESH,
        )

    def landed(target, recv_sem):
        remote(target, target, s_left.at[0], recv_sem, (me, seq)).wait_recv()

    def vec_copy(t):
        return remote(vbuf.at[t], vland.at[t], s_v.at[t], r_v.at[t], partners[t])

    vbuf[0] = vec[...]
    vec_copy(0).start()
    for i in range(len(chunks)):
        chunk_copy(i).wait()
        for q in range(0, CHUNK, BS):
            turned[(chunks[i][2] + q) // BS] = held[i % HELD, :, q : q + BS].T
        if i + HELD < len(chunks):
            chunk_copy(i + HELD).start()
    for copy in copies:
        copy.wait()

    group = wide * SUBS
    total = n * SUBS

    def item_of(k):
        xs = far_first(x, wide, k % wide)
        zs = far_first(z, deep, k // group)
        sub = (k // wide) % SUBS
        return xs, zs, sub, (zs * wide + xs) * SUBS + sub

    def swap(k):
        return remote(stage.at[k % STAGED], land_c.at[k % RING], s_c.at[k % STAGED], r_c.at[k % RING], (me, mate))

    def cross(item):
        return remote(acc.at[item, pl.ds(other_at, lone)], land_y.at[item], s_y.at[item], r_y.at[item], (me, (tall - 1 - y) * CORES + c))

    def grads(k, core, ref, first):
        xs, zs, sub, item = item_of(k)
        base = (zs * wide + xs) * slots + core * half + sub * size

        def one(i, _):
            ref[first, i] = dot(turned[left_at[base + i]], right[right_at[base + i]]).astype(ref.dtype)
            return 0

        lax.fori_loop(0, size, one, 0, unroll=min(4, size))

    def add(item, at, length, ref, first):
        def one(i, _):
            acc[item, at + i] = acc[item, at + i] + ref[first + (i,)]
            return 0

        lax.fori_loop(0, length, one, 0, unroll=min(3, length))

    def step_x(k, begin_it):
        xs, zs, sub, item = item_of(k)
        for below, step in ((True, 1), (False, -1)):
            to = entry(x + step, wide, below, xs)
            sent = remote(acc.at[item, pl.ds(bulk_at, bulk)], land_x.at[to, zs * SUBS + sub], s_x.at[item],
                          r_x.at[to, zs * SUBS + sub], (me + step, seq))

            @pl.when((xs - x) * step > 0)
            def _():
                if begin_it:
                    sent.start()
                else:
                    sent.wait_send()

    def take_x(k):
        xs, zs, sub, item = item_of(k)
        for below, step in ((True, 1), (False, -1)):
            comes = ((xs - x) * step >= 0) & (x - step >= 0) & (x - step < wide)
            at = entry(x, wide, below, xs)

            @pl.when(comes)
            def _():
                landed(land_x.at[at, zs * SUBS + sub], r_x.at[at, zs * SUBS + sub])
                add(item, bulk_at, bulk, land_x, (at, zs * SUBS + sub))

    def step_z(k, begin_it):
        xs, zs, sub, item = item_of(k)
        for below, step in ((True, 1), (False, -1)):
            to = entry(z + step, deep, below, zs)
            sent = remote(acc.at[item, pl.ds(bulk_at, bulk)], land_z.at[to, sub], s_z.at[zs * SUBS + sub], r_z.at[to, sub],
                          (me + step * wide, seq))

            @pl.when((zs - z) * step > 0)
            def _():
                if begin_it:
                    sent.start()
                else:
                    sent.wait_send()

    def take_z(k):
        xs, zs, sub, item = item_of(k)
        for below, step in ((True, 1), (False, -1)):
            comes = ((zs - z) * step >= 0) & (z - step >= 0) & (z - step < deep)
            at = entry(z, deep, below, zs)

            @pl.when(comes)
            def _():
                landed(land_z.at[at, sub], r_z.at[at, sub])
                add(item, bulk_at, bulk, land_z, (at, sub))

    planes = bits(tall)

    def swap_plane(t, sub):
        mine = pl.ds(bulk_at, bulk)
        return remote(acc.at[me * SUBS + sub, mine], fin.at[t, sub, mine], s_f.at[t, sub], r_f.at[t, sub], (me, (y ^ planes[t]) * CORES + c))

    def take_plane(t, sub):
        item = me * SUBS + sub
        theirs = pl.ds((1 - y) * lone if lone else 0, bulk)
        landed(fin.at[t, sub, theirs], r_f.at[t, sub])
        swap_plane(t, sub).wait_send()
        add(item, lone, size - 2 * lone, fin.at[t, sub, pl.ds(lone, size - 2 * lone)], ())
        if lone:
            cross(item).wait_send()
            acc[item, pl.ds(other_at, lone)] = fin[t, sub, pl.ds(other_at, lone)]

    def swap_core(sub):
        return remote(acc.at[me * SUBS + sub], out.at[pl.ds(c * half + sub * size, size)], s_m.at[sub], r_m.at[sub], (me, mate))

    late_z = LATE_Z + PER_HOP * jnp.minimum(z, deep - 1 - z)

    def turn_of(k, _):
        @pl.when(k < total)
        def _():
            @pl.when(k >= STAGED)
            def _():
                swap(k - STAGED).wait_send()

            grads(k, 1 - c, stage, k % STAGED)

            @pl.when(k >= RING)
            def _():
                pl.semaphore_wait(free, 1)

            swap(k).start()
            grads(k, c, acc, item_of(k)[3])

        for t in range(1, rounds + 1):
            @pl.when(k == t)
            def _(t=t):
                landed(vland.at[t - 1], r_v.at[t - 1])
                vbuf[t] = vbuf[t - 1] + vland[t - 1]
                if t < rounds:
                    vec_copy(t).start()
                else:
                    vec_out[...] = vbuf[t]

        b = k - LATE_ADD

        @pl.when((b >= 0) & (b < total))
        def _():
            item = item_of(b)[3]
            landed(land_c.at[b % RING], r_c.at[b % RING])
            add(item, 0, size, land_c, (b % RING,))

            @pl.when(b < total - RING)
            def _():
                pl.semaphore_signal(free, inc=1, device_id=(me, mate), device_id_type=MESH)

            if lone:
                cross(item).start()

        b = k - LATE_X

        @pl.when((b >= 0) & (b < total))
        def _():
            item = item_of(b)[3]
            if lone:
                landed(land_y.at[item], r_y.at[item])
                add(item, lone_at, lone, land_y, (item,))
            if wide > 2:
                @pl.when(item_of(b)[0] != x)
                def _():
                    take_x(b)
            step_x(b, True)

        b = k - late_z

        @pl.when((b >= 0) & (b < total) & (b % wide == wide - 1))
        def _():
            take_x(b)
            take_z(b)
            step_z(b, True)
            if planes:
                @pl.when(item_of(b)[1] == z)
                def _():
                    swap_plane(0, item_of(b)[2]).start()

        return 0

    lax.fori_loop(0, total + LATE_Z + PER_HOP * ((deep - 1) // 2), turn_of, 0)

    def finish(k, _):
        if lone:
            item = item_of(k)[3]

            @pl.when(item // SUBS != me)
            def _():
                cross(item).wait_send()

        step_x(k, False)

        @pl.when(k % wide == wide - 1)
        def _():
            step_z(k, False)

        return 0

    for t in range(len(planes)):
        for sub in range(SUBS):
            if t:
                swap_plane(t, sub).start()
        for sub in range(SUBS):
            take_plane(t, sub)
            if t == len(planes) - 1:
                swap_core(sub).start()
                out[pl.ds(c * half + sub * size, size)] = acc[me * SUBS + sub]
    lax.fori_loop(0, total, finish, 0)
    for k in range(max(total - STAGED, 0), total):
        swap(k).wait_send()
    for t in range(rounds):
        vec_copy(t).wait_send()
    for sub in range(SUBS):
        swap_core(sub).wait_send()
        landed(out.at[pl.ds((1 - c) * half + sub * size, size)], r_m.at[sub])


def reduce_blocks(grid, slots, left_at, right_at, lefts, rights, vec):
    wide, tall, deep = grid
    n = wide * deep
    half, size, lone, bulk = split_of(slots, tall)
    tile = (BS, BS)
    low = lefts[0].dtype
    tokens = lefts[0].shape[0]
    widths = [[a.shape[1] for a in lefts], [a.shape[1] for a in rights]]
    sem = pltpu.SemaphoreType.DMA
    rounds = sum(length.bit_length() - 1 for length in (CORES, wide, tall, deep))
    planes = max(tall.bit_length() - 1, 1)
    items = n * SUBS
    buf = lambda *lead: pltpu.VMEM(lead + tile, low)
    smem, vmem, hbm = (pl.BlockSpec(memory_space=m) for m in (pltpu.SMEM, pltpu.VMEM, pl.ANY))
    return pl.pallas_call(
        functools.partial(reduce_kernel, grid, slots, widths),
        out_shape=(jax.ShapeDtypeStruct((slots,) + tile, low), jax.ShapeDtypeStruct(vec.shape, vec.dtype)),
        in_specs=[smem, smem, vmem] + [hbm] * (len(lefts) + len(rights)),
        out_specs=(vmem, vmem),
        scratch_shapes=[
            pltpu.VMEM((sum(widths[0]) // BS, BS, tokens), low), pltpu.VMEM((sum(widths[1]) // BS, tokens, BS), low), pltpu.VMEM((HELD, tokens, CHUNK), low),
            buf(items, size), buf(STAGED, size), buf(RING, size), buf(items, max(lone, 1)), buf(entries(wide), deep * SUBS, bulk),
            buf(entries(deep), SUBS, bulk), buf(planes, SUBS, size),
            pltpu.VMEM((rounds + 1,) + vec.shape, vec.dtype), pltpu.VMEM((rounds,) + vec.shape, vec.dtype),
            sem((HELD,)), sem((len(rights),)), sem((STAGED,)), sem((RING,)), sem((items,)), sem((items,)), sem((items,)),
            sem((entries(wide), deep * SUBS)), sem((deep * SUBS,)), sem((entries(deep), SUBS)),
            sem((planes, SUBS)), sem((planes, SUBS)), sem((SUBS,)), sem((SUBS,)), sem((rounds,)), sem((rounds,)),
            pltpu.SemaphoreType.REGULAR,
        ],
        compiler_params=pltpu.CompilerParams(collective_id=1, has_side_effects=True, vmem_limit_bytes=63 << 20),
        name="reduce_blocks",
    )(left_at, right_at, vec, *lefts, *rights)


STEP_BLOCKS = 32
DEPTH = 4


def assemble_kernel(table, blocks, w_in, w_out, w_ff, w_down, wide, tall, s_in, s_out):
    outs = []
    for ref in (w_in, w_out, w_ff, w_down):
        rows, cols = ref.shape
        per_row = cols // BS
        deep = STEP_BLOCKS // per_row
        for r in range(rows // (BS * deep)):
            outs.append((ref, r * BS * deep, deep, per_row))

    def target(step):
        ref, at, deep, per_row = outs[step]
        slot = step % DEPTH
        return (wide.at[slot] if deep == 1 else tall.at[slot]), ref.at[pl.ds(at, BS * deep)], deep, per_row

    def fetch(step):
        buffer, _, deep, per_row = target(step)

        def one(i, _):
            rows = pl.ds(pl.multiple_of(i // per_row * BS, BS), BS)
            cols = pl.ds(pl.multiple_of(i % per_row * BS, BS), BS)
            pltpu.make_async_copy(blocks.at[table[step * STEP_BLOCKS + i]], buffer.at[rows, cols], s_in.at[step % DEPTH]).start()
            return 0

        lax.fori_loop(0, STEP_BLOCKS, one, 0)

    def put(step):
        buffer, place_to, _, _ = target(step)
        return pltpu.make_async_copy(buffer, place_to, s_out.at[step % DEPTH])

    steps = len(outs)
    for step in range(min(DEPTH - 1, steps)):
        fetch(step)
    for step in range(steps):
        buffer, place_to, _, _ = target(step)
        pltpu.make_async_copy(place_to, buffer, s_in.at[step % DEPTH]).wait()
        put(step).start()
        ahead = step + DEPTH - 1
        if ahead < steps:
            if step >= 1:
                put(step - 1).wait()
            fetch(ahead)
    for step in range(max(steps - DEPTH, 0), steps):
        put(step).wait()


def slots_in_order(block_of_slot, order):
    match = jnp.array(order, jnp.int32)[:, None] == block_of_slot[None, :]
    return jnp.sum(jnp.where(match, jnp.arange(block_of_slot.shape[0], dtype=jnp.int32)[None, :], 0), axis=1)


def values_of(block_of_slot, values):
    match = block_of_slot[:, None] == jnp.arange(len(values), dtype=jnp.int32)[None, :]
    return jnp.sum(jnp.where(match, jnp.array(values, jnp.int32)[None, :], 0), axis=1)


def grad_tables():
    lefts, rights = [], []
    left_base = right_base = 0
    for members, beside in ((WIDE_IN, True), (TALL_OUT, False), (WIDE_FF, True), (TALL_FF, False)):
        for m in members:
            rows, cols = SHAPES[m]
            for r in range(0, rows, BS):
                for q in range(0, cols, BS):
                    lefts.append((left_base + r) // BS)
                    rights.append((right_base + q) // BS)
            if beside:
                right_base += cols
            else:
                left_base += rows
        if beside:
            left_base += rows
        else:
            right_base += cols
    return lefts, rights


def assemble(blocks, table):
    shapes = [(D, sum(SHAPES[m][1] for m in WIDE_IN)), (sum(SHAPES[m][0] for m in TALL_OUT), D), (D, 2 * FF), (FF, D)]
    hbm = pl.BlockSpec(memory_space=pl.ANY)
    return pl.pallas_call(
        assemble_kernel,
        out_shape=tuple(jax.ShapeDtypeStruct(shape, BF16) for shape in shapes),
        grid_spec=pltpu.PrefetchScalarGridSpec(
            num_scalar_prefetch=1, grid=(1,), in_specs=[hbm], out_specs=(hbm,) * 4,
            scratch_shapes=[
                pltpu.VMEM((DEPTH, BS, STEP_BLOCKS * BS), BF16),
                pltpu.VMEM((DEPTH, STEP_BLOCKS // (D // BS) * BS, D), BF16),
                pltpu.SemaphoreType.DMA((DEPTH,)), pltpu.SemaphoreType.DMA((DEPTH,)),
            ],
        ),
        compiler_params=kernel_params(),
        name="assemble",
    )(table, blocks)


SHAMPOO = 8


def shampoo_kernel(norm, total, master, left, right, left_root, right_root, grad, new_left, new_right, new_master, low):
    for i in range(SHAMPOO):
        g = total[i]
        value = g.astype(F32) * norm
        grad[i] = value
        new_left[i] = 0.5 * left[i] + dot_nt(g, g) * (0.5 * norm * norm / BS)
        new_right[i] = 0.5 * right[i] + dot_tn(g, g) * (0.5 * norm * norm / BS)
        inner = dot(g, right_root[i].astype(BF16))
        moved = dot(left_root[i].astype(BF16), inner.astype(BF16)) * (LR_MATRIX * norm)
        fresh = master[i] - moved
        new_master[i] = fresh
        low[i] = fresh.astype(BF16)


def shampoo(norm, total, master, left, right, left_root, right_root):
    slots = total.shape[0]
    spec = pl.BlockSpec((SHAMPOO, BS, BS), lambda i: (i, 0, 0))
    full = jax.ShapeDtypeStruct(master.shape, F32)
    return pl.pallas_call(
        functools.partial(shampoo_kernel, norm),
        out_shape=(full, full, full, full, jax.ShapeDtypeStruct(master.shape, BF16)),
        grid=(slots // SHAMPOO,),
        in_specs=[spec] * 6,
        out_specs=(spec,) * 5,
        compiler_params=kernel_params(),
        name="shampoo",
    )(total, master, left, right, left_root, right_root)


BLOCK = 256
HALO = 8


def lane_index(shape):
    return lax.broadcasted_iota(jnp.int32, shape, len(shape) - 1)


def conv_tile(extended, taps, marks, count):
    total = jnp.broadcast_to(taps[KERNEL : KERNEL + 1, :], (count, extended.shape[1]))
    for tap in range(KERNEL):
        total = total + taps[tap : tap + 1, :] * near_rows(extended, tap, count) * marks[:, tap : tap + 1]
    return total


def near_rows(extended, tap, count):
    back = REACH - tap
    moved = pltpu.roll(extended, back, 0) if back else extended
    return moved[HALO : HALO + count, :]


def softplus(v):
    return jnp.maximum(v, 0.0) + jnp.log(1.0 + jnp.exp(-jnp.abs(v)))


def chunk_decays(raw, params):
    delta = softplus(raw + params[0:1, :])
    decay = -delta * jnp.exp(params[1:2, :])
    block = raw.shape[0] if raw.shape[0] < BLOCK else BLOCK
    rows = lax.broadcasted_iota(jnp.int32, (block, block), 0)
    lower = (rows >= lane_index((block, block))).astype(F32)
    sums = [dot(lower, decay[i : i + block, :], HIGHEST) for i in range(0, raw.shape[0], block)]
    return delta, decay, jnp.concatenate(sums, axis=0)


def end_weights(delta, sums, marks):
    last = sums[-1:, :]
    return jnp.exp(last - sums) * delta * marks[:, 5:6], jnp.exp(last) * marks[-1:, 4:5]


def spread_matrix():
    rows = lax.broadcasted_iota(jnp.int32, (LANES, INNER), 0)
    return (rows == lane_index((LANES, INNER)) // HEAD).astype(F32)


def mix_first_kernel(proj_x, proj_bc, halo, taps, params, raw, marks, xbc, decays, decays_t, state, factor):
    tokens = raw.shape[0]
    mark = marks[...]
    for ref, at in ((proj_x, 0), (proj_bc, INNER)):
        step = 256
        for q in range(0, ref.shape[1], step):
            cols = slice(at + q, at + q + step)
            own = ref[:, q : q + step].astype(BF16).astype(F32)
            extended = jnp.concatenate([halo[:, cols].astype(F32), own], axis=0)
            value = conv_tile(extended, taps[:, cols], mark, tokens)
            xbc[:, cols] = (value * sigmoid(value)).astype(BF16)
    delta, decay, sums = chunk_decays(raw[...], params[...])
    decays[0] = delta
    decays[1] = sums
    decays_t[...] = sums.T
    spread = spread_matrix()
    total = jnp.zeros((NSTATE, INNER), F32)
    product = jnp.ones((1, LANES), F32)
    for i in range(0, tokens, BLOCK):
        rows = slice(i, i + BLOCK)
        weight, own = end_weights(delta[rows], sums[rows], mark[rows])
        weighted = (xbc[rows, :INNER].astype(F32) * dot(weight.astype(BF16), spread.astype(BF16))).astype(BF16)
        keep = dot(jnp.broadcast_to(own, (8, LANES)), spread, HIGHEST)[0:1]
        total = keep * total + dot_tn(xbc[rows, INNER : INNER + NSTATE], weighted)
        product = product * own
    state[...] = total.astype(BF16)
    factor[...] = jnp.broadcast_to(product, factor.shape)


def mix_first(proj, halo, taps, params, raw, marks):
    tokens = raw.shape[0]
    vmem = pl.BlockSpec(memory_space=pltpu.VMEM)
    return pl.pallas_call(
        mix_first_kernel,
        out_shape=(
            jax.ShapeDtypeStruct((tokens, CHANNELS), BF16),
            jax.ShapeDtypeStruct((2, tokens, LANES), F32),
            jax.ShapeDtypeStruct((LANES, tokens), F32),
            jax.ShapeDtypeStruct((NSTATE, INNER), BF16),
            jax.ShapeDtypeStruct((8, LANES), F32),
        ),
        grid=(1,),
        in_specs=[
            pl.BlockSpec((tokens, INNER), lambda i: (0, 1)),
            pl.BlockSpec((tokens, 2 * NSTATE), lambda i: (0, 2 * INNER // (2 * NSTATE))),
            vmem, vmem, vmem, vmem, vmem,
        ],
        out_specs=(vmem,) * 5,
        compiler_params=kernel_params(),
        name="mix_first",
    )(proj, proj, halo, taps, params, raw, marks)


def attend(left, right, mark_rows, mark_cols):
    return jnp.where(mark_rows & mark_cols, dot_nt(left, right), 0.0)


def halves(tile):
    low = lane_index(tile.shape) < HEAD
    zero = jnp.zeros_like(tile)
    return jnp.where(low, tile, zero), jnp.where(low, zero, tile)


def pair_column(values, a):
    return values[:, a * HEAD : a * HEAD + 1]


def mix_second_kernel(x, b, c, z, decays, decays_t, marks, labels, incoming, skip, gain, y, normed, states,
                      wide_sums, wide_delta, wide_end, keep, near, b_t, state, gated, squares):
    j = pl.program_id(0)
    tokens = x.shape[0]
    blocks = tokens // BLOCK
    cols = pl.ds(pl.multiple_of(j * LANES, LANES), LANES)

    @pl.when(j == 0)
    def _():
        spread = spread_matrix()
        rows = lax.broadcasted_iota(jnp.int32, (BLOCK, BLOCK), 0)
        ordered = rows >= lane_index((BLOCK, BLOCK))
        for i in range(blocks):
            at = slice(i * BLOCK, (i + 1) * BLOCK)
            mark = marks[at]
            same = mark[:, 6:7] == labels[0:1, at]
            near[i] = jnp.where(ordered & same, dot_nt(c[at], b[at]), 0.0)
            b_t[i] = b[at].T
            weight, own = end_weights(decays[0, at], decays[1, at], mark)
            wide_end[at] = dot(weight.astype(BF16), spread.astype(BF16)).astype(BF16)
            wide_sums[at] = dot(decays[1, at], spread, HIGHEST)
            wide_delta[at] = dot(decays[0, at].astype(BF16), spread.astype(BF16)).astype(BF16)
            keep[i] = dot(jnp.broadcast_to(own, (8, LANES)), spread, HIGHEST)
        squares[...] = jnp.zeros_like(squares)

    state[...] = incoming[...].astype(F32)
    for i in range(blocks):
        at = slice(i * BLOCK, (i + 1) * BLOCK)
        states[i] = state[...]
        tile = x[at].astype(F32)
        scaled = (tile * wide_delta[at, cols].astype(F32)).astype(BF16)
        sums = wide_sums[at, cols]
        total = jnp.zeros((BLOCK, LANES), F32)
        for a, part in enumerate(halves(scaled)):
            row = decays_t[pl.ds(2 * j + a, 1), at]
            weight = near[i] * jnp.exp(jnp.minimum(pair_column(sums, a) - row, 0.0))
            total = total + dot(weight.astype(BF16), part)
        carried = dot(c[at], state[...].astype(BF16))
        total = total + carried * jnp.exp(sums) * marks[at, 4:5] + skip[0:1, cols] * tile
        y[at] = total
        gate = z[at]
        gate = total * gate * sigmoid(gate)
        gated[at, cols] = gate
        squares[at] += gate * gate
        weighted = (tile * wide_end[at, cols].astype(F32)).astype(BF16)
        state[...] = keep[i, 0:1, cols] * state[...] + dot(b_t[i], weighted)
    states[blocks] = state[...]

    @pl.when(j == PAIRS - 1)
    def _():
        for i in range(blocks):
            at = slice(i * BLOCK, (i + 1) * BLOCK)
            scale = lax.rsqrt(jnp.sum(squares[at], axis=1, keepdims=True) / INNER + EPS)
            normed[at] = (gated[at] * scale * gain[0:1, :]).astype(BF16)


def mix_second(xbc, proj, decays, decays_t, marks, labels, incoming, skip, gain):
    tokens = xbc.shape[0]
    blocks = tokens // BLOCK
    tile = pl.BlockSpec((tokens, LANES), lambda j: (0, j))
    return pl.pallas_call(
        mix_second_kernel,
        out_shape=(
            jax.ShapeDtypeStruct((tokens, INNER), F32),
            jax.ShapeDtypeStruct((tokens, INNER), BF16),
            jax.ShapeDtypeStruct((blocks + 1, NSTATE, INNER), F32),
        ),
        grid=(PAIRS,),
        in_specs=[
            tile,
            pl.BlockSpec((tokens, NSTATE), lambda j: (0, INNER // NSTATE)),
            pl.BlockSpec((tokens, NSTATE), lambda j: (0, INNER // NSTATE + 1)),
            tile,
            whole(decays.shape), whole(decays_t.shape), whole(marks.shape), whole(labels.shape),
            pl.BlockSpec((NSTATE, LANES), lambda j: (0, j)),
            whole(skip.shape), whole(gain.shape),
        ],
        out_specs=(tile, whole((tokens, INNER)), pl.BlockSpec((blocks + 1, NSTATE, LANES), lambda j: (0, 0, j))),
        scratch_shapes=[
            pltpu.VMEM((tokens, INNER), F32), pltpu.VMEM((tokens, INNER), BF16), pltpu.VMEM((tokens, INNER), BF16),
            pltpu.VMEM((blocks, 8, INNER), F32), pltpu.VMEM((blocks, BLOCK, BLOCK), F32),
            pltpu.VMEM((blocks, NSTATE, BLOCK), BF16), pltpu.VMEM((NSTATE, LANES), F32),
            pltpu.VMEM((tokens, INNER), F32), pltpu.VMEM((tokens, LANES), F32),
        ],
        compiler_params=kernel_params(),
        name="mix_second",
    )(xbc, xbc, xbc, proj, decays, decays_t, marks, labels, incoming, skip, gain)


def gate_back_kernel(grad, y, z, gain, c, decays, marks, g_y, g_z, g_gain, g_state):
    step = pl.program_id(0)
    value, gate = y[...], z[...]
    opened = sigmoid(gate)
    swish = gate * opened
    gated = value * swish
    scale = lax.rsqrt(jnp.mean(gated * gated, axis=1, keepdims=True) + EPS)
    unit = gated * scale
    given = grad[...]
    scaled = given * gain[0:1, :]
    g_gated = scale * (scaled - unit * jnp.mean(scaled * unit, axis=1, keepdims=True))
    fresh = g_gated * swish
    g_y[...] = fresh.astype(BF16)
    g_z[...] = (g_gated * value * (opened + swish * (1.0 - opened))).astype(BF16)
    spread = spread_matrix()
    sums = decays[1]
    mark = marks[...]
    entry_weight = jnp.exp(sums) * mark[:, 4:5]
    own = jnp.exp(sums[-1:, :]) * mark[-1:, 4:5]
    keep = dot(jnp.broadcast_to(own, (8, LANES)), spread, HIGHEST)[0:1]
    weighted = (fresh * dot(entry_weight.astype(BF16), spread.astype(BF16))).astype(BF16)
    local = dot_tn(c[...], weighted)
    gains = jnp.broadcast_to(jnp.sum(given * unit, axis=0, keepdims=True), g_gain.shape)

    @pl.when(step == 0)
    def _():
        g_state[...] = local
        g_gain[...] = gains

    @pl.when(step > 0)
    def _():
        g_state[...] = keep * g_state[...] + local
        g_gain[...] += gains


def gate_back(grad, y, proj, gain, xbc, decays, marks):
    tokens = y.shape[0]
    blocks = tokens // BLOCK
    rows = lambda width, col: pl.BlockSpec((BLOCK, width), lambda i: (blocks - 1 - i, col))
    return pl.pallas_call(
        gate_back_kernel,
        out_shape=(
            jax.ShapeDtypeStruct((tokens, INNER), BF16),
            jax.ShapeDtypeStruct((tokens, INNER), BF16),
            jax.ShapeDtypeStruct((8, INNER), F32),
            jax.ShapeDtypeStruct((NSTATE, INNER), F32),
        ),
        grid=(blocks,),
        in_specs=[
            rows(INNER, 0), rows(INNER, 0), rows(INNER, 0), whole(gain.shape), rows(NSTATE, INNER // NSTATE + 1),
            pl.BlockSpec((2, BLOCK, LANES), lambda i: (0, blocks - 1 - i, 0)), rows(LANES, 0),
        ],
        out_specs=(rows(INNER, 0), rows(INNER, 0), whole((8, INNER)), whole((NSTATE, INNER))),
        compiler_params=kernel_params(),
        name="gate_back",
    )(grad, y, proj, gain, xbc, decays, marks)


def conv_back(grad, extended, taps, marks, count):
    acc = conv_tile(extended, taps, marks, count)
    opened = sigmoid(acc)
    g_acc = grad * (opened + acc * opened * (1.0 - opened))
    width = g_acc.shape[1]
    weights, result = [], jnp.zeros((HALO + count, width), F32)
    for tap in range(KERNEL):
        marked = g_acc * marks[:, tap : tap + 1]
        weights.append(jnp.sum(marked * near_rows(extended, tap, count), axis=0, keepdims=True))
        spread = jnp.concatenate([jnp.zeros((HALO, width), F32), marked * taps[tap : tap + 1, :]], axis=0)
        back = REACH - tap
        result = result + (pltpu.roll(spread, HALO + count - back, 0) if back else spread)
    weights.append(jnp.sum(g_acc, axis=0, keepdims=True))
    weights.append(jnp.zeros((8 - KERNEL - 1, width), F32))
    return result, jnp.concatenate(weights, axis=0)


def mix_back_kernel(x, b, c, proj_x, proj_bc, halo, taps, y, g_y, decays, decays_t, raw, params, marks, labels, states, leaving, skip,
                    g_conv, g_rim, g_taps, g_raw, g_params,
                    wide_sums, wide_delta, wide_end, wide_skip, keep, near, c_t, state, g_near, g_b, g_c, g_cum, g_delta, g_skip, ends):
    j = pl.program_id(0)
    tokens = x.shape[0]
    blocks = tokens // BLOCK
    cols = pl.ds(pl.multiple_of(j * LANES, LANES), LANES)
    lane = lane_index((LANES, LANES))
    gather = ((lax.broadcasted_iota(jnp.int32, (LANES, LANES), 0) // HEAD + 2 * j) == lane).astype(BF16)

    def collect(values):
        high = values.astype(BF16)
        return dot(high, gather) + dot((values - high.astype(F32)).astype(BF16), gather)

    @pl.when(j == 0)
    def _():
        spread = spread_matrix()
        rows = lax.broadcasted_iota(jnp.int32, (BLOCK, BLOCK), 0)
        ordered = rows <= lane_index((BLOCK, BLOCK))
        for i in range(blocks):
            at = slice(i * BLOCK, (i + 1) * BLOCK)
            mark = marks[at]
            same = mark[:, 6:7] == labels[0:1, at]
            near[i] = jnp.where(ordered & same, dot_nt(b[at], c[at]), 0.0)
            c_t[i] = c[at].T
            weight, own = end_weights(decays[0, at], decays[1, at], mark)
            end_only = jnp.exp(decays[1, at][-1:, :] - decays[1, at]) * mark[:, 5:6]
            wide_end[at] = dot(end_only.astype(BF16), spread.astype(BF16)).astype(BF16)
            wide_sums[at] = dot(decays[1, at], spread, HIGHEST)
            wide_delta[at] = dot(decays[0, at].astype(BF16), spread.astype(BF16)).astype(BF16)
            keep[i] = dot(jnp.broadcast_to(own, (8, LANES)), spread, HIGHEST)
        for ref in (g_near, g_b, g_c, g_cum, g_delta, g_skip, ends):
            ref[...] = jnp.zeros_like(ref)

    state[...] = leaving[...].astype(F32)
    g_x = []
    for i in range(blocks - 1, -1, -1):
        at = slice(i * BLOCK, (i + 1) * BLOCK)
        tile = x[at].astype(F32)
        step = wide_delta[at, cols].astype(F32)
        scaled = tile * step
        low_scaled = scaled.astype(BF16)
        sums = wide_sums[at, cols]
        end = wide_end[at, cols].astype(F32)
        given = g_y[at]
        low_state = state[...].astype(BF16)
        ends[i] += collect(jnp.broadcast_to(jnp.sum(states[i + 1] * state[...], axis=0, keepdims=True), (8, LANES)))
        total = end * dot(b[at], low_state)
        for a, (part, grad) in enumerate(zip(halves(low_scaled), halves(given))):
            row = decays_t[pl.ds(2 * j + a, 1), at]
            decay = jnp.exp(jnp.minimum(row - pair_column(sums, a), 0.0))
            total = total + dot((near[i] * decay).astype(BF16), grad)
            g_near[i] += decay * dot_nt(part, given)
        given = given.astype(F32)
        entry = jnp.exp(sums) * marks[at, 4:5]
        reached = (given * entry).astype(BF16)
        g_b[at] += dot_nt((scaled * end).astype(BF16), low_state)
        g_c[at] += dot_nt(reached, states[i].astype(BF16))
        own_skip = skip[0:1, cols]
        g_cum[at] += collect(given * (y[at] - own_skip * tile) - scaled * total)
        g_delta[at] += collect(total * tile)
        g_skip[...] += collect(jnp.broadcast_to(jnp.sum(given * tile, axis=0, keepdims=True), (8, LANES)))
        g_x.append(step * total + own_skip * given)
        state[...] = keep[i, 0:1, cols] * state[...] + dot(c_t[i], reached)

    mark = marks[...]
    own = proj_x[...].astype(BF16).astype(F32)
    extended = jnp.concatenate([halo[:, cols].astype(F32), own], axis=0)
    result, weights = conv_back(jnp.concatenate(g_x[::-1], axis=0), extended, taps[:, cols], mark, tokens)
    g_rim[:HALO, cols] = result[:HALO]
    g_rim[HALO:, cols] = result[tokens:]
    g_conv[:, cols] = result[HALO:].astype(BF16)
    g_taps[:, cols] = weights

    @pl.when(j == PAIRS - 1)
    def _():
        for i in range(blocks):
            at = slice(i * BLOCK, (i + 1) * BLOCK)
            rows = lax.broadcasted_iota(jnp.int32, (BLOCK, BLOCK), 0)
            seen = (rows <= lane_index((BLOCK, BLOCK))) & (marks[at, 6:7] == labels[0:1, at])
            grad = jnp.where(seen, g_near[i], 0.0)
            g_b[at] += dot(grad.astype(BF16), c[at])
            g_c[at] += dot(grad.T.astype(BF16), b[at])
        for k, ref in enumerate((g_b, g_c)):
            at = slice(INNER + k * NSTATE, INNER + (k + 1) * NSTATE)
            own = proj_bc[:, k * NSTATE : (k + 1) * NSTATE].astype(BF16).astype(F32)
            extended = jnp.concatenate([halo[:, at].astype(F32), own], axis=0)
            result, weights = conv_back(ref[...], extended, taps[:, at], mark, tokens)
            g_rim[:HALO, at] = result[:HALO]
            g_rim[HALO:, at] = result[tokens:]
            g_conv[:, at] = result[HALO:].astype(BF16)
            g_taps[:, at] = weights
        rate = -jnp.exp(params[1:2, :])
        bias_sum = jnp.zeros((1, LANES), F32)
        rate_sum = jnp.zeros((1, LANES), F32)
        rows = lax.broadcasted_iota(jnp.int32, (BLOCK, BLOCK), 0)
        upper = (rows <= lane_index((BLOCK, BLOCK))).astype(F32)
        for i in range(blocks):
            at = slice(i * BLOCK, (i + 1) * BLOCK)
            g_decay = dot(upper, g_cum[at], HIGHEST) + ends[i, 0:1, :]
            delta = decays[0, at]
            full = g_delta[at] + g_decay * rate
            full = full * sigmoid(raw[at] + params[0:1, :])
            g_raw[at] = full.astype(BF16)
            bias_sum = bias_sum + jnp.sum(full, axis=0, keepdims=True)
            rate_sum = rate_sum + jnp.sum(g_decay * delta * rate, axis=0, keepdims=True)
        g_params[...] = jnp.concatenate([bias_sum, rate_sum, g_skip[0:1, :], jnp.zeros((5, LANES), F32)], axis=0)


def mix_back(xbc, proj, halo, taps, y, g_y, decays, decays_t, raw, params, marks, labels, states, leaving, skip):
    tokens = xbc.shape[0]
    blocks = tokens // BLOCK
    tile = pl.BlockSpec((tokens, LANES), lambda j: (0, j))
    acc = lambda *shape: pltpu.VMEM(shape, F32)
    return pl.pallas_call(
        mix_back_kernel,
        out_shape=(
            jax.ShapeDtypeStruct((tokens, CHANNELS), BF16),
            jax.ShapeDtypeStruct((2 * HALO, CHANNELS), F32),
            jax.ShapeDtypeStruct((8, CHANNELS), F32),
            jax.ShapeDtypeStruct((tokens, LANES), BF16),
            jax.ShapeDtypeStruct((8, LANES), F32),
        ),
        grid=(PAIRS,),
        in_specs=[
            tile,
            pl.BlockSpec((tokens, NSTATE), lambda j: (0, INNER // NSTATE)),
            pl.BlockSpec((tokens, NSTATE), lambda j: (0, INNER // NSTATE + 1)),
            pl.BlockSpec((tokens, LANES), lambda j: (0, PAIRS + j)),
            pl.BlockSpec((tokens, 2 * NSTATE), lambda j: (0, 2 * INNER // (2 * NSTATE))),
            whole(halo.shape), whole(taps.shape), tile, tile,
            whole(decays.shape), whole(decays_t.shape), whole(raw.shape), whole(params.shape), whole(marks.shape), whole(labels.shape),
            pl.BlockSpec((blocks + 1, NSTATE, LANES), lambda j: (0, 0, j)),
            pl.BlockSpec((NSTATE, LANES), lambda j: (0, j)),
            whole(skip.shape),
        ],
        out_specs=(
            whole((tokens, CHANNELS)), whole((2 * HALO, CHANNELS)), whole((8, CHANNELS)), whole((tokens, LANES)), whole((8, LANES)),
        ),
        scratch_shapes=[
            acc(tokens, INNER), pltpu.VMEM((tokens, INNER), BF16), pltpu.VMEM((tokens, INNER), BF16), acc(8, LANES),
            acc(blocks, 8, INNER), acc(blocks, BLOCK, BLOCK), pltpu.VMEM((blocks, NSTATE, BLOCK), BF16), acc(NSTATE, LANES),
            acc(blocks, BLOCK, BLOCK), acc(tokens, NSTATE), acc(tokens, NSTATE), acc(tokens, LANES), acc(tokens, LANES),
            acc(8, LANES), acc(blocks, 8, LANES),
        ],
        compiler_params=kernel_params(),
        name="mix_back",
    )(xbc, xbc, xbc, proj, proj, halo, taps, y, g_y, decays, decays_t, raw, params, marks, labels, states, leaving, skip)


QBLOCK = 256
GROUPS = HEADS // KV_HEADS
QPAIRS = QDIM // LANES
SCALE = 1.0 / math.sqrt(HEAD)


def swap_halves(values):
    half = HEAD // 2
    front = lane_index(values.shape) % HEAD < half
    width = values.shape[-1]
    return jnp.where(front, pltpu.roll(values, width - half, 1), pltpu.roll(values, half, 1))


def turn(values, cosine, sine):
    return values * cosine + swap_halves(values) * sine


def rope_kernel(*refs):
    queries, (k, v, cosine, sine, q_out, kv_out) = refs[:QPAIRS], refs[QPAIRS:]
    cos, sin = cosine[...], sine[...]
    for p, q in enumerate(queries):
        q_out[:, p * LANES : (p + 1) * LANES] = turn(q[...], cos, sin).astype(BF16)
    kv_out[:, :KDIM] = turn(k[...], cos, sin).astype(BF16)
    kv_out[:, KDIM:] = v[...].astype(BF16)


def rope_all(proj, cosine, sine):
    tokens = proj.shape[0]
    start = 2 * INNER + 2 * NSTATE
    return pl.pallas_call(
        rope_kernel,
        out_shape=(jax.ShapeDtypeStruct((tokens, QDIM), BF16), jax.ShapeDtypeStruct((tokens, 2 * KDIM), BF16)),
        grid=(1,),
        in_specs=[
            pl.BlockSpec((tokens, LANES), lambda i, p=p: (0, start // LANES + p)) for p in range(QPAIRS + 2)
        ] + [whole(cosine.shape), whole(sine.shape)],
        out_specs=(whole((tokens, QDIM)), whole((tokens, 2 * KDIM))),
        compiler_params=kernel_params(),
        name="rope",
    )(*[proj] * (QPAIRS + 2), cosine, sine)


def both_sides(tile, both):
    low = lane_index(tile.shape) < HEAD
    zero = jnp.zeros_like(tile)
    moved = pltpu.roll(tile.astype(F32), HEAD, 1).astype(tile.dtype)
    both[0, 0] = jnp.where(low, tile, zero)
    both[0, 1] = jnp.where(low, zero, moved)
    both[1, 0] = jnp.where(low, moved, zero)
    both[1, 1] = jnp.where(low, zero, tile)


def attend_kernel(q, kv, key_labels, marks, context, stats, keys, values):
    block, pair = pl.program_id(0), pl.program_id(1)
    window = DOC_MOST + QBLOCK
    start = pl.multiple_of(block * QBLOCK, QBLOCK)

    @pl.when((block == 0) & (pair == 0))
    def _():
        both_sides(kv[:, :KDIM], keys)
        both_sides(kv[:, KDIM:], values)

    group = pair // (GROUPS // 2)
    rows = lax.broadcasted_iota(jnp.int32, (QBLOCK, window), 0)
    cols = lane_index((QBLOCK, window))
    seen = (cols <= rows + DOC_MOST) & (marks[:, 6:7] == key_labels[0, 0:1, :])
    total = jnp.zeros((QBLOCK, LANES), F32)
    found = jnp.zeros((QBLOCK, LANES), F32)
    for a in range(2):
        scores = dot_nt(q[...], keys[group, a, pl.ds(start, window), :]) * SCALE
        scores = jnp.where(seen, scores, NEG_BIG)
        most = jnp.max(scores, axis=1, keepdims=True)
        probs = jnp.exp(scores - most)
        mass = jnp.sum(probs, axis=1, keepdims=True)
        probs = probs * (1.0 / mass)
        total = total + dot(probs.astype(BF16), values[group, a, pl.ds(start, window), :])
        found = jnp.where(lane_index(found.shape) == a, most + jnp.log(mass), found)
    context[...] = total.astype(BF16)
    stats[0] = found.T[0:8, :]


def attend(q, kv, key_labels, marks):
    tokens = q.shape[0]
    blocks = tokens // QBLOCK
    tile = pl.BlockSpec((QBLOCK, LANES), lambda i, p: (i, p))
    return pl.pallas_call(
        attend_kernel,
        out_shape=(jax.ShapeDtypeStruct((tokens, QDIM), BF16), jax.ShapeDtypeStruct((QPAIRS, 8, tokens), F32)),
        grid=(blocks, QPAIRS),
        in_specs=[
            tile, whole(kv.shape), pl.BlockSpec((1,) + key_labels.shape[1:], lambda i, p: (i, 0, 0)),
            pl.BlockSpec((QBLOCK, LANES), lambda i, p: (i, 0)),
        ],
        out_specs=(tile, pl.BlockSpec((1, 8, QBLOCK), lambda i, p: (p, 0, i))),
        scratch_shapes=[pltpu.VMEM((2, 2) + (kv.shape[0], LANES), BF16)] * 2,
        compiler_params=kernel_params(),
        name="attend",
    )(q, kv, key_labels, marks)


def attend_back_kernel(q, kv, given, key_marks, query_labels, stats, cosine, sine, g_q, g_kv, keys, values, g_key, g_value):
    block, pair = pl.program_id(0), pl.program_id(1)
    window = DOC_MOST + QBLOCK
    start = pl.multiple_of(block * QBLOCK, QBLOCK)

    @pl.when((block == 0) & (pair == 0))
    def _():
        both_sides(kv[:, :KDIM], keys)
        both_sides(kv[:, KDIM:], values)
        g_key[...] = jnp.zeros_like(g_key)
        g_value[...] = jnp.zeros_like(g_value)

    group = pair // (GROUPS // 2)
    rows = lax.broadcasted_iota(jnp.int32, (window, QBLOCK), 0)
    cols = lane_index((window, QBLOCK))
    seen = (rows <= cols + DOC_MOST) & (key_marks[0, :, 0:1] == query_labels[0:1, :])
    at = pl.ds(start, window)
    query, grad = q[...], given[...].astype(BF16)
    total = jnp.zeros((QBLOCK, LANES), F32)
    for a, (query_part, grad_part) in enumerate(zip(halves(query), halves(grad))):
        key = keys[group, a, at, :]
        scores = jnp.where(seen, dot_nt(key, query) * SCALE, NEG_BIG)
        probs = jnp.exp(scores - stats[0, a : a + 1, :])
        g_probs = dot_nt(values[group, a, at, :], grad)
        mean = jnp.sum(probs * g_probs, axis=0, keepdims=True)
        g_scores = (probs * (g_probs - mean)).astype(BF16)
        g_key[group, at] += dot(g_scores, query_part) * SCALE
        g_value[group, at] += dot(probs.astype(BF16), grad_part)
        total = total + dot_tn(g_scores, key)
    g_q[...] = turn(total * SCALE, cosine[...], -sine[...]).astype(BF16)

    @pl.when((block == pl.num_programs(0) - 1) & (pair == QPAIRS - 1))
    def _():
        for k, ref in enumerate((g_key, g_value)):
            first = ref[0] + pltpu.roll(ref[0], HEAD, 1)
            second = ref[1] + pltpu.roll(ref[1], HEAD, 1)
            g_kv[:, k * KDIM : (k + 1) * KDIM] = jnp.where(lane_index(first.shape) < HEAD, first, second).astype(BF16)


def attend_back(q, kv, given, key_marks, query_labels, stats, cosine, sine):
    tokens = q.shape[0]
    blocks = tokens // QBLOCK
    tile = pl.BlockSpec((QBLOCK, LANES), lambda i, p: (i, p))
    row = pl.BlockSpec((QBLOCK, LANES), lambda i, p: (i, 0))
    return pl.pallas_call(
        attend_back_kernel,
        out_shape=(jax.ShapeDtypeStruct((tokens, QDIM), BF16), jax.ShapeDtypeStruct(kv.shape, BF16)),
        grid=(blocks, QPAIRS),
        in_specs=[
            tile, whole(kv.shape), pl.BlockSpec((QBLOCK, LANES), lambda i, p: (i, PAIRS + p)),
            pl.BlockSpec((1,) + key_marks.shape[1:], lambda i, p: (i, 0, 0)),
            pl.BlockSpec((8, QBLOCK), lambda i, p: (0, i)),
            pl.BlockSpec((1, 8, QBLOCK), lambda i, p: (p, 0, i)), row, row,
        ],
        out_specs=(tile, whole(kv.shape)),
        scratch_shapes=[pltpu.VMEM((2, 2) + (kv.shape[0], LANES), BF16)] * 2 + [pltpu.VMEM((2, kv.shape[0], LANES), F32)] * 2,
        compiler_params=kernel_params(),
        name="attend_back",
    )(q, kv, given, key_marks, query_labels, stats, cosine, sine)


def turn_back_kernel(g_kv, cosine, sine, out):
    out[:, :KDIM] = turn(g_kv[:, :KDIM], cosine[...], -sine[...]).astype(BF16)
    out[:, KDIM:] = g_kv[:, KDIM:].astype(BF16)


def turn_back(g_kv, cosine, sine):
    return pl.pallas_call(
        turn_back_kernel, out_shape=jax.ShapeDtypeStruct(g_kv.shape, BF16), compiler_params=kernel_params(), name="turn_back",
    )(g_kv, cosine, sine)


def ungroup(rows, micro):
    seq = lax.axis_size("seq")
    each = seq // micro
    here = lax.axis_index("seq")
    order = here // each
    cut = rows.reshape((micro, rows.shape[0] // micro) + rows.shape[1:])
    pieces = []
    for t in range(micro):
        pairs = [(((j + t) % micro) * each + j // micro, j) for j in range(seq)]
        pieces.append(lax.ppermute(lax.dynamic_index_in_dim(cut, (order - t) % micro, 0, False), "seq", pairs))
    stacked = jnp.stack(pieces)
    return jnp.stack([lax.dynamic_index_in_dim(stacked, (m - here) % micro, 0, False) for m in range(micro)])


def along(value, steps, micro):
    seq = lax.axis_size("seq")
    each = seq // micro
    pairs = [(s, s + steps) for s in range(seq) if 0 <= s % each + steps < each]
    return lax.ppermute(value, "seq", pairs)


def pad_rows(*rows):
    width = rows[0].shape[-1]
    return jnp.concatenate([r.reshape(-1, width) for r in rows] + [jnp.zeros((8 - sum(r.size // width for r in rows), width), F32)], axis=0)


def shards(grid, tokens, cotangent, doc_ids, master_blocks, block_of_slot, left_stats, right_stats, left_roots, right_roots,
           vector_params, first_moment, second_moment, adam_step):
    micro, piece = tokens.shape[:2]
    seq = lax.axis_size("seq")
    each = seq // micro
    count = micro * piece
    here = lax.axis_index("seq")
    rank = here % each
    start = rank * count
    slots = master_blocks.shape[0]

    orders = all_orders()
    table = slots_in_order(block_of_slot, sum(orders, []))
    left_at, right_at = (values_of(block_of_slot, values) for values in grad_tables())
    gathered, rows, given, labels_all = gather_blocks(grid, master_blocks, tokens, cotangent, doc_ids)
    w_in, w_out, w_ff, w_down = assemble(gathered.reshape(-1, BS, BS), table)
    rows, given = rows.reshape(count, D), given.reshape(count, D)
    gain_in, gain_mid, gain_mix, conv_weight, conv_bias, dt_bias, a_log, skip, w_dt = unpack_vectors(vector_params)
    w_dt = jnp.pad(w_dt.reshape(D, HEADS_SSM), ((0, 0), (0, LANES - HEADS_SSM))).astype(BF16)
    taps = pad_rows(conv_weight.reshape(KERNEL, CHANNELS), conv_bias)
    lane_pad = lambda v: jnp.pad(v, (0, LANES - HEADS_SSM))
    params = pad_rows(lane_pad(dt_bias), lane_pad(a_log))
    wide_skip = pad_rows(jnp.repeat(skip, HEAD))
    wide_gain = pad_rows(gain_mix)

    row = lax.dynamic_index_in_dim(labels_all, here // each, 1, False).reshape(-1)
    before = jnp.concatenate([jnp.full((DOC_MOST,), -1, jnp.int32), row])
    window = lax.dynamic_slice_in_dim(before, start, DOC_MOST + count)
    labels = window[DOC_MOST:]
    blocks = count // BLOCK
    columns = [(window[DOC_MOST - REACH + tap : DOC_MOST - REACH + tap + count] == labels).astype(F32) for tap in range(KERNEL)]
    by_block = labels.reshape(blocks, BLOCK)
    entries_at = window[DOC_MOST - 1 : DOC_MOST - 1 + count].reshape(blocks, BLOCK)[:, :1]
    columns.append((by_block == entries_at).astype(F32).reshape(-1))
    columns.append((by_block == by_block[:, -1:]).astype(F32).reshape(-1))
    columns.append(labels.astype(F32))
    marks = jnp.pad(jnp.stack(columns, axis=1), ((0, 0), (0, LANES - len(columns))))
    label_rows = jnp.broadcast_to(labels.astype(F32)[None], (8, count))
    far = jnp.stack([window[i : i + DOC_MOST + QBLOCK] for i in range(0, count, QBLOCK)]).astype(F32)
    key_labels = jnp.broadcast_to(far[:, None, :], (far.shape[0], 8, far.shape[1]))
    key_marks = jnp.broadcast_to(far[:, :, None], far.shape + (8,))
    first = jnp.sum((row[None, :] < labels[:, None]).astype(jnp.int32), axis=1)
    positions = (start + jnp.arange(count) - first).astype(F32)
    half = HEAD // 2
    frequency = jnp.exp(jnp.arange(half, dtype=F32) * (-2.0 * math.log(THETA) / HEAD))
    angles = positions[:, None] * frequency[None, :]
    cos, sin = jnp.cos(angles), jnp.sin(angles)
    cosine = jnp.concatenate([cos] * 4, axis=1)
    sine = jnp.concatenate([-sin, sin] * 2, axis=1)

    inputs = rows.astype(F32)
    normed_in = (inputs * rms_scale(inputs) * gain_in).astype(BF16)
    proj = dot(normed_in, w_in)
    raw = dot(normed_in, w_dt)
    halo = along(proj[count - HALO :, INNER : INNER + CHANNELS].astype(BF16), 1, micro)
    q, kv = rope_all(proj, cosine, sine)
    xbc, decays, decays_t, state, factor = mix_first(proj, halo, taps, params, raw, marks)
    past = min(each - 1, -(-DOC_MOST // count))
    earlier = [along(kv, back, micro) for back in range(past, 0, -1)]
    if past * count < DOC_MOST:
        earlier.insert(0, jnp.zeros((DOC_MOST - past * count, kv.shape[1]), BF16))
    reach = jnp.concatenate(earlier + [kv], axis=0)[-(DOC_MOST + count) :]
    wide = lambda f: jnp.repeat(f[0, :HEADS_SSM], HEAD)[None]
    incoming = along(state, each - 1, micro).astype(F32) if each > 1 else jnp.zeros(state.shape, F32)
    for back in range(each - 2, 0, -1):
        incoming = along(state, back, micro).astype(F32) + wide(along(factor, back, micro)) * incoming
    y, normed_ssm, states = mix_second(xbc, proj, decays, decays_t, marks, label_rows, incoming, wide_skip, wide_gain)
    context, stats = attend(q, reach, key_labels, marks)
    hidden = inputs + (dot(normed_ssm, w_out[:INNER]) + dot(context, w_out[INNER:]))
    normed_mid = (hidden * rms_scale(hidden) * gain_mid).astype(BF16)
    both = dot(normed_mid, w_ff)
    gate, upper = both[:, :FF], both[:, FF:]
    opened = sigmoid(gate)
    mixed = (gate * opened * upper).astype(BF16)
    layer_out = ungroup((hidden + dot(mixed, w_down)).astype(BF16), micro)

    g_mixed = dot_nt(given, w_down)
    g_gate = g_mixed * upper * (opened + gate * opened * (1.0 - opened))
    g_ff = jnp.concatenate([g_gate.astype(BF16), (g_mixed * gate * opened).astype(BF16)], axis=1)

    def norm_back(grad, values, gain):
        scale = rms_scale(values)
        unit = values * scale
        scaled = grad * gain
        return scale * (scaled - unit * jnp.mean(scaled * unit, axis=1, keepdims=True)), jnp.sum(grad * unit, axis=0)

    g_values, g_gain_mid = norm_back(dot_nt(g_ff, w_ff), hidden, gain_mid)
    g_hidden = given.astype(F32) + g_values
    hidden_low = g_hidden.astype(BF16)
    g_out = dot_nt(hidden_low, w_out)
    g_y, g_z, g_gain_mix, g_state = gate_back(g_out, y, proj, wide_gain, xbc, decays, marks)
    low_state = g_state.astype(BF16)
    leaving = along(low_state, 1 - each, micro).astype(F32) if each > 1 else jnp.zeros(state.shape, F32)
    for ahead in range(each - 2, 0, -1):
        leaving = along(low_state, -ahead, micro).astype(F32) + wide(along(factor, -ahead, micro)) * leaving
    g_q, g_reach = attend_back(q, reach, g_out, key_marks, label_rows, stats, cosine, sine)
    g_conv, g_rim, g_taps, g_raw, g_params = mix_back(
        xbc, proj, halo, taps, y, g_y, decays, decays_t, raw, params, marks, label_rows, states, leaving, wide_skip
    )
    g_kv = g_reach[-count:].astype(F32)
    for back in range(1, past + 1):
        low = max(0, DOC_MOST - back * count)
        part = g_reach[low : DOC_MOST - (back - 1) * count]
        moved = along(part, -back, micro).astype(F32)
        g_kv = g_kv + jnp.pad(moved, ((count - part.shape[0], 0), (0, 0)))
    g_kv = turn_back(g_kv, cosine, sine)
    rim = along(g_rim[:HALO], -1, micro)
    g_conv = lax.dynamic_update_slice(g_conv, (g_rim[HALO:] + rim).astype(BF16), (count - HALO, 0))
    g_in = jnp.concatenate([g_z, g_conv, g_q, g_kv], axis=1)
    g_values, g_gain_in = norm_back(dot_nt(g_in, w_in) + dot_nt(g_raw, w_dt), inputs, gain_in)
    grad_tokens = ungroup((g_values + g_hidden).astype(BF16), micro).astype(F32)
    g_w_dt = dot_tn(normed_in, g_raw)

    parts = [g_gain_in, g_gain_mid, g_gain_mix[0], g_taps[:KERNEL].reshape(-1), g_taps[KERNEL]]
    parts += [g_params[i, :HEADS_SSM] for i in range(3)] + [g_w_dt[:, :HEADS_SSM].reshape(-1)]
    width = vector_params.shape[0]
    height = -(-width // (8 * LANES)) * 8
    vector = jnp.concatenate(parts + [jnp.zeros((height * LANES - width,), F32)]).reshape(height, LANES)
    total, vector = reduce_blocks(grid, slots, left_at, right_at, [normed_in, normed_ssm, context, normed_mid, mixed],
                                  [g_z, g_conv, g_q, g_kv, hidden_low, g_ff, given], vector)
    norm = 1.0 / math.sqrt(count * seq * lax.axis_size("dp"))
    updates = shampoo(norm, total, master_blocks, left_stats, right_stats, left_roots, right_roots)
    g_vector = vector.reshape(-1)[:width] * norm
    step = adam_step[0].astype(F32)
    new_first = BETA_ONE * first_moment + (1.0 - BETA_ONE) * g_vector
    new_second = BETA_TWO * second_moment + (1.0 - BETA_TWO) * g_vector * g_vector
    first_hat = new_first / (1.0 - jnp.power(BETA_ONE, step))
    second_hat = new_second / (1.0 - jnp.power(BETA_TWO, step))
    new_vector = vector_params - LR_VECTOR * first_hat / (jnp.sqrt(second_hat) + ADAM_EPS)
    return (layer_out, grad_tokens) + tuple(updates) + (g_vector, new_vector, new_first, new_second)


def solution(mesh):
    line, block, copied = P("dp", "seq", None), P("dp", None, None), P()
    return jax.shard_map(
        functools.partial(shards, grid_of(mesh)),
        mesh=mesh,
        in_specs=(line, line, P("dp", "seq"), block, copied, block, block, block, block, copied, copied, copied, copied),
        out_specs=(line, line) + (block,) * 5 + (copied,) * 4,
        check_vma=False,
    )
```

```python
import functools
import math

import jax
import jax.numpy as jnp
from jax import lax
from jax.experimental import pallas as pl
from jax.experimental.pallas import tpu as pltpu
from jax.sharding import PartitionSpec as P

D = 1024
HEADS_SSM = 24
HEAD = 64
NSTATE = 128
HEADS = 8
KV_HEADS = 2
FF = 2048
KERNEL = 4
BS = 128
DOC_MOST = 512
INNER = HEADS_SSM * HEAD
CHANNELS = INNER + 2 * NSTATE
REACH = KERNEL - 1
QDIM = HEADS * HEAD
KDIM = KV_HEADS * HEAD
LANES = 128
PAIRS = INNER // LANES

EPS = 1e-05
THETA = 100000000000.0
LR_MATRIX = 0.02
LR_VECTOR = 0.08
BETA_ONE = 0.9
BETA_TWO = 0.999
ADAM_EPS = 1e-08
NEG_BIG = -1e30
F32 = jnp.float32
BF16 = jnp.bfloat16
HIGHEST = lax.Precision.HIGHEST
VMEM_MOST = 60 << 20

SHAPES = (
    (D, INNER), (D, INNER), (D, 2 * NSTATE), (D, QDIM), (D, KDIM), (D, KDIM),
    (INNER, D), (QDIM, D), (D, FF), (D, FF), (FF, D),
)
WIDE_IN, TALL_OUT, WIDE_FF, TALL_FF = (0, 1, 2, 3, 4, 5), (6, 7), (8, 9), (10,)
SIZES = (D, D, INNER, KERNEL * CHANNELS, CHANNELS, HEADS_SSM, HEADS_SSM, HEADS_SSM, D * HEADS_SSM)


def block_offsets():
    starts, total = [], 0
    for rows, cols in SHAPES:
        starts.append(total)
        total += rows // BS * (cols // BS)
    return starts


def wide_order(members):
    starts = block_offsets()
    rows = SHAPES[members[0]][0] // BS
    return [starts[m] + r * (SHAPES[m][1] // BS) + q for r in range(rows) for m in members for q in range(SHAPES[m][1] // BS)]


def tall_order(members):
    starts = block_offsets()
    return [starts[m] + i for m in members for i in range(SHAPES[m][0] // BS * (SHAPES[m][1] // BS))]


def all_orders():
    return [wide_order(WIDE_IN), tall_order(TALL_OUT), wide_order(WIDE_FF), tall_order(TALL_FF)]


def unpack_vectors(flat):
    result, offset = [], 0
    for count in SIZES:
        result.append(flat[offset : offset + count])
        offset += count
    return result


def dot(left, right, precision=None):
    return jnp.dot(left, right, preferred_element_type=F32, precision=precision)


def dot_nt(left, right):
    return lax.dot_general(left, right, (((1,), (1,)), ((), ())), preferred_element_type=F32)


def dot_tn(left, right):
    return lax.dot_general(left, right, (((0,), (0,)), ((), ())), preferred_element_type=F32)


def sigmoid(v):
    return 1.0 / (1.0 + jnp.exp(-v))


def rms_scale(values):
    return lax.rsqrt(jnp.mean(values * values, axis=-1, keepdims=True) + EPS)


def kernel_params(**more):
    return pltpu.CompilerParams(vmem_limit_bytes=VMEM_MOST, **more)


def whole(shape):
    return pl.BlockSpec(shape, lambda *_: (0,) * len(shape))


MESH = pl.DeviceIdType.MESH
CORES = 2
PIECES = 3
APART = 5 / 16


def grid_of(mesh):
    try:
        wide = len({device.coords[0] for device in mesh.devices.flat})
    except AttributeError:
        wide = mesh.shape["seq"] // CORES
    return wide, mesh.shape["seq"] // CORES, mesh.shape["dp"] // wide


def parts_of(slots, tall):
    half = slots // CORES
    size = half // PIECES
    lone = round(size * APART) if tall == 2 and size >= 8 else 0
    return half, size, lone, size - lone


def place(grid):
    wide, tall, deep = grid
    dp, seq = lax.axis_index("dp"), lax.axis_index("seq")
    return dp % wide, seq // CORES, dp // wide, seq % CORES


def gather_kernel(grid, slots, master, tokens, cotangent, docs, out, rows, given, labels, wide_own, src, bounce,
                  sem_own, sem_load, sz, rz, sx, rx, sy, ry, sc, rc, s_rows, r_rows, s_docs, r_docs):
    wide, tall, deep = grid
    x, y, z, c = place(grid)
    half, size, lone, bulk = parts_of(slots, tall)
    me = z * wide + x
    seq = y * CORES + c
    base = c * half
    bulk_at = y * (size - bulk)
    lone_at = y * bulk
    other_at = (1 - y) * bulk if lone else 0
    mate = y * CORES + (1 - c)
    over = (tall - 1 - y) * CORES + c
    peers = tall * CORES
    micro = tokens.shape[0]
    each = peers // micro

    loads = []
    for k in range(CORES):
        part = pl.ds(((c + k) % CORES) * half, half)
        loads.append((part, pltpu.make_async_copy(master.at[part], wide_own.at[part], sem_load.at[k])))
        loads[-1][1].start()

    barrier = pltpu.get_barrier_semaphore()
    count = jnp.int32(0)
    for step_by, at, length in ((wide, z, deep), (1, x, wide)):
        for step in (1, -1):
            ok = (at + step >= 0) & (at + step < length)
            there = me + step * step_by

            @pl.when(ok)
            def _(there=there):
                pl.semaphore_signal(barrier, inc=1, device_id=(there, seq), device_id_type=MESH)

            count = count + ok.astype(jnp.int32)
    for k in range(1, peers):
        pl.semaphore_signal(barrier, inc=1, device_id=(me, (seq + k) % peers), device_id_type=MESH)
    pl.semaphore_wait(barrier, count + (peers - 1))
    both = ((0, 1), (1, -1))
    yes = jnp.bool_(True)

    def piece(shard, at, length):
        return out.at[shard, pl.ds(at, length)]

    def run(begin_it):
        def send(ok, source, target, send_sem, recv_sem, device):
            copy = pltpu.make_async_remote_copy(
                src_ref=source, dst_ref=target, send_sem=send_sem, recv_sem=recv_sem,
                device_id=device, device_id_type=MESH,
            )

            @pl.when(ok)
            def _():
                if begin_it:
                    copy.start()
                else:
                    copy.wait_send()

        def arrived(ok, target, recv_sem):
            if begin_it:
                copy = pltpu.make_async_remote_copy(
                    src_ref=target, dst_ref=target, send_sem=sem_own.at[0], recv_sem=recv_sem,
                    device_id=(me, seq), device_id_type=MESH,
                )

                @pl.when(ok)
                def _():
                    copy.wait_recv()

        def pass_on(ok, shard, sub):
            at = base + sub * size
            mine = piece(shard, at + bulk_at, bulk)
            send(ok, mine, mine, sc.at[0, shard, sub], rc.at[0, shard, sub], (me, mate))
            if lone:
                mine = piece(shard, at + lone_at, lone)
                send(ok, mine, mine, sy.at[shard, sub], ry.at[shard, sub], (me, over))

        def along_x(ok, zs, dirs, hop, sub, own):
            for d, step in dirs:
                shard = zs * wide + x - step * hop
                go = ok & (x + step >= 0) & (x + step < wide)
                at = base + sub * size + bulk_at
                source = src.at[pl.ds(at, bulk)] if own else piece(shard, at, bulk)
                send(go, source, piece(shard, at, bulk), sx.at[d, hop, zs, sub], rx.at[d, hop + 1, zs, sub], (me + step, seq))

        def columns(s):
            return [(yes, z)] if s == 0 else [((z - step * s >= 0) & (z - step * s < deep), z - step * s) for _, step in both]

        def x_in(s, hop, sub):
            for ok, zs in columns(s):
                for d, step in both:
                    from_x = x - step * hop
                    come = ok & (from_x >= 0) & (from_x < wide)
                    shard = zs * wide + from_x
                    arrived(come, piece(shard, base + sub * size + bulk_at, bulk), rx.at[d, hop, zs, sub])
                    along_x(come, zs, ((d, step),), hop, sub, False)
                    pass_on(come, shard, sub)

        def y_in(ok, shard, sub):
            if lone:
                mine = piece(shard, base + sub * size + other_at, lone)
                arrived(ok, mine, ry.at[shard, sub])
                send(ok, mine, mine, sc.at[1, shard, sub], rc.at[1, shard, sub], (me, mate))

        def y_all(s, sub):
            for ok, zs in columns(s):
                if s > 0:
                    y_in(ok, zs * wide + x, sub)
                for hop in range(1, wide):
                    for _, step in both:
                        from_x = x - step * hop
                        y_in(ok & (from_x >= 0) & (from_x < wide), zs * wide + from_x, sub)

        def z_step(s, sub):
            for d, step in both:
                zs = z - step * s
                ok = (zs >= 0) & (zs < deep)
                shard = zs * wide + x
                at = base + sub * size + bulk_at
                mine = piece(shard, at, bulk)
                if s:
                    arrived(ok, mine, rz.at[d, s, sub])
                go = ok & (z + step >= 0) & (z + step < deep)
                source = mine if s else src.at[pl.ds(at, bulk)]
                if s + 1 < deep:
                    send(go, source, mine, sz.at[d, s, sub], rz.at[d, s + 1, sub], (me + step * wide, seq))
                if s:
                    along_x(ok, zs, both, 0, sub, False)
                    pass_on(ok, shard, sub)
            if s == 0:
                along_x(yes, z, both, 0, sub, True)

        for s in range(deep):
            def one(sub, _, s=s):
                z_step(s, sub)
                if s:
                    for hop in range(1, wide):
                        x_in(s - 1, hop, sub)
                if s >= 2:
                    y_all(s - 2, sub)
                return 0

            lax.fori_loop(0, PIECES, one, 0)
            if s == 0:
                local(begin_it, send, arrived)

        def last_x(sub, _):
            for hop in range(1, wide):
                x_in(deep - 1, hop, sub)
            if deep > 1:
                y_all(deep - 2, sub)
            return 0

        def last_y(sub, _):
            y_all(deep - 1, sub)
            return 0

        lax.fori_loop(0, PIECES, last_x, 0)
        lax.fori_loop(0, PIECES, last_y, 0)

    def convert(k):
        part, copy = loads[k]
        copy.wait()
        base_at = ((c + k) % CORES) * half

        def one(i, _):
            src[base_at + i] = wide_own[base_at + i].astype(src.dtype)
            return 0

        lax.fori_loop(0, half, one, 0, unroll=2)

    keep = pltpu.make_async_copy(src, out.at[me], sem_load.at[0])
    at_home = []
    for t in range(micro):
        m = (seq + t) % micro
        there = m * each + seq // micro
        for k, (source, target) in enumerate(((tokens, rows), (cotangent, given))):
            place_to = target.at[seq % micro]
            take = pltpu.make_async_copy(source.at[m], bounce.at[k], sem_own.at[k])
            put = pltpu.make_async_copy(bounce.at[k], place_to, sem_own.at[k])
            at_home.append((there == seq, take, put))

    def local(begin_it, send, arrived):
        for t in range(micro):
            m = (seq + t) % micro
            there = m * each + seq // micro
            for k, (source, target) in enumerate(((tokens, rows), (cotangent, given))):
                send(there != seq, source.at[m], target.at[seq % micro], s_rows.at[k, t], r_rows.at[k, seq % micro], (me, there))
        if begin_it:
            labels[seq] = docs[...]
        for k in range(1, peers):
            send(yes, docs, labels.at[seq], s_docs.at[k], r_docs.at[seq], (me, (seq + k) % peers))
        if begin_it:
            for ok, take, _ in at_home:
                @pl.when(ok)
                def _(take=take):
                    take.start()
            convert(1)
            keep.start()
            for ok, take, put in at_home:
                @pl.when(ok)
                def _(take=take, put=put):
                    take.wait()
                    put.start()

    convert(0)
    run(True)
    keep.wait()
    for ok, take, put in at_home:
        @pl.when(ok)
        def _(put=put):
            put.wait()

    def came(ok, target, recv_sem):
        @pl.when(ok)
        def _():
            pltpu.make_async_remote_copy(
                src_ref=target, dst_ref=target, send_sem=sem_own.at[0], recv_sem=recv_sem,
                device_id=(me, seq), device_id_type=MESH,
            ).wait_recv()

    for q in range(micro):
        source = seq % each * micro + q
        for k, target in enumerate((rows, given)):
            came(source != seq, target.at[q], r_rows.at[k, q])
    for k in range(1, peers):
        source = (seq + k) % peers
        came(yes, labels.at[source], r_docs.at[source])

    def last(i, _):
        shard, sub = i // PIECES, i % PIECES
        at = (1 - c) * half + sub * size
        came(shard != me, piece(shard, at + bulk_at, bulk), rc.at[0, shard, sub])
        if lone:
            came(shard != me, piece(shard, at + other_at, lone), rc.at[1, shard, sub])
        return 0

    lax.fori_loop(0, wide * deep * PIECES, last, 0)
    run(False)


def gather_blocks(grid, master, tokens, cotangent, docs):
    wide, tall, deep = grid
    slots = master.shape[0]
    n = wide * deep
    peers = tall * CORES
    micro = tokens.shape[0]
    low = tokens.dtype
    sem = pltpu.SemaphoreType.DMA
    hbm = pl.BlockSpec(memory_space=pl.ANY)
    vmem = pl.BlockSpec(memory_space=pltpu.VMEM)
    return pl.pallas_call(
        functools.partial(gather_kernel, grid, slots),
        out_shape=(
            jax.ShapeDtypeStruct((n,) + master.shape, low),
            jax.ShapeDtypeStruct(tokens.shape, low), jax.ShapeDtypeStruct(tokens.shape, low),
            jax.ShapeDtypeStruct((peers,) + docs.shape, docs.dtype),
        ),
        in_specs=[hbm, hbm, hbm, vmem],
        out_specs=(hbm, hbm, hbm, vmem),
        scratch_shapes=[
            pltpu.VMEM(master.shape, master.dtype), pltpu.VMEM(master.shape, low), pltpu.VMEM((2,) + tokens.shape[1:], low),
            sem((2,)), sem((CORES,)),
            sem((2, deep, PIECES)), sem((2, deep + 1, PIECES)),
            sem((2, wide, deep, PIECES)), sem((2, wide + 1, deep, PIECES)),
            sem((n, PIECES)), sem((n, PIECES)),
            sem((2, n, PIECES)), sem((2, n, PIECES)),
            sem((2, micro)), sem((2, micro)), sem((peers,)), sem((peers,)),
        ],
        compiler_params=pltpu.CompilerParams(collective_id=0, has_side_effects=True, vmem_limit_bytes=60 << 20),
        name="gather_blocks",
    )(master, tokens, cotangent, docs)

def far_first(at, size, i):
    above, below = size - 1 - at, at
    less, more = jnp.minimum(above, below), jnp.maximum(above, below)
    long_side = jnp.where(above >= below, 1, -1)
    j = i - (more - less)
    near = at + jnp.where(j % 2 == 0, 1, -1) * (less - j // 2)
    return jnp.where(j < 0, at + long_side * (more - i), near)


def entry(at, size, source_below, target):
    lower = jnp.where(at > 0, size - at, 0) if size > 2 else 0
    return target - at if source_below else lower + at - target


def entries(size):
    return size + 1 if size > 2 else 1

SUBS = 3
LONE = 5 / 16
RING = 6
STAGED = 3
LATE_ADD, LATE_X, LATE_Z, PER_HOP = 1, 3, 6, 3
CHUNK = 512
HELD = 12


def split_of(slots, tall):
    half = slots // CORES
    piece = half // SUBS
    lone = round(piece * LONE) if tall == 2 and piece >= 8 else 0
    return half, piece, lone, piece - lone


def reduce_kernel(grid, slots, widths, left_at, right_at, vec, *refs):
    wide, tall, deep = grid
    count = sum(len(w) for w in widths)
    arrays = refs[:count]
    (out, vec_out, turned, right, held, acc, stage, land_c, land_y, land_x, land_z, fin, vbuf, vland,
     s_left, s_right, s_c, r_c, s_y, r_y, s_x, r_x, s_z, r_z, s_f, r_f, s_m, r_m, s_v, r_v, free) = refs[count:]
    n = wide * deep
    x, y, z, c = place(grid)
    half, size, lone, bulk = split_of(slots, tall)
    me = z * wide + x
    seq = y * CORES + c
    mate = y * CORES + (1 - c)
    bulk_at = y * lone
    lone_at = y * bulk
    other_at = (1 - y) * bulk
    bits = lambda length: [1 << b for b in range(length.bit_length() - 1)]
    partners = [(me, mate)]
    partners += [(me, (y ^ b) * CORES + c) for b in bits(tall)]
    partners += [(z * wide + (x ^ b), seq) for b in bits(wide)]
    partners += [((z ^ b) * wide + x, seq) for b in bits(deep)]
    rounds = len(partners)

    chunks, k, at = [], 0, 0
    for width in widths[0]:
        for q in range(0, width, CHUNK):
            chunks.append((k, q, at + q))
        k, at = k + 1, at + width

    def chunk_copy(i):
        k, q, _ = chunks[i]
        return pltpu.make_async_copy(arrays[k].at[:, pl.ds(q, CHUNK)], held.at[i % HELD], s_left.at[i % HELD])

    ahead = min(HELD, len(chunks))
    for i in range(ahead):
        chunk_copy(i).start()
    copies, at = [], 0
    for width in widths[1]:
        def one(q, _, k=k, at=at):
            cols = pl.ds(pl.multiple_of(q * BS, BS), BS)
            pltpu.make_async_copy(arrays[k].at[:, cols], right.at[at + q], s_right.at[k - len(widths[0])]).start()
            return 0

        lax.fori_loop(0, width // BS, one, 0)
        part = right.at[pl.ds(at, width // BS)]
        copies.append(pltpu.make_async_copy(part, part, s_right.at[k - len(widths[0])]))
        k, at = k + 1, at + width // BS

    barrier = pltpu.get_barrier_semaphore()
    awaited = jnp.int32(0)
    for step_by, at, length in ((wide, z, deep), (1, x, wide)):
        for step in (1, -1):
            ok = (at + step >= 0) & (at + step < length)

            @pl.when(ok)
            def _(there=me + step * step_by):
                pl.semaphore_signal(barrier, inc=1, device_id=(there, seq), device_id_type=MESH)

            awaited = awaited + ok.astype(jnp.int32)
    for device in partners:
        pl.semaphore_signal(barrier, inc=1, device_id=device, device_id_type=MESH)
    pl.semaphore_wait(barrier, awaited + rounds)

    def remote(source, target, send_sem, recv_sem, device):
        return pltpu.make_async_remote_copy(
            src_ref=source, dst_ref=target, send_sem=send_sem, recv_sem=recv_sem,
            device_id=device, device_id_type=MESH,
        )

    def landed(target, recv_sem):
        remote(target, target, s_left.at[0], recv_sem, (me, seq)).wait_recv()

    def vec_copy(t):
        return remote(vbuf.at[t], vland.at[t], s_v.at[t], r_v.at[t], partners[t])

    vbuf[0] = vec[...]
    vec_copy(0).start()
    for i in range(len(chunks)):
        chunk_copy(i).wait()
        for q in range(0, CHUNK, BS):
            turned[(chunks[i][2] + q) // BS] = held[i % HELD, :, q : q + BS].T
        if i + HELD < len(chunks):
            chunk_copy(i + HELD).start()
    for copy in copies:
        copy.wait()

    group = wide * SUBS
    total = n * SUBS

    def item_of(k):
        xs = far_first(x, wide, k % wide)
        zs = far_first(z, deep, k // group)
        sub = (k // wide) % SUBS
        return xs, zs, sub, (zs * wide + xs) * SUBS + sub

    def swap(k):
        return remote(stage.at[k % STAGED], land_c.at[k % RING], s_c.at[k % STAGED], r_c.at[k % RING], (me, mate))

    def cross(item):
        return remote(acc.at[item, pl.ds(other_at, lone)], land_y.at[item], s_y.at[item], r_y.at[item], (me, (tall - 1 - y) * CORES + c))

    def grads(k, core, ref, first):
        xs, zs, sub, item = item_of(k)
        base = (zs * wide + xs) * slots + core * half + sub * size

        def one(i, _):
            ref[first, i] = dot(turned[left_at[base + i]], right[right_at[base + i]]).astype(ref.dtype)
            return 0

        lax.fori_loop(0, size, one, 0, unroll=min(4, size))

    def add(item, at, length, ref, first):
        def one(i, _):
            acc[item, at + i] = acc[item, at + i] + ref[first + (i,)]
            return 0

        lax.fori_loop(0, length, one, 0, unroll=min(3, length))

    def step_x(k, begin_it):
        xs, zs, sub, item = item_of(k)
        for below, step in ((True, 1), (False, -1)):
            to = entry(x + step, wide, below, xs)
            sent = remote(acc.at[item, pl.ds(bulk_at, bulk)], land_x.at[to, zs * SUBS + sub], s_x.at[item],
                          r_x.at[to, zs * SUBS + sub], (me + step, seq))

            @pl.when((xs - x) * step > 0)
            def _():
                if begin_it:
                    sent.start()
                else:
                    sent.wait_send()

    def take_x(k):
        xs, zs, sub, item = item_of(k)
        for below, step in ((True, 1), (False, -1)):
            comes = ((xs - x) * step >= 0) & (x - step >= 0) & (x - step < wide)
            at = entry(x, wide, below, xs)

            @pl.when(comes)
            def _():
                landed(land_x.at[at, zs * SUBS + sub], r_x.at[at, zs * SUBS + sub])
                add(item, bulk_at, bulk, land_x, (at, zs * SUBS + sub))

    def step_z(k, begin_it):
        xs, zs, sub, item = item_of(k)
        for below, step in ((True, 1), (False, -1)):
            to = entry(z + step, deep, below, zs)
            sent = remote(acc.at[item, pl.ds(bulk_at, bulk)], land_z.at[to, sub], s_z.at[zs * SUBS + sub], r_z.at[to, sub],
                          (me + step * wide, seq))

            @pl.when((zs - z) * step > 0)
            def _():
                if begin_it:
                    sent.start()
                else:
                    sent.wait_send()

    def take_z(k):
        xs, zs, sub, item = item_of(k)
        for below, step in ((True, 1), (False, -1)):
            comes = ((zs - z) * step >= 0) & (z - step >= 0) & (z - step < deep)
            at = entry(z, deep, below, zs)

            @pl.when(comes)
            def _():
                landed(land_z.at[at, sub], r_z.at[at, sub])
                add(item, bulk_at, bulk, land_z, (at, sub))

    planes = bits(tall)

    def swap_plane(t, sub):
        mine = pl.ds(bulk_at, bulk)
        return remote(acc.at[me * SUBS + sub, mine], fin.at[t, sub, mine], s_f.at[t, sub], r_f.at[t, sub], (me, (y ^ planes[t]) * CORES + c))

    def take_plane(t, sub):
        item = me * SUBS + sub
        theirs = pl.ds((1 - y) * lone if lone else 0, bulk)
        landed(fin.at[t, sub, theirs], r_f.at[t, sub])
        swap_plane(t, sub).wait_send()
        add(item, lone, size - 2 * lone, fin.at[t, sub, pl.ds(lone, size - 2 * lone)], ())
        if lone:
            cross(item).wait_send()
            acc[item, pl.ds(other_at, lone)] = fin[t, sub, pl.ds(other_at, lone)]

    def swap_core(sub):
        return remote(acc.at[me * SUBS + sub], out.at[pl.ds(c * half + sub * size, size)], s_m.at[sub], r_m.at[sub], (me, mate))

    late_z = LATE_Z + PER_HOP * jnp.minimum(z, deep - 1 - z)

    def turn_of(k, _):
        @pl.when(k < total)
        def _():
            @pl.when(k >= STAGED)
            def _():
                swap(k - STAGED).wait_send()

            grads(k, 1 - c, stage, k % STAGED)

            @pl.when(k >= RING)
            def _():
                pl.semaphore_wait(free, 1)

            swap(k).start()
            grads(k, c, acc, item_of(k)[3])

        for t in range(1, rounds + 1):
            @pl.when(k == t)
            def _(t=t):
                landed(vland.at[t - 1], r_v.at[t - 1])
                vbuf[t] = vbuf[t - 1] + vland[t - 1]
                if t < rounds:
                    vec_copy(t).start()
                else:
                    vec_out[...] = vbuf[t]

        b = k - LATE_ADD

        @pl.when((b >= 0) & (b < total))
        def _():
            item = item_of(b)[3]
            landed(land_c.at[b % RING], r_c.at[b % RING])
            add(item, 0, size, land_c, (b % RING,))

            @pl.when(b < total - RING)
            def _():
                pl.semaphore_signal(free, inc=1, device_id=(me, mate), device_id_type=MESH)

            if lone:
                cross(item).start()

        b = k - LATE_X

        @pl.when((b >= 0) & (b < total))
        def _():
            item = item_of(b)[3]
            if lone:
                landed(land_y.at[item], r_y.at[item])
                add(item, lone_at, lone, land_y, (item,))
            if wide > 2:
                @pl.when(item_of(b)[0] != x)
                def _():
                    take_x(b)
            step_x(b, True)

        b = k - late_z

        @pl.when((b >= 0) & (b < total) & (b % wide == wide - 1))
        def _():
            take_x(b)
            take_z(b)
            step_z(b, True)
            if planes:
                @pl.when(item_of(b)[1] == z)
                def _():
                    swap_plane(0, item_of(b)[2]).start()

        return 0

    lax.fori_loop(0, total + LATE_Z + PER_HOP * ((deep - 1) // 2), turn_of, 0)

    def finish(k, _):
        if lone:
            item = item_of(k)[3]

            @pl.when(item // SUBS != me)
            def _():
                cross(item).wait_send()

        step_x(k, False)

        @pl.when(k % wide == wide - 1)
        def _():
            step_z(k, False)

        return 0

    for t in range(len(planes)):
        for sub in range(SUBS):
            if t:
                swap_plane(t, sub).start()
        for sub in range(SUBS):
            take_plane(t, sub)
            if t == len(planes) - 1:
                swap_core(sub).start()
                out[pl.ds(c * half + sub * size, size)] = acc[me * SUBS + sub]
    lax.fori_loop(0, total, finish, 0)
    for k in range(max(total - STAGED, 0), total):
        swap(k).wait_send()
    for t in range(rounds):
        vec_copy(t).wait_send()
    for sub in range(SUBS):
        swap_core(sub).wait_send()
        landed(out.at[pl.ds((1 - c) * half + sub * size, size)], r_m.at[sub])


def reduce_blocks(grid, slots, left_at, right_at, lefts, rights, vec):
    wide, tall, deep = grid
    n = wide * deep
    half, size, lone, bulk = split_of(slots, tall)
    tile = (BS, BS)
    low = lefts[0].dtype
    tokens = lefts[0].shape[0]
    widths = [[a.shape[1] for a in lefts], [a.shape[1] for a in rights]]
    sem = pltpu.SemaphoreType.DMA
    rounds = sum(length.bit_length() - 1 for length in (CORES, wide, tall, deep))
    planes = max(tall.bit_length() - 1, 1)
    items = n * SUBS
    buf = lambda *lead: pltpu.VMEM(lead + tile, low)
    smem, vmem, hbm = (pl.BlockSpec(memory_space=m) for m in (pltpu.SMEM, pltpu.VMEM, pl.ANY))
    return pl.pallas_call(
        functools.partial(reduce_kernel, grid, slots, widths),
        out_shape=(jax.ShapeDtypeStruct((slots,) + tile, low), jax.ShapeDtypeStruct(vec.shape, vec.dtype)),
        in_specs=[smem, smem, vmem] + [hbm] * (len(lefts) + len(rights)),
        out_specs=(vmem, vmem),
        scratch_shapes=[
            pltpu.VMEM((sum(widths[0]) // BS, BS, tokens), low), pltpu.VMEM((sum(widths[1]) // BS, tokens, BS), low), pltpu.VMEM((HELD, tokens, CHUNK), low),
            buf(items, size), buf(STAGED, size), buf(RING, size), buf(items, max(lone, 1)), buf(entries(wide), deep * SUBS, bulk),
            buf(entries(deep), SUBS, bulk), buf(planes, SUBS, size),
            pltpu.VMEM((rounds + 1,) + vec.shape, vec.dtype), pltpu.VMEM((rounds,) + vec.shape, vec.dtype),
            sem((HELD,)), sem((len(rights),)), sem((STAGED,)), sem((RING,)), sem((items,)), sem((items,)), sem((items,)),
            sem((entries(wide), deep * SUBS)), sem((deep * SUBS,)), sem((entries(deep), SUBS)),
            sem((planes, SUBS)), sem((planes, SUBS)), sem((SUBS,)), sem((SUBS,)), sem((rounds,)), sem((rounds,)),
            pltpu.SemaphoreType.REGULAR,
        ],
        compiler_params=pltpu.CompilerParams(collective_id=1, has_side_effects=True, vmem_limit_bytes=63 << 20),
        name="reduce_blocks",
    )(left_at, right_at, vec, *lefts, *rights)


STEP_BLOCKS = 32
DEPTH = 4


def assemble_kernel(table, blocks, w_in, w_out, w_ff, w_down, wide, tall, s_in, s_out):
    outs = []
    for ref in (w_in, w_out, w_ff, w_down):
        rows, cols = ref.shape
        per_row = cols // BS
        deep = STEP_BLOCKS // per_row
        for r in range(rows // (BS * deep)):
            outs.append((ref, r * BS * deep, deep, per_row))

    def target(step):
        ref, at, deep, per_row = outs[step]
        slot = step % DEPTH
        return (wide.at[slot] if deep == 1 else tall.at[slot]), ref.at[pl.ds(at, BS * deep)], deep, per_row

    def fetch(step):
        buffer, _, deep, per_row = target(step)

        def one(i, _):
            rows = pl.ds(pl.multiple_of(i // per_row * BS, BS), BS)
            cols = pl.ds(pl.multiple_of(i % per_row * BS, BS), BS)
            pltpu.make_async_copy(blocks.at[table[step * STEP_BLOCKS + i]], buffer.at[rows, cols], s_in.at[step % DEPTH]).start()
            return 0

        lax.fori_loop(0, STEP_BLOCKS, one, 0)

    def put(step):
        buffer, place_to, _, _ = target(step)
        return pltpu.make_async_copy(buffer, place_to, s_out.at[step % DEPTH])

    steps = len(outs)
    for step in range(min(DEPTH - 1, steps)):
        fetch(step)
    for step in range(steps):
        buffer, place_to, _, _ = target(step)
        pltpu.make_async_copy(place_to, buffer, s_in.at[step % DEPTH]).wait()
        put(step).start()
        ahead = step + DEPTH - 1
        if ahead < steps:
            if step >= 1:
                put(step - 1).wait()
            fetch(ahead)
    for step in range(max(steps - DEPTH, 0), steps):
        put(step).wait()


def slots_in_order(block_of_slot, order):
    match = jnp.array(order, jnp.int32)[:, None] == block_of_slot[None, :]
    return jnp.sum(jnp.where(match, jnp.arange(block_of_slot.shape[0], dtype=jnp.int32)[None, :], 0), axis=1)


def values_of(block_of_slot, values):
    match = block_of_slot[:, None] == jnp.arange(len(values), dtype=jnp.int32)[None, :]
    return jnp.sum(jnp.where(match, jnp.array(values, jnp.int32)[None, :], 0), axis=1)


def grad_tables():
    lefts, rights = [], []
    left_base = right_base = 0
    for members, beside in ((WIDE_IN, True), (TALL_OUT, False), (WIDE_FF, True), (TALL_FF, False)):
        for m in members:
            rows, cols = SHAPES[m]
            for r in range(0, rows, BS):
                for q in range(0, cols, BS):
                    lefts.append((left_base + r) // BS)
                    rights.append((right_base + q) // BS)
            if beside:
                right_base += cols
            else:
                left_base += rows
        if beside:
            left_base += rows
        else:
            right_base += cols
    return lefts, rights


def assemble(blocks, table):
    shapes = [(D, sum(SHAPES[m][1] for m in WIDE_IN)), (sum(SHAPES[m][0] for m in TALL_OUT), D), (D, 2 * FF), (FF, D)]
    hbm = pl.BlockSpec(memory_space=pl.ANY)
    return pl.pallas_call(
        assemble_kernel,
        out_shape=tuple(jax.ShapeDtypeStruct(shape, BF16) for shape in shapes),
        grid_spec=pltpu.PrefetchScalarGridSpec(
            num_scalar_prefetch=1, grid=(1,), in_specs=[hbm], out_specs=(hbm,) * 4,
            scratch_shapes=[
                pltpu.VMEM((DEPTH, BS, STEP_BLOCKS * BS), BF16),
                pltpu.VMEM((DEPTH, STEP_BLOCKS // (D // BS) * BS, D), BF16),
                pltpu.SemaphoreType.DMA((DEPTH,)), pltpu.SemaphoreType.DMA((DEPTH,)),
            ],
        ),
        compiler_params=kernel_params(),
        name="assemble",
    )(table, blocks)


SHAMPOO = 24


def shampoo_kernel(norm, total, master, left, right, left_root, right_root, grad, new_left, new_right, new_master, low):
    scale = 0.5 * norm * norm / BS
    for i in range(0, total.shape[0], 2):
        pair = (i, i + 1)
        rows = jnp.concatenate([total[k] for k in pair], axis=0)
        cols = jnp.concatenate([total[k] for k in pair], axis=1)
        outer = dot_nt(rows, rows) * scale
        inner = dot_tn(cols, cols) * scale
        moved = dot(rows, jnp.concatenate([right_root[k] for k in pair], axis=1).astype(BF16))
        moved = jnp.concatenate([moved[:BS, :BS], moved[BS:, BS:]], axis=1).astype(BF16)
        moved = dot(jnp.concatenate([left_root[k] for k in pair], axis=0).astype(BF16), moved) * (LR_MATRIX * norm)
        for k, at in zip(pair, (slice(0, BS), slice(BS, 2 * BS))):
            grad[k] = total[k].astype(F32) * norm
            new_left[k] = 0.5 * left[k] + outer[at, at]
            new_right[k] = 0.5 * right[k] + inner[at, at]
            fresh = master[k] - moved[at, at]
            new_master[k] = fresh
            low[k] = fresh.astype(BF16)


def shampoo(norm, total, master, left, right, left_root, right_root):
    slots = total.shape[0]
    each = math.gcd(slots, SHAMPOO)
    spec = pl.BlockSpec((each, BS, BS), lambda i: (i, 0, 0))
    full = jax.ShapeDtypeStruct(master.shape, F32)
    return pl.pallas_call(
        functools.partial(shampoo_kernel, norm),
        out_shape=(full, full, full, full, jax.ShapeDtypeStruct(master.shape, BF16)),
        grid=(slots // each,),
        in_specs=[spec] * 6,
        out_specs=(spec,) * 5,
        compiler_params=kernel_params(),
        name="shampoo",
    )(total, master, left, right, left_root, right_root)


BLOCK = 256
HALO = 8


def lane_index(shape):
    return lax.broadcasted_iota(jnp.int32, shape, len(shape) - 1)


def conv_tile(extended, taps, marks, count):
    total = jnp.broadcast_to(taps[KERNEL : KERNEL + 1, :], (count, extended.shape[1]))
    for tap in range(KERNEL):
        total = total + taps[tap : tap + 1, :] * near_rows(extended, tap, count) * marks[:, tap : tap + 1]
    return total


def near_rows(extended, tap, count):
    back = REACH - tap
    moved = pltpu.roll(extended, back, 0) if back else extended
    return moved[HALO : HALO + count, :]


def softplus(v):
    return jnp.maximum(v, 0.0) + jnp.log(1.0 + jnp.exp(-jnp.abs(v)))


def chunk_decays(raw, params):
    delta = softplus(raw + params[0:1, :])
    decay = -delta * jnp.exp(params[1:2, :])
    block = raw.shape[0] if raw.shape[0] < BLOCK else BLOCK
    rows = lax.broadcasted_iota(jnp.int32, (block, block), 0)
    lower = (rows >= lane_index((block, block))).astype(F32)
    sums = [dot(lower, decay[i : i + block, :], HIGHEST) for i in range(0, raw.shape[0], block)]
    return delta, decay, jnp.concatenate(sums, axis=0)


def end_weights(delta, sums, marks):
    last = sums[-1:, :]
    return jnp.exp(last - sums) * delta * marks[:, 5:6], jnp.exp(last) * marks[-1:, 4:5]


def spread_matrix():
    rows = lax.broadcasted_iota(jnp.int32, (LANES, INNER), 0)
    return (rows == lane_index((LANES, INNER)) // HEAD).astype(F32)


def mix_first_kernel(proj_x, proj_bc, halo, taps, params, raw, marks, xbc, decays, decays_t, state, factor):
    tokens = raw.shape[0]
    mark = marks[...]
    for ref, at in ((proj_x, 0), (proj_bc, INNER)):
        step = 256
        for q in range(0, ref.shape[1], step):
            cols = slice(at + q, at + q + step)
            own = ref[:, q : q + step].astype(F32)
            extended = jnp.concatenate([halo[:, cols].astype(F32), own], axis=0)
            value = conv_tile(extended, taps[:, cols], mark, tokens)
            xbc[:, cols] = (value * sigmoid(value)).astype(BF16)
    delta, decay, sums = chunk_decays(raw[...], params[...])
    decays[0] = delta
    decays[1] = sums
    for i in range(tokens // BLOCK):
        decays_t[i] = sums[i * BLOCK : (i + 1) * BLOCK].T
    spread = spread_matrix()
    total = jnp.zeros((NSTATE, INNER), F32)
    product = jnp.ones((1, LANES), F32)
    for i in range(0, tokens, BLOCK):
        rows = slice(i, i + BLOCK)
        weight, own = end_weights(delta[rows], sums[rows], mark[rows])
        weighted = (xbc[rows, :INNER].astype(F32) * dot(weight.astype(BF16), spread.astype(BF16))).astype(BF16)
        keep = dot(jnp.broadcast_to(own, (8, LANES)), spread, HIGHEST)[0:1]
        total = keep * total + dot_tn(xbc[rows, INNER : INNER + NSTATE], weighted)
        product = product * own
    state[...] = total.astype(BF16)
    factor[...] = jnp.broadcast_to(product, factor.shape)


def mix_first(proj, halo, taps, params, raw, marks):
    tokens = raw.shape[0]
    vmem = pl.BlockSpec(memory_space=pltpu.VMEM)
    return pl.pallas_call(
        mix_first_kernel,
        out_shape=(
            jax.ShapeDtypeStruct((tokens, CHANNELS), BF16),
            jax.ShapeDtypeStruct((2, tokens, LANES), F32),
            jax.ShapeDtypeStruct((tokens // BLOCK, LANES, BLOCK), F32),
            jax.ShapeDtypeStruct((NSTATE, INNER), BF16),
            jax.ShapeDtypeStruct((8, LANES), F32),
        ),
        grid=(1,),
        in_specs=[
            pl.BlockSpec((tokens, INNER), lambda i: (0, 1)),
            pl.BlockSpec((tokens, 2 * NSTATE), lambda i: (0, 2 * INNER // (2 * NSTATE))),
            vmem, vmem, vmem, vmem, vmem,
        ],
        out_specs=(vmem,) * 5,
        compiler_params=kernel_params(),
        name="mix_first",
    )(proj, proj, halo, taps, params, raw, marks)


def attend(left, right, mark_rows, mark_cols):
    return jnp.where(mark_rows & mark_cols, dot_nt(left, right), 0.0)


def halves(tile):
    low = lane_index(tile.shape) < HEAD
    zero = jnp.zeros_like(tile)
    return jnp.where(low, tile, zero), jnp.where(low, zero, tile)


def pair_column(values, a):
    return values[:, a * HEAD : a * HEAD + 1]


def mix_second_kernel(x, b, c, z, decays, decays_t, marks, labels, incoming, skip, gain, y, normed, states,
                      wide_sums, wide_delta, wide_end, keep, near, b_t, state, gated, squares):
    j = pl.program_id(0)
    tokens = x.shape[0]
    blocks = tokens // BLOCK
    cols = pl.ds(pl.multiple_of(j * LANES, LANES), LANES)

    @pl.when(j == 0)
    def _():
        spread = spread_matrix()
        rows = lax.broadcasted_iota(jnp.int32, (BLOCK, BLOCK), 0)
        ordered = rows >= lane_index((BLOCK, BLOCK))
        for i in range(blocks):
            at = slice(i * BLOCK, (i + 1) * BLOCK)
            mark = marks[at]
            same = mark[:, 6:7] == labels[0:1, at]
            near[i] = jnp.where(ordered & same, dot_nt(c[at], b[at]), 0.0)
            b_t[i] = b[at].T
            weight, own = end_weights(decays[0, at], decays[1, at], mark)
            wide_end[at] = dot(weight.astype(BF16), spread.astype(BF16)).astype(BF16)
            wide_sums[at] = dot(decays[1, at], spread, HIGHEST)
            wide_delta[at] = dot(decays[0, at].astype(BF16), spread.astype(BF16)).astype(BF16)
            keep[i] = dot(jnp.broadcast_to(own, (8, LANES)), spread, HIGHEST)
        squares[...] = jnp.zeros_like(squares)

    state[...] = incoming[...].astype(F32)
    for i in range(blocks):
        at = slice(i * BLOCK, (i + 1) * BLOCK)
        states[i] = state[...]
        tile = x[at].astype(F32)
        scaled = (tile * wide_delta[at, cols].astype(F32)).astype(BF16)
        sums = wide_sums[at, cols]
        total = jnp.zeros((BLOCK, LANES), F32)
        for a, part in enumerate(halves(scaled)):
            row = decays_t[i, pl.ds(2 * j + a, 1), :]
            weight = near[i] * jnp.exp(jnp.minimum(pair_column(sums, a) - row, 0.0))
            total = total + dot(weight.astype(BF16), part)
        carried = dot(c[at], state[...].astype(BF16))
        total = total + carried * jnp.exp(sums) * marks[at, 4:5] + skip[0:1, cols] * tile
        y[at] = total
        gate = z[at].astype(F32)
        gate = total * gate * sigmoid(gate)
        gated[at, cols] = gate
        squares[at] += gate * gate
        weighted = (tile * wide_end[at, cols].astype(F32)).astype(BF16)
        state[...] = keep[i, 0:1, cols] * state[...] + dot(b_t[i], weighted)
    states[blocks] = state[...]

    @pl.when(j == PAIRS - 1)
    def _():
        for i in range(blocks):
            at = slice(i * BLOCK, (i + 1) * BLOCK)
            scale = lax.rsqrt(jnp.sum(squares[at], axis=1, keepdims=True) / INNER + EPS)
            normed[at] = (gated[at] * scale * gain[0:1, :]).astype(BF16)


def mix_second(xbc, proj, decays, decays_t, marks, labels, incoming, skip, gain):
    tokens = xbc.shape[0]
    blocks = tokens // BLOCK
    tile = pl.BlockSpec((tokens, LANES), lambda j: (0, j))
    return pl.pallas_call(
        mix_second_kernel,
        out_shape=(
            jax.ShapeDtypeStruct((tokens, INNER), F32),
            jax.ShapeDtypeStruct((tokens, INNER), BF16),
            jax.ShapeDtypeStruct((blocks + 1, NSTATE, INNER), F32),
        ),
        grid=(PAIRS,),
        in_specs=[
            tile,
            pl.BlockSpec((tokens, NSTATE), lambda j: (0, INNER // NSTATE)),
            pl.BlockSpec((tokens, NSTATE), lambda j: (0, INNER // NSTATE + 1)),
            tile,
            whole(decays.shape), whole(decays_t.shape), whole(marks.shape), whole(labels.shape),
            pl.BlockSpec((NSTATE, LANES), lambda j: (0, j)),
            whole(skip.shape), whole(gain.shape),
        ],
        out_specs=(tile, whole((tokens, INNER)), pl.BlockSpec((blocks + 1, NSTATE, LANES), lambda j: (0, 0, j))),
        scratch_shapes=[
            pltpu.VMEM((tokens, INNER), F32), pltpu.VMEM((tokens, INNER), BF16), pltpu.VMEM((tokens, INNER), BF16),
            pltpu.VMEM((blocks, 8, INNER), F32), pltpu.VMEM((blocks, BLOCK, BLOCK), F32),
            pltpu.VMEM((blocks, NSTATE, BLOCK), BF16), pltpu.VMEM((NSTATE, LANES), F32),
            pltpu.VMEM((tokens, INNER), F32), pltpu.VMEM((tokens, LANES), F32),
        ],
        compiler_params=kernel_params(),
        name="mix_second",
    )(xbc, xbc, xbc, proj, decays, decays_t, marks, labels, incoming, skip, gain)


def gate_back_kernel(grad, y, z, gain, c, decays, marks, g_y, g_z, g_gain, g_state):
    step = pl.program_id(0)
    value, gate = y[...], z[...].astype(F32)
    opened = sigmoid(gate)
    swish = gate * opened
    gated = value * swish
    scale = lax.rsqrt(jnp.mean(gated * gated, axis=1, keepdims=True) + EPS)
    unit = gated * scale
    given = grad[...].astype(F32)
    scaled = given * gain[0:1, :]
    g_gated = scale * (scaled - unit * jnp.mean(scaled * unit, axis=1, keepdims=True))
    fresh = g_gated * swish
    g_y[...] = fresh.astype(BF16)
    g_z[...] = (g_gated * value * (opened + swish * (1.0 - opened))).astype(BF16)
    spread = spread_matrix()
    sums = decays[1]
    mark = marks[...]
    entry_weight = jnp.exp(sums) * mark[:, 4:5]
    own = jnp.exp(sums[-1:, :]) * mark[-1:, 4:5]
    keep = dot(jnp.broadcast_to(own, (8, LANES)), spread, HIGHEST)[0:1]
    weighted = (fresh * dot(entry_weight.astype(BF16), spread.astype(BF16))).astype(BF16)
    local = dot_tn(c[...], weighted)
    gains = jnp.broadcast_to(jnp.sum(given * unit, axis=0, keepdims=True), g_gain.shape)

    @pl.when(step == 0)
    def _():
        g_state[...] = local
        g_gain[...] = gains

    @pl.when(step > 0)
    def _():
        g_state[...] = keep * g_state[...] + local
        g_gain[...] += gains


def gate_back(grad, y, proj, gain, xbc, decays, marks):
    tokens = y.shape[0]
    blocks = tokens // BLOCK
    rows = lambda width, col: pl.BlockSpec((BLOCK, width), lambda i: (blocks - 1 - i, col))
    return pl.pallas_call(
        gate_back_kernel,
        out_shape=(
            jax.ShapeDtypeStruct((tokens, INNER), BF16),
            jax.ShapeDtypeStruct((tokens, INNER), BF16),
            jax.ShapeDtypeStruct((8, INNER), F32),
            jax.ShapeDtypeStruct((NSTATE, INNER), F32),
        ),
        grid=(blocks,),
        in_specs=[
            rows(INNER, 0), rows(INNER, 0), rows(INNER, 0), whole(gain.shape), rows(NSTATE, INNER // NSTATE + 1),
            pl.BlockSpec((2, BLOCK, LANES), lambda i: (0, blocks - 1 - i, 0)), rows(LANES, 0),
        ],
        out_specs=(rows(INNER, 0), rows(INNER, 0), whole((8, INNER)), whole((NSTATE, INNER))),
        compiler_params=kernel_params(),
        name="gate_back",
    )(grad, y, proj, gain, xbc, decays, marks)


def conv_back(grad, extended, taps, marks, count):
    acc = conv_tile(extended, taps, marks, count)
    opened = sigmoid(acc)
    g_acc = grad * (opened + acc * opened * (1.0 - opened))
    width = g_acc.shape[1]
    weights, result = [], jnp.zeros((HALO + count, width), F32)
    for tap in range(KERNEL):
        marked = g_acc * marks[:, tap : tap + 1]
        weights.append(jnp.sum(marked * near_rows(extended, tap, count), axis=0, keepdims=True))
        spread = jnp.concatenate([jnp.zeros((HALO, width), F32), marked * taps[tap : tap + 1, :]], axis=0)
        back = REACH - tap
        result = result + (pltpu.roll(spread, HALO + count - back, 0) if back else spread)
    weights.append(jnp.sum(g_acc, axis=0, keepdims=True))
    weights.append(jnp.zeros((8 - KERNEL - 1, width), F32))
    return result, jnp.concatenate(weights, axis=0)


def mix_back_kernel(x, b, c, proj_x, proj_bc, halo, taps, y, g_y, decays, decays_t, raw, params, marks, labels, states, leaving, skip,
                    g_conv, g_rim, g_taps, g_raw, g_params,
                    wide_sums, wide_delta, wide_end, wide_skip, keep, near, c_t, state, g_near, g_b, g_c, g_cum, g_delta, g_skip, ends):
    j = pl.program_id(0)
    tokens = x.shape[0]
    blocks = tokens // BLOCK
    cols = pl.ds(pl.multiple_of(j * LANES, LANES), LANES)
    lane = lane_index((LANES, LANES))
    gather = ((lax.broadcasted_iota(jnp.int32, (LANES, LANES), 0) // HEAD + 2 * j) == lane).astype(BF16)

    def collect(values):
        high = values.astype(BF16)
        return dot(high, gather) + dot((values - high.astype(F32)).astype(BF16), gather)

    @pl.when(j == 0)
    def _():
        spread = spread_matrix()
        rows = lax.broadcasted_iota(jnp.int32, (BLOCK, BLOCK), 0)
        ordered = rows <= lane_index((BLOCK, BLOCK))
        for i in range(blocks):
            at = slice(i * BLOCK, (i + 1) * BLOCK)
            mark = marks[at]
            same = mark[:, 6:7] == labels[0:1, at]
            near[i] = jnp.where(ordered & same, dot_nt(b[at], c[at]), 0.0)
            c_t[i] = c[at].T
            weight, own = end_weights(decays[0, at], decays[1, at], mark)
            end_only = jnp.exp(decays[1, at][-1:, :] - decays[1, at]) * mark[:, 5:6]
            wide_end[at] = dot(end_only.astype(BF16), spread.astype(BF16)).astype(BF16)
            wide_sums[at] = dot(decays[1, at], spread, HIGHEST)
            wide_delta[at] = dot(decays[0, at].astype(BF16), spread.astype(BF16)).astype(BF16)
            keep[i] = dot(jnp.broadcast_to(own, (8, LANES)), spread, HIGHEST)
        for ref in (g_near, g_b, g_c, g_cum, g_delta, g_skip, ends):
            ref[...] = jnp.zeros_like(ref)

    state[...] = leaving[...].astype(F32)
    g_x = []
    for i in range(blocks - 1, -1, -1):
        at = slice(i * BLOCK, (i + 1) * BLOCK)
        tile = x[at].astype(F32)
        step = wide_delta[at, cols].astype(F32)
        scaled = tile * step
        low_scaled = scaled.astype(BF16)
        sums = wide_sums[at, cols]
        end = wide_end[at, cols].astype(F32)
        given = g_y[at]
        low_state = state[...].astype(BF16)
        ends[i] += collect(jnp.broadcast_to(jnp.sum(states[i + 1] * state[...], axis=0, keepdims=True), (8, LANES)))
        total = end * dot(b[at], low_state)
        for a, (part, grad) in enumerate(zip(halves(low_scaled), halves(given))):
            row = decays_t[i, pl.ds(2 * j + a, 1), :]
            decay = jnp.exp(jnp.minimum(row - pair_column(sums, a), 0.0))
            total = total + dot((near[i] * decay).astype(BF16), grad)
            g_near[i] += decay * dot_nt(part, given)
        given = given.astype(F32)
        entry = jnp.exp(sums) * marks[at, 4:5]
        reached = (given * entry).astype(BF16)
        g_b[at] += dot_nt((scaled * end).astype(BF16), low_state)
        g_c[at] += dot_nt(reached, states[i].astype(BF16))
        own_skip = skip[0:1, cols]
        g_cum[at] += collect(given * (y[at] - own_skip * tile) - scaled * total)
        g_delta[at] += collect(total * tile)
        g_skip[...] += collect(jnp.broadcast_to(jnp.sum(given * tile, axis=0, keepdims=True), (8, LANES)))
        g_x.append(step * total + own_skip * given)
        state[...] = keep[i, 0:1, cols] * state[...] + dot(c_t[i], reached)

    mark = marks[...]
    own = proj_x[...].astype(F32)
    extended = jnp.concatenate([halo[:, cols].astype(F32), own], axis=0)
    result, weights = conv_back(jnp.concatenate(g_x[::-1], axis=0), extended, taps[:, cols], mark, tokens)
    g_rim[:HALO, cols] = result[:HALO]
    g_rim[HALO:, cols] = result[tokens:]
    g_conv[:, cols] = result[HALO:].astype(BF16)
    g_taps[:, cols] = weights

    @pl.when(j == PAIRS - 1)
    def _():
        for i in range(blocks):
            at = slice(i * BLOCK, (i + 1) * BLOCK)
            rows = lax.broadcasted_iota(jnp.int32, (BLOCK, BLOCK), 0)
            seen = (rows <= lane_index((BLOCK, BLOCK))) & (marks[at, 6:7] == labels[0:1, at])
            grad = jnp.where(seen, g_near[i], 0.0)
            g_b[at] += dot(grad.astype(BF16), c[at])
            g_c[at] += dot(grad.T.astype(BF16), b[at])
        for k, ref in enumerate((g_b, g_c)):
            at = slice(INNER + k * NSTATE, INNER + (k + 1) * NSTATE)
            own = proj_bc[:, k * NSTATE : (k + 1) * NSTATE].astype(F32)
            extended = jnp.concatenate([halo[:, at].astype(F32), own], axis=0)
            result, weights = conv_back(ref[...], extended, taps[:, at], mark, tokens)
            g_rim[:HALO, at] = result[:HALO]
            g_rim[HALO:, at] = result[tokens:]
            g_conv[:, at] = result[HALO:].astype(BF16)
            g_taps[:, at] = weights
        rate = -jnp.exp(params[1:2, :])
        bias_sum = jnp.zeros((1, LANES), F32)
        rate_sum = jnp.zeros((1, LANES), F32)
        rows = lax.broadcasted_iota(jnp.int32, (BLOCK, BLOCK), 0)
        upper = (rows <= lane_index((BLOCK, BLOCK))).astype(F32)
        for i in range(blocks):
            at = slice(i * BLOCK, (i + 1) * BLOCK)
            g_decay = dot(upper, g_cum[at], HIGHEST) + ends[i, 0:1, :]
            delta = decays[0, at]
            full = g_delta[at] + g_decay * rate
            full = full * sigmoid(raw[at] + params[0:1, :])
            g_raw[at] = full.astype(BF16)
            bias_sum = bias_sum + jnp.sum(full, axis=0, keepdims=True)
            rate_sum = rate_sum + jnp.sum(g_decay * delta * rate, axis=0, keepdims=True)
        g_params[...] = jnp.concatenate([bias_sum, rate_sum, g_skip[0:1, :], jnp.zeros((5, LANES), F32)], axis=0)


def mix_back(xbc, proj, halo, taps, y, g_y, decays, decays_t, raw, params, marks, labels, states, leaving, skip):
    tokens = xbc.shape[0]
    blocks = tokens // BLOCK
    tile = pl.BlockSpec((tokens, LANES), lambda j: (0, j))
    acc = lambda *shape: pltpu.VMEM(shape, F32)
    return pl.pallas_call(
        mix_back_kernel,
        out_shape=(
            jax.ShapeDtypeStruct((tokens, CHANNELS), BF16),
            jax.ShapeDtypeStruct((2 * HALO, CHANNELS), F32),
            jax.ShapeDtypeStruct((8, CHANNELS), F32),
            jax.ShapeDtypeStruct((tokens, LANES), BF16),
            jax.ShapeDtypeStruct((8, LANES), F32),
        ),
        grid=(PAIRS,),
        in_specs=[
            tile,
            pl.BlockSpec((tokens, NSTATE), lambda j: (0, INNER // NSTATE)),
            pl.BlockSpec((tokens, NSTATE), lambda j: (0, INNER // NSTATE + 1)),
            pl.BlockSpec((tokens, LANES), lambda j: (0, PAIRS + j)),
            pl.BlockSpec((tokens, 2 * NSTATE), lambda j: (0, 2 * INNER // (2 * NSTATE))),
            whole(halo.shape), whole(taps.shape), tile, tile,
            whole(decays.shape), whole(decays_t.shape), whole(raw.shape), whole(params.shape), whole(marks.shape), whole(labels.shape),
            pl.BlockSpec((blocks + 1, NSTATE, LANES), lambda j: (0, 0, j)),
            pl.BlockSpec((NSTATE, LANES), lambda j: (0, j)),
            whole(skip.shape),
        ],
        out_specs=(
            whole((tokens, CHANNELS)), whole((2 * HALO, CHANNELS)), whole((8, CHANNELS)), whole((tokens, LANES)), whole((8, LANES)),
        ),
        scratch_shapes=[
            acc(tokens, INNER), pltpu.VMEM((tokens, INNER), BF16), pltpu.VMEM((tokens, INNER), BF16), acc(8, LANES),
            acc(blocks, 8, INNER), acc(blocks, BLOCK, BLOCK), pltpu.VMEM((blocks, NSTATE, BLOCK), BF16), acc(NSTATE, LANES),
            acc(blocks, BLOCK, BLOCK), acc(tokens, NSTATE), acc(tokens, NSTATE), acc(tokens, LANES), acc(tokens, LANES),
            acc(8, LANES), acc(blocks, 8, LANES),
        ],
        compiler_params=kernel_params(),
        name="mix_back",
    )(xbc, xbc, xbc, proj, proj, halo, taps, y, g_y, decays, decays_t, raw, params, marks, labels, states, leaving, skip)


QBLOCK = 256
GROUPS = HEADS // KV_HEADS
QPAIRS = QDIM // LANES
SCALE = 1.0 / math.sqrt(HEAD)


def swap_halves(values):
    half = HEAD // 2
    front = lane_index(values.shape) % HEAD < half
    width = values.shape[-1]
    return jnp.where(front, pltpu.roll(values, width - half, 1), pltpu.roll(values, half, 1))


def turn(values, cosine, sine):
    return values * cosine + swap_halves(values) * sine


def rope_kernel(*refs):
    queries, (k, v, cosine, sine, q_out, kv_out) = refs[:QPAIRS], refs[QPAIRS:]
    cos, sin = cosine[...], sine[...]
    for p, q in enumerate(queries):
        q_out[:, p * LANES : (p + 1) * LANES] = turn(q[...].astype(F32), cos, sin).astype(BF16)
    kv_out[:, :KDIM] = turn(k[...].astype(F32), cos, sin).astype(BF16)
    kv_out[:, KDIM:] = v[...].astype(BF16)


def rope_all(proj, cosine, sine):
    tokens = proj.shape[0]
    start = 2 * INNER + 2 * NSTATE
    return pl.pallas_call(
        rope_kernel,
        out_shape=(jax.ShapeDtypeStruct((tokens, QDIM), BF16), jax.ShapeDtypeStruct((tokens, 2 * KDIM), BF16)),
        grid=(1,),
        in_specs=[
            pl.BlockSpec((tokens, LANES), lambda i, p=p: (0, start // LANES + p)) for p in range(QPAIRS + 2)
        ] + [whole(cosine.shape), whole(sine.shape)],
        out_specs=(whole((tokens, QDIM)), whole((tokens, 2 * KDIM))),
        compiler_params=kernel_params(),
        name="rope",
    )(*[proj] * (QPAIRS + 2), cosine, sine)


def both_sides(tile, both):
    low = lane_index(tile.shape) < HEAD
    zero = jnp.zeros_like(tile)
    moved = pltpu.roll(tile.astype(F32), HEAD, 1).astype(tile.dtype)
    both[0, 0] = jnp.where(low, tile, zero)
    both[0, 1] = jnp.where(low, zero, moved)
    both[1, 0] = jnp.where(low, moved, zero)
    both[1, 1] = jnp.where(low, zero, tile)


def attend_kernel(q, kv, key_labels, marks, context, stats, keys, values):
    block, pair = pl.program_id(0), pl.program_id(1)
    window = DOC_MOST + QBLOCK
    start = pl.multiple_of(block * QBLOCK, QBLOCK)

    @pl.when((block == 0) & (pair == 0))
    def _():
        both_sides(kv[:, :KDIM], keys)
        both_sides(kv[:, KDIM:], values)

    group = pair // (GROUPS // 2)
    rows = lax.broadcasted_iota(jnp.int32, (QBLOCK, window), 0)
    cols = lane_index((QBLOCK, window))
    seen = (cols <= rows + DOC_MOST) & (marks[:, 6:7] == key_labels[0, 0:1, :])
    total = jnp.zeros((QBLOCK, LANES), F32)
    found = jnp.zeros((QBLOCK, LANES), F32)
    for a in range(2):
        scores = dot_nt(q[...], keys[group, a, pl.ds(start, window), :]) * SCALE
        scores = jnp.where(seen, scores, NEG_BIG)
        most = jnp.max(scores, axis=1, keepdims=True)
        probs = jnp.exp(scores - most)
        mass = jnp.sum(probs, axis=1, keepdims=True)
        probs = probs * (1.0 / mass)
        total = total + dot(probs.astype(BF16), values[group, a, pl.ds(start, window), :])
        found = jnp.where(lane_index(found.shape) == a, most + jnp.log(mass), found)
    context[...] = total.astype(BF16)
    stats[0] = found.T[0:8, :]


def attend(q, kv, key_labels, marks):
    tokens = q.shape[0]
    blocks = tokens // QBLOCK
    tile = pl.BlockSpec((QBLOCK, LANES), lambda i, p: (i, p))
    return pl.pallas_call(
        attend_kernel,
        out_shape=(jax.ShapeDtypeStruct((tokens, QDIM), BF16), jax.ShapeDtypeStruct((QPAIRS, 8, tokens), F32)),
        grid=(blocks, QPAIRS),
        in_specs=[
            tile, whole(kv.shape), pl.BlockSpec((1,) + key_labels.shape[1:], lambda i, p: (i, 0, 0)),
            pl.BlockSpec((QBLOCK, LANES), lambda i, p: (i, 0)),
        ],
        out_specs=(tile, pl.BlockSpec((1, 8, QBLOCK), lambda i, p: (p, 0, i))),
        scratch_shapes=[pltpu.VMEM((2, 2) + (kv.shape[0], LANES), BF16)] * 2,
        compiler_params=kernel_params(),
        name="attend",
    )(q, kv, key_labels, marks)


def attend_back_kernel(q, kv, given, key_marks, query_labels, stats, cosine, sine, g_q, g_kv, keys, values, g_key, g_value):
    block, pair = pl.program_id(0), pl.program_id(1)
    window = DOC_MOST + QBLOCK
    start = pl.multiple_of(block * QBLOCK, QBLOCK)

    @pl.when((block == 0) & (pair == 0))
    def _():
        both_sides(kv[:, :KDIM], keys)
        both_sides(kv[:, KDIM:], values)
        g_key[...] = jnp.zeros_like(g_key)
        g_value[...] = jnp.zeros_like(g_value)

    group = pair // (GROUPS // 2)
    rows = lax.broadcasted_iota(jnp.int32, (window, QBLOCK), 0)
    cols = lane_index((window, QBLOCK))
    seen = (rows <= cols + DOC_MOST) & (key_marks[0, :, 0:1] == query_labels[0:1, :])
    at = pl.ds(start, window)
    query, grad = q[...], given[...]
    total = jnp.zeros((QBLOCK, LANES), F32)
    for a, (query_part, grad_part) in enumerate(zip(halves(query), halves(grad))):
        key = keys[group, a, at, :]
        scores = jnp.where(seen, dot_nt(key, query) * SCALE, NEG_BIG)
        probs = jnp.exp(scores - stats[0, a : a + 1, :])
        g_probs = dot_nt(values[group, a, at, :], grad)
        mean = jnp.sum(probs * g_probs, axis=0, keepdims=True)
        g_scores = (probs * (g_probs - mean)).astype(BF16)
        g_key[group, at] += dot(g_scores, query_part) * SCALE
        g_value[group, at] += dot(probs.astype(BF16), grad_part)
        total = total + dot_tn(g_scores, key)
    g_q[...] = turn(total * SCALE, cosine[...], -sine[...]).astype(BF16)

    @pl.when((block == pl.num_programs(0) - 1) & (pair == QPAIRS - 1))
    def _():
        for k, ref in enumerate((g_key, g_value)):
            first = ref[0] + pltpu.roll(ref[0], HEAD, 1)
            second = ref[1] + pltpu.roll(ref[1], HEAD, 1)
            g_kv[:, k * KDIM : (k + 1) * KDIM] = jnp.where(lane_index(first.shape) < HEAD, first, second).astype(BF16)


def attend_back(q, kv, given, key_marks, query_labels, stats, cosine, sine):
    tokens = q.shape[0]
    blocks = tokens // QBLOCK
    tile = pl.BlockSpec((QBLOCK, LANES), lambda i, p: (i, p))
    row = pl.BlockSpec((QBLOCK, LANES), lambda i, p: (i, 0))
    return pl.pallas_call(
        attend_back_kernel,
        out_shape=(jax.ShapeDtypeStruct((tokens, QDIM), BF16), jax.ShapeDtypeStruct(kv.shape, BF16)),
        grid=(blocks, QPAIRS),
        in_specs=[
            tile, whole(kv.shape), pl.BlockSpec((QBLOCK, LANES), lambda i, p: (i, PAIRS + p)),
            pl.BlockSpec((1,) + key_marks.shape[1:], lambda i, p: (i, 0, 0)),
            pl.BlockSpec((8, QBLOCK), lambda i, p: (0, i)),
            pl.BlockSpec((1, 8, QBLOCK), lambda i, p: (p, 0, i)), row, row,
        ],
        out_specs=(tile, whole(kv.shape)),
        scratch_shapes=[pltpu.VMEM((2, 2) + (kv.shape[0], LANES), BF16)] * 2 + [pltpu.VMEM((2, kv.shape[0], LANES), F32)] * 2,
        compiler_params=kernel_params(),
        name="attend_back",
    )(q, kv, given, key_marks, query_labels, stats, cosine, sine)


def turn_back_kernel(g_kv, cosine, sine, out):
    out[:, :KDIM] = turn(g_kv[:, :KDIM], cosine[...], -sine[...]).astype(BF16)
    out[:, KDIM:] = g_kv[:, KDIM:].astype(BF16)


def turn_back(g_kv, cosine, sine):
    return pl.pallas_call(
        turn_back_kernel, out_shape=jax.ShapeDtypeStruct(g_kv.shape, BF16), compiler_params=kernel_params(), name="turn_back",
    )(g_kv, cosine, sine)


def ungroup(rows, micro):
    seq = lax.axis_size("seq")
    each = seq // micro
    here = lax.axis_index("seq")
    order = here // each
    cut = rows.reshape((micro, rows.shape[0] // micro) + rows.shape[1:])
    pieces = []
    for t in range(micro):
        pairs = [(((j + t) % micro) * each + j // micro, j) for j in range(seq)]
        pieces.append(lax.ppermute(lax.dynamic_index_in_dim(cut, (order - t) % micro, 0, False), "seq", pairs))
    results = []
    for m in range(micro):
        chosen = pieces[0]
        for t in range(1, micro):
            chosen = jnp.where((m - here) % micro == t, pieces[t], chosen)
        results.append(chosen)
    return jnp.stack(results)


def along(value, steps, micro):
    seq = lax.axis_size("seq")
    each = seq // micro
    pairs = [(s, s + steps) for s in range(seq) if 0 <= s % each + steps < each]
    return lax.ppermute(value, "seq", pairs)


def pad_rows(*rows):
    width = rows[0].shape[-1]
    return jnp.concatenate([r.reshape(-1, width) for r in rows] + [jnp.zeros((8 - sum(r.size // width for r in rows), width), F32)], axis=0)


def shards(grid, tokens, cotangent, doc_ids, master_blocks, block_of_slot, left_stats, right_stats, left_roots, right_roots,
           vector_params, first_moment, second_moment, adam_step):
    micro, piece = tokens.shape[:2]
    seq = lax.axis_size("seq")
    each = seq // micro
    count = micro * piece
    here = lax.axis_index("seq")
    rank = here % each
    start = rank * count
    slots = master_blocks.shape[0]

    orders = all_orders()
    table = slots_in_order(block_of_slot, sum(orders, []))
    left_at, right_at = (values_of(block_of_slot, values) for values in grad_tables())
    gathered, rows, given, labels_all = gather_blocks(grid, master_blocks, tokens, cotangent, doc_ids)
    w_in, w_out, w_ff, w_down = assemble(gathered.reshape(-1, BS, BS), table)
    rows, given = rows.reshape(count, D), given.reshape(count, D)
    gain_in, gain_mid, gain_mix, conv_weight, conv_bias, dt_bias, a_log, skip, w_dt = unpack_vectors(vector_params)
    w_dt = jnp.pad(w_dt.reshape(D, HEADS_SSM), ((0, 0), (0, LANES - HEADS_SSM))).astype(BF16)
    taps = pad_rows(conv_weight.reshape(KERNEL, CHANNELS), conv_bias)
    lane_pad = lambda v: jnp.pad(v, (0, LANES - HEADS_SSM))
    params = pad_rows(lane_pad(dt_bias), lane_pad(a_log))
    wide_skip = pad_rows(jnp.repeat(skip, HEAD))
    wide_gain = pad_rows(gain_mix)

    row = lax.dynamic_index_in_dim(labels_all, here // each, 1, False).reshape(-1)
    before = jnp.concatenate([jnp.full((DOC_MOST,), -1, jnp.int32), row])
    window = lax.dynamic_slice_in_dim(before, start, DOC_MOST + count)
    labels = window[DOC_MOST:]
    blocks = count // BLOCK
    columns = [(window[DOC_MOST - REACH + tap : DOC_MOST - REACH + tap + count] == labels).astype(F32) for tap in range(KERNEL)]
    by_block = labels.reshape(blocks, BLOCK)
    entries_at = window[DOC_MOST - 1 : DOC_MOST - 1 + count].reshape(blocks, BLOCK)[:, :1]
    columns.append((by_block == entries_at).astype(F32).reshape(-1))
    columns.append((by_block == by_block[:, -1:]).astype(F32).reshape(-1))
    columns.append(labels.astype(F32))
    marks = jnp.pad(jnp.stack(columns, axis=1), ((0, 0), (0, LANES - len(columns))))
    label_rows = jnp.broadcast_to(labels.astype(F32)[None], (8, count))
    far = jnp.stack([window[i : i + DOC_MOST + QBLOCK] for i in range(0, count, QBLOCK)]).astype(F32)
    key_labels = jnp.broadcast_to(far[:, None, :], (far.shape[0], 8, far.shape[1]))
    key_marks = jnp.broadcast_to(far[:, :, None], far.shape + (8,))
    first = jnp.sum((row[None, :] < labels[:, None]).astype(jnp.int32), axis=1)
    positions = (start + jnp.arange(count) - first).astype(F32)
    half = HEAD // 2
    frequency = jnp.exp(jnp.arange(half, dtype=F32) * (-2.0 * math.log(THETA) / HEAD))
    angles = positions[:, None] * frequency[None, :]
    cos, sin = jnp.cos(angles), jnp.sin(angles)
    cosine = jnp.concatenate([cos] * 4, axis=1)
    sine = jnp.concatenate([-sin, sin] * 2, axis=1)

    inputs = rows.astype(F32)
    normed_in = (inputs * rms_scale(inputs) * gain_in).astype(BF16)
    proj = dot(normed_in, w_in).astype(BF16)
    raw = dot(normed_in, w_dt)
    halo = along(proj[count - HALO :, INNER : INNER + CHANNELS], 1, micro)
    q, kv = rope_all(proj, cosine, sine)
    xbc, decays, decays_t, state, factor = mix_first(proj, halo, taps, params, raw, marks)
    past = min(each - 1, -(-DOC_MOST // count))
    earlier = [along(kv, back, micro) for back in range(past, 0, -1)]
    if past * count < DOC_MOST:
        earlier.insert(0, jnp.zeros((DOC_MOST - past * count, kv.shape[1]), BF16))
    reach = jnp.concatenate(earlier + [kv], axis=0)[-(DOC_MOST + count) :]
    wide = lambda f: jnp.repeat(f[0, :HEADS_SSM], HEAD)[None]
    incoming = along(state, each - 1, micro).astype(F32) if each > 1 else jnp.zeros(state.shape, F32)
    for back in range(each - 2, 0, -1):
        incoming = along(state, back, micro).astype(F32) + wide(along(factor, back, micro)) * incoming
    y, normed_ssm, states = mix_second(xbc, proj, decays, decays_t, marks, label_rows, incoming, wide_skip, wide_gain)
    context, stats = attend(q, reach, key_labels, marks)
    hidden = inputs + (dot(normed_ssm, w_out[:INNER]) + dot(context, w_out[INNER:]))
    normed_mid = (hidden * rms_scale(hidden) * gain_mid).astype(BF16)
    both = dot(normed_mid, w_ff).astype(BF16)
    gate, upper = both[:, :FF].astype(F32), both[:, FF:].astype(F32)
    opened = sigmoid(gate)
    mixed = (gate * opened * upper).astype(BF16)
    layer_out = ungroup((hidden + dot(mixed, w_down)).astype(BF16), micro)

    g_mixed = dot_nt(given, w_down)
    g_gate = g_mixed * upper * (opened + gate * opened * (1.0 - opened))
    g_ff = jnp.concatenate([g_gate.astype(BF16), (g_mixed * gate * opened).astype(BF16)], axis=1)

    def norm_back(grad, values, gain):
        scale = rms_scale(values)
        unit = values * scale
        scaled = grad * gain
        return scale * (scaled - unit * jnp.mean(scaled * unit, axis=1, keepdims=True)), jnp.sum(grad * unit, axis=0)

    g_values, g_gain_mid = norm_back(dot_nt(g_ff, w_ff), hidden, gain_mid)
    g_hidden = given.astype(F32) + g_values
    hidden_low = g_hidden.astype(BF16)
    g_out = dot_nt(hidden_low, w_out).astype(BF16)
    g_y, g_z, g_gain_mix, g_state = gate_back(g_out, y, proj, wide_gain, xbc, decays, marks)
    low_state = g_state.astype(BF16)
    leaving = along(low_state, 1 - each, micro).astype(F32) if each > 1 else jnp.zeros(state.shape, F32)
    for ahead in range(each - 2, 0, -1):
        leaving = along(low_state, -ahead, micro).astype(F32) + wide(along(factor, -ahead, micro)) * leaving
    g_q, g_reach = attend_back(q, reach, g_out, key_marks, label_rows, stats, cosine, sine)
    g_conv, g_rim, g_taps, g_raw, g_params = mix_back(
        xbc, proj, halo, taps, y, g_y, decays, decays_t, raw, params, marks, label_rows, states, leaving, wide_skip
    )
    g_kv = g_reach[-count:].astype(F32)
    for back in range(1, past + 1):
        low = max(0, DOC_MOST - back * count)
        part = g_reach[low : DOC_MOST - (back - 1) * count]
        moved = along(part, -back, micro).astype(F32)
        g_kv = g_kv + jnp.pad(moved, ((count - part.shape[0], 0), (0, 0)))
    g_kv = turn_back(g_kv, cosine, sine)
    rim = along(g_rim[:HALO], -1, micro)
    g_conv = lax.dynamic_update_slice(g_conv, (g_rim[HALO:] + rim).astype(BF16), (count - HALO, 0))
    g_in = jnp.concatenate([g_z, g_conv, g_q, g_kv], axis=1)
    g_values, g_gain_in = norm_back(dot_nt(g_in, w_in) + dot_nt(g_raw, w_dt), inputs, gain_in)
    grad_tokens = ungroup((g_values + g_hidden).astype(BF16), micro).astype(F32)
    g_w_dt = dot_tn(normed_in, g_raw)

    parts = [g_gain_in, g_gain_mid, g_gain_mix[0], g_taps[:KERNEL].reshape(-1), g_taps[KERNEL]]
    parts += [g_params[i, :HEADS_SSM] for i in range(3)] + [g_w_dt[:, :HEADS_SSM].reshape(-1)]
    width = vector_params.shape[0]
    height = -(-width // (8 * LANES)) * 8
    vector = jnp.concatenate(parts + [jnp.zeros((height * LANES - width,), F32)]).reshape(height, LANES)
    total, vector = reduce_blocks(grid, slots, left_at, right_at, [normed_in, normed_ssm, context, normed_mid, mixed],
                                  [g_z, g_conv, g_q, g_kv, hidden_low, g_ff, given], vector)
    norm = 1.0 / math.sqrt(count * seq * lax.axis_size("dp"))
    updates = shampoo(norm, total, master_blocks, left_stats, right_stats, left_roots, right_roots)
    g_vector = vector.reshape(-1)[:width] * norm
    step = adam_step[0].astype(F32)
    new_first = BETA_ONE * first_moment + (1.0 - BETA_ONE) * g_vector
    new_second = BETA_TWO * second_moment + (1.0 - BETA_TWO) * g_vector * g_vector
    first_hat = new_first / (1.0 - jnp.power(BETA_ONE, step))
    second_hat = new_second / (1.0 - jnp.power(BETA_TWO, step))
    new_vector = vector_params - LR_VECTOR * first_hat / (jnp.sqrt(second_hat) + ADAM_EPS)
    return (layer_out, grad_tokens) + tuple(updates) + (g_vector, new_vector, new_first, new_second)


def solution(mesh):
    line, block, copied = P("dp", "seq", None), P("dp", None, None), P()
    return jax.shard_map(
        functools.partial(shards, grid_of(mesh)),
        mesh=mesh,
        in_specs=(line, line, P("dp", "seq"), block, copied, block, block, block, block, copied, copied, copied, copied),
        out_specs=(line, line) + (block,) * 5 + (copied,) * 4,
        check_vma=False,
    )
```

```python
import functools
import math

import jax
import jax.numpy as jnp
from jax import lax
from jax.experimental import pallas as pl
from jax.experimental.pallas import tpu as pltpu
from jax.sharding import PartitionSpec as P

D = 1024
HEADS_SSM = 24
HEAD = 64
NSTATE = 128
HEADS = 8
KV_HEADS = 2
FF = 2048
KERNEL = 4
BS = 128
DOC_MOST = 512
INNER = HEADS_SSM * HEAD
CHANNELS = INNER + 2 * NSTATE
REACH = KERNEL - 1
QDIM = HEADS * HEAD
KDIM = KV_HEADS * HEAD
LANES = 128
PAIRS = INNER // LANES

EPS = 1e-05
THETA = 100000000000.0
LR_MATRIX = 0.02
LR_VECTOR = 0.08
BETA_ONE = 0.9
BETA_TWO = 0.999
ADAM_EPS = 1e-08
NEG_BIG = -1e30
F32 = jnp.float32
BF16 = jnp.bfloat16
HIGHEST = lax.Precision.HIGHEST
VMEM_MOST = 60 << 20

SHAPES = (
    (D, INNER), (D, INNER), (D, 2 * NSTATE), (D, QDIM), (D, KDIM), (D, KDIM),
    (INNER, D), (QDIM, D), (D, FF), (D, FF), (FF, D),
)
WIDE_IN, TALL_OUT, WIDE_FF, TALL_FF = (0, 1, 2, 3, 4, 5), (6, 7), (8, 9), (10,)
SIZES = (D, D, INNER, KERNEL * CHANNELS, CHANNELS, HEADS_SSM, HEADS_SSM, HEADS_SSM, D * HEADS_SSM)


def block_offsets():
    starts, total = [], 0
    for rows, cols in SHAPES:
        starts.append(total)
        total += rows // BS * (cols // BS)
    return starts


def wide_order(members):
    starts = block_offsets()
    rows = SHAPES[members[0]][0] // BS
    return [starts[m] + r * (SHAPES[m][1] // BS) + q for r in range(rows) for m in members for q in range(SHAPES[m][1] // BS)]


def tall_order(members):
    starts = block_offsets()
    return [starts[m] + i for m in members for i in range(SHAPES[m][0] // BS * (SHAPES[m][1] // BS))]


def all_orders():
    return [wide_order(WIDE_IN), tall_order(TALL_OUT), wide_order(WIDE_FF), tall_order(TALL_FF)]


def unpack_vectors(flat):
    result, offset = [], 0
    for count in SIZES:
        result.append(flat[offset : offset + count])
        offset += count
    return result


def dot(left, right, precision=None):
    return jnp.dot(left, right, preferred_element_type=F32, precision=precision)


def dot_nt(left, right):
    return lax.dot_general(left, right, (((1,), (1,)), ((), ())), preferred_element_type=F32)


def dot_tn(left, right):
    return lax.dot_general(left, right, (((0,), (0,)), ((), ())), preferred_element_type=F32)


def sigmoid(v):
    return 1.0 / (1.0 + jnp.exp(-v))


def rms_scale(values):
    return lax.rsqrt(jnp.mean(values * values, axis=-1, keepdims=True) + EPS)


def kernel_params(**more):
    return pltpu.CompilerParams(vmem_limit_bytes=VMEM_MOST, **more)


def whole(shape):
    return pl.BlockSpec(shape, lambda *_: (0,) * len(shape))


MESH = pl.DeviceIdType.MESH
CORES = 2
PIECES = 3
APART = 5 / 16


def grid_of(mesh):
    try:
        wide = len({device.coords[0] for device in mesh.devices.flat})
    except AttributeError:
        wide = mesh.shape["seq"] // CORES
    return wide, mesh.shape["seq"] // CORES, mesh.shape["dp"] // wide


def parts_of(slots, tall):
    half = slots // CORES
    size = half // PIECES
    lone = round(size * APART) if tall == 2 and size >= 8 else 0
    return half, size, lone, size - lone


def place(grid):
    wide, tall, deep = grid
    dp, seq = lax.axis_index("dp"), lax.axis_index("seq")
    return dp % wide, seq // CORES, dp // wide, seq % CORES


def gather_kernel(grid, slots, master, tokens, cotangent, docs, out, rows, given, labels, wide_own, src, bounce,
                  sem_own, sem_load, sz, rz, sx, rx, sy, ry, sc, rc, s_rows, r_rows, s_docs, r_docs):
    wide, tall, deep = grid
    x, y, z, c = place(grid)
    half, size, lone, bulk = parts_of(slots, tall)
    me = z * wide + x
    seq = y * CORES + c
    base = c * half
    bulk_at = y * (size - bulk)
    lone_at = y * bulk
    other_at = (1 - y) * bulk if lone else 0
    mate = y * CORES + (1 - c)
    over = (tall - 1 - y) * CORES + c
    peers = tall * CORES
    micro = tokens.shape[0]
    each = peers // micro

    loads = []
    for k in range(CORES):
        part = pl.ds(((c + k) % CORES) * half, half)
        loads.append((part, pltpu.make_async_copy(master.at[part], wide_own.at[part], sem_load.at[k])))
        loads[-1][1].start()

    barrier = pltpu.get_barrier_semaphore()
    count = jnp.int32(0)
    for step_by, at, length in ((wide, z, deep), (1, x, wide)):
        for step in (1, -1):
            ok = (at + step >= 0) & (at + step < length)
            there = me + step * step_by

            @pl.when(ok)
            def _(there=there):
                pl.semaphore_signal(barrier, inc=1, device_id=(there, seq), device_id_type=MESH)

            count = count + ok.astype(jnp.int32)
    for k in range(1, peers):
        pl.semaphore_signal(barrier, inc=1, device_id=(me, (seq + k) % peers), device_id_type=MESH)
    pl.semaphore_wait(barrier, count + (peers - 1))
    both = ((0, 1), (1, -1))
    yes = jnp.bool_(True)

    def piece(shard, at, length):
        return out.at[shard, pl.ds(at, length)]

    def run(begin_it):
        def send(ok, source, target, send_sem, recv_sem, device):
            copy = pltpu.make_async_remote_copy(
                src_ref=source, dst_ref=target, send_sem=send_sem, recv_sem=recv_sem,
                device_id=device, device_id_type=MESH,
            )

            @pl.when(ok)
            def _():
                if begin_it:
                    copy.start()
                else:
                    copy.wait_send()

        def arrived(ok, target, recv_sem):
            if begin_it:
                copy = pltpu.make_async_remote_copy(
                    src_ref=target, dst_ref=target, send_sem=sem_own.at[0], recv_sem=recv_sem,
                    device_id=(me, seq), device_id_type=MESH,
                )

                @pl.when(ok)
                def _():
                    copy.wait_recv()

        def pass_on(ok, shard, sub):
            at = base + sub * size
            mine = piece(shard, at + bulk_at, bulk)
            send(ok, mine, mine, sc.at[0, shard, sub], rc.at[0, shard, sub], (me, mate))
            if lone:
                mine = piece(shard, at + lone_at, lone)
                send(ok, mine, mine, sy.at[shard, sub], ry.at[shard, sub], (me, over))

        def along_x(ok, zs, dirs, hop, sub, own):
            for d, step in dirs:
                shard = zs * wide + x - step * hop
                go = ok & (x + step >= 0) & (x + step < wide)
                at = base + sub * size + bulk_at
                source = src.at[pl.ds(at, bulk)] if own else piece(shard, at, bulk)
                send(go, source, piece(shard, at, bulk), sx.at[d, hop, zs, sub], rx.at[d, hop + 1, zs, sub], (me + step, seq))

        def columns(s):
            return [(yes, z)] if s == 0 else [((z - step * s >= 0) & (z - step * s < deep), z - step * s) for _, step in both]

        def x_in(s, hop, sub):
            for ok, zs in columns(s):
                for d, step in both:
                    from_x = x - step * hop
                    come = ok & (from_x >= 0) & (from_x < wide)
                    shard = zs * wide + from_x
                    arrived(come, piece(shard, base + sub * size + bulk_at, bulk), rx.at[d, hop, zs, sub])
                    along_x(come, zs, ((d, step),), hop, sub, False)
                    pass_on(come, shard, sub)

        def y_in(ok, shard, sub):
            if lone:
                mine = piece(shard, base + sub * size + other_at, lone)
                arrived(ok, mine, ry.at[shard, sub])
                send(ok, mine, mine, sc.at[1, shard, sub], rc.at[1, shard, sub], (me, mate))

        def y_all(s, sub):
            for ok, zs in columns(s):
                if s > 0:
                    y_in(ok, zs * wide + x, sub)
                for hop in range(1, wide):
                    for _, step in both:
                        from_x = x - step * hop
                        y_in(ok & (from_x >= 0) & (from_x < wide), zs * wide + from_x, sub)

        def z_step(s, sub):
            for d, step in both:
                zs = z - step * s
                ok = (zs >= 0) & (zs < deep)
                shard = zs * wide + x
                at = base + sub * size + bulk_at
                mine = piece(shard, at, bulk)
                if s:
                    arrived(ok, mine, rz.at[d, s, sub])
                go = ok & (z + step >= 0) & (z + step < deep)
                source = mine if s else src.at[pl.ds(at, bulk)]
                if s + 1 < deep:
                    send(go, source, mine, sz.at[d, s, sub], rz.at[d, s + 1, sub], (me + step * wide, seq))
                if s:
                    along_x(ok, zs, both, 0, sub, False)
                    pass_on(ok, shard, sub)
            if s == 0:
                along_x(yes, z, both, 0, sub, True)

        for s in range(deep):
            def one(sub, _, s=s):
                z_step(s, sub)
                if s:
                    for hop in range(1, wide):
                        x_in(s - 1, hop, sub)
                if s >= 2:
                    y_all(s - 2, sub)
                return 0

            lax.fori_loop(0, PIECES, one, 0)
            if s == 0:
                local(begin_it, send, arrived)

        def last_x(sub, _):
            for hop in range(1, wide):
                x_in(deep - 1, hop, sub)
            if deep > 1:
                y_all(deep - 2, sub)
            return 0

        def last_y(sub, _):
            y_all(deep - 1, sub)
            return 0

        lax.fori_loop(0, PIECES, last_x, 0)
        lax.fori_loop(0, PIECES, last_y, 0)

    def convert(k):
        part, copy = loads[k]
        copy.wait()
        base_at = ((c + k) % CORES) * half

        def one(i, _):
            src[base_at + i] = wide_own[base_at + i].astype(src.dtype)
            return 0

        lax.fori_loop(0, half, one, 0, unroll=2)

    keep = pltpu.make_async_copy(src, out.at[me], sem_load.at[0])
    at_home = []
    for t in range(micro):
        m = (seq + t) % micro
        there = m * each + seq // micro
        for k, (source, target) in enumerate(((tokens, rows), (cotangent, given))):
            place_to = target.at[seq % micro]
            take = pltpu.make_async_copy(source.at[m], bounce.at[k], sem_own.at[k])
            put = pltpu.make_async_copy(bounce.at[k], place_to, sem_own.at[k])
            at_home.append((there == seq, take, put))

    def local(begin_it, send, arrived):
        for t in range(micro):
            m = (seq + t) % micro
            there = m * each + seq // micro
            for k, (source, target) in enumerate(((tokens, rows), (cotangent, given))):
                send(there != seq, source.at[m], target.at[seq % micro], s_rows.at[k, t], r_rows.at[k, seq % micro], (me, there))
        if begin_it:
            labels[seq] = docs[...]
        for k in range(1, peers):
            send(yes, docs, labels.at[seq], s_docs.at[k], r_docs.at[seq], (me, (seq + k) % peers))
        if begin_it:
            for ok, take, _ in at_home:
                @pl.when(ok)
                def _(take=take):
                    take.start()
            convert(1)
            keep.start()
            for ok, take, put in at_home:
                @pl.when(ok)
                def _(take=take, put=put):
                    take.wait()
                    put.start()

    convert(0)
    run(True)
    keep.wait()
    for ok, take, put in at_home:
        @pl.when(ok)
        def _(put=put):
            put.wait()

    def came(ok, target, recv_sem):
        @pl.when(ok)
        def _():
            pltpu.make_async_remote_copy(
                src_ref=target, dst_ref=target, send_sem=sem_own.at[0], recv_sem=recv_sem,
                device_id=(me, seq), device_id_type=MESH,
            ).wait_recv()

    for q in range(micro):
        source = seq % each * micro + q
        for k, target in enumerate((rows, given)):
            came(source != seq, target.at[q], r_rows.at[k, q])
    for k in range(1, peers):
        source = (seq + k) % peers
        came(yes, labels.at[source], r_docs.at[source])

    def last(i, _):
        shard, sub = i // PIECES, i % PIECES
        at = (1 - c) * half + sub * size
        came(shard != me, piece(shard, at + bulk_at, bulk), rc.at[0, shard, sub])
        if lone:
            came(shard != me, piece(shard, at + other_at, lone), rc.at[1, shard, sub])
        return 0

    lax.fori_loop(0, wide * deep * PIECES, last, 0)
    run(False)


def gather_blocks(grid, master, tokens, cotangent, docs):
    wide, tall, deep = grid
    slots = master.shape[0]
    n = wide * deep
    peers = tall * CORES
    micro = tokens.shape[0]
    low = tokens.dtype
    sem = pltpu.SemaphoreType.DMA
    hbm = pl.BlockSpec(memory_space=pl.ANY)
    vmem = pl.BlockSpec(memory_space=pltpu.VMEM)
    return pl.pallas_call(
        functools.partial(gather_kernel, grid, slots),
        out_shape=(
            jax.ShapeDtypeStruct((n,) + master.shape, low),
            jax.ShapeDtypeStruct(tokens.shape, low), jax.ShapeDtypeStruct(tokens.shape, low),
            jax.ShapeDtypeStruct((peers,) + docs.shape, docs.dtype),
        ),
        in_specs=[hbm, hbm, hbm, vmem],
        out_specs=(hbm, hbm, hbm, vmem),
        scratch_shapes=[
            pltpu.VMEM(master.shape, master.dtype), pltpu.VMEM(master.shape, low), pltpu.VMEM((2,) + tokens.shape[1:], low),
            sem((2,)), sem((CORES,)),
            sem((2, deep, PIECES)), sem((2, deep + 1, PIECES)),
            sem((2, wide, deep, PIECES)), sem((2, wide + 1, deep, PIECES)),
            sem((n, PIECES)), sem((n, PIECES)),
            sem((2, n, PIECES)), sem((2, n, PIECES)),
            sem((2, micro)), sem((2, micro)), sem((peers,)), sem((peers,)),
        ],
        compiler_params=pltpu.CompilerParams(collective_id=0, has_side_effects=True, vmem_limit_bytes=60 << 20),
        name="gather_blocks",
    )(master, tokens, cotangent, docs)

def far_first(at, size, i):
    above, below = size - 1 - at, at
    less, more = jnp.minimum(above, below), jnp.maximum(above, below)
    long_side = jnp.where(above >= below, 1, -1)
    j = i - (more - less)
    near = at + jnp.where(j % 2 == 0, 1, -1) * (less - j // 2)
    return jnp.where(j < 0, at + long_side * (more - i), near)


def entry(at, size, source_below, target):
    lower = jnp.where(at > 0, size - at, 0) if size > 2 else 0
    return target - at if source_below else lower + at - target


def entries(size):
    return size + 1 if size > 2 else 1

SUBS = 3
LONE = 5 / 16
RING = 6
STAGED = 3
LATE_ADD, LATE_X, LATE_Z, PER_HOP = 1, 3, 6, 3
CHUNK = 512
HELD = 12


def split_of(slots, tall):
    half = slots // CORES
    piece = half // SUBS
    lone = round(piece * LONE) if tall == 2 and piece >= 8 else 0
    return half, piece, lone, piece - lone


def reduce_kernel(grid, slots, widths, left_at, right_at, vec, *refs):
    wide, tall, deep = grid
    count = sum(len(w) for w in widths)
    arrays = refs[:count]
    (out, vec_out, turned, right, held, acc, stage, land_c, land_y, land_x, land_z, fin, vbuf, vland,
     s_left, s_right, s_c, r_c, s_y, r_y, s_x, r_x, s_z, r_z, s_f, r_f, s_m, r_m, s_v, r_v, free) = refs[count:]
    n = wide * deep
    x, y, z, c = place(grid)
    half, size, lone, bulk = split_of(slots, tall)
    me = z * wide + x
    seq = y * CORES + c
    mate = y * CORES + (1 - c)
    bulk_at = y * lone
    lone_at = y * bulk
    other_at = (1 - y) * bulk
    bits = lambda length: [1 << b for b in range(length.bit_length() - 1)]
    partners = [(me, mate)]
    partners += [(me, (y ^ b) * CORES + c) for b in bits(tall)]
    partners += [(z * wide + (x ^ b), seq) for b in bits(wide)]
    partners += [((z ^ b) * wide + x, seq) for b in bits(deep)]
    rounds = len(partners)

    chunks, k, at = [], 0, 0
    for width in widths[0]:
        for q in range(0, width, CHUNK):
            chunks.append((k, q, at + q))
        k, at = k + 1, at + width

    def chunk_copy(i):
        k, q, _ = chunks[i]
        return pltpu.make_async_copy(arrays[k].at[:, pl.ds(q, CHUNK)], held.at[i % HELD], s_left.at[i % HELD])

    ahead = min(HELD, len(chunks))
    for i in range(ahead):
        chunk_copy(i).start()
    copies, at = [], 0
    for width in widths[1]:
        def one(q, _, k=k, at=at):
            cols = pl.ds(pl.multiple_of(q * BS, BS), BS)
            pltpu.make_async_copy(arrays[k].at[:, cols], right.at[at + q], s_right.at[k - len(widths[0])]).start()
            return 0

        lax.fori_loop(0, width // BS, one, 0)
        part = right.at[pl.ds(at, width // BS)]
        copies.append(pltpu.make_async_copy(part, part, s_right.at[k - len(widths[0])]))
        k, at = k + 1, at + width // BS

    barrier = pltpu.get_barrier_semaphore()
    awaited = jnp.int32(0)
    for step_by, at, length in ((wide, z, deep), (1, x, wide)):
        for step in (1, -1):
            ok = (at + step >= 0) & (at + step < length)

            @pl.when(ok)
            def _(there=me + step * step_by):
                pl.semaphore_signal(barrier, inc=1, device_id=(there, seq), device_id_type=MESH)

            awaited = awaited + ok.astype(jnp.int32)
    for device in partners:
        pl.semaphore_signal(barrier, inc=1, device_id=device, device_id_type=MESH)
    pl.semaphore_wait(barrier, awaited + rounds)

    def remote(source, target, send_sem, recv_sem, device):
        return pltpu.make_async_remote_copy(
            src_ref=source, dst_ref=target, send_sem=send_sem, recv_sem=recv_sem,
            device_id=device, device_id_type=MESH,
        )

    def landed(target, recv_sem):
        remote(target, target, s_left.at[0], recv_sem, (me, seq)).wait_recv()

    def vec_copy(t):
        return remote(vbuf.at[t], vland.at[t], s_v.at[t], r_v.at[t], partners[t])

    vbuf[0] = vec[...]
    vec_copy(0).start()
    for i in range(len(chunks)):
        chunk_copy(i).wait()
        for q in range(0, CHUNK, BS):
            turned[(chunks[i][2] + q) // BS] = held[i % HELD, :, q : q + BS].T
        if i + HELD < len(chunks):
            chunk_copy(i + HELD).start()
    for copy in copies:
        copy.wait()

    group = wide * SUBS
    total = n * SUBS

    def item_of(k):
        xs = far_first(x, wide, k % wide)
        zs = far_first(z, deep, k // group)
        sub = (k // wide) % SUBS
        return xs, zs, sub, (zs * wide + xs) * SUBS + sub

    def swap(k):
        return remote(stage.at[k % STAGED], land_c.at[k % RING], s_c.at[k % STAGED], r_c.at[k % RING], (me, mate))

    def cross(item):
        return remote(acc.at[item, pl.ds(other_at, lone)], land_y.at[item], s_y.at[item], r_y.at[item], (me, (tall - 1 - y) * CORES + c))

    def grads(k, core, ref, first):
        xs, zs, sub, item = item_of(k)
        base = (zs * wide + xs) * slots + core * half + sub * size

        def one(i, _):
            ref[first, i] = dot(turned[left_at[base + i]], right[right_at[base + i]]).astype(ref.dtype)
            return 0

        lax.fori_loop(0, size, one, 0, unroll=min(4, size))

    def add(item, at, length, ref, first):
        def one(i, _):
            acc[item, at + i] = acc[item, at + i] + ref[first + (i,)]
            return 0

        lax.fori_loop(0, length, one, 0, unroll=min(3, length))

    def step_x(k, begin_it):
        xs, zs, sub, item = item_of(k)
        for below, step in ((True, 1), (False, -1)):
            to = entry(x + step, wide, below, xs)
            sent = remote(acc.at[item, pl.ds(bulk_at, bulk)], land_x.at[to, zs * SUBS + sub], s_x.at[item],
                          r_x.at[to, zs * SUBS + sub], (me + step, seq))

            @pl.when((xs - x) * step > 0)
            def _():
                if begin_it:
                    sent.start()
                else:
                    sent.wait_send()

    def take_x(k):
        xs, zs, sub, item = item_of(k)
        for below, step in ((True, 1), (False, -1)):
            comes = ((xs - x) * step >= 0) & (x - step >= 0) & (x - step < wide)
            at = entry(x, wide, below, xs)

            @pl.when(comes)
            def _():
                landed(land_x.at[at, zs * SUBS + sub], r_x.at[at, zs * SUBS + sub])
                add(item, bulk_at, bulk, land_x, (at, zs * SUBS + sub))

    def step_z(k, begin_it):
        xs, zs, sub, item = item_of(k)
        for below, step in ((True, 1), (False, -1)):
            to = entry(z + step, deep, below, zs)
            sent = remote(acc.at[item, pl.ds(bulk_at, bulk)], land_z.at[to, sub], s_z.at[zs * SUBS + sub], r_z.at[to, sub],
                          (me + step * wide, seq))

            @pl.when((zs - z) * step > 0)
            def _():
                if begin_it:
                    sent.start()
                else:
                    sent.wait_send()

    def take_z(k):
        xs, zs, sub, item = item_of(k)
        for below, step in ((True, 1), (False, -1)):
            comes = ((zs - z) * step >= 0) & (z - step >= 0) & (z - step < deep)
            at = entry(z, deep, below, zs)

            @pl.when(comes)
            def _():
                landed(land_z.at[at, sub], r_z.at[at, sub])
                add(item, bulk_at, bulk, land_z, (at, sub))

    planes = bits(tall)

    def swap_plane(t, sub):
        mine = pl.ds(bulk_at, bulk)
        return remote(acc.at[me * SUBS + sub, mine], fin.at[t, sub, mine], s_f.at[t, sub], r_f.at[t, sub], (me, (y ^ planes[t]) * CORES + c))

    def take_plane(t, sub):
        item = me * SUBS + sub
        theirs = pl.ds((1 - y) * lone if lone else 0, bulk)
        landed(fin.at[t, sub, theirs], r_f.at[t, sub])
        swap_plane(t, sub).wait_send()
        add(item, lone, size - 2 * lone, fin.at[t, sub, pl.ds(lone, size - 2 * lone)], ())
        if lone:
            cross(item).wait_send()
            acc[item, pl.ds(other_at, lone)] = fin[t, sub, pl.ds(other_at, lone)]

    def swap_core(sub):
        return remote(acc.at[me * SUBS + sub], out.at[pl.ds(c * half + sub * size, size)], s_m.at[sub], r_m.at[sub], (me, mate))

    late_z = LATE_Z + PER_HOP * jnp.minimum(z, deep - 1 - z)

    def turn_of(k, _):
        @pl.when(k < total)
        def _():
            @pl.when(k >= STAGED)
            def _():
                swap(k - STAGED).wait_send()

            grads(k, 1 - c, stage, k % STAGED)

            @pl.when(k >= RING)
            def _():
                pl.semaphore_wait(free, 1)

            swap(k).start()
            grads(k, c, acc, item_of(k)[3])

        for t in range(1, rounds + 1):
            @pl.when(k == t)
            def _(t=t):
                landed(vland.at[t - 1], r_v.at[t - 1])
                vbuf[t] = vbuf[t - 1] + vland[t - 1]
                if t < rounds:
                    vec_copy(t).start()
                else:
                    vec_out[...] = vbuf[t]

        b = k - LATE_ADD

        @pl.when((b >= 0) & (b < total))
        def _():
            item = item_of(b)[3]
            landed(land_c.at[b % RING], r_c.at[b % RING])
            add(item, 0, size, land_c, (b % RING,))

            @pl.when(b < total - RING)
            def _():
                pl.semaphore_signal(free, inc=1, device_id=(me, mate), device_id_type=MESH)

            if lone:
                cross(item).start()

        b = k - LATE_X

        @pl.when((b >= 0) & (b < total))
        def _():
            item = item_of(b)[3]
            if lone:
                landed(land_y.at[item], r_y.at[item])
                add(item, lone_at, lone, land_y, (item,))
            if wide > 2:
                @pl.when(item_of(b)[0] != x)
                def _():
                    take_x(b)
            step_x(b, True)

        b = k - late_z

        @pl.when((b >= 0) & (b < total) & (b % wide == wide - 1))
        def _():
            take_x(b)
            take_z(b)
            step_z(b, True)
            if planes:
                @pl.when(item_of(b)[1] == z)
                def _():
                    swap_plane(0, item_of(b)[2]).start()

        return 0

    lax.fori_loop(0, total + LATE_Z + PER_HOP * ((deep - 1) // 2), turn_of, 0)

    def finish(k, _):
        if lone:
            item = item_of(k)[3]

            @pl.when(item // SUBS != me)
            def _():
                cross(item).wait_send()

        step_x(k, False)

        @pl.when(k % wide == wide - 1)
        def _():
            step_z(k, False)

        return 0

    for t in range(len(planes)):
        for sub in range(SUBS):
            if t:
                swap_plane(t, sub).start()
        for sub in range(SUBS):
            take_plane(t, sub)
            if t == len(planes) - 1:
                swap_core(sub).start()
                out[pl.ds(c * half + sub * size, size)] = acc[me * SUBS + sub]
    lax.fori_loop(0, total, finish, 0)
    for k in range(max(total - STAGED, 0), total):
        swap(k).wait_send()
    for t in range(rounds):
        vec_copy(t).wait_send()
    for sub in range(SUBS):
        swap_core(sub).wait_send()
        landed(out.at[pl.ds((1 - c) * half + sub * size, size)], r_m.at[sub])


def reduce_blocks(grid, slots, left_at, right_at, lefts, rights, vec):
    wide, tall, deep = grid
    n = wide * deep
    half, size, lone, bulk = split_of(slots, tall)
    tile = (BS, BS)
    low = lefts[0].dtype
    tokens = lefts[0].shape[0]
    widths = [[a.shape[1] for a in lefts], [a.shape[1] for a in rights]]
    sem = pltpu.SemaphoreType.DMA
    rounds = sum(length.bit_length() - 1 for length in (CORES, wide, tall, deep))
    planes = max(tall.bit_length() - 1, 1)
    items = n * SUBS
    buf = lambda *lead: pltpu.VMEM(lead + tile, low)
    smem, vmem, hbm = (pl.BlockSpec(memory_space=m) for m in (pltpu.SMEM, pltpu.VMEM, pl.ANY))
    return pl.pallas_call(
        functools.partial(reduce_kernel, grid, slots, widths),
        out_shape=(jax.ShapeDtypeStruct((slots,) + tile, low), jax.ShapeDtypeStruct(vec.shape, vec.dtype)),
        in_specs=[smem, smem, vmem] + [hbm] * (len(lefts) + len(rights)),
        out_specs=(vmem, vmem),
        scratch_shapes=[
            pltpu.VMEM((sum(widths[0]) // BS, BS, tokens), low), pltpu.VMEM((sum(widths[1]) // BS, tokens, BS), low), pltpu.VMEM((HELD, tokens, CHUNK), low),
            buf(items, size), buf(STAGED, size), buf(RING, size), buf(items, max(lone, 1)), buf(entries(wide), deep * SUBS, bulk),
            buf(entries(deep), SUBS, bulk), buf(planes, SUBS, size),
            pltpu.VMEM((rounds + 1,) + vec.shape, vec.dtype), pltpu.VMEM((rounds,) + vec.shape, vec.dtype),
            sem((HELD,)), sem((len(rights),)), sem((STAGED,)), sem((RING,)), sem((items,)), sem((items,)), sem((items,)),
            sem((entries(wide), deep * SUBS)), sem((deep * SUBS,)), sem((entries(deep), SUBS)),
            sem((planes, SUBS)), sem((planes, SUBS)), sem((SUBS,)), sem((SUBS,)), sem((rounds,)), sem((rounds,)),
            pltpu.SemaphoreType.REGULAR,
        ],
        compiler_params=pltpu.CompilerParams(collective_id=1, has_side_effects=True, vmem_limit_bytes=63 << 20),
        name="reduce_blocks",
    )(left_at, right_at, vec, *lefts, *rights)


BLOCK = 256
HALO = 8


def lane_index(shape):
    return lax.broadcasted_iota(jnp.int32, shape, len(shape) - 1)


def conv_tile(extended, taps, marks, count):
    total = jnp.broadcast_to(taps[KERNEL : KERNEL + 1, :], (count, extended.shape[1]))
    for tap in range(KERNEL):
        total = total + taps[tap : tap + 1, :] * near_rows(extended, tap, count) * marks[:, tap : tap + 1]
    return total


def near_rows(extended, tap, count):
    back = REACH - tap
    moved = pltpu.roll(extended, back, 0) if back else extended
    return moved[HALO : HALO + count, :]


def softplus(v):
    return jnp.maximum(v, 0.0) + jnp.log(1.0 + jnp.exp(-jnp.abs(v)))


def chunk_decays(raw, params):
    delta = softplus(raw + params[0:1, :])
    decay = -delta * jnp.exp(params[1:2, :])
    block = raw.shape[0] if raw.shape[0] < BLOCK else BLOCK
    rows = lax.broadcasted_iota(jnp.int32, (block, block), 0)
    lower = (rows >= lane_index((block, block))).astype(F32)
    sums = [dot(lower, decay[i : i + block, :], HIGHEST) for i in range(0, raw.shape[0], block)]
    return delta, decay, jnp.concatenate(sums, axis=0)


def end_weights(delta, sums, marks):
    last = sums[-1:, :]
    return jnp.exp(last - sums) * delta * marks[:, 5:6], jnp.exp(last) * marks[-1:, 4:5]


def spread_matrix():
    rows = lax.broadcasted_iota(jnp.int32, (LANES, INNER), 0)
    return (rows == lane_index((LANES, INNER)) // HEAD).astype(F32)


def mix_first_kernel(proj_x, proj_bc, halo, taps, params, raw, marks, xbc, decays, decays_t, state, factor):
    tokens = raw.shape[0]
    mark = marks[...]
    for ref, at in ((proj_x, 0), (proj_bc, INNER)):
        step = 256
        for q in range(0, ref.shape[1], step):
            cols = slice(at + q, at + q + step)
            own = ref[:, q : q + step].astype(F32)
            extended = jnp.concatenate([halo[:, cols].astype(F32), own], axis=0)
            value = conv_tile(extended, taps[:, cols], mark, tokens)
            xbc[:, cols] = (value * sigmoid(value)).astype(BF16)
    delta, decay, sums = chunk_decays(raw[...], params[...])
    decays[0] = delta
    decays[1] = sums
    for i in range(tokens // BLOCK):
        decays_t[i] = sums[i * BLOCK : (i + 1) * BLOCK].T
    spread = spread_matrix()
    total = jnp.zeros((NSTATE, INNER), F32)
    product = jnp.ones((1, LANES), F32)
    for i in range(0, tokens, BLOCK):
        rows = slice(i, i + BLOCK)
        weight, own = end_weights(delta[rows], sums[rows], mark[rows])
        weighted = (xbc[rows, :INNER].astype(F32) * dot(weight.astype(BF16), spread.astype(BF16))).astype(BF16)
        keep = dot(jnp.broadcast_to(own, (8, LANES)), spread, HIGHEST)[0:1]
        total = keep * total + dot_tn(xbc[rows, INNER : INNER + NSTATE], weighted)
        product = product * own
    state[...] = total.astype(BF16)
    factor[...] = jnp.broadcast_to(product, factor.shape)


def mix_first(proj, halo, taps, params, raw, marks):
    tokens = raw.shape[0]
    vmem = pl.BlockSpec(memory_space=pltpu.VMEM)
    return pl.pallas_call(
        mix_first_kernel,
        out_shape=(
            jax.ShapeDtypeStruct((tokens, CHANNELS), BF16),
            jax.ShapeDtypeStruct((2, tokens, LANES), F32),
            jax.ShapeDtypeStruct((tokens // BLOCK, LANES, BLOCK), F32),
            jax.ShapeDtypeStruct((NSTATE, INNER), BF16),
            jax.ShapeDtypeStruct((8, LANES), F32),
        ),
        grid=(1,),
        in_specs=[
            pl.BlockSpec((tokens, INNER), lambda i: (0, 1)),
            pl.BlockSpec((tokens, 2 * NSTATE), lambda i: (0, 2 * INNER // (2 * NSTATE))),
            vmem, vmem, vmem, vmem, vmem,
        ],
        out_specs=(vmem,) * 5,
        compiler_params=kernel_params(),
        name="mix_first",
    )(proj, proj, halo, taps, params, raw, marks)


def attend(left, right, mark_rows, mark_cols):
    return jnp.where(mark_rows & mark_cols, dot_nt(left, right), 0.0)


def halves(tile):
    low = lane_index(tile.shape) < HEAD
    zero = jnp.zeros_like(tile)
    return jnp.where(low, tile, zero), jnp.where(low, zero, tile)


def pair_column(values, a):
    return values[:, a * HEAD : a * HEAD + 1]


def mix_second_kernel(x, b, c, z, decays, decays_t, marks, labels, incoming, skip, gain, y, normed, states,
                      wide_sums, wide_delta, wide_end, keep, near, b_t, state, gated, squares):
    j = pl.program_id(0)
    tokens = x.shape[0]
    blocks = tokens // BLOCK
    cols = pl.ds(pl.multiple_of(j * LANES, LANES), LANES)

    @pl.when(j == 0)
    def _():
        spread = spread_matrix()
        rows = lax.broadcasted_iota(jnp.int32, (BLOCK, BLOCK), 0)
        ordered = rows >= lane_index((BLOCK, BLOCK))
        for i in range(blocks):
            at = slice(i * BLOCK, (i + 1) * BLOCK)
            mark = marks[at]
            same = mark[:, 6:7] == labels[0:1, at]
            near[i] = jnp.where(ordered & same, dot_nt(c[at], b[at]), 0.0)
            b_t[i] = b[at].T
            weight, own = end_weights(decays[0, at], decays[1, at], mark)
            wide_end[at] = dot(weight.astype(BF16), spread.astype(BF16)).astype(BF16)
            wide_sums[at] = dot(decays[1, at], spread, HIGHEST)
            wide_delta[at] = dot(decays[0, at].astype(BF16), spread.astype(BF16)).astype(BF16)
            keep[i] = dot(jnp.broadcast_to(own, (8, LANES)), spread, HIGHEST)
        squares[...] = jnp.zeros_like(squares)

    state[...] = incoming[...].astype(F32)
    for i in range(blocks):
        at = slice(i * BLOCK, (i + 1) * BLOCK)
        states[i] = state[...]
        tile = x[at].astype(F32)
        scaled = (tile * wide_delta[at, cols].astype(F32)).astype(BF16)
        sums = wide_sums[at, cols]
        total = jnp.zeros((BLOCK, LANES), F32)
        for a, part in enumerate(halves(scaled)):
            row = decays_t[i, pl.ds(2 * j + a, 1), :]
            weight = near[i] * jnp.exp(jnp.minimum(pair_column(sums, a) - row, 0.0))
            total = total + dot(weight.astype(BF16), part)
        carried = dot(c[at], state[...].astype(BF16))
        total = total + carried * jnp.exp(sums) * marks[at, 4:5] + skip[0:1, cols] * tile
        y[at] = total
        gate = z[at].astype(F32)
        gate = total * gate * sigmoid(gate)
        gated[at, cols] = gate
        squares[at] += gate * gate
        weighted = (tile * wide_end[at, cols].astype(F32)).astype(BF16)
        state[...] = keep[i, 0:1, cols] * state[...] + dot(b_t[i], weighted)
    states[blocks] = state[...]

    @pl.when(j == PAIRS - 1)
    def _():
        for i in range(blocks):
            at = slice(i * BLOCK, (i + 1) * BLOCK)
            scale = lax.rsqrt(jnp.sum(squares[at], axis=1, keepdims=True) / INNER + EPS)
            normed[at] = (gated[at] * scale * gain[0:1, :]).astype(BF16)


def mix_second(xbc, proj, decays, decays_t, marks, labels, incoming, skip, gain):
    tokens = xbc.shape[0]
    blocks = tokens // BLOCK
    tile = pl.BlockSpec((tokens, LANES), lambda j: (0, j))
    return pl.pallas_call(
        mix_second_kernel,
        out_shape=(
            jax.ShapeDtypeStruct((tokens, INNER), F32),
            jax.ShapeDtypeStruct((tokens, INNER), BF16),
            jax.ShapeDtypeStruct((blocks + 1, NSTATE, INNER), F32),
        ),
        grid=(PAIRS,),
        in_specs=[
            tile,
            pl.BlockSpec((tokens, NSTATE), lambda j: (0, INNER // NSTATE)),
            pl.BlockSpec((tokens, NSTATE), lambda j: (0, INNER // NSTATE + 1)),
            tile,
            whole(decays.shape), whole(decays_t.shape), whole(marks.shape), whole(labels.shape),
            pl.BlockSpec((NSTATE, LANES), lambda j: (0, j)),
            whole(skip.shape), whole(gain.shape),
        ],
        out_specs=(tile, whole((tokens, INNER)), pl.BlockSpec((blocks + 1, NSTATE, LANES), lambda j: (0, 0, j))),
        scratch_shapes=[
            pltpu.VMEM((tokens, INNER), F32), pltpu.VMEM((tokens, INNER), BF16), pltpu.VMEM((tokens, INNER), BF16),
            pltpu.VMEM((blocks, 8, INNER), F32), pltpu.VMEM((blocks, BLOCK, BLOCK), F32),
            pltpu.VMEM((blocks, NSTATE, BLOCK), BF16), pltpu.VMEM((NSTATE, LANES), F32),
            pltpu.VMEM((tokens, INNER), F32), pltpu.VMEM((tokens, LANES), F32),
        ],
        compiler_params=kernel_params(),
        name="mix_second",
    )(xbc, xbc, xbc, proj, decays, decays_t, marks, labels, incoming, skip, gain)


def gate_back_kernel(grad, y, z, gain, c, decays, marks, g_y, g_z, g_gain, g_state):
    step = pl.program_id(0)
    value, gate = y[...], z[...].astype(F32)
    opened = sigmoid(gate)
    swish = gate * opened
    gated = value * swish
    scale = lax.rsqrt(jnp.mean(gated * gated, axis=1, keepdims=True) + EPS)
    unit = gated * scale
    given = grad[...].astype(F32)
    scaled = given * gain[0:1, :]
    g_gated = scale * (scaled - unit * jnp.mean(scaled * unit, axis=1, keepdims=True))
    fresh = g_gated * swish
    g_y[...] = fresh.astype(BF16)
    g_z[...] = (g_gated * value * (opened + swish * (1.0 - opened))).astype(BF16)
    spread = spread_matrix()
    sums = decays[1]
    mark = marks[...]
    entry_weight = jnp.exp(sums) * mark[:, 4:5]
    own = jnp.exp(sums[-1:, :]) * mark[-1:, 4:5]
    keep = dot(jnp.broadcast_to(own, (8, LANES)), spread, HIGHEST)[0:1]
    weighted = (fresh * dot(entry_weight.astype(BF16), spread.astype(BF16))).astype(BF16)
    local = dot_tn(c[...], weighted)
    gains = jnp.broadcast_to(jnp.sum(given * unit, axis=0, keepdims=True), g_gain.shape)

    @pl.when(step == 0)
    def _():
        g_state[...] = local
        g_gain[...] = gains

    @pl.when(step > 0)
    def _():
        g_state[...] = keep * g_state[...] + local
        g_gain[...] += gains


def gate_back(grad, y, proj, gain, xbc, decays, marks):
    tokens = y.shape[0]
    blocks = tokens // BLOCK
    rows = lambda width, col: pl.BlockSpec((BLOCK, width), lambda i: (blocks - 1 - i, col))
    return pl.pallas_call(
        gate_back_kernel,
        out_shape=(
            jax.ShapeDtypeStruct((tokens, INNER), BF16),
            jax.ShapeDtypeStruct((tokens, INNER), BF16),
            jax.ShapeDtypeStruct((8, INNER), F32),
            jax.ShapeDtypeStruct((NSTATE, INNER), F32),
        ),
        grid=(blocks,),
        in_specs=[
            rows(INNER, 0), rows(INNER, 0), rows(INNER, 0), whole(gain.shape), rows(NSTATE, INNER // NSTATE + 1),
            pl.BlockSpec((2, BLOCK, LANES), lambda i: (0, blocks - 1 - i, 0)), rows(LANES, 0),
        ],
        out_specs=(rows(INNER, 0), rows(INNER, 0), whole((8, INNER)), whole((NSTATE, INNER))),
        compiler_params=kernel_params(),
        name="gate_back",
    )(grad, y, proj, gain, xbc, decays, marks)


def conv_back(grad, extended, taps, marks, count):
    acc = conv_tile(extended, taps, marks, count)
    opened = sigmoid(acc)
    g_acc = grad * (opened + acc * opened * (1.0 - opened))
    width = g_acc.shape[1]
    weights, result = [], jnp.zeros((HALO + count, width), F32)
    for tap in range(KERNEL):
        marked = g_acc * marks[:, tap : tap + 1]
        weights.append(jnp.sum(marked * near_rows(extended, tap, count), axis=0, keepdims=True))
        spread = jnp.concatenate([jnp.zeros((HALO, width), F32), marked * taps[tap : tap + 1, :]], axis=0)
        back = REACH - tap
        result = result + (pltpu.roll(spread, HALO + count - back, 0) if back else spread)
    weights.append(jnp.sum(g_acc, axis=0, keepdims=True))
    weights.append(jnp.zeros((8 - KERNEL - 1, width), F32))
    return result, jnp.concatenate(weights, axis=0)


def mix_back_kernel(x, b, c, proj_x, proj_bc, halo, taps, y, g_y, decays, decays_t, raw, params, marks, labels, states, leaving, skip,
                    g_conv, g_rim, g_taps, g_raw, g_params,
                    wide_sums, wide_delta, wide_end, wide_skip, keep, near, c_t, state, g_near, g_b, g_c, g_cum, g_delta, g_skip, ends):
    j = pl.program_id(0)
    tokens = x.shape[0]
    blocks = tokens // BLOCK
    cols = pl.ds(pl.multiple_of(j * LANES, LANES), LANES)
    lane = lane_index((LANES, LANES))
    gather = ((lax.broadcasted_iota(jnp.int32, (LANES, LANES), 0) // HEAD + 2 * j) == lane).astype(BF16)

    def collect(values):
        high = values.astype(BF16)
        return dot(high, gather) + dot((values - high.astype(F32)).astype(BF16), gather)

    @pl.when(j == 0)
    def _():
        spread = spread_matrix()
        rows = lax.broadcasted_iota(jnp.int32, (BLOCK, BLOCK), 0)
        ordered = rows <= lane_index((BLOCK, BLOCK))
        for i in range(blocks):
            at = slice(i * BLOCK, (i + 1) * BLOCK)
            mark = marks[at]
            same = mark[:, 6:7] == labels[0:1, at]
            near[i] = jnp.where(ordered & same, dot_nt(b[at], c[at]), 0.0)
            c_t[i] = c[at].T
            weight, own = end_weights(decays[0, at], decays[1, at], mark)
            end_only = jnp.exp(decays[1, at][-1:, :] - decays[1, at]) * mark[:, 5:6]
            wide_end[at] = dot(end_only.astype(BF16), spread.astype(BF16)).astype(BF16)
            wide_sums[at] = dot(decays[1, at], spread, HIGHEST)
            wide_delta[at] = dot(decays[0, at].astype(BF16), spread.astype(BF16)).astype(BF16)
            keep[i] = dot(jnp.broadcast_to(own, (8, LANES)), spread, HIGHEST)
        for ref in (g_near, g_b, g_c, g_cum, g_delta, g_skip, ends):
            ref[...] = jnp.zeros_like(ref)

    state[...] = leaving[...].astype(F32)
    g_x = []
    for i in range(blocks - 1, -1, -1):
        at = slice(i * BLOCK, (i + 1) * BLOCK)
        tile = x[at].astype(F32)
        step = wide_delta[at, cols].astype(F32)
        scaled = tile * step
        low_scaled = scaled.astype(BF16)
        sums = wide_sums[at, cols]
        end = wide_end[at, cols].astype(F32)
        given = g_y[at]
        low_state = state[...].astype(BF16)
        ends[i] += collect(jnp.broadcast_to(jnp.sum(states[i + 1] * state[...], axis=0, keepdims=True), (8, LANES)))
        total = end * dot(b[at], low_state)
        for a, (part, grad) in enumerate(zip(halves(low_scaled), halves(given))):
            row = decays_t[i, pl.ds(2 * j + a, 1), :]
            decay = jnp.exp(jnp.minimum(row - pair_column(sums, a), 0.0))
            total = total + dot((near[i] * decay).astype(BF16), grad)
            g_near[i] += decay * dot_nt(part, given)
        given = given.astype(F32)
        entry = jnp.exp(sums) * marks[at, 4:5]
        reached = (given * entry).astype(BF16)
        g_b[at] += dot_nt((scaled * end).astype(BF16), low_state)
        g_c[at] += dot_nt(reached, states[i].astype(BF16))
        own_skip = skip[0:1, cols]
        g_cum[at] += collect(given * (y[at] - own_skip * tile) - scaled * total)
        g_delta[at] += collect(total * tile)
        g_skip[...] += collect(jnp.broadcast_to(jnp.sum(given * tile, axis=0, keepdims=True), (8, LANES)))
        g_x.append(step * total + own_skip * given)
        state[...] = keep[i, 0:1, cols] * state[...] + dot(c_t[i], reached)

    mark = marks[...]
    own = proj_x[...].astype(F32)
    extended = jnp.concatenate([halo[:, cols].astype(F32), own], axis=0)
    result, weights = conv_back(jnp.concatenate(g_x[::-1], axis=0), extended, taps[:, cols], mark, tokens)
    g_rim[:HALO, cols] = result[:HALO]
    g_rim[HALO:, cols] = result[tokens:]
    g_conv[:, cols] = result[HALO:].astype(BF16)
    g_taps[:, cols] = weights

    @pl.when(j == PAIRS - 1)
    def _():
        for i in range(blocks):
            at = slice(i * BLOCK, (i + 1) * BLOCK)
            rows = lax.broadcasted_iota(jnp.int32, (BLOCK, BLOCK), 0)
            seen = (rows <= lane_index((BLOCK, BLOCK))) & (marks[at, 6:7] == labels[0:1, at])
            grad = jnp.where(seen, g_near[i], 0.0)
            g_b[at] += dot(grad.astype(BF16), c[at])
            g_c[at] += dot(grad.T.astype(BF16), b[at])
        for k, ref in enumerate((g_b, g_c)):
            at = slice(INNER + k * NSTATE, INNER + (k + 1) * NSTATE)
            own = proj_bc[:, k * NSTATE : (k + 1) * NSTATE].astype(F32)
            extended = jnp.concatenate([halo[:, at].astype(F32), own], axis=0)
            result, weights = conv_back(ref[...], extended, taps[:, at], mark, tokens)
            g_rim[:HALO, at] = result[:HALO]
            g_rim[HALO:, at] = result[tokens:]
            g_conv[:, at] = result[HALO:].astype(BF16)
            g_taps[:, at] = weights
        rate = -jnp.exp(params[1:2, :])
        bias_sum = jnp.zeros((1, LANES), F32)
        rate_sum = jnp.zeros((1, LANES), F32)
        rows = lax.broadcasted_iota(jnp.int32, (BLOCK, BLOCK), 0)
        upper = (rows <= lane_index((BLOCK, BLOCK))).astype(F32)
        for i in range(blocks):
            at = slice(i * BLOCK, (i + 1) * BLOCK)
            g_decay = dot(upper, g_cum[at], HIGHEST) + ends[i, 0:1, :]
            delta = decays[0, at]
            full = g_delta[at] + g_decay * rate
            full = full * sigmoid(raw[at] + params[0:1, :])
            g_raw[at] = full.astype(BF16)
            bias_sum = bias_sum + jnp.sum(full, axis=0, keepdims=True)
            rate_sum = rate_sum + jnp.sum(g_decay * delta * rate, axis=0, keepdims=True)
        g_params[...] = jnp.concatenate([bias_sum, rate_sum, g_skip[0:1, :], jnp.zeros((5, LANES), F32)], axis=0)


def mix_back(xbc, proj, halo, taps, y, g_y, decays, decays_t, raw, params, marks, labels, states, leaving, skip):
    tokens = xbc.shape[0]
    blocks = tokens // BLOCK
    tile = pl.BlockSpec((tokens, LANES), lambda j: (0, j))
    acc = lambda *shape: pltpu.VMEM(shape, F32)
    return pl.pallas_call(
        mix_back_kernel,
        out_shape=(
            jax.ShapeDtypeStruct((tokens, CHANNELS), BF16),
            jax.ShapeDtypeStruct((2 * HALO, CHANNELS), F32),
            jax.ShapeDtypeStruct((8, CHANNELS), F32),
            jax.ShapeDtypeStruct((tokens, LANES), BF16),
            jax.ShapeDtypeStruct((8, LANES), F32),
        ),
        grid=(PAIRS,),
        in_specs=[
            tile,
            pl.BlockSpec((tokens, NSTATE), lambda j: (0, INNER // NSTATE)),
            pl.BlockSpec((tokens, NSTATE), lambda j: (0, INNER // NSTATE + 1)),
            pl.BlockSpec((tokens, LANES), lambda j: (0, PAIRS + j)),
            pl.BlockSpec((tokens, 2 * NSTATE), lambda j: (0, 2 * INNER // (2 * NSTATE))),
            whole(halo.shape), whole(taps.shape), tile, tile,
            whole(decays.shape), whole(decays_t.shape), whole(raw.shape), whole(params.shape), whole(marks.shape), whole(labels.shape),
            pl.BlockSpec((blocks + 1, NSTATE, LANES), lambda j: (0, 0, j)),
            pl.BlockSpec((NSTATE, LANES), lambda j: (0, j)),
            whole(skip.shape),
        ],
        out_specs=(
            whole((tokens, CHANNELS)), whole((2 * HALO, CHANNELS)), whole((8, CHANNELS)), whole((tokens, LANES)), whole((8, LANES)),
        ),
        scratch_shapes=[
            acc(tokens, INNER), pltpu.VMEM((tokens, INNER), BF16), pltpu.VMEM((tokens, INNER), BF16), acc(8, LANES),
            acc(blocks, 8, INNER), acc(blocks, BLOCK, BLOCK), pltpu.VMEM((blocks, NSTATE, BLOCK), BF16), acc(NSTATE, LANES),
            acc(blocks, BLOCK, BLOCK), acc(tokens, NSTATE), acc(tokens, NSTATE), acc(tokens, LANES), acc(tokens, LANES),
            acc(8, LANES), acc(blocks, 8, LANES),
        ],
        compiler_params=kernel_params(),
        name="mix_back",
    )(xbc, xbc, xbc, proj, proj, halo, taps, y, g_y, decays, decays_t, raw, params, marks, labels, states, leaving, skip)


QBLOCK = 256
GROUPS = HEADS // KV_HEADS
QPAIRS = QDIM // LANES
SCALE = 1.0 / math.sqrt(HEAD)


def swap_halves(values):
    half = HEAD // 2
    front = lane_index(values.shape) % HEAD < half
    width = values.shape[-1]
    return jnp.where(front, pltpu.roll(values, width - half, 1), pltpu.roll(values, half, 1))


def turn(values, cosine, sine):
    return values * cosine + swap_halves(values) * sine


def both_sides(tile, both):
    low = lane_index(tile.shape) < HEAD
    zero = jnp.zeros_like(tile)
    moved = pltpu.roll(tile.astype(F32), HEAD, 1).astype(tile.dtype)
    both[0, 0] = jnp.where(low, tile, zero)
    both[0, 1] = jnp.where(low, zero, moved)
    both[1, 0] = jnp.where(low, moved, zero)
    both[1, 1] = jnp.where(low, zero, tile)


def attend_kernel(q, kv, key_labels, marks, context, stats, keys, values):
    block, pair = pl.program_id(0), pl.program_id(1)
    window = DOC_MOST + QBLOCK
    start = pl.multiple_of(block * QBLOCK, QBLOCK)

    @pl.when((block == 0) & (pair == 0))
    def _():
        both_sides(kv[:, :KDIM], keys)
        both_sides(kv[:, KDIM:], values)

    group = pair // (GROUPS // 2)
    rows = lax.broadcasted_iota(jnp.int32, (QBLOCK, window), 0)
    cols = lane_index((QBLOCK, window))
    seen = (cols <= rows + DOC_MOST) & (marks[:, 6:7] == key_labels[0, 0:1, :])
    total = jnp.zeros((QBLOCK, LANES), F32)
    found = jnp.zeros((QBLOCK, LANES), F32)
    for a in range(2):
        scores = dot_nt(q[...], keys[group, a, pl.ds(start, window), :]) * SCALE
        scores = jnp.where(seen, scores, NEG_BIG)
        most = jnp.max(scores, axis=1, keepdims=True)
        probs = jnp.exp(scores - most)
        mass = jnp.sum(probs, axis=1, keepdims=True)
        probs = probs * (1.0 / mass)
        total = total + dot(probs.astype(BF16), values[group, a, pl.ds(start, window), :])
        found = jnp.where(lane_index(found.shape) == a, most + jnp.log(mass), found)
    context[...] = total.astype(BF16)
    stats[0] = found.T[0:8, :]


def attend(q, kv, key_labels, marks):
    tokens = q.shape[0]
    blocks = tokens // QBLOCK
    tile = pl.BlockSpec((QBLOCK, LANES), lambda i, p: (i, p))
    return pl.pallas_call(
        attend_kernel,
        out_shape=(jax.ShapeDtypeStruct((tokens, QDIM), BF16), jax.ShapeDtypeStruct((QPAIRS, 8, tokens), F32)),
        grid=(blocks, QPAIRS),
        in_specs=[
            tile, whole(kv.shape), pl.BlockSpec((1,) + key_labels.shape[1:], lambda i, p: (i, 0, 0)),
            pl.BlockSpec((QBLOCK, LANES), lambda i, p: (i, 0)),
        ],
        out_specs=(tile, pl.BlockSpec((1, 8, QBLOCK), lambda i, p: (p, 0, i))),
        scratch_shapes=[pltpu.VMEM((2, 2) + (kv.shape[0], LANES), BF16)] * 2,
        compiler_params=kernel_params(),
        name="attend",
    )(q, kv, key_labels, marks)


def attend_back_kernel(q, kv, given, key_marks, query_labels, stats, cosine, sine, g_q, g_kv, keys, values, g_key, g_value):
    block, pair = pl.program_id(0), pl.program_id(1)
    window = DOC_MOST + QBLOCK
    start = pl.multiple_of(block * QBLOCK, QBLOCK)

    @pl.when((block == 0) & (pair == 0))
    def _():
        both_sides(kv[:, :KDIM], keys)
        both_sides(kv[:, KDIM:], values)
        g_key[...] = jnp.zeros_like(g_key)
        g_value[...] = jnp.zeros_like(g_value)

    group = pair // (GROUPS // 2)
    rows = lax.broadcasted_iota(jnp.int32, (window, QBLOCK), 0)
    cols = lane_index((window, QBLOCK))
    seen = (rows <= cols + DOC_MOST) & (key_marks[0, :, 0:1] == query_labels[0:1, :])
    at = pl.ds(start, window)
    query, grad = q[...], given[...]
    total = jnp.zeros((QBLOCK, LANES), F32)
    for a, (query_part, grad_part) in enumerate(zip(halves(query), halves(grad))):
        key = keys[group, a, at, :]
        scores = jnp.where(seen, dot_nt(key, query) * SCALE, NEG_BIG)
        probs = jnp.exp(scores - stats[0, a : a + 1, :])
        g_probs = dot_nt(values[group, a, at, :], grad)
        mean = jnp.sum(probs * g_probs, axis=0, keepdims=True)
        g_scores = (probs * (g_probs - mean)).astype(BF16)
        g_key[group, at] += dot(g_scores, query_part) * SCALE
        g_value[group, at] += dot(probs.astype(BF16), grad_part)
        total = total + dot_tn(g_scores, key)
    g_q[...] = turn(total * SCALE, cosine[...], -sine[...]).astype(BF16)

    @pl.when((block == pl.num_programs(0) - 1) & (pair == QPAIRS - 1))
    def _():
        for k, ref in enumerate((g_key, g_value)):
            first = ref[0] + pltpu.roll(ref[0], HEAD, 1)
            second = ref[1] + pltpu.roll(ref[1], HEAD, 1)
            g_kv[:, k * KDIM : (k + 1) * KDIM] = jnp.where(lane_index(first.shape) < HEAD, first, second).astype(BF16)


def attend_back(q, kv, given, key_marks, query_labels, stats, cosine, sine):
    tokens = q.shape[0]
    blocks = tokens // QBLOCK
    tile = pl.BlockSpec((QBLOCK, LANES), lambda i, p: (i, p))
    row = pl.BlockSpec((QBLOCK, LANES), lambda i, p: (i, 0))
    return pl.pallas_call(
        attend_back_kernel,
        out_shape=(jax.ShapeDtypeStruct((tokens, QDIM), BF16), jax.ShapeDtypeStruct(kv.shape, BF16)),
        grid=(blocks, QPAIRS),
        in_specs=[
            tile, whole(kv.shape), pl.BlockSpec((QBLOCK, LANES), lambda i, p: (i, PAIRS + p)),
            pl.BlockSpec((1,) + key_marks.shape[1:], lambda i, p: (i, 0, 0)),
            pl.BlockSpec((8, QBLOCK), lambda i, p: (0, i)),
            pl.BlockSpec((1, 8, QBLOCK), lambda i, p: (p, 0, i)), row, row,
        ],
        out_specs=(tile, whole(kv.shape)),
        scratch_shapes=[pltpu.VMEM((2, 2) + (kv.shape[0], LANES), BF16)] * 2 + [pltpu.VMEM((2, kv.shape[0], LANES), F32)] * 2,
        compiler_params=kernel_params(),
        name="attend_back",
    )(q, kv, given, key_marks, query_labels, stats, cosine, sine)


def turn_back_kernel(g_kv, cosine, sine, out):
    out[:, :KDIM] = turn(g_kv[:, :KDIM], cosine[...], -sine[...]).astype(BF16)
    out[:, KDIM:] = g_kv[:, KDIM:].astype(BF16)


def turn_back(g_kv, cosine, sine):
    return pl.pallas_call(
        turn_back_kernel, out_shape=jax.ShapeDtypeStruct(g_kv.shape, BF16), compiler_params=kernel_params(), name="turn_back",
    )(g_kv, cosine, sine)


FF_TILE = 512


def feed_kernel(hidden, given, gain, w_gate, w_up, w_down, normed, mixed, g_gate, g_up, result, g_hidden, low, g_gain, total, g_mid):
    j = pl.program_id(0)

    @pl.when(j == 0)
    def _():
        values = hidden[...]
        normed[...] = (values * rms_scale(values) * gain[0:1, :]).astype(BF16)

    gate = dot(normed[...], w_gate[...])
    upper = dot(normed[...], w_up[...])
    grad = dot_nt(given[...], w_down[...])
    opened = sigmoid(gate)
    swish = gate * opened
    product = (swish * upper).astype(BF16)
    left = (grad * upper * (opened + swish * (1.0 - opened))).astype(BF16)
    right = (grad * swish).astype(BF16)
    mixed[...] = product
    g_gate[...] = left
    g_up[...] = right
    forward = dot(product, w_down[...])
    backward = dot_nt(left, w_gate[...]) + dot_nt(right, w_up[...])

    @pl.when(j == 0)
    def _():
        total[...] = forward
        g_mid[...] = backward

    @pl.when(j > 0)
    def _():
        total[...] += forward
        g_mid[...] += backward

    @pl.when(j == pl.num_programs(0) - 1)
    def _():
        values = hidden[...]
        result[...] = (values + total[...]).astype(BF16)
        scale = rms_scale(values)
        unit = values * scale
        back = g_mid[...]
        scaled = back * gain[0:1, :]
        fresh = given[...].astype(F32) + scale * (scaled - unit * jnp.mean(scaled * unit, axis=1, keepdims=True))
        g_hidden[...] = fresh
        low[...] = fresh.astype(BF16)
        g_gain[...] = jnp.broadcast_to(jnp.sum(back * unit, axis=0, keepdims=True), g_gain.shape)


def feed(hidden, given, gain, w_ff, w_down):
    tokens = hidden.shape[0]
    tiles = FF // FF_TILE
    rows = whole((tokens, D))
    tile = pl.BlockSpec((tokens, FF_TILE), lambda j: (0, j))
    return pl.pallas_call(
        feed_kernel,
        out_shape=(
            jax.ShapeDtypeStruct((tokens, D), BF16),
            jax.ShapeDtypeStruct((tokens, FF), BF16), jax.ShapeDtypeStruct((tokens, FF), BF16), jax.ShapeDtypeStruct((tokens, FF), BF16),
            jax.ShapeDtypeStruct((tokens, D), BF16), jax.ShapeDtypeStruct((tokens, D), F32), jax.ShapeDtypeStruct((tokens, D), BF16),
            jax.ShapeDtypeStruct((8, D), F32),
        ),
        grid=(tiles,),
        in_specs=[
            rows, rows, whole((8, D)),
            pl.BlockSpec((D, FF_TILE), lambda j: (0, j)), pl.BlockSpec((D, FF_TILE), lambda j: (0, tiles + j)),
            pl.BlockSpec((FF_TILE, D), lambda j: (j, 0)),
        ],
        out_specs=(rows, tile, tile, tile, rows, rows, rows, whole((8, D))),
        scratch_shapes=[pltpu.VMEM((tokens, D), F32), pltpu.VMEM((tokens, D), F32)],
        compiler_params=kernel_params(),
        name="feed",
    )(hidden, given, gain, w_ff, w_ff, w_down)


STEP_BLOCKS = 32
DEPTH = 4


def project_kernel(table, blocks, rows, gain, w_dt, cosine, sine, w_in, w_out, w_ff, w_down, proj, q_out, kv_out, normed, raw, halo,
                   held, wide, tall, s_first, s_put, s_in, s_out):
    across = held.shape[1] // BS
    down = held.shape[0] // BS

    def first(r):
        def one(i, _):
            cols = pl.ds(pl.multiple_of(i * BS, BS), BS)
            pltpu.make_async_copy(blocks.at[table[r * across + i]], held.at[pl.ds(r * BS, BS), cols], s_first.at[r]).start()
            return 0

        lax.fori_loop(0, across, one, 0)

    outs = []
    for ref in (w_out, w_ff, w_down):
        count, cols = ref.shape
        per_row = cols // BS
        deep = STEP_BLOCKS // per_row
        for r in range(count // (BS * deep)):
            outs.append((ref, r * BS * deep, deep, per_row))

    def target(step):
        ref, at, deep, per_row = outs[step]
        slot = step % DEPTH
        return (wide.at[slot] if deep == 1 else tall.at[slot]), ref.at[pl.ds(at, BS * deep)], per_row

    def fetch(step):
        buffer, _, per_row = target(step)

        def one(i, _):
            block_rows = pl.ds(pl.multiple_of(i // per_row * BS, BS), BS)
            cols = pl.ds(pl.multiple_of(i % per_row * BS, BS), BS)
            source = blocks.at[table[down * across + step * STEP_BLOCKS + i]]
            pltpu.make_async_copy(source, buffer.at[block_rows, cols], s_in.at[step % DEPTH]).start()
            return 0

        lax.fori_loop(0, STEP_BLOCKS, one, 0)

    def put(step):
        buffer, place_to, _ = target(step)
        return pltpu.make_async_copy(buffer, place_to, s_out.at[step % DEPTH])

    steps = len(outs)

    def advance(step):
        buffer, place_to, _ = target(step)
        pltpu.make_async_copy(place_to, buffer, s_in.at[step % DEPTH]).wait()
        put(step).start()
        ahead = step + DEPTH - 1
        if ahead < steps:
            if step >= 1:
                put(step - 1).wait()
            fetch(ahead)

    for r in range(down):
        first(r)
    for step in range(min(DEPTH - 1, steps)):
        fetch(step)
    values = rows[...].astype(F32)
    low = (values * rms_scale(values) * gain[0:1, :]).astype(BF16)
    normed[...] = low
    raw[...] = dot(low, w_dt[...])
    for r in range(down):
        part = held.at[pl.ds(r * BS, BS)]
        pltpu.make_async_copy(part, part, s_first.at[r]).wait()
    whole_put = pltpu.make_async_copy(held, w_in, s_put.at[0])
    whole_put.start()
    cos, sin = cosine[...], sine[...]
    tokens = rows.shape[0]
    plain = proj.shape[1]
    cuts = [(at, min(512, plain - at)) for at in range(0, plain, 512)] + [(plain, QDIM), (plain + QDIM, 2 * KDIM)]
    done = 0
    for k, (at, width) in enumerate(cuts):
        value = dot(normed[...], held[:, at : at + width])
        if at < plain:
            proj[:, at : at + width] = value.astype(BF16)
        elif at == plain:
            for p in range(QPAIRS):
                lanes = slice(p * LANES, (p + 1) * LANES)
                q_out[:, lanes] = turn(value[:, lanes], cos, sin).astype(BF16)
        else:
            kv_out[:, :KDIM] = turn(value[:, :KDIM], cos, sin).astype(BF16)
            kv_out[:, KDIM:] = value[:, KDIM:].astype(BF16)
        goal = steps * (k + 1) // len(cuts)
        for step in range(done, goal):
            advance(step)
        done = goal
    halo[...] = proj[tokens - halo.shape[0] :, INNER:]
    for step in range(max(steps - DEPTH, 0), steps):
        put(step).wait()
    whole_put.wait()


def slots_in_order(block_of_slot, order):
    match = jnp.array(order, jnp.int32)[:, None] == block_of_slot[None, :]
    return jnp.sum(jnp.where(match, jnp.arange(block_of_slot.shape[0], dtype=jnp.int32)[None, :], 0), axis=1)


def values_of(block_of_slot, values):
    match = block_of_slot[:, None] == jnp.arange(len(values), dtype=jnp.int32)[None, :]
    return jnp.sum(jnp.where(match, jnp.array(values, jnp.int32)[None, :], 0), axis=1)


def grad_tables():
    lefts, rights = [], []
    left_base = right_base = 0
    for members, beside in ((WIDE_IN, True), (TALL_OUT, False), (WIDE_FF, True), (TALL_FF, False)):
        for m in members:
            rows, cols = SHAPES[m]
            for r in range(0, rows, BS):
                for q in range(0, cols, BS):
                    lefts.append((left_base + r) // BS)
                    rights.append((right_base + q) // BS)
            if beside:
                right_base += cols
            else:
                left_base += rows
        if beside:
            left_base += rows
        else:
            right_base += cols
    return lefts, rights


def project(blocks, table, rows, gain, w_dt, cosine, sine):
    tokens = rows.shape[0]
    total = sum(SHAPES[m][1] for m in WIDE_IN)
    plain = total - QDIM - 2 * KDIM
    shapes = [(D, total), (sum(SHAPES[m][0] for m in TALL_OUT), D), (D, 2 * FF), (FF, D)]
    results = [(tokens, plain), (tokens, QDIM), (tokens, 2 * KDIM), (tokens, D), (tokens, LANES), (HALO, CHANNELS)]
    kinds = [BF16, BF16, BF16, BF16, F32, BF16]
    hbm = pl.BlockSpec(memory_space=pl.ANY)
    vmem = pl.BlockSpec(memory_space=pltpu.VMEM)
    return pl.pallas_call(
        project_kernel,
        out_shape=tuple(jax.ShapeDtypeStruct(shape, BF16) for shape in shapes)
        + tuple(jax.ShapeDtypeStruct(shape, kind) for shape, kind in zip(results, kinds)),
        grid_spec=pltpu.PrefetchScalarGridSpec(
            num_scalar_prefetch=1, grid=(1,), in_specs=[hbm] + [vmem] * 5, out_specs=(hbm,) * 4 + (vmem,) * 6,
            scratch_shapes=[
                pltpu.VMEM((D, total), BF16),
                pltpu.VMEM((DEPTH, BS, STEP_BLOCKS * BS), BF16),
                pltpu.VMEM((DEPTH, STEP_BLOCKS // (D // BS) * BS, D), BF16),
                pltpu.SemaphoreType.DMA((D // BS,)), pltpu.SemaphoreType.DMA((1,)),
                pltpu.SemaphoreType.DMA((DEPTH,)), pltpu.SemaphoreType.DMA((DEPTH,)),
            ],
        ),
        compiler_params=kernel_params(),
        name="project",
    )(table, blocks, rows, gain, w_dt, cosine, sine)


SHAMPOO = 24


def shampoo_kernel(norm, total, master, left, right, left_root, right_root, grad, new_left, new_right, new_master, low):
    scale = 0.5 * norm * norm / BS
    for i in range(0, total.shape[0], 2):
        pair = (i, i + 1)
        rows = jnp.concatenate([total[k] for k in pair], axis=0)
        cols = jnp.concatenate([total[k] for k in pair], axis=1)
        outer = dot_nt(rows, rows) * scale
        inner = dot_tn(cols, cols) * scale
        moved = dot(rows, jnp.concatenate([right_root[k] for k in pair], axis=1).astype(BF16))
        moved = jnp.concatenate([moved[:BS, :BS], moved[BS:, BS:]], axis=1).astype(BF16)
        moved = dot(jnp.concatenate([left_root[k] for k in pair], axis=0).astype(BF16), moved) * (LR_MATRIX * norm)
        for k, at in zip(pair, (slice(0, BS), slice(BS, 2 * BS))):
            grad[k] = total[k].astype(F32) * norm
            new_left[k] = 0.5 * left[k] + outer[at, at]
            new_right[k] = 0.5 * right[k] + inner[at, at]
            fresh = master[k] - moved[at, at]
            new_master[k] = fresh
            low[k] = fresh.astype(BF16)


def shampoo(norm, total, master, left, right, left_root, right_root):
    slots = total.shape[0]
    each = math.gcd(slots, SHAMPOO)
    spec = pl.BlockSpec((each, BS, BS), lambda i: (i, 0, 0))
    full = jax.ShapeDtypeStruct(master.shape, F32)
    return pl.pallas_call(
        functools.partial(shampoo_kernel, norm),
        out_shape=(full, full, full, full, jax.ShapeDtypeStruct(master.shape, BF16)),
        grid=(slots // each,),
        in_specs=[spec] * 6,
        out_specs=(spec,) * 5,
        compiler_params=kernel_params(),
        name="shampoo",
    )(total, master, left, right, left_root, right_root)


def ungroup(values, micro):
    seq = lax.axis_size("seq")
    each = seq // micro
    here = lax.axis_index("seq")
    order = here // each
    stacked = jnp.stack(values)
    cut = stacked.reshape((len(values), micro, -1) + stacked.shape[2:])
    pieces = []
    for t in range(micro):
        pairs = [(((j + t) % micro) * each + j // micro, j) for j in range(seq)]
        pieces.append(lax.ppermute(lax.dynamic_index_in_dim(cut, (order - t) % micro, 1, False), "seq", pairs))
    results = []
    for m in range(micro):
        chosen = pieces[0]
        for t in range(1, micro):
            chosen = jnp.where((m - here) % micro == t, pieces[t], chosen)
        results.append(chosen)
    return [jnp.stack([chosen[k] for chosen in results]) for k in range(len(values))]


def along(value, steps, micro):
    seq = lax.axis_size("seq")
    each = seq // micro
    pairs = [(s, s + steps) for s in range(seq) if 0 <= s % each + steps < each]
    return lax.ppermute(value, "seq", pairs)


def pad_rows(*rows):
    width = rows[0].shape[-1]
    return jnp.concatenate([r.reshape(-1, width) for r in rows] + [jnp.zeros((8 - sum(r.size // width for r in rows), width), F32)], axis=0)


def shards(grid, tokens, cotangent, doc_ids, master_blocks, block_of_slot, left_stats, right_stats, left_roots, right_roots,
           vector_params, first_moment, second_moment, adam_step):
    micro, piece = tokens.shape[:2]
    seq = lax.axis_size("seq")
    each = seq // micro
    count = micro * piece
    here = lax.axis_index("seq")
    rank = here % each
    start = rank * count
    slots = master_blocks.shape[0]

    orders = all_orders()
    table = slots_in_order(block_of_slot, sum(orders, []))
    left_at, right_at = (values_of(block_of_slot, values) for values in grad_tables())
    gathered, rows, given, labels_all = gather_blocks(grid, master_blocks, tokens, cotangent, doc_ids)
    rows, given = rows.reshape(count, D), given.reshape(count, D)
    gain_in, gain_mid, gain_mix, conv_weight, conv_bias, dt_bias, a_log, skip, w_dt = unpack_vectors(vector_params)
    w_dt = jnp.pad(w_dt.reshape(D, HEADS_SSM), ((0, 0), (0, LANES - HEADS_SSM))).astype(BF16)
    taps = pad_rows(conv_weight.reshape(KERNEL, CHANNELS), conv_bias)
    lane_pad = lambda v: jnp.pad(v, (0, LANES - HEADS_SSM))
    params = pad_rows(lane_pad(dt_bias), lane_pad(a_log))
    wide_skip = pad_rows(jnp.repeat(skip, HEAD))
    wide_gain = pad_rows(gain_mix)

    row = lax.dynamic_index_in_dim(labels_all, here // each, 1, False).reshape(-1)
    before = jnp.concatenate([jnp.full((DOC_MOST,), -1, jnp.int32), row])
    window = lax.dynamic_slice_in_dim(before, start, DOC_MOST + count)
    labels = window[DOC_MOST:]
    blocks = count // BLOCK
    columns = [(window[DOC_MOST - REACH + tap : DOC_MOST - REACH + tap + count] == labels).astype(F32) for tap in range(KERNEL)]
    by_block = labels.reshape(blocks, BLOCK)
    entries_at = window[DOC_MOST - 1 : DOC_MOST - 1 + count].reshape(blocks, BLOCK)[:, :1]
    columns.append((by_block == entries_at).astype(F32).reshape(-1))
    columns.append((by_block == by_block[:, -1:]).astype(F32).reshape(-1))
    columns.append(labels.astype(F32))
    marks = jnp.pad(jnp.stack(columns, axis=1), ((0, 0), (0, LANES - len(columns))))
    label_rows = jnp.broadcast_to(labels.astype(F32)[None], (8, count))
    far = jnp.stack([window[i : i + DOC_MOST + QBLOCK] for i in range(0, count, QBLOCK)]).astype(F32)
    key_labels = jnp.broadcast_to(far[:, None, :], (far.shape[0], 8, far.shape[1]))
    key_marks = jnp.broadcast_to(far[:, :, None], far.shape + (8,))
    first = jnp.sum((row[None, :] < labels[:, None]).astype(jnp.int32), axis=1)
    positions = (start + jnp.arange(count) - first).astype(F32)
    half = HEAD // 2
    frequency = jnp.exp(jnp.arange(half, dtype=F32) * (-2.0 * math.log(THETA) / HEAD))
    angles = positions[:, None] * frequency[None, :]
    cos, sin = jnp.cos(angles), jnp.sin(angles)
    cosine = jnp.concatenate([cos] * 4, axis=1)
    sine = jnp.concatenate([-sin, sin] * 2, axis=1)

    inputs = rows.astype(F32)
    w_in, w_out, w_ff, w_down, proj, q, kv, normed_in, raw, halo = project(
        gathered.reshape(-1, BS, BS), table, rows, pad_rows(gain_in), w_dt, cosine, sine
    )
    halo = along(halo, 1, micro)
    xbc, decays, decays_t, state, factor = mix_first(proj, halo, taps, params, raw, marks)
    past = min(each - 1, -(-DOC_MOST // count))
    earlier = [along(kv, back, micro) for back in range(past, 0, -1)]
    if past * count < DOC_MOST:
        earlier.insert(0, jnp.zeros((DOC_MOST - past * count, kv.shape[1]), BF16))
    reach = jnp.concatenate(earlier + [kv], axis=0)[-(DOC_MOST + count) :]
    wide = lambda f: jnp.repeat(f[0, :HEADS_SSM], HEAD)[None]
    incoming = along(state, each - 1, micro).astype(F32) if each > 1 else jnp.zeros(state.shape, F32)
    for back in range(each - 2, 0, -1):
        incoming = along(state, back, micro).astype(F32) + wide(along(factor, back, micro)) * incoming
    y, normed_ssm, states = mix_second(xbc, proj, decays, decays_t, marks, label_rows, incoming, wide_skip, wide_gain)
    context, stats = attend(q, reach, key_labels, marks)
    hidden = inputs + (dot(normed_ssm, w_out[:INNER]) + dot(context, w_out[INNER:]))
    def norm_back(grad, values, gain):
        scale = rms_scale(values)
        unit = values * scale
        scaled = grad * gain
        return scale * (scaled - unit * jnp.mean(scaled * unit, axis=1, keepdims=True)), jnp.sum(grad * unit, axis=0)

    normed_mid, mixed, g_gate, g_up, result, g_hidden, hidden_low, g_gain_mid = feed(hidden, given, pad_rows(gain_mid), w_ff, w_down)
    (layer_out,) = ungroup([result], micro)
    g_out = dot_nt(hidden_low, w_out).astype(BF16)
    g_y, g_z, g_gain_mix, g_state = gate_back(g_out, y, proj, wide_gain, xbc, decays, marks)
    low_state = g_state.astype(BF16)
    leaving = along(low_state, 1 - each, micro).astype(F32) if each > 1 else jnp.zeros(state.shape, F32)
    for ahead in range(each - 2, 0, -1):
        leaving = along(low_state, -ahead, micro).astype(F32) + wide(along(factor, -ahead, micro)) * leaving
    g_q, g_reach = attend_back(q, reach, g_out, key_marks, label_rows, stats, cosine, sine)
    g_conv, g_rim, g_taps, g_raw, g_params = mix_back(
        xbc, proj, halo, taps, y, g_y, decays, decays_t, raw, params, marks, label_rows, states, leaving, wide_skip
    )
    g_kv = g_reach[-count:].astype(F32)
    for back in range(1, past + 1):
        low = max(0, DOC_MOST - back * count)
        part = g_reach[low : DOC_MOST - (back - 1) * count]
        moved = along(part, -back, micro).astype(F32)
        g_kv = g_kv + jnp.pad(moved, ((count - part.shape[0], 0), (0, 0)))
    g_kv = turn_back(g_kv, cosine, sine)
    rim = along(g_rim[:HALO], -1, micro)
    g_conv = lax.dynamic_update_slice(g_conv, (g_rim[HALO:] + rim).astype(BF16), (count - HALO, 0))
    g_in = jnp.concatenate([g_z, g_conv, g_q, g_kv], axis=1)
    g_values, g_gain_in = norm_back(dot_nt(g_in, w_in) + dot_nt(g_raw, w_dt), inputs, gain_in)
    (grad_tokens,) = ungroup([(g_values + g_hidden).astype(BF16)], micro)
    grad_tokens = grad_tokens.astype(F32)
    g_w_dt = dot_tn(normed_in, g_raw)

    parts = [g_gain_in, g_gain_mid[0], g_gain_mix[0], g_taps[:KERNEL].reshape(-1), g_taps[KERNEL]]
    parts += [g_params[i, :HEADS_SSM] for i in range(3)] + [g_w_dt[:, :HEADS_SSM].reshape(-1)]
    width = vector_params.shape[0]
    height = -(-width // (8 * LANES)) * 8
    vector = jnp.concatenate(parts + [jnp.zeros((height * LANES - width,), F32)]).reshape(height, LANES)
    total, vector = reduce_blocks(grid, slots, left_at, right_at, [normed_in, normed_ssm, context, normed_mid, mixed],
                                  [g_z, g_conv, g_q, g_kv, hidden_low, g_gate, g_up, given], vector)
    norm = 1.0 / math.sqrt(count * seq * lax.axis_size("dp"))
    updates = shampoo(norm, total, master_blocks, left_stats, right_stats, left_roots, right_roots)
    g_vector = vector.reshape(-1)[:width] * norm
    step = adam_step[0].astype(F32)
    new_first = BETA_ONE * first_moment + (1.0 - BETA_ONE) * g_vector
    new_second = BETA_TWO * second_moment + (1.0 - BETA_TWO) * g_vector * g_vector
    first_hat = new_first / (1.0 - jnp.power(BETA_ONE, step))
    second_hat = new_second / (1.0 - jnp.power(BETA_TWO, step))
    new_vector = vector_params - LR_VECTOR * first_hat / (jnp.sqrt(second_hat) + ADAM_EPS)
    return (layer_out, grad_tokens) + tuple(updates) + (g_vector, new_vector, new_first, new_second)


def solution(mesh):
    line, block, copied = P("dp", "seq", None), P("dp", None, None), P()
    return jax.shard_map(
        functools.partial(shards, grid_of(mesh)),
        mesh=mesh,
        in_specs=(line, line, P("dp", "seq"), block, copied, block, block, block, block, copied, copied, copied, copied),
        out_specs=(line, line) + (block,) * 5 + (copied,) * 4,
        check_vma=False,
    )
```

```python
import functools
import math

import jax
import jax.numpy as jnp
from jax import lax
from jax.experimental import pallas as pl
from jax.experimental.pallas import tpu as pltpu
from jax.sharding import PartitionSpec as P

D = 1024
HEADS_SSM = 24
HEAD = 64
NSTATE = 128
HEADS = 8
KV_HEADS = 2
FF = 2048
KERNEL = 4
BS = 128
DOC_MOST = 512
INNER = HEADS_SSM * HEAD
CHANNELS = INNER + 2 * NSTATE
REACH = KERNEL - 1
QDIM = HEADS * HEAD
KDIM = KV_HEADS * HEAD
LANES = 128
PAIRS = INNER // LANES

EPS = 1e-05
THETA = 100000000000.0
LR_MATRIX = 0.02
LR_VECTOR = 0.08
BETA_ONE = 0.9
BETA_TWO = 0.999
ADAM_EPS = 1e-08
NEG_BIG = -1e30
F32 = jnp.float32
BF16 = jnp.bfloat16
HIGHEST = lax.Precision.HIGHEST
VMEM_MOST = 60 << 20

SHAPES = (
    (D, INNER), (D, INNER), (D, 2 * NSTATE), (D, QDIM), (D, KDIM), (D, KDIM),
    (INNER, D), (QDIM, D), (D, FF), (D, FF), (FF, D),
)
WIDE_IN, TALL_OUT, WIDE_FF, TALL_FF = (0, 1, 2, 3, 4, 5), (6, 7), (8, 9), (10,)
SIZES = (D, D, INNER, KERNEL * CHANNELS, CHANNELS, HEADS_SSM, HEADS_SSM, HEADS_SSM, D * HEADS_SSM)


def block_offsets():
    starts, total = [], 0
    for rows, cols in SHAPES:
        starts.append(total)
        total += rows // BS * (cols // BS)
    return starts


def wide_order(members):
    starts = block_offsets()
    rows = SHAPES[members[0]][0] // BS
    return [starts[m] + r * (SHAPES[m][1] // BS) + q for r in range(rows) for m in members for q in range(SHAPES[m][1] // BS)]


def tall_order(members):
    starts = block_offsets()
    return [starts[m] + i for m in members for i in range(SHAPES[m][0] // BS * (SHAPES[m][1] // BS))]


def all_orders():
    return [wide_order(WIDE_IN), tall_order(TALL_OUT), wide_order(WIDE_FF), tall_order(TALL_FF)]


def unpack_vectors(flat):
    result, offset = [], 0
    for count in SIZES:
        result.append(flat[offset : offset + count])
        offset += count
    return result


def dot(left, right, precision=None):
    return jnp.dot(left, right, preferred_element_type=F32, precision=precision)


def dot_nt(left, right):
    return lax.dot_general(left, right, (((1,), (1,)), ((), ())), preferred_element_type=F32)


def dot_tn(left, right):
    return lax.dot_general(left, right, (((0,), (0,)), ((), ())), preferred_element_type=F32)


def sigmoid(v):
    return 1.0 / (1.0 + jnp.exp(-v))


def rms_scale(values):
    return lax.rsqrt(jnp.mean(values * values, axis=-1, keepdims=True) + EPS)


def kernel_params(**more):
    return pltpu.CompilerParams(vmem_limit_bytes=VMEM_MOST, **more)


def whole(shape):
    return pl.BlockSpec(shape, lambda *_: (0,) * len(shape))


MESH = pl.DeviceIdType.MESH
CORES = 2
PIECES = 3
APART = 5 / 16


def grid_of(mesh):
    try:
        wide = len({device.coords[0] for device in mesh.devices.flat})
    except AttributeError:
        wide = mesh.shape["seq"] // CORES
    return wide, mesh.shape["seq"] // CORES, mesh.shape["dp"] // wide


def parts_of(slots, tall):
    half = slots // CORES
    size = half // PIECES
    lone = round(size * APART) if tall == 2 and size >= 8 else 0
    return half, size, lone, size - lone


def place(grid):
    wide, tall, deep = grid
    dp, seq = lax.axis_index("dp"), lax.axis_index("seq")
    return dp % wide, seq // CORES, dp // wide, seq % CORES


def gather_kernel(grid, slots, master, tokens, cotangent, docs, out, rows, given, labels, wide_own, src, bounce,
                  sem_own, sem_load, sz, rz, sx, rx, sy, ry, sc, rc, s_rows, r_rows, s_docs, r_docs):
    wide, tall, deep = grid
    x, y, z, c = place(grid)
    half, size, lone, bulk = parts_of(slots, tall)
    me = z * wide + x
    seq = y * CORES + c
    base = c * half
    bulk_at = y * (size - bulk)
    lone_at = y * bulk
    other_at = (1 - y) * bulk if lone else 0
    mate = y * CORES + (1 - c)
    over = (tall - 1 - y) * CORES + c
    peers = tall * CORES
    micro = tokens.shape[0]
    each = peers // micro

    loads = []
    for k in range(CORES):
        part = pl.ds(((c + k) % CORES) * half, half)
        loads.append((part, pltpu.make_async_copy(master.at[part], wide_own.at[part], sem_load.at[k])))
        loads[-1][1].start()

    barrier = pltpu.get_barrier_semaphore()
    count = jnp.int32(0)
    for step_by, at, length in ((wide, z, deep), (1, x, wide)):
        for step in (1, -1):
            ok = (at + step >= 0) & (at + step < length)
            there = me + step * step_by

            @pl.when(ok)
            def _(there=there):
                pl.semaphore_signal(barrier, inc=1, device_id=(there, seq), device_id_type=MESH)

            count = count + ok.astype(jnp.int32)
    for k in range(1, peers):
        pl.semaphore_signal(barrier, inc=1, device_id=(me, (seq + k) % peers), device_id_type=MESH)
    pl.semaphore_wait(barrier, count + (peers - 1))
    both = ((0, 1), (1, -1))
    yes = jnp.bool_(True)

    def piece(shard, at, length):
        return out.at[shard, pl.ds(at, length)]

    def run(begin_it):
        def send(ok, source, target, send_sem, recv_sem, device):
            copy = pltpu.make_async_remote_copy(
                src_ref=source, dst_ref=target, send_sem=send_sem, recv_sem=recv_sem,
                device_id=device, device_id_type=MESH,
            )

            @pl.when(ok)
            def _():
                if begin_it:
                    copy.start()
                else:
                    copy.wait_send()

        def arrived(ok, target, recv_sem):
            if begin_it:
                copy = pltpu.make_async_remote_copy(
                    src_ref=target, dst_ref=target, send_sem=sem_own.at[0], recv_sem=recv_sem,
                    device_id=(me, seq), device_id_type=MESH,
                )

                @pl.when(ok)
                def _():
                    copy.wait_recv()

        def pass_on(ok, shard, sub):
            at = base + sub * size
            mine = piece(shard, at + bulk_at, bulk)
            send(ok, mine, mine, sc.at[0, shard, sub], rc.at[0, shard, sub], (me, mate))
            if lone:
                mine = piece(shard, at + lone_at, lone)
                send(ok, mine, mine, sy.at[shard, sub], ry.at[shard, sub], (me, over))

        def along_x(ok, zs, dirs, hop, sub, own):
            for d, step in dirs:
                shard = zs * wide + x - step * hop
                go = ok & (x + step >= 0) & (x + step < wide)
                at = base + sub * size + bulk_at
                source = src.at[pl.ds(at, bulk)] if own else piece(shard, at, bulk)
                send(go, source, piece(shard, at, bulk), sx.at[d, hop, zs, sub], rx.at[d, hop + 1, zs, sub], (me + step, seq))

        def columns(s):
            return [(yes, z)] if s == 0 else [((z - step * s >= 0) & (z - step * s < deep), z - step * s) for _, step in both]

        def x_in(s, hop, sub):
            for ok, zs in columns(s):
                for d, step in both:
                    from_x = x - step * hop
                    come = ok & (from_x >= 0) & (from_x < wide)
                    shard = zs * wide + from_x
                    arrived(come, piece(shard, base + sub * size + bulk_at, bulk), rx.at[d, hop, zs, sub])
                    along_x(come, zs, ((d, step),), hop, sub, False)
                    pass_on(come, shard, sub)

        def y_in(ok, shard, sub):
            if lone:
                mine = piece(shard, base + sub * size + other_at, lone)
                arrived(ok, mine, ry.at[shard, sub])
                send(ok, mine, mine, sc.at[1, shard, sub], rc.at[1, shard, sub], (me, mate))

        def y_all(s, sub):
            for ok, zs in columns(s):
                if s > 0:
                    y_in(ok, zs * wide + x, sub)
                for hop in range(1, wide):
                    for _, step in both:
                        from_x = x - step * hop
                        y_in(ok & (from_x >= 0) & (from_x < wide), zs * wide + from_x, sub)

        def z_step(s, sub):
            for d, step in both:
                zs = z - step * s
                ok = (zs >= 0) & (zs < deep)
                shard = zs * wide + x
                at = base + sub * size + bulk_at
                mine = piece(shard, at, bulk)
                if s:
                    arrived(ok, mine, rz.at[d, s, sub])
                go = ok & (z + step >= 0) & (z + step < deep)
                source = mine if s else src.at[pl.ds(at, bulk)]
                if s + 1 < deep:
                    send(go, source, mine, sz.at[d, s, sub], rz.at[d, s + 1, sub], (me + step * wide, seq))
                if s:
                    along_x(ok, zs, both, 0, sub, False)
                    pass_on(ok, shard, sub)
            if s == 0:
                along_x(yes, z, both, 0, sub, True)

        for s in range(deep):
            def one(sub, _, s=s):
                z_step(s, sub)
                if s:
                    for hop in range(1, wide):
                        x_in(s - 1, hop, sub)
                if s >= 2:
                    y_all(s - 2, sub)
                return 0

            lax.fori_loop(0, PIECES, one, 0)
            if s == 0:
                local(begin_it, send, arrived)

        def last_x(sub, _):
            for hop in range(1, wide):
                x_in(deep - 1, hop, sub)
            if deep > 1:
                y_all(deep - 2, sub)
            return 0

        def last_y(sub, _):
            y_all(deep - 1, sub)
            return 0

        lax.fori_loop(0, PIECES, last_x, 0)
        lax.fori_loop(0, PIECES, last_y, 0)

    def convert(k):
        part, copy = loads[k]
        copy.wait()
        base_at = ((c + k) % CORES) * half

        def one(i, _):
            src[base_at + i] = wide_own[base_at + i].astype(src.dtype)
            return 0

        lax.fori_loop(0, half, one, 0, unroll=2)

    keep = pltpu.make_async_copy(src, out.at[me], sem_load.at[0])
    at_home = []
    for t in range(micro):
        m = (seq + t) % micro
        there = m * each + seq // micro
        for k, (source, target) in enumerate(((tokens, rows), (cotangent, given))):
            place_to = target.at[seq % micro]
            take = pltpu.make_async_copy(source.at[m], bounce.at[k], sem_own.at[k])
            put = pltpu.make_async_copy(bounce.at[k], place_to, sem_own.at[k])
            at_home.append((there == seq, take, put))

    def local(begin_it, send, arrived):
        for t in range(micro):
            m = (seq + t) % micro
            there = m * each + seq // micro
            for k, (source, target) in enumerate(((tokens, rows), (cotangent, given))):
                send(there != seq, source.at[m], target.at[seq % micro], s_rows.at[k, t], r_rows.at[k, seq % micro], (me, there))
        if begin_it:
            labels[seq] = docs[...]
        for k in range(1, peers):
            send(yes, docs, labels.at[seq], s_docs.at[k], r_docs.at[seq], (me, (seq + k) % peers))
        if begin_it:
            for ok, take, _ in at_home:
                @pl.when(ok)
                def _(take=take):
                    take.start()
            convert(1)
            keep.start()
            for ok, take, put in at_home:
                @pl.when(ok)
                def _(take=take, put=put):
                    take.wait()
                    put.start()

    convert(0)
    run(True)
    keep.wait()
    for ok, take, put in at_home:
        @pl.when(ok)
        def _(put=put):
            put.wait()

    def came(ok, target, recv_sem):
        @pl.when(ok)
        def _():
            pltpu.make_async_remote_copy(
                src_ref=target, dst_ref=target, send_sem=sem_own.at[0], recv_sem=recv_sem,
                device_id=(me, seq), device_id_type=MESH,
            ).wait_recv()

    for q in range(micro):
        source = seq % each * micro + q
        for k, target in enumerate((rows, given)):
            came(source != seq, target.at[q], r_rows.at[k, q])
    for k in range(1, peers):
        source = (seq + k) % peers
        came(yes, labels.at[source], r_docs.at[source])

    def last(i, _):
        shard, sub = i // PIECES, i % PIECES
        at = (1 - c) * half + sub * size
        came(shard != me, piece(shard, at + bulk_at, bulk), rc.at[0, shard, sub])
        if lone:
            came(shard != me, piece(shard, at + other_at, lone), rc.at[1, shard, sub])
        return 0

    lax.fori_loop(0, wide * deep * PIECES, last, 0)
    run(False)


def gather_blocks(grid, master, tokens, cotangent, docs):
    wide, tall, deep = grid
    slots = master.shape[0]
    n = wide * deep
    peers = tall * CORES
    micro = tokens.shape[0]
    low = tokens.dtype
    sem = pltpu.SemaphoreType.DMA
    hbm = pl.BlockSpec(memory_space=pl.ANY)
    vmem = pl.BlockSpec(memory_space=pltpu.VMEM)
    return pl.pallas_call(
        functools.partial(gather_kernel, grid, slots),
        out_shape=(
            jax.ShapeDtypeStruct((n,) + master.shape, low),
            jax.ShapeDtypeStruct(tokens.shape, low), jax.ShapeDtypeStruct(tokens.shape, low),
            jax.ShapeDtypeStruct((peers,) + docs.shape, docs.dtype),
        ),
        in_specs=[hbm, hbm, hbm, vmem],
        out_specs=(hbm, hbm, hbm, vmem),
        scratch_shapes=[
            pltpu.VMEM(master.shape, master.dtype), pltpu.VMEM(master.shape, low), pltpu.VMEM((2,) + tokens.shape[1:], low),
            sem((2,)), sem((CORES,)),
            sem((2, deep, PIECES)), sem((2, deep + 1, PIECES)),
            sem((2, wide, deep, PIECES)), sem((2, wide + 1, deep, PIECES)),
            sem((n, PIECES)), sem((n, PIECES)),
            sem((2, n, PIECES)), sem((2, n, PIECES)),
            sem((2, micro)), sem((2, micro)), sem((peers,)), sem((peers,)),
        ],
        compiler_params=pltpu.CompilerParams(collective_id=0, has_side_effects=True, vmem_limit_bytes=60 << 20),
        name="gather_blocks",
    )(master, tokens, cotangent, docs)

def far_first(at, size, i):
    above, below = size - 1 - at, at
    less, more = jnp.minimum(above, below), jnp.maximum(above, below)
    long_side = jnp.where(above >= below, 1, -1)
    j = i - (more - less)
    near = at + jnp.where(j % 2 == 0, 1, -1) * (less - j // 2)
    return jnp.where(j < 0, at + long_side * (more - i), near)


def entry(at, size, source_below, target):
    lower = jnp.where(at > 0, size - at, 0) if size > 2 else 0
    return target - at if source_below else lower + at - target


def entries(size):
    return size + 1 if size > 2 else 1

SUBS = 3
LONE = 5 / 16
RING = 6
STAGED = 3
LATE_ADD, LATE_X, LATE_Z, PER_HOP = 1, 3, 6, 3
CHUNK = 512
HELD = 12


def split_of(slots, tall):
    half = slots // CORES
    piece = half // SUBS
    lone = round(piece * LONE) if tall == 2 and piece >= 8 else 0
    return half, piece, lone, piece - lone


def reduce_kernel(grid, slots, widths, left_at, right_at, vec, *refs):
    wide, tall, deep = grid
    count = sum(len(w) for w in widths)
    arrays = refs[:count]
    (out, vec_out, turned, right, held, acc, stage, land_c, land_y, land_x, land_z, fin, vbuf, vland,
     s_left, s_right, s_c, r_c, s_y, r_y, s_x, r_x, s_z, r_z, s_f, r_f, s_m, r_m, s_v, r_v, free) = refs[count:]
    n = wide * deep
    x, y, z, c = place(grid)
    half, size, lone, bulk = split_of(slots, tall)
    me = z * wide + x
    seq = y * CORES + c
    mate = y * CORES + (1 - c)
    bulk_at = y * lone
    lone_at = y * bulk
    other_at = (1 - y) * bulk
    bits = lambda length: [1 << b for b in range(length.bit_length() - 1)]
    partners = [(me, mate)]
    partners += [(me, (y ^ b) * CORES + c) for b in bits(tall)]
    partners += [(z * wide + (x ^ b), seq) for b in bits(wide)]
    partners += [((z ^ b) * wide + x, seq) for b in bits(deep)]
    rounds = len(partners)

    chunks, k, at = [], 0, 0
    for width in widths[0]:
        for q in range(0, width, CHUNK):
            chunks.append((k, q, at + q))
        k, at = k + 1, at + width

    def chunk_copy(i):
        k, q, _ = chunks[i]
        return pltpu.make_async_copy(arrays[k].at[:, pl.ds(q, CHUNK)], held.at[i % HELD], s_left.at[i % HELD])

    ahead = min(HELD, len(chunks))
    for i in range(ahead):
        chunk_copy(i).start()
    copies, at = [], 0
    for width in widths[1]:
        def one(q, _, k=k, at=at):
            cols = pl.ds(pl.multiple_of(q * BS, BS), BS)
            pltpu.make_async_copy(arrays[k].at[:, cols], right.at[at + q], s_right.at[k - len(widths[0])]).start()
            return 0

        lax.fori_loop(0, width // BS, one, 0)
        part = right.at[pl.ds(at, width // BS)]
        copies.append(pltpu.make_async_copy(part, part, s_right.at[k - len(widths[0])]))
        k, at = k + 1, at + width // BS

    barrier = pltpu.get_barrier_semaphore()
    awaited = jnp.int32(0)
    for step_by, at, length in ((wide, z, deep), (1, x, wide)):
        for step in (1, -1):
            ok = (at + step >= 0) & (at + step < length)

            @pl.when(ok)
            def _(there=me + step * step_by):
                pl.semaphore_signal(barrier, inc=1, device_id=(there, seq), device_id_type=MESH)

            awaited = awaited + ok.astype(jnp.int32)
    for device in partners:
        pl.semaphore_signal(barrier, inc=1, device_id=device, device_id_type=MESH)
    pl.semaphore_wait(barrier, awaited + rounds)

    def remote(source, target, send_sem, recv_sem, device):
        return pltpu.make_async_remote_copy(
            src_ref=source, dst_ref=target, send_sem=send_sem, recv_sem=recv_sem,
            device_id=device, device_id_type=MESH,
        )

    def landed(target, recv_sem):
        remote(target, target, s_left.at[0], recv_sem, (me, seq)).wait_recv()

    def vec_copy(t):
        return remote(vbuf.at[t], vland.at[t], s_v.at[t], r_v.at[t], partners[t])

    vbuf[0] = vec[...]
    vec_copy(0).start()
    for i in range(len(chunks)):
        chunk_copy(i).wait()
        for q in range(0, CHUNK, BS):
            turned[(chunks[i][2] + q) // BS] = held[i % HELD, :, q : q + BS].T
        if i + HELD < len(chunks):
            chunk_copy(i + HELD).start()
    for copy in copies:
        copy.wait()

    group = wide * SUBS
    total = n * SUBS

    def item_of(k):
        xs = far_first(x, wide, k % wide)
        zs = far_first(z, deep, k // group)
        sub = (k // wide) % SUBS
        return xs, zs, sub, (zs * wide + xs) * SUBS + sub

    def swap(k):
        return remote(stage.at[k % STAGED], land_c.at[k % RING], s_c.at[k % STAGED], r_c.at[k % RING], (me, mate))

    def cross(item):
        return remote(acc.at[item, pl.ds(other_at, lone)], land_y.at[item], s_y.at[item], r_y.at[item], (me, (tall - 1 - y) * CORES + c))

    def grads(k, core, ref, first):
        xs, zs, sub, item = item_of(k)
        base = (zs * wide + xs) * slots + core * half + sub * size

        def one(i, _):
            ref[first, i] = dot(turned[left_at[base + i]], right[right_at[base + i]]).astype(ref.dtype)
            return 0

        lax.fori_loop(0, size, one, 0, unroll=min(4, size))

    def add(item, at, length, ref, first):
        def one(i, _):
            acc[item, at + i] = acc[item, at + i] + ref[first + (i,)]
            return 0

        lax.fori_loop(0, length, one, 0, unroll=min(3, length))

    def step_x(k, begin_it):
        xs, zs, sub, item = item_of(k)
        for below, step in ((True, 1), (False, -1)):
            to = entry(x + step, wide, below, xs)
            sent = remote(acc.at[item, pl.ds(bulk_at, bulk)], land_x.at[to, zs * SUBS + sub], s_x.at[item],
                          r_x.at[to, zs * SUBS + sub], (me + step, seq))

            @pl.when((xs - x) * step > 0)
            def _():
                if begin_it:
                    sent.start()
                else:
                    sent.wait_send()

    def take_x(k):
        xs, zs, sub, item = item_of(k)
        for below, step in ((True, 1), (False, -1)):
            comes = ((xs - x) * step >= 0) & (x - step >= 0) & (x - step < wide)
            at = entry(x, wide, below, xs)

            @pl.when(comes)
            def _():
                landed(land_x.at[at, zs * SUBS + sub], r_x.at[at, zs * SUBS + sub])
                add(item, bulk_at, bulk, land_x, (at, zs * SUBS + sub))

    def step_z(k, begin_it):
        xs, zs, sub, item = item_of(k)
        for below, step in ((True, 1), (False, -1)):
            to = entry(z + step, deep, below, zs)
            sent = remote(acc.at[item, pl.ds(bulk_at, bulk)], land_z.at[to, sub], s_z.at[zs * SUBS + sub], r_z.at[to, sub],
                          (me + step * wide, seq))

            @pl.when((zs - z) * step > 0)
            def _():
                if begin_it:
                    sent.start()
                else:
                    sent.wait_send()

    def take_z(k):
        xs, zs, sub, item = item_of(k)
        for below, step in ((True, 1), (False, -1)):
            comes = ((zs - z) * step >= 0) & (z - step >= 0) & (z - step < deep)
            at = entry(z, deep, below, zs)

            @pl.when(comes)
            def _():
                landed(land_z.at[at, sub], r_z.at[at, sub])
                add(item, bulk_at, bulk, land_z, (at, sub))

    planes = bits(tall)

    def swap_plane(t, sub):
        mine = pl.ds(bulk_at, bulk)
        return remote(acc.at[me * SUBS + sub, mine], fin.at[t, sub, mine], s_f.at[t, sub], r_f.at[t, sub], (me, (y ^ planes[t]) * CORES + c))

    def take_plane(t, sub):
        item = me * SUBS + sub
        theirs = pl.ds((1 - y) * lone if lone else 0, bulk)
        landed(fin.at[t, sub, theirs], r_f.at[t, sub])
        swap_plane(t, sub).wait_send()
        add(item, lone, size - 2 * lone, fin.at[t, sub, pl.ds(lone, size - 2 * lone)], ())
        if lone:
            cross(item).wait_send()
            acc[item, pl.ds(other_at, lone)] = fin[t, sub, pl.ds(other_at, lone)]

    def swap_core(sub):
        return remote(acc.at[me * SUBS + sub], out.at[pl.ds(c * half + sub * size, size)], s_m.at[sub], r_m.at[sub], (me, mate))

    late_z = LATE_Z + PER_HOP * jnp.minimum(z, deep - 1 - z)

    def turn_of(k, _):
        @pl.when(k < total)
        def _():
            @pl.when(k >= STAGED)
            def _():
                swap(k - STAGED).wait_send()

            grads(k, 1 - c, stage, k % STAGED)

            @pl.when(k >= RING)
            def _():
                pl.semaphore_wait(free, 1)

            swap(k).start()
            grads(k, c, acc, item_of(k)[3])

        for t in range(1, rounds + 1):
            @pl.when(k == t)
            def _(t=t):
                landed(vland.at[t - 1], r_v.at[t - 1])
                vbuf[t] = vbuf[t - 1] + vland[t - 1]
                if t < rounds:
                    vec_copy(t).start()
                else:
                    vec_out[...] = vbuf[t]

        b = k - LATE_ADD

        @pl.when((b >= 0) & (b < total))
        def _():
            item = item_of(b)[3]
            landed(land_c.at[b % RING], r_c.at[b % RING])
            add(item, 0, size, land_c, (b % RING,))

            @pl.when(b < total - RING)
            def _():
                pl.semaphore_signal(free, inc=1, device_id=(me, mate), device_id_type=MESH)

            if lone:
                cross(item).start()

        b = k - LATE_X

        @pl.when((b >= 0) & (b < total))
        def _():
            item = item_of(b)[3]
            if lone:
                landed(land_y.at[item], r_y.at[item])
                add(item, lone_at, lone, land_y, (item,))
            if wide > 2:
                @pl.when(item_of(b)[0] != x)
                def _():
                    take_x(b)
            step_x(b, True)

        b = k - late_z

        @pl.when((b >= 0) & (b < total) & (b % wide == wide - 1))
        def _():
            take_x(b)
            take_z(b)
            step_z(b, True)
            if planes:
                @pl.when(item_of(b)[1] == z)
                def _():
                    swap_plane(0, item_of(b)[2]).start()

        return 0

    lax.fori_loop(0, total + LATE_Z + PER_HOP * ((deep - 1) // 2), turn_of, 0)

    def finish(k, _):
        if lone:
            item = item_of(k)[3]

            @pl.when(item // SUBS != me)
            def _():
                cross(item).wait_send()

        step_x(k, False)

        @pl.when(k % wide == wide - 1)
        def _():
            step_z(k, False)

        return 0

    for t in range(len(planes)):
        for sub in range(SUBS):
            if t:
                swap_plane(t, sub).start()
        for sub in range(SUBS):
            take_plane(t, sub)
            if t == len(planes) - 1:
                swap_core(sub).start()
                out[pl.ds(c * half + sub * size, size)] = acc[me * SUBS + sub]
    lax.fori_loop(0, total, finish, 0)
    for k in range(max(total - STAGED, 0), total):
        swap(k).wait_send()
    for t in range(rounds):
        vec_copy(t).wait_send()
    for sub in range(SUBS):
        swap_core(sub).wait_send()
        landed(out.at[pl.ds((1 - c) * half + sub * size, size)], r_m.at[sub])


def reduce_blocks(grid, slots, left_at, right_at, lefts, rights, vec):
    wide, tall, deep = grid
    n = wide * deep
    half, size, lone, bulk = split_of(slots, tall)
    tile = (BS, BS)
    low = lefts[0].dtype
    tokens = lefts[0].shape[0]
    widths = [[a.shape[1] for a in lefts], [a.shape[1] for a in rights]]
    sem = pltpu.SemaphoreType.DMA
    rounds = sum(length.bit_length() - 1 for length in (CORES, wide, tall, deep))
    planes = max(tall.bit_length() - 1, 1)
    items = n * SUBS
    buf = lambda *lead: pltpu.VMEM(lead + tile, low)
    smem, vmem, hbm = (pl.BlockSpec(memory_space=m) for m in (pltpu.SMEM, pltpu.VMEM, pl.ANY))
    return pl.pallas_call(
        functools.partial(reduce_kernel, grid, slots, widths),
        out_shape=(jax.ShapeDtypeStruct((slots,) + tile, low), jax.ShapeDtypeStruct(vec.shape, vec.dtype)),
        in_specs=[smem, smem, vmem] + [hbm] * (len(lefts) + len(rights)),
        out_specs=(vmem, vmem),
        scratch_shapes=[
            pltpu.VMEM((sum(widths[0]) // BS, BS, tokens), low), pltpu.VMEM((sum(widths[1]) // BS, tokens, BS), low), pltpu.VMEM((HELD, tokens, CHUNK), low),
            buf(items, size), buf(STAGED, size), buf(RING, size), buf(items, max(lone, 1)), buf(entries(wide), deep * SUBS, bulk),
            buf(entries(deep), SUBS, bulk), buf(planes, SUBS, size),
            pltpu.VMEM((rounds + 1,) + vec.shape, vec.dtype), pltpu.VMEM((rounds,) + vec.shape, vec.dtype),
            sem((HELD,)), sem((len(rights),)), sem((STAGED,)), sem((RING,)), sem((items,)), sem((items,)), sem((items,)),
            sem((entries(wide), deep * SUBS)), sem((deep * SUBS,)), sem((entries(deep), SUBS)),
            sem((planes, SUBS)), sem((planes, SUBS)), sem((SUBS,)), sem((SUBS,)), sem((rounds,)), sem((rounds,)),
            pltpu.SemaphoreType.REGULAR,
        ],
        compiler_params=pltpu.CompilerParams(collective_id=1, has_side_effects=True, vmem_limit_bytes=63 << 20),
        name="reduce_blocks",
    )(left_at, right_at, vec, *lefts, *rights)


BLOCK = 256
HALO = 8


def lane_index(shape):
    return lax.broadcasted_iota(jnp.int32, shape, len(shape) - 1)


def conv_tile(extended, taps, marks, count):
    total = jnp.broadcast_to(taps[KERNEL : KERNEL + 1, :], (count, extended.shape[1]))
    for tap in range(KERNEL):
        total = total + taps[tap : tap + 1, :] * near_rows(extended, tap, count) * marks[:, tap : tap + 1]
    return total


def near_rows(extended, tap, count):
    back = REACH - tap
    moved = pltpu.roll(extended, back, 0) if back else extended
    return moved[HALO : HALO + count, :]


def softplus(v):
    return jnp.maximum(v, 0.0) + jnp.log(1.0 + jnp.exp(-jnp.abs(v)))


def chunk_decays(raw, params):
    delta = softplus(raw + params[0:1, :])
    decay = -delta * jnp.exp(params[1:2, :])
    block = raw.shape[0] if raw.shape[0] < BLOCK else BLOCK
    rows = lax.broadcasted_iota(jnp.int32, (block, block), 0)
    lower = (rows >= lane_index((block, block))).astype(F32)
    sums = [dot(lower, decay[i : i + block, :], HIGHEST) for i in range(0, raw.shape[0], block)]
    return delta, decay, jnp.concatenate(sums, axis=0)


def end_weights(delta, sums, marks):
    last = sums[-1:, :]
    return jnp.exp(last - sums) * delta * marks[:, 5:6], jnp.exp(last) * marks[-1:, 4:5]


def spread_matrix():
    rows = lax.broadcasted_iota(jnp.int32, (LANES, INNER), 0)
    return (rows == lane_index((LANES, INNER)) // HEAD).astype(F32)


def mix_first_kernel(proj_x, proj_bc, halo, taps, params, raw, marks, xbc, decays, decays_t, state, factor):
    tokens = raw.shape[0]
    mark = marks[...]
    for ref, at in ((proj_x, 0), (proj_bc, INNER)):
        step = 256
        for q in range(0, ref.shape[1], step):
            cols = slice(at + q, at + q + step)
            own = ref[:, q : q + step].astype(F32)
            extended = jnp.concatenate([halo[:, cols].astype(F32), own], axis=0)
            value = conv_tile(extended, taps[:, cols], mark, tokens)
            xbc[:, cols] = (value * sigmoid(value)).astype(BF16)
    delta, decay, sums = chunk_decays(raw[...], params[...])
    decays[0] = delta
    decays[1] = sums
    for i in range(tokens // BLOCK):
        decays_t[i] = sums[i * BLOCK : (i + 1) * BLOCK].T
    spread = spread_matrix()
    total = jnp.zeros((NSTATE, INNER), F32)
    product = jnp.ones((1, LANES), F32)
    for i in range(0, tokens, BLOCK):
        rows = slice(i, i + BLOCK)
        weight, own = end_weights(delta[rows], sums[rows], mark[rows])
        weighted = (xbc[rows, :INNER].astype(F32) * dot(weight.astype(BF16), spread.astype(BF16))).astype(BF16)
        keep = dot(jnp.broadcast_to(own, (8, LANES)), spread, HIGHEST)[0:1]
        total = keep * total + dot_tn(xbc[rows, INNER : INNER + NSTATE], weighted)
        product = product * own
    state[...] = total.astype(BF16)
    factor[...] = jnp.broadcast_to(product, factor.shape)


def mix_first(proj, halo, taps, params, raw, marks):
    tokens = raw.shape[0]
    vmem = pl.BlockSpec(memory_space=pltpu.VMEM)
    return pl.pallas_call(
        mix_first_kernel,
        out_shape=(
            jax.ShapeDtypeStruct((tokens, CHANNELS), BF16),
            jax.ShapeDtypeStruct((2, tokens, LANES), F32),
            jax.ShapeDtypeStruct((tokens // BLOCK, LANES, BLOCK), F32),
            jax.ShapeDtypeStruct((NSTATE, INNER), BF16),
            jax.ShapeDtypeStruct((8, LANES), F32),
        ),
        grid=(1,),
        in_specs=[
            pl.BlockSpec((tokens, INNER), lambda i: (0, 1)),
            pl.BlockSpec((tokens, 2 * NSTATE), lambda i: (0, 2 * INNER // (2 * NSTATE))),
            vmem, vmem, vmem, vmem, vmem,
        ],
        out_specs=(vmem,) * 5,
        compiler_params=kernel_params(),
        name="mix_first",
    )(proj, proj, halo, taps, params, raw, marks)


def attend(left, right, mark_rows, mark_cols):
    return jnp.where(mark_rows & mark_cols, dot_nt(left, right), 0.0)


def halves(tile):
    low = lane_index(tile.shape) < HEAD
    zero = jnp.zeros_like(tile)
    return jnp.where(low, tile, zero), jnp.where(low, zero, tile)


def pair_column(values, a):
    return values[:, a * HEAD : a * HEAD + 1]


def mix_second_kernel(x, b, c, z, decays, decays_t, marks, labels, incoming, skip, gain, y, normed, states,
                      wide_sums, wide_delta, wide_end, keep, near, b_t, state, gated, squares):
    j = pl.program_id(0)
    tokens = x.shape[0]
    blocks = tokens // BLOCK
    cols = pl.ds(pl.multiple_of(j * LANES, LANES), LANES)

    @pl.when(j == 0)
    def _():
        spread = spread_matrix()
        rows = lax.broadcasted_iota(jnp.int32, (BLOCK, BLOCK), 0)
        ordered = rows >= lane_index((BLOCK, BLOCK))
        for i in range(blocks):
            at = slice(i * BLOCK, (i + 1) * BLOCK)
            mark = marks[at]
            same = mark[:, 6:7] == labels[0:1, at]
            near[i] = jnp.where(ordered & same, dot_nt(c[at], b[at]), 0.0)
            b_t[i] = b[at].T
            weight, own = end_weights(decays[0, at], decays[1, at], mark)
            wide_end[at] = dot(weight.astype(BF16), spread.astype(BF16)).astype(BF16)
            wide_sums[at] = dot(decays[1, at], spread, HIGHEST)
            wide_delta[at] = dot(decays[0, at].astype(BF16), spread.astype(BF16)).astype(BF16)
            keep[i] = dot(jnp.broadcast_to(own, (8, LANES)), spread, HIGHEST)
        squares[...] = jnp.zeros_like(squares)

    state[...] = incoming[...].astype(F32)
    for i in range(blocks):
        at = slice(i * BLOCK, (i + 1) * BLOCK)
        states[i] = state[...]
        tile = x[at].astype(F32)
        scaled = (tile * wide_delta[at, cols].astype(F32)).astype(BF16)
        sums = wide_sums[at, cols]
        total = jnp.zeros((BLOCK, LANES), F32)
        for a, part in enumerate(halves(scaled)):
            row = decays_t[i, pl.ds(2 * j + a, 1), :]
            weight = near[i] * jnp.exp(jnp.minimum(pair_column(sums, a) - row, 0.0))
            total = total + dot(weight.astype(BF16), part)
        carried = dot(c[at], state[...].astype(BF16))
        total = total + carried * jnp.exp(sums) * marks[at, 4:5] + skip[0:1, cols] * tile
        y[at] = total
        gate = z[at].astype(F32)
        gate = total * gate * sigmoid(gate)
        gated[at, cols] = gate
        squares[at] += gate * gate
        weighted = (tile * wide_end[at, cols].astype(F32)).astype(BF16)
        state[...] = keep[i, 0:1, cols] * state[...] + dot(b_t[i], weighted)
    states[blocks] = state[...]

    @pl.when(j == PAIRS - 1)
    def _():
        for i in range(blocks):
            at = slice(i * BLOCK, (i + 1) * BLOCK)
            scale = lax.rsqrt(jnp.sum(squares[at], axis=1, keepdims=True) / INNER + EPS)
            normed[at] = (gated[at] * scale * gain[0:1, :]).astype(BF16)


def mix_second(xbc, proj, decays, decays_t, marks, labels, incoming, skip, gain):
    tokens = xbc.shape[0]
    blocks = tokens // BLOCK
    tile = pl.BlockSpec((tokens, LANES), lambda j: (0, j))
    return pl.pallas_call(
        mix_second_kernel,
        out_shape=(
            jax.ShapeDtypeStruct((tokens, INNER), F32),
            jax.ShapeDtypeStruct((tokens, INNER), BF16),
            jax.ShapeDtypeStruct((blocks + 1, NSTATE, INNER), F32),
        ),
        grid=(PAIRS,),
        in_specs=[
            tile,
            pl.BlockSpec((tokens, NSTATE), lambda j: (0, INNER // NSTATE)),
            pl.BlockSpec((tokens, NSTATE), lambda j: (0, INNER // NSTATE + 1)),
            tile,
            whole(decays.shape), whole(decays_t.shape), whole(marks.shape), whole(labels.shape),
            pl.BlockSpec((NSTATE, LANES), lambda j: (0, j)),
            whole(skip.shape), whole(gain.shape),
        ],
        out_specs=(tile, whole((tokens, INNER)), pl.BlockSpec((blocks + 1, NSTATE, LANES), lambda j: (0, 0, j))),
        scratch_shapes=[
            pltpu.VMEM((tokens, INNER), F32), pltpu.VMEM((tokens, INNER), BF16), pltpu.VMEM((tokens, INNER), BF16),
            pltpu.VMEM((blocks, 8, INNER), F32), pltpu.VMEM((blocks, BLOCK, BLOCK), F32),
            pltpu.VMEM((blocks, NSTATE, BLOCK), BF16), pltpu.VMEM((NSTATE, LANES), F32),
            pltpu.VMEM((tokens, INNER), F32), pltpu.VMEM((tokens, LANES), F32),
        ],
        compiler_params=kernel_params(),
        name="mix_second",
    )(xbc, xbc, xbc, proj, decays, decays_t, marks, labels, incoming, skip, gain)


def gate_back_kernel(grad, y, z, gain, c, decays, marks, g_y, g_z, g_gain, g_state):
    step = pl.program_id(0)
    value, gate = y[...], z[...].astype(F32)
    opened = sigmoid(gate)
    swish = gate * opened
    gated = value * swish
    scale = lax.rsqrt(jnp.mean(gated * gated, axis=1, keepdims=True) + EPS)
    unit = gated * scale
    given = grad[...].astype(F32)
    scaled = given * gain[0:1, :]
    g_gated = scale * (scaled - unit * jnp.mean(scaled * unit, axis=1, keepdims=True))
    fresh = g_gated * swish
    g_y[...] = fresh.astype(BF16)
    g_z[...] = (g_gated * value * (opened + swish * (1.0 - opened))).astype(BF16)
    spread = spread_matrix()
    sums = decays[1]
    mark = marks[...]
    entry_weight = jnp.exp(sums) * mark[:, 4:5]
    own = jnp.exp(sums[-1:, :]) * mark[-1:, 4:5]
    keep = dot(jnp.broadcast_to(own, (8, LANES)), spread, HIGHEST)[0:1]
    weighted = (fresh * dot(entry_weight.astype(BF16), spread.astype(BF16))).astype(BF16)
    local = dot_tn(c[...], weighted)
    gains = jnp.sum(given * unit, axis=0, keepdims=True)

    @pl.when(step == 0)
    def _():
        g_state[...] = local
        g_gain[...] = gains

    @pl.when(step > 0)
    def _():
        g_state[...] = keep * g_state[...] + local
        g_gain[...] += gains


def gate_back(grad, y, proj, gain, xbc, decays, marks):
    tokens = y.shape[0]
    blocks = tokens // BLOCK
    rows = lambda width, col: pl.BlockSpec((BLOCK, width), lambda i: (blocks - 1 - i, col))
    return pl.pallas_call(
        gate_back_kernel,
        out_shape=(
            jax.ShapeDtypeStruct((tokens, INNER), BF16),
            jax.ShapeDtypeStruct((tokens, INNER), BF16),
            jax.ShapeDtypeStruct((1, INNER), F32),
            jax.ShapeDtypeStruct((NSTATE, INNER), F32),
        ),
        grid=(blocks,),
        in_specs=[
            rows(INNER, 0), rows(INNER, 0), rows(INNER, 0), whole(gain.shape), rows(NSTATE, INNER // NSTATE + 1),
            pl.BlockSpec((2, BLOCK, LANES), lambda i: (0, blocks - 1 - i, 0)), rows(LANES, 0),
        ],
        out_specs=(rows(INNER, 0), rows(INNER, 0), whole((1, INNER)), whole((NSTATE, INNER))),
        compiler_params=kernel_params(),
        name="gate_back",
    )(grad, y, proj, gain, xbc, decays, marks)


def conv_back(grad, extended, taps, marks, count):
    acc = conv_tile(extended, taps, marks, count)
    opened = sigmoid(acc)
    g_acc = grad * (opened + acc * opened * (1.0 - opened))
    width = g_acc.shape[1]
    weights, result = [], jnp.zeros((HALO + count, width), F32)
    for tap in range(KERNEL):
        marked = g_acc * marks[:, tap : tap + 1]
        weights.append(jnp.sum(marked * near_rows(extended, tap, count), axis=0, keepdims=True))
        spread = jnp.concatenate([jnp.zeros((HALO, width), F32), marked * taps[tap : tap + 1, :]], axis=0)
        back = REACH - tap
        result = result + (pltpu.roll(spread, HALO + count - back, 0) if back else spread)
    weights.append(jnp.sum(g_acc, axis=0, keepdims=True))
    weights.append(jnp.zeros((8 - KERNEL - 1, width), F32))
    return result, jnp.concatenate(weights, axis=0)


def mix_back_kernel(x, b, c, proj_x, proj_bc, halo, taps, y, g_y, decays, decays_t, raw, params, marks, labels, states, leaving, skip,
                    g_conv, g_rim, g_taps, g_raw, g_params,
                    wide_sums, wide_delta, wide_end, wide_skip, keep, near, c_t, state, g_near, g_b, g_c, g_cum, g_delta, g_skip, ends):
    j = pl.program_id(0)
    tokens = x.shape[0]
    blocks = tokens // BLOCK
    cols = pl.ds(pl.multiple_of(j * LANES, LANES), LANES)
    lane = lane_index((LANES, LANES))
    gather = ((lax.broadcasted_iota(jnp.int32, (LANES, LANES), 0) // HEAD + 2 * j) == lane).astype(BF16)

    def collect(values):
        high = values.astype(BF16)
        return dot(high, gather) + dot((values - high.astype(F32)).astype(BF16), gather)

    @pl.when(j == 0)
    def _():
        spread = spread_matrix()
        rows = lax.broadcasted_iota(jnp.int32, (BLOCK, BLOCK), 0)
        ordered = rows <= lane_index((BLOCK, BLOCK))
        for i in range(blocks):
            at = slice(i * BLOCK, (i + 1) * BLOCK)
            mark = marks[at]
            same = mark[:, 6:7] == labels[0:1, at]
            near[i] = jnp.where(ordered & same, dot_nt(b[at], c[at]), 0.0)
            c_t[i] = c[at].T
            weight, own = end_weights(decays[0, at], decays[1, at], mark)
            end_only = jnp.exp(decays[1, at][-1:, :] - decays[1, at]) * mark[:, 5:6]
            wide_end[at] = dot(end_only.astype(BF16), spread.astype(BF16)).astype(BF16)
            wide_sums[at] = dot(decays[1, at], spread, HIGHEST)
            wide_delta[at] = dot(decays[0, at].astype(BF16), spread.astype(BF16)).astype(BF16)
            keep[i] = dot(jnp.broadcast_to(own, (8, LANES)), spread, HIGHEST)
        for ref in (g_near, g_b, g_c, g_cum, g_delta, g_skip, ends):
            ref[...] = jnp.zeros_like(ref)

    state[...] = leaving[...].astype(F32)
    g_x = []
    for i in range(blocks - 1, -1, -1):
        at = slice(i * BLOCK, (i + 1) * BLOCK)
        tile = x[at].astype(F32)
        step = wide_delta[at, cols].astype(F32)
        scaled = tile * step
        low_scaled = scaled.astype(BF16)
        sums = wide_sums[at, cols]
        end = wide_end[at, cols].astype(F32)
        given = g_y[at]
        low_state = state[...].astype(BF16)
        ends[i] += collect(jnp.broadcast_to(jnp.sum(states[i + 1] * state[...], axis=0, keepdims=True), (8, LANES)))
        total = end * dot(b[at], low_state)
        for a, (part, grad) in enumerate(zip(halves(low_scaled), halves(given))):
            row = decays_t[i, pl.ds(2 * j + a, 1), :]
            decay = jnp.exp(jnp.minimum(row - pair_column(sums, a), 0.0))
            total = total + dot((near[i] * decay).astype(BF16), grad)
            g_near[i] += decay * dot_nt(part, given)
        given = given.astype(F32)
        entry = jnp.exp(sums) * marks[at, 4:5]
        reached = (given * entry).astype(BF16)
        g_b[at] += dot_nt((scaled * end).astype(BF16), low_state)
        g_c[at] += dot_nt(reached, states[i].astype(BF16))
        own_skip = skip[0:1, cols]
        g_cum[at] += collect(given * (y[at] - own_skip * tile) - scaled * total)
        g_delta[at] += collect(total * tile)
        g_skip[...] += collect(jnp.broadcast_to(jnp.sum(given * tile, axis=0, keepdims=True), (8, LANES)))
        g_x.append(step * total + own_skip * given)
        state[...] = keep[i, 0:1, cols] * state[...] + dot(c_t[i], reached)

    mark = marks[...]
    own = proj_x[...].astype(F32)
    extended = jnp.concatenate([halo[:, cols].astype(F32), own], axis=0)
    result, weights = conv_back(jnp.concatenate(g_x[::-1], axis=0), extended, taps[:, cols], mark, tokens)
    g_rim[:HALO, cols] = result[:HALO]
    g_rim[HALO:, cols] = result[tokens:]
    g_conv[:, cols] = result[HALO:].astype(BF16)
    g_taps[:, cols] = weights

    @pl.when(j == PAIRS - 1)
    def _():
        for i in range(blocks):
            at = slice(i * BLOCK, (i + 1) * BLOCK)
            rows = lax.broadcasted_iota(jnp.int32, (BLOCK, BLOCK), 0)
            seen = (rows <= lane_index((BLOCK, BLOCK))) & (marks[at, 6:7] == labels[0:1, at])
            grad = jnp.where(seen, g_near[i], 0.0)
            g_b[at] += dot(grad.astype(BF16), c[at])
            g_c[at] += dot(grad.T.astype(BF16), b[at])
        for k, ref in enumerate((g_b, g_c)):
            at = slice(INNER + k * NSTATE, INNER + (k + 1) * NSTATE)
            own = proj_bc[:, k * NSTATE : (k + 1) * NSTATE].astype(F32)
            extended = jnp.concatenate([halo[:, at].astype(F32), own], axis=0)
            result, weights = conv_back(ref[...], extended, taps[:, at], mark, tokens)
            g_rim[:HALO, at] = result[:HALO]
            g_rim[HALO:, at] = result[tokens:]
            g_conv[:, at] = result[HALO:].astype(BF16)
            g_taps[:, at] = weights
        rate = -jnp.exp(params[1:2, :])
        bias_sum = jnp.zeros((1, LANES), F32)
        rate_sum = jnp.zeros((1, LANES), F32)
        rows = lax.broadcasted_iota(jnp.int32, (BLOCK, BLOCK), 0)
        upper = (rows <= lane_index((BLOCK, BLOCK))).astype(F32)
        for i in range(blocks):
            at = slice(i * BLOCK, (i + 1) * BLOCK)
            g_decay = dot(upper, g_cum[at], HIGHEST) + ends[i, 0:1, :]
            delta = decays[0, at]
            full = g_delta[at] + g_decay * rate
            full = full * sigmoid(raw[at] + params[0:1, :])
            g_raw[at] = full.astype(BF16)
            bias_sum = bias_sum + jnp.sum(full, axis=0, keepdims=True)
            rate_sum = rate_sum + jnp.sum(g_decay * delta * rate, axis=0, keepdims=True)
        g_params[...] = jnp.concatenate([bias_sum, rate_sum, g_skip[0:1, :], jnp.zeros((5, LANES), F32)], axis=0)


def mix_back(xbc, proj, halo, taps, y, g_y, decays, decays_t, raw, params, marks, labels, states, leaving, skip):
    tokens = xbc.shape[0]
    blocks = tokens // BLOCK
    tile = pl.BlockSpec((tokens, LANES), lambda j: (0, j))
    acc = lambda *shape: pltpu.VMEM(shape, F32)
    return pl.pallas_call(
        mix_back_kernel,
        out_shape=(
            jax.ShapeDtypeStruct((tokens, CHANNELS), BF16),
            jax.ShapeDtypeStruct((2 * HALO, CHANNELS), F32),
            jax.ShapeDtypeStruct((8, CHANNELS), F32),
            jax.ShapeDtypeStruct((tokens, LANES), BF16),
            jax.ShapeDtypeStruct((8, LANES), F32),
        ),
        grid=(PAIRS,),
        in_specs=[
            tile,
            pl.BlockSpec((tokens, NSTATE), lambda j: (0, INNER // NSTATE)),
            pl.BlockSpec((tokens, NSTATE), lambda j: (0, INNER // NSTATE + 1)),
            pl.BlockSpec((tokens, LANES), lambda j: (0, PAIRS + j)),
            pl.BlockSpec((tokens, 2 * NSTATE), lambda j: (0, 2 * INNER // (2 * NSTATE))),
            whole(halo.shape), whole(taps.shape), tile, tile,
            whole(decays.shape), whole(decays_t.shape), whole(raw.shape), whole(params.shape), whole(marks.shape), whole(labels.shape),
            pl.BlockSpec((blocks + 1, NSTATE, LANES), lambda j: (0, 0, j)),
            pl.BlockSpec((NSTATE, LANES), lambda j: (0, j)),
            whole(skip.shape),
        ],
        out_specs=(
            whole((tokens, CHANNELS)), whole((2 * HALO, CHANNELS)), whole((8, CHANNELS)), whole((tokens, LANES)), whole((8, LANES)),
        ),
        scratch_shapes=[
            acc(tokens, INNER), pltpu.VMEM((tokens, INNER), BF16), pltpu.VMEM((tokens, INNER), BF16), acc(8, LANES),
            acc(blocks, 8, INNER), acc(blocks, BLOCK, BLOCK), pltpu.VMEM((blocks, NSTATE, BLOCK), BF16), acc(NSTATE, LANES),
            acc(blocks, BLOCK, BLOCK), acc(tokens, NSTATE), acc(tokens, NSTATE), acc(tokens, LANES), acc(tokens, LANES),
            acc(8, LANES), acc(blocks, 8, LANES),
        ],
        compiler_params=kernel_params(),
        name="mix_back",
    )(xbc, xbc, xbc, proj, proj, halo, taps, y, g_y, decays, decays_t, raw, params, marks, labels, states, leaving, skip)


QBLOCK = 256
GROUPS = HEADS // KV_HEADS
QPAIRS = QDIM // LANES
SCALE = 1.0 / math.sqrt(HEAD)


def swap_halves(values):
    half = HEAD // 2
    front = lane_index(values.shape) % HEAD < half
    width = values.shape[-1]
    return jnp.where(front, pltpu.roll(values, width - half, 1), pltpu.roll(values, half, 1))


def turn(values, cosine, sine):
    return values * cosine + swap_halves(values) * sine


def both_sides(tile, both):
    low = lane_index(tile.shape) < HEAD
    zero = jnp.zeros_like(tile)
    moved = pltpu.roll(tile.astype(F32), HEAD, 1).astype(tile.dtype)
    both[0, 0] = jnp.where(low, tile, zero)
    both[0, 1] = jnp.where(low, zero, moved)
    both[1, 0] = jnp.where(low, moved, zero)
    both[1, 1] = jnp.where(low, zero, tile)


def attend_kernel(q, kv, key_labels, marks, context, stats, keys, values):
    block, pair = pl.program_id(0), pl.program_id(1)
    window = DOC_MOST + QBLOCK
    start = pl.multiple_of(block * QBLOCK, QBLOCK)

    @pl.when((block == 0) & (pair == 0))
    def _():
        both_sides(kv[:, :KDIM], keys)
        both_sides(kv[:, KDIM:], values)

    group = pair // (GROUPS // 2)
    rows = lax.broadcasted_iota(jnp.int32, (QBLOCK, window), 0)
    cols = lane_index((QBLOCK, window))
    seen = (cols <= rows + DOC_MOST) & (marks[:, 6:7] == key_labels[0, 0:1, :])
    total = jnp.zeros((QBLOCK, LANES), F32)
    found = jnp.zeros((QBLOCK, LANES), F32)
    for a in range(2):
        scores = dot_nt(q[...], keys[group, a, pl.ds(start, window), :]) * SCALE
        scores = jnp.where(seen, scores, NEG_BIG)
        most = jnp.max(scores, axis=1, keepdims=True)
        probs = jnp.exp(scores - most)
        mass = jnp.sum(probs, axis=1, keepdims=True)
        probs = probs * (1.0 / mass)
        total = total + dot(probs.astype(BF16), values[group, a, pl.ds(start, window), :])
        found = jnp.where(lane_index(found.shape) == a, most + jnp.log(mass), found)
    context[...] = total.astype(BF16)
    stats[0] = found.T[0:8, :]


def attend(q, kv, key_labels, marks):
    tokens = q.shape[0]
    blocks = tokens // QBLOCK
    tile = pl.BlockSpec((QBLOCK, LANES), lambda i, p: (i, p))
    return pl.pallas_call(
        attend_kernel,
        out_shape=(jax.ShapeDtypeStruct((tokens, QDIM), BF16), jax.ShapeDtypeStruct((QPAIRS, 8, tokens), F32)),
        grid=(blocks, QPAIRS),
        in_specs=[
            tile, whole(kv.shape), pl.BlockSpec((1,) + key_labels.shape[1:], lambda i, p: (i, 0, 0)),
            pl.BlockSpec((QBLOCK, LANES), lambda i, p: (i, 0)),
        ],
        out_specs=(tile, pl.BlockSpec((1, 8, QBLOCK), lambda i, p: (p, 0, i))),
        scratch_shapes=[pltpu.VMEM((2, 2) + (kv.shape[0], LANES), BF16)] * 2,
        compiler_params=kernel_params(),
        name="attend",
    )(q, kv, key_labels, marks)


def attend_back_kernel(q, kv, given, key_marks, query_labels, stats, cosine, sine, g_q, g_kv, keys, values, g_key, g_value):
    block, pair = pl.program_id(0), pl.program_id(1)
    window = DOC_MOST + QBLOCK
    start = pl.multiple_of(block * QBLOCK, QBLOCK)

    @pl.when((block == 0) & (pair == 0))
    def _():
        both_sides(kv[:, :KDIM], keys)
        both_sides(kv[:, KDIM:], values)
        g_key[...] = jnp.zeros_like(g_key)
        g_value[...] = jnp.zeros_like(g_value)

    group = pair // (GROUPS // 2)
    rows = lax.broadcasted_iota(jnp.int32, (window, QBLOCK), 0)
    cols = lane_index((window, QBLOCK))
    seen = (rows <= cols + DOC_MOST) & (key_marks[0, :, 0:1] == query_labels[0:1, :])
    at = pl.ds(start, window)
    query, grad = q[...], given[...]
    total = jnp.zeros((QBLOCK, LANES), F32)
    for a, (query_part, grad_part) in enumerate(zip(halves(query), halves(grad))):
        key = keys[group, a, at, :]
        scores = jnp.where(seen, dot_nt(key, query) * SCALE, NEG_BIG)
        probs = jnp.exp(scores - stats[0, a : a + 1, :])
        g_probs = dot_nt(values[group, a, at, :], grad)
        mean = jnp.sum(probs * g_probs, axis=0, keepdims=True)
        g_scores = (probs * (g_probs - mean)).astype(BF16)
        g_key[group, at] += dot(g_scores, query_part) * SCALE
        g_value[group, at] += dot(probs.astype(BF16), grad_part)
        total = total + dot_tn(g_scores, key)
    g_q[...] = turn(total * SCALE, cosine[...], -sine[...]).astype(BF16)

    @pl.when((block == pl.num_programs(0) - 1) & (pair == QPAIRS - 1))
    def _():
        for k, ref in enumerate((g_key, g_value)):
            first = ref[0] + pltpu.roll(ref[0], HEAD, 1)
            second = ref[1] + pltpu.roll(ref[1], HEAD, 1)
            g_kv[:, k * KDIM : (k + 1) * KDIM] = jnp.where(lane_index(first.shape) < HEAD, first, second).astype(BF16)


def attend_back(q, kv, given, key_marks, query_labels, stats, cosine, sine):
    tokens = q.shape[0]
    blocks = tokens // QBLOCK
    tile = pl.BlockSpec((QBLOCK, LANES), lambda i, p: (i, p))
    row = pl.BlockSpec((QBLOCK, LANES), lambda i, p: (i, 0))
    return pl.pallas_call(
        attend_back_kernel,
        out_shape=(jax.ShapeDtypeStruct((tokens, QDIM), BF16), jax.ShapeDtypeStruct(kv.shape, BF16)),
        grid=(blocks, QPAIRS),
        in_specs=[
            tile, whole(kv.shape), pl.BlockSpec((QBLOCK, LANES), lambda i, p: (i, PAIRS + p)),
            pl.BlockSpec((1,) + key_marks.shape[1:], lambda i, p: (i, 0, 0)),
            pl.BlockSpec((8, QBLOCK), lambda i, p: (0, i)),
            pl.BlockSpec((1, 8, QBLOCK), lambda i, p: (p, 0, i)), row, row,
        ],
        out_specs=(tile, whole(kv.shape)),
        scratch_shapes=[pltpu.VMEM((2, 2) + (kv.shape[0], LANES), BF16)] * 2 + [pltpu.VMEM((2, kv.shape[0], LANES), F32)] * 2,
        compiler_params=kernel_params(),
        name="attend_back",
    )(q, kv, given, key_marks, query_labels, stats, cosine, sine)


def turn_back_kernel(g_kv, cosine, sine, out):
    out[:, :KDIM] = turn(g_kv[:, :KDIM], cosine[...], -sine[...]).astype(BF16)
    out[:, KDIM:] = g_kv[:, KDIM:].astype(BF16)


def turn_back(g_kv, cosine, sine):
    return pl.pallas_call(
        turn_back_kernel, out_shape=jax.ShapeDtypeStruct(g_kv.shape, BF16), compiler_params=kernel_params(), name="turn_back",
    )(g_kv, cosine, sine)


FF_TILE = 512


def feed_kernel(rows, scanned, context, given, gain, w_out, w_gate, w_up, w_down,
                normed, mixed, g_gate, g_up, result, g_hidden, low, g_gain, g_out, hidden, total, g_mid):
    j = pl.program_id(0)

    @pl.when(j == 0)
    def _():
        values = rows[...].astype(F32) + (dot(scanned[...], w_out[:INNER, :]) + dot(context[...], w_out[INNER:, :]))
        hidden[...] = values
        normed[...] = (values * rms_scale(values) * gain[0:1, :]).astype(BF16)

    gate = dot(normed[...], w_gate[...])
    upper = dot(normed[...], w_up[...])
    grad = dot_nt(given[...], w_down[...])
    opened = sigmoid(gate)
    swish = gate * opened
    product = (swish * upper).astype(BF16)
    left = (grad * upper * (opened + swish * (1.0 - opened))).astype(BF16)
    right = (grad * swish).astype(BF16)
    mixed[...] = product
    g_gate[...] = left
    g_up[...] = right
    forward = dot(product, w_down[...])
    backward = dot_nt(left, w_gate[...]) + dot_nt(right, w_up[...])

    @pl.when(j == 0)
    def _():
        total[...] = forward
        g_mid[...] = backward

    @pl.when(j > 0)
    def _():
        total[...] += forward
        g_mid[...] += backward

    @pl.when(j == pl.num_programs(0) - 1)
    def _():
        values = hidden[...]
        result[...] = (values + total[...]).astype(BF16)
        scale = rms_scale(values)
        unit = values * scale
        back = g_mid[...]
        scaled = back * gain[0:1, :]
        fresh = given[...].astype(F32) + scale * (scaled - unit * jnp.mean(scaled * unit, axis=1, keepdims=True))
        g_hidden[...] = fresh
        low[...] = fresh.astype(BF16)
        g_gain[...] = jnp.sum(back * unit, axis=0, keepdims=True)
        for at in range(0, g_out.shape[1], FF_TILE):
            g_out[:, at : at + FF_TILE] = dot_nt(low[...], w_out[at : at + FF_TILE, :]).astype(BF16)


def feed(inputs, scanned, context, given, gain, w_out, w_ff, w_down):
    tokens = inputs.shape[0]
    tiles = FF // FF_TILE
    rows = whole((tokens, D))
    once = lambda a: pl.BlockSpec(a.shape, lambda j: (0, 0), pipeline_mode=pl.Buffered(1))
    tile = pl.BlockSpec((tokens, FF_TILE), lambda j: (0, j))
    return pl.pallas_call(
        feed_kernel,
        out_shape=(
            jax.ShapeDtypeStruct((tokens, D), BF16),
            jax.ShapeDtypeStruct((tokens, FF), BF16), jax.ShapeDtypeStruct((tokens, FF), BF16), jax.ShapeDtypeStruct((tokens, FF), BF16),
            jax.ShapeDtypeStruct((tokens, D), BF16), jax.ShapeDtypeStruct((tokens, D), F32), jax.ShapeDtypeStruct((tokens, D), BF16),
            jax.ShapeDtypeStruct((1, D), F32), jax.ShapeDtypeStruct((tokens, INNER + QDIM), BF16),
        ),
        grid=(tiles,),
        in_specs=[
            once(inputs), once(scanned), once(context), once(given), once(gain), once(w_out),
            pl.BlockSpec((D, FF_TILE), lambda j: (0, j)), pl.BlockSpec((D, FF_TILE), lambda j: (0, tiles + j)),
            pl.BlockSpec((FF_TILE, D), lambda j: (j, 0)),
        ],
        out_specs=(rows, tile, tile, tile, rows, rows, rows, whole((1, D)), whole((tokens, INNER + QDIM))),
        scratch_shapes=[pltpu.VMEM((tokens, D), F32)] * 3,
        compiler_params=kernel_params(),
        name="feed",
    )(inputs, scanned, context, given, gain, w_out, w_ff, w_ff, w_down)


STEP_BLOCKS = 32
DEPTH = 4


def project_kernel(table, blocks, rows, gain, w_dt, cosine, sine, w_in, w_out, w_ff, w_down, proj, q_out, kv_out, normed, raw, halo,
                   held, wide, tall, s_first, s_put, s_in, s_out):
    across = held.shape[1] // BS
    down = held.shape[0] // BS

    def first(r):
        def one(i, _):
            cols = pl.ds(pl.multiple_of(i * BS, BS), BS)
            pltpu.make_async_copy(blocks.at[table[r * across + i]], held.at[pl.ds(r * BS, BS), cols], s_first.at[r]).start()
            return 0

        lax.fori_loop(0, across, one, 0)

    outs = []
    for ref in (w_out, w_ff, w_down):
        count, cols = ref.shape
        per_row = cols // BS
        deep = STEP_BLOCKS // per_row
        for r in range(count // (BS * deep)):
            outs.append((ref, r * BS * deep, deep, per_row))

    def target(step):
        ref, at, deep, per_row = outs[step]
        slot = step % DEPTH
        return (wide.at[slot] if deep == 1 else tall.at[slot]), ref.at[pl.ds(at, BS * deep)], per_row

    def fetch(step):
        buffer, _, per_row = target(step)

        def one(i, _):
            block_rows = pl.ds(pl.multiple_of(i // per_row * BS, BS), BS)
            cols = pl.ds(pl.multiple_of(i % per_row * BS, BS), BS)
            source = blocks.at[table[down * across + step * STEP_BLOCKS + i]]
            pltpu.make_async_copy(source, buffer.at[block_rows, cols], s_in.at[step % DEPTH]).start()
            return 0

        lax.fori_loop(0, STEP_BLOCKS, one, 0)

    def put(step):
        buffer, place_to, _ = target(step)
        return pltpu.make_async_copy(buffer, place_to, s_out.at[step % DEPTH])

    steps = len(outs)

    def advance(step):
        buffer, place_to, _ = target(step)
        pltpu.make_async_copy(place_to, buffer, s_in.at[step % DEPTH]).wait()
        put(step).start()
        ahead = step + DEPTH - 1
        if ahead < steps:
            if step >= 1:
                put(step - 1).wait()
            fetch(ahead)

    for r in range(down):
        first(r)
    for step in range(min(DEPTH - 1, steps)):
        fetch(step)
    values = rows[...].astype(F32)
    low = (values * rms_scale(values) * gain[0:1, :]).astype(BF16)
    normed[...] = low
    raw[...] = dot(low, w_dt[...])
    for r in range(down):
        part = held.at[pl.ds(r * BS, BS)]
        pltpu.make_async_copy(part, part, s_first.at[r]).wait()
    whole_put = pltpu.make_async_copy(held, w_in, s_put.at[0])
    whole_put.start()
    cos, sin = cosine[...], sine[...]
    tokens = rows.shape[0]
    plain = proj.shape[1]
    cuts = [(at, min(512, plain - at)) for at in range(0, plain, 512)] + [(plain, QDIM), (plain + QDIM, 2 * KDIM)]
    done = 0
    for k, (at, width) in enumerate(cuts):
        value = dot(normed[...], held[:, at : at + width])
        if at < plain:
            proj[:, at : at + width] = value.astype(BF16)
        elif at == plain:
            for p in range(QPAIRS):
                lanes = slice(p * LANES, (p + 1) * LANES)
                q_out[:, lanes] = turn(value[:, lanes], cos, sin).astype(BF16)
        else:
            kv_out[:, :KDIM] = turn(value[:, :KDIM], cos, sin).astype(BF16)
            kv_out[:, KDIM:] = value[:, KDIM:].astype(BF16)
        goal = steps * (k + 1) // len(cuts)
        for step in range(done, goal):
            advance(step)
        done = goal
    halo[...] = proj[tokens - halo.shape[0] :, INNER:]
    for step in range(max(steps - DEPTH, 0), steps):
        put(step).wait()
    whole_put.wait()


def slots_in_order(block_of_slot, order):
    match = jnp.array(order, jnp.int32)[:, None] == block_of_slot[None, :]
    return jnp.sum(jnp.where(match, jnp.arange(block_of_slot.shape[0], dtype=jnp.int32)[None, :], 0), axis=1)


def values_of(block_of_slot, values):
    match = block_of_slot[:, None] == jnp.arange(len(values), dtype=jnp.int32)[None, :]
    return jnp.sum(jnp.where(match, jnp.array(values, jnp.int32)[None, :], 0), axis=1)


def grad_tables():
    lefts, rights = [], []
    left_base = right_base = 0
    for members, beside in ((WIDE_IN, True), (TALL_OUT, False), (WIDE_FF, True), (TALL_FF, False)):
        for m in members:
            rows, cols = SHAPES[m]
            for r in range(0, rows, BS):
                for q in range(0, cols, BS):
                    lefts.append((left_base + r) // BS)
                    rights.append((right_base + q) // BS)
            if beside:
                right_base += cols
            else:
                left_base += rows
        if beside:
            left_base += rows
        else:
            right_base += cols
    return lefts, rights


def project(blocks, table, rows, gain, w_dt, cosine, sine):
    tokens = rows.shape[0]
    total = sum(SHAPES[m][1] for m in WIDE_IN)
    plain = total - QDIM - 2 * KDIM
    shapes = [(D, total), (sum(SHAPES[m][0] for m in TALL_OUT), D), (D, 2 * FF), (FF, D)]
    results = [(tokens, plain), (tokens, QDIM), (tokens, 2 * KDIM), (tokens, D), (tokens, LANES), (HALO, CHANNELS)]
    kinds = [BF16, BF16, BF16, BF16, F32, BF16]
    hbm = pl.BlockSpec(memory_space=pl.ANY)
    vmem = pl.BlockSpec(memory_space=pltpu.VMEM)
    return pl.pallas_call(
        project_kernel,
        out_shape=tuple(jax.ShapeDtypeStruct(shape, BF16) for shape in shapes)
        + tuple(jax.ShapeDtypeStruct(shape, kind) for shape, kind in zip(results, kinds)),
        grid_spec=pltpu.PrefetchScalarGridSpec(
            num_scalar_prefetch=1, grid=(1,), in_specs=[hbm] + [vmem] * 5, out_specs=(hbm,) * 4 + (vmem,) * 6,
            scratch_shapes=[
                pltpu.VMEM((D, total), BF16),
                pltpu.VMEM((DEPTH, BS, STEP_BLOCKS * BS), BF16),
                pltpu.VMEM((DEPTH, STEP_BLOCKS // (D // BS) * BS, D), BF16),
                pltpu.SemaphoreType.DMA((D // BS,)), pltpu.SemaphoreType.DMA((1,)),
                pltpu.SemaphoreType.DMA((DEPTH,)), pltpu.SemaphoreType.DMA((DEPTH,)),
            ],
        ),
        compiler_params=kernel_params(),
        name="project",
    )(table, blocks, rows, gain, w_dt, cosine, sine)


SHAMPOO = 24


def shampoo_kernel(norm, total, master, left, right, left_root, right_root, grad, new_left, new_right, new_master, low):
    scale = 0.5 * norm * norm / BS
    for i in range(0, total.shape[0], 2):
        pair = (i, i + 1)
        rows = jnp.concatenate([total[k] for k in pair], axis=0)
        cols = jnp.concatenate([total[k] for k in pair], axis=1)
        outer = dot_nt(rows, rows) * scale
        inner = dot_tn(cols, cols) * scale
        moved = dot(rows, jnp.concatenate([right_root[k] for k in pair], axis=1).astype(BF16))
        moved = jnp.concatenate([moved[:BS, :BS], moved[BS:, BS:]], axis=1).astype(BF16)
        moved = dot(jnp.concatenate([left_root[k] for k in pair], axis=0).astype(BF16), moved) * (LR_MATRIX * norm)
        for k, at in zip(pair, (slice(0, BS), slice(BS, 2 * BS))):
            grad[k] = total[k].astype(F32) * norm
            new_left[k] = 0.5 * left[k] + outer[at, at]
            new_right[k] = 0.5 * right[k] + inner[at, at]
            fresh = master[k] - moved[at, at]
            new_master[k] = fresh
            low[k] = fresh.astype(BF16)


def shampoo(norm, total, master, left, right, left_root, right_root):
    slots = total.shape[0]
    each = math.gcd(slots, SHAMPOO)
    spec = pl.BlockSpec((each, BS, BS), lambda i: (i, 0, 0))
    full = jax.ShapeDtypeStruct(master.shape, F32)
    return pl.pallas_call(
        functools.partial(shampoo_kernel, norm),
        out_shape=(full, full, full, full, jax.ShapeDtypeStruct(master.shape, BF16)),
        grid=(slots // each,),
        in_specs=[spec] * 6,
        out_specs=(spec,) * 5,
        compiler_params=kernel_params(),
        name="shampoo",
    )(total, master, left, right, left_root, right_root)


def ungroup(values, micro):
    seq = lax.axis_size("seq")
    each = seq // micro
    here = lax.axis_index("seq")
    order = here // each
    stacked = jnp.stack(values)
    cut = stacked.reshape((len(values), micro, -1) + stacked.shape[2:])
    pieces = []
    for t in range(micro):
        pairs = [(((j + t) % micro) * each + j // micro, j) for j in range(seq)]
        pieces.append(lax.ppermute(lax.dynamic_index_in_dim(cut, (order - t) % micro, 1, False), "seq", pairs))
    results = []
    for m in range(micro):
        chosen = pieces[0]
        for t in range(1, micro):
            chosen = jnp.where((m - here) % micro == t, pieces[t], chosen)
        results.append(chosen)
    return [jnp.stack([chosen[k] for chosen in results]) for k in range(len(values))]


def along(value, steps, micro):
    seq = lax.axis_size("seq")
    each = seq // micro
    pairs = [(s, s + steps) for s in range(seq) if 0 <= s % each + steps < each]
    return lax.ppermute(value, "seq", pairs)


def pad_rows(*rows):
    width = rows[0].shape[-1]
    return jnp.concatenate([r.reshape(-1, width) for r in rows] + [jnp.zeros((8 - sum(r.size // width for r in rows), width), F32)], axis=0)


def shards(grid, tokens, cotangent, doc_ids, master_blocks, block_of_slot, left_stats, right_stats, left_roots, right_roots,
           vector_params, first_moment, second_moment, adam_step):
    micro, piece = tokens.shape[:2]
    seq = lax.axis_size("seq")
    each = seq // micro
    count = micro * piece
    here = lax.axis_index("seq")
    rank = here % each
    start = rank * count
    slots = master_blocks.shape[0]

    orders = all_orders()
    table = slots_in_order(block_of_slot, sum(orders, []))
    left_at, right_at = (values_of(block_of_slot, values) for values in grad_tables())
    gathered, rows, given, labels_all = gather_blocks(grid, master_blocks, tokens, cotangent, doc_ids)
    rows, given = rows.reshape(count, D), given.reshape(count, D)
    gain_in, gain_mid, gain_mix, conv_weight, conv_bias, dt_bias, a_log, skip, w_dt = unpack_vectors(vector_params)
    w_dt = jnp.pad(w_dt.reshape(D, HEADS_SSM), ((0, 0), (0, LANES - HEADS_SSM))).astype(BF16)
    taps = pad_rows(conv_weight.reshape(KERNEL, CHANNELS), conv_bias)
    lane_pad = lambda v: jnp.pad(v, (0, LANES - HEADS_SSM))
    params = pad_rows(lane_pad(dt_bias), lane_pad(a_log))
    wide_skip = jnp.repeat(skip, HEAD)[None]
    wide_gain = gain_mix[None]

    row = lax.dynamic_index_in_dim(labels_all, here // each, 1, False).reshape(-1)
    before = jnp.concatenate([jnp.full((DOC_MOST,), -1, jnp.int32), row])
    window = lax.dynamic_slice_in_dim(before, start, DOC_MOST + count)
    labels = window[DOC_MOST:]
    blocks = count // BLOCK
    columns = [(window[DOC_MOST - REACH + tap : DOC_MOST - REACH + tap + count] == labels).astype(F32) for tap in range(KERNEL)]
    by_block = labels.reshape(blocks, BLOCK)
    entries_at = window[DOC_MOST - 1 : DOC_MOST - 1 + count].reshape(blocks, BLOCK)[:, :1]
    columns.append((by_block == entries_at).astype(F32).reshape(-1))
    columns.append((by_block == by_block[:, -1:]).astype(F32).reshape(-1))
    columns.append(labels.astype(F32))
    marks = jnp.pad(jnp.stack(columns, axis=1), ((0, 0), (0, LANES - len(columns))))
    label_rows = jnp.broadcast_to(labels.astype(F32)[None], (8, count))
    far = jnp.stack([window[i : i + DOC_MOST + QBLOCK] for i in range(0, count, QBLOCK)]).astype(F32)
    key_labels = jnp.broadcast_to(far[:, None, :], (far.shape[0], 8, far.shape[1]))
    key_marks = jnp.broadcast_to(far[:, :, None], far.shape + (8,))
    first = jnp.sum((row[None, :] < labels[:, None]).astype(jnp.int32), axis=1)
    positions = (start + jnp.arange(count) - first).astype(F32)
    half = HEAD // 2
    frequency = jnp.exp(jnp.arange(half, dtype=F32) * (-2.0 * math.log(THETA) / HEAD))
    angles = positions[:, None] * jnp.tile(frequency, LANES // half)[None, :]
    cosine = jnp.cos(angles)
    sine = jnp.sin(angles) * jnp.where(jnp.arange(LANES) % HEAD < half, -1.0, 1.0).astype(F32)[None, :]

    inputs = rows.astype(F32)
    w_in, w_out, w_ff, w_down, proj, q, kv, normed_in, raw, halo = project(
        gathered.reshape(-1, BS, BS), table, rows, gain_in[None], w_dt, cosine, sine
    )
    halo = along(halo, 1, micro)
    xbc, decays, decays_t, state, factor = mix_first(proj, halo, taps, params, raw, marks)
    past = min(each - 1, -(-DOC_MOST // count))
    earlier = [along(kv, back, micro) for back in range(past, 0, -1)]
    if past * count < DOC_MOST:
        earlier.insert(0, jnp.zeros((DOC_MOST - past * count, kv.shape[1]), BF16))
    reach = jnp.concatenate(earlier + [kv], axis=0)[-(DOC_MOST + count) :]
    wide = lambda f: jnp.repeat(f[0, :HEADS_SSM], HEAD)[None]
    incoming = along(state, each - 1, micro).astype(F32) if each > 1 else jnp.zeros(state.shape, F32)
    for back in range(each - 2, 0, -1):
        incoming = along(state, back, micro).astype(F32) + wide(along(factor, back, micro)) * incoming
    y, normed_ssm, states = mix_second(xbc, proj, decays, decays_t, marks, label_rows, incoming, wide_skip, wide_gain)
    context, stats = attend(q, reach, key_labels, marks)
    def norm_back(grad, values, gain):
        scale = rms_scale(values)
        unit = values * scale
        scaled = grad * gain
        return scale * (scaled - unit * jnp.mean(scaled * unit, axis=1, keepdims=True)), jnp.sum(grad * unit, axis=0)

    normed_mid, mixed, g_gate, g_up, result, g_hidden, hidden_low, g_gain_mid, g_out = feed(
        rows, normed_ssm, context, given, gain_mid[None], w_out, w_ff, w_down
    )
    (layer_out,) = ungroup([result], micro)
    g_y, g_z, g_gain_mix, g_state = gate_back(g_out, y, proj, wide_gain, xbc, decays, marks)
    low_state = g_state.astype(BF16)
    leaving = along(low_state, 1 - each, micro).astype(F32) if each > 1 else jnp.zeros(state.shape, F32)
    for ahead in range(each - 2, 0, -1):
        leaving = along(low_state, -ahead, micro).astype(F32) + wide(along(factor, -ahead, micro)) * leaving
    g_q, g_reach = attend_back(q, reach, g_out, key_marks, label_rows, stats, cosine, sine)
    g_conv, g_rim, g_taps, g_raw, g_params = mix_back(
        xbc, proj, halo, taps, y, g_y, decays, decays_t, raw, params, marks, label_rows, states, leaving, wide_skip
    )
    g_kv = g_reach[-count:].astype(F32)
    for back in range(1, past + 1):
        low = max(0, DOC_MOST - back * count)
        part = g_reach[low : DOC_MOST - (back - 1) * count]
        moved = along(part, -back, micro).astype(F32)
        g_kv = g_kv + jnp.pad(moved, ((count - part.shape[0], 0), (0, 0)))
    g_kv = turn_back(g_kv, cosine, sine)
    rim = along(g_rim[:HALO], -1, micro)
    g_conv = lax.dynamic_update_slice(g_conv, (g_rim[HALO:] + rim).astype(BF16), (count - HALO, 0))
    g_in = jnp.concatenate([g_z, g_conv, g_q, g_kv], axis=1)
    g_values, g_gain_in = norm_back(dot_nt(g_in, w_in) + dot_nt(g_raw, w_dt), inputs, gain_in)
    (grad_tokens,) = ungroup([(g_values + g_hidden).astype(BF16)], micro)
    grad_tokens = grad_tokens.astype(F32)
    g_w_dt = dot_tn(normed_in, g_raw)

    parts = [g_gain_in, g_gain_mid[0], g_gain_mix[0], g_taps[:KERNEL].reshape(-1), g_taps[KERNEL]]
    parts += [g_params[i, :HEADS_SSM] for i in range(3)] + [g_w_dt[:, :HEADS_SSM].reshape(-1)]
    width = vector_params.shape[0]
    height = -(-width // (8 * LANES)) * 8
    vector = jnp.concatenate(parts + [jnp.zeros((height * LANES - width,), F32)]).reshape(height, LANES)
    total, vector = reduce_blocks(grid, slots, left_at, right_at, [normed_in, normed_ssm, context, normed_mid, mixed],
                                  [g_z, g_conv, g_q, g_kv, hidden_low, g_gate, g_up, given], vector)
    norm = 1.0 / math.sqrt(count * seq * lax.axis_size("dp"))
    updates = shampoo(norm, total, master_blocks, left_stats, right_stats, left_roots, right_roots)
    g_vector = vector.reshape(-1)[:width] * norm
    step = adam_step[0].astype(F32)
    new_first = BETA_ONE * first_moment + (1.0 - BETA_ONE) * g_vector
    new_second = BETA_TWO * second_moment + (1.0 - BETA_TWO) * g_vector * g_vector
    first_hat = new_first / (1.0 - jnp.power(BETA_ONE, step))
    second_hat = new_second / (1.0 - jnp.power(BETA_TWO, step))
    new_vector = vector_params - LR_VECTOR * first_hat / (jnp.sqrt(second_hat) + ADAM_EPS)
    return (layer_out, grad_tokens) + tuple(updates) + (g_vector, new_vector, new_first, new_second)


def solution(mesh):
    line, block, copied = P("dp", "seq", None), P("dp", None, None), P()
    return jax.shard_map(
        functools.partial(shards, grid_of(mesh)),
        mesh=mesh,
        in_specs=(line, line, P("dp", "seq"), block, copied, block, block, block, block, copied, copied, copied, copied),
        out_specs=(line, line) + (block,) * 5 + (copied,) * 4,
        check_vma=False,
    )
```

```python
import functools
import math

import jax
import jax.numpy as jnp
from jax import lax
from jax.experimental import pallas as pl
from jax.experimental.pallas import tpu as pltpu
from jax.sharding import PartitionSpec as P

D = 1024
HEADS_SSM = 24
HEAD = 64
NSTATE = 128
HEADS = 8
KV_HEADS = 2
FF = 2048
KERNEL = 4
BS = 128
DOC_MOST = 512
INNER = HEADS_SSM * HEAD
CHANNELS = INNER + 2 * NSTATE
REACH = KERNEL - 1
QDIM = HEADS * HEAD
KDIM = KV_HEADS * HEAD
LANES = 128
PAIRS = INNER // LANES

EPS = 1e-05
THETA = 100000000000.0
LR_MATRIX = 0.02
LR_VECTOR = 0.08
BETA_ONE = 0.9
BETA_TWO = 0.999
ADAM_EPS = 1e-08
NEG_BIG = -1e30
F32 = jnp.float32
BF16 = jnp.bfloat16
HIGHEST = lax.Precision.HIGHEST
VMEM_MOST = 60 << 20

SHAPES = (
    (D, INNER), (D, INNER), (D, 2 * NSTATE), (D, QDIM), (D, KDIM), (D, KDIM),
    (INNER, D), (QDIM, D), (D, FF), (D, FF), (FF, D),
)
WIDE_IN, TALL_OUT, WIDE_FF, TALL_FF = (0, 1, 2, 3, 4, 5), (6, 7), (8, 9), (10,)
SIZES = (D, D, INNER, KERNEL * CHANNELS, CHANNELS, HEADS_SSM, HEADS_SSM, HEADS_SSM, D * HEADS_SSM)


def block_offsets():
    starts, total = [], 0
    for rows, cols in SHAPES:
        starts.append(total)
        total += rows // BS * (cols // BS)
    return starts


def wide_order(members):
    starts = block_offsets()
    rows = SHAPES[members[0]][0] // BS
    return [starts[m] + r * (SHAPES[m][1] // BS) + q for r in range(rows) for m in members for q in range(SHAPES[m][1] // BS)]


def tall_order(members):
    starts = block_offsets()
    return [starts[m] + i for m in members for i in range(SHAPES[m][0] // BS * (SHAPES[m][1] // BS))]


def all_orders():
    return [wide_order(WIDE_IN), tall_order(TALL_OUT), wide_order(WIDE_FF), tall_order(TALL_FF)]


def unpack_vectors(flat):
    result, offset = [], 0
    for count in SIZES:
        result.append(flat[offset : offset + count])
        offset += count
    return result


def dot(left, right, precision=None):
    return jnp.dot(left, right, preferred_element_type=F32, precision=precision)


def dot_nt(left, right):
    return lax.dot_general(left, right, (((1,), (1,)), ((), ())), preferred_element_type=F32)


def dot_tn(left, right):
    return lax.dot_general(left, right, (((0,), (0,)), ((), ())), preferred_element_type=F32)


def sigmoid(v):
    return 1.0 / (1.0 + jnp.exp(-v))


def rms_scale(values):
    return lax.rsqrt(jnp.mean(values * values, axis=-1, keepdims=True) + EPS)


def kernel_params(**more):
    return pltpu.CompilerParams(vmem_limit_bytes=VMEM_MOST, **more)


def whole(shape):
    return pl.BlockSpec(shape, lambda *_: (0,) * len(shape))


MESH = pl.DeviceIdType.MESH
CORES = 2
PIECES = 3
APART = 5 / 16


def grid_of(mesh):
    try:
        wide = len({device.coords[0] for device in mesh.devices.flat})
    except AttributeError:
        wide = mesh.shape["seq"] // CORES
    return wide, mesh.shape["seq"] // CORES, mesh.shape["dp"] // wide


def parts_of(slots, tall):
    half = slots // CORES
    size = half // PIECES
    lone = round(size * APART) if tall == 2 and size >= 8 else 0
    return half, size, lone, size - lone


def place(grid):
    wide, tall, deep = grid
    dp, seq = lax.axis_index("dp"), lax.axis_index("seq")
    return dp % wide, seq // CORES, dp // wide, seq % CORES


def gather_kernel(grid, slots, master, tokens, cotangent, docs, out, rows, given, labels, wide_own, src, bounce,
                  sem_own, sem_load, sz, rz, sx, rx, sy, ry, sc, rc, s_rows, r_rows, s_docs, r_docs):
    wide, tall, deep = grid
    x, y, z, c = place(grid)
    half, size, lone, bulk = parts_of(slots, tall)
    me = z * wide + x
    seq = y * CORES + c
    base = c * half
    bulk_at = y * (size - bulk)
    lone_at = y * bulk
    other_at = (1 - y) * bulk if lone else 0
    mate = y * CORES + (1 - c)
    over = (tall - 1 - y) * CORES + c
    peers = tall * CORES
    micro = tokens.shape[0]
    each = peers // micro

    loads = []
    for k in range(CORES):
        part = pl.ds(((c + k) % CORES) * half, half)
        loads.append((part, pltpu.make_async_copy(master.at[part], wide_own.at[part], sem_load.at[k])))
        loads[-1][1].start()

    barrier = pltpu.get_barrier_semaphore()
    count = jnp.int32(0)
    for step_by, at, length in ((wide, z, deep), (1, x, wide)):
        for step in (1, -1):
            ok = (at + step >= 0) & (at + step < length)
            there = me + step * step_by

            @pl.when(ok)
            def _(there=there):
                pl.semaphore_signal(barrier, inc=1, device_id=(there, seq), device_id_type=MESH)

            count = count + ok.astype(jnp.int32)
    for k in range(1, peers):
        pl.semaphore_signal(barrier, inc=1, device_id=(me, (seq + k) % peers), device_id_type=MESH)
    pl.semaphore_wait(barrier, count + (peers - 1))
    both = ((0, 1), (1, -1))
    yes = jnp.bool_(True)

    def piece(shard, at, length):
        return out.at[shard, pl.ds(at, length)]

    def run(begin_it):
        def send(ok, source, target, send_sem, recv_sem, device):
            copy = pltpu.make_async_remote_copy(
                src_ref=source, dst_ref=target, send_sem=send_sem, recv_sem=recv_sem,
                device_id=device, device_id_type=MESH,
            )

            @pl.when(ok)
            def _():
                if begin_it:
                    copy.start()
                else:
                    copy.wait_send()

        def arrived(ok, target, recv_sem):
            if begin_it:
                copy = pltpu.make_async_remote_copy(
                    src_ref=target, dst_ref=target, send_sem=sem_own.at[0], recv_sem=recv_sem,
                    device_id=(me, seq), device_id_type=MESH,
                )

                @pl.when(ok)
                def _():
                    copy.wait_recv()

        def pass_on(ok, shard, sub):
            at = base + sub * size
            mine = piece(shard, at + bulk_at, bulk)
            send(ok, mine, mine, sc.at[0, shard, sub], rc.at[0, shard, sub], (me, mate))
            if lone:
                mine = piece(shard, at + lone_at, lone)
                send(ok, mine, mine, sy.at[shard, sub], ry.at[shard, sub], (me, over))

        def along_x(ok, zs, dirs, hop, sub, own):
            for d, step in dirs:
                shard = zs * wide + x - step * hop
                go = ok & (x + step >= 0) & (x + step < wide)
                at = base + sub * size + bulk_at
                source = src.at[pl.ds(at, bulk)] if own else piece(shard, at, bulk)
                send(go, source, piece(shard, at, bulk), sx.at[d, hop, zs, sub], rx.at[d, hop + 1, zs, sub], (me + step, seq))

        def columns(s):
            return [(yes, z)] if s == 0 else [((z - step * s >= 0) & (z - step * s < deep), z - step * s) for _, step in both]

        def x_in(s, hop, sub):
            for ok, zs in columns(s):
                for d, step in both:
                    from_x = x - step * hop
                    come = ok & (from_x >= 0) & (from_x < wide)
                    shard = zs * wide + from_x
                    arrived(come, piece(shard, base + sub * size + bulk_at, bulk), rx.at[d, hop, zs, sub])
                    along_x(come, zs, ((d, step),), hop, sub, False)
                    pass_on(come, shard, sub)

        def y_in(ok, shard, sub):
            if lone:
                mine = piece(shard, base + sub * size + other_at, lone)
                arrived(ok, mine, ry.at[shard, sub])
                send(ok, mine, mine, sc.at[1, shard, sub], rc.at[1, shard, sub], (me, mate))

        def y_all(s, sub):
            for ok, zs in columns(s):
                if s > 0:
                    y_in(ok, zs * wide + x, sub)
                for hop in range(1, wide):
                    for _, step in both:
                        from_x = x - step * hop
                        y_in(ok & (from_x >= 0) & (from_x < wide), zs * wide + from_x, sub)

        def z_step(s, sub):
            for d, step in both:
                zs = z - step * s
                ok = (zs >= 0) & (zs < deep)
                shard = zs * wide + x
                at = base + sub * size + bulk_at
                mine = piece(shard, at, bulk)
                if s:
                    arrived(ok, mine, rz.at[d, s, sub])
                go = ok & (z + step >= 0) & (z + step < deep)
                source = mine if s else src.at[pl.ds(at, bulk)]
                if s + 1 < deep:
                    send(go, source, mine, sz.at[d, s, sub], rz.at[d, s + 1, sub], (me + step * wide, seq))
                if s:
                    along_x(ok, zs, both, 0, sub, False)
                    pass_on(ok, shard, sub)
            if s == 0:
                along_x(yes, z, both, 0, sub, True)

        for s in range(deep):
            def one(sub, _, s=s):
                z_step(s, sub)
                if s:
                    for hop in range(1, wide):
                        x_in(s - 1, hop, sub)
                if s >= 2:
                    y_all(s - 2, sub)
                return 0

            lax.fori_loop(0, PIECES, one, 0)
            if s == 0:
                local(begin_it, send, arrived)

        def last_x(sub, _):
            for hop in range(1, wide):
                x_in(deep - 1, hop, sub)
            if deep > 1:
                y_all(deep - 2, sub)
            return 0

        def last_y(sub, _):
            y_all(deep - 1, sub)
            return 0

        lax.fori_loop(0, PIECES, last_x, 0)
        lax.fori_loop(0, PIECES, last_y, 0)

    def convert(k):
        part, copy = loads[k]
        copy.wait()
        base_at = ((c + k) % CORES) * half

        def one(i, _):
            src[base_at + i] = wide_own[base_at + i].astype(src.dtype)
            return 0

        lax.fori_loop(0, half, one, 0, unroll=2)

    keep = pltpu.make_async_copy(src, out.at[me], sem_load.at[0])
    at_home = []
    for t in range(micro):
        m = (seq + t) % micro
        there = m * each + seq // micro
        for k, (source, target) in enumerate(((tokens, rows), (cotangent, given))):
            place_to = target.at[seq % micro]
            take = pltpu.make_async_copy(source.at[m], bounce.at[k], sem_own.at[k])
            put = pltpu.make_async_copy(bounce.at[k], place_to, sem_own.at[k])
            at_home.append((there == seq, take, put))

    def local(begin_it, send, arrived):
        for t in range(micro):
            m = (seq + t) % micro
            there = m * each + seq // micro
            for k, (source, target) in enumerate(((tokens, rows), (cotangent, given))):
                send(there != seq, source.at[m], target.at[seq % micro], s_rows.at[k, t], r_rows.at[k, seq % micro], (me, there))
        if begin_it:
            labels[seq] = docs[...]
        for k in range(1, peers):
            send(yes, docs, labels.at[seq], s_docs.at[k], r_docs.at[seq], (me, (seq + k) % peers))
        if begin_it:
            for ok, take, _ in at_home:
                @pl.when(ok)
                def _(take=take):
                    take.start()
            convert(1)
            keep.start()
            for ok, take, put in at_home:
                @pl.when(ok)
                def _(take=take, put=put):
                    take.wait()
                    put.start()

    convert(0)
    run(True)
    keep.wait()
    for ok, take, put in at_home:
        @pl.when(ok)
        def _(put=put):
            put.wait()

    def came(ok, target, recv_sem):
        @pl.when(ok)
        def _():
            pltpu.make_async_remote_copy(
                src_ref=target, dst_ref=target, send_sem=sem_own.at[0], recv_sem=recv_sem,
                device_id=(me, seq), device_id_type=MESH,
            ).wait_recv()

    for q in range(micro):
        source = seq % each * micro + q
        for k, target in enumerate((rows, given)):
            came(source != seq, target.at[q], r_rows.at[k, q])
    for k in range(1, peers):
        source = (seq + k) % peers
        came(yes, labels.at[source], r_docs.at[source])

    def last(i, _):
        shard, sub = i // PIECES, i % PIECES
        at = (1 - c) * half + sub * size
        came(shard != me, piece(shard, at + bulk_at, bulk), rc.at[0, shard, sub])
        if lone:
            came(shard != me, piece(shard, at + other_at, lone), rc.at[1, shard, sub])
        return 0

    lax.fori_loop(0, wide * deep * PIECES, last, 0)
    run(False)


def gather_blocks(grid, master, tokens, cotangent, docs):
    wide, tall, deep = grid
    slots = master.shape[0]
    n = wide * deep
    peers = tall * CORES
    micro = tokens.shape[0]
    low = tokens.dtype
    sem = pltpu.SemaphoreType.DMA
    hbm = pl.BlockSpec(memory_space=pl.ANY)
    vmem = pl.BlockSpec(memory_space=pltpu.VMEM)
    return pl.pallas_call(
        functools.partial(gather_kernel, grid, slots),
        out_shape=(
            jax.ShapeDtypeStruct((n,) + master.shape, low),
            jax.ShapeDtypeStruct(tokens.shape, low), jax.ShapeDtypeStruct(tokens.shape, low),
            jax.ShapeDtypeStruct((peers,) + docs.shape, docs.dtype),
        ),
        in_specs=[hbm, hbm, hbm, vmem],
        out_specs=(hbm, hbm, hbm, vmem),
        scratch_shapes=[
            pltpu.VMEM(master.shape, master.dtype), pltpu.VMEM(master.shape, low), pltpu.VMEM((2,) + tokens.shape[1:], low),
            sem((2,)), sem((CORES,)),
            sem((2, deep, PIECES)), sem((2, deep + 1, PIECES)),
            sem((2, wide, deep, PIECES)), sem((2, wide + 1, deep, PIECES)),
            sem((n, PIECES)), sem((n, PIECES)),
            sem((2, n, PIECES)), sem((2, n, PIECES)),
            sem((2, micro)), sem((2, micro)), sem((peers,)), sem((peers,)),
        ],
        compiler_params=pltpu.CompilerParams(collective_id=0, has_side_effects=True, vmem_limit_bytes=60 << 20),
        name="gather_blocks",
    )(master, tokens, cotangent, docs)

def far_first(at, size, i):
    above, below = size - 1 - at, at
    less, more = jnp.minimum(above, below), jnp.maximum(above, below)
    long_side = jnp.where(above >= below, 1, -1)
    j = i - (more - less)
    near = at + jnp.where(j % 2 == 0, 1, -1) * (less - j // 2)
    return jnp.where(j < 0, at + long_side * (more - i), near)


def entry(at, size, source_below, target):
    lower = jnp.where(at > 0, size - at, 0) if size > 2 else 0
    return target - at if source_below else lower + at - target


def entries(size):
    return size + 1 if size > 2 else 1

SUBS = 3
LONE = 5 / 16
RING = 6
STAGED = 3
LATE_ADD, LATE_X, LATE_Z, PER_HOP = 1, 3, 6, 3
CHUNK = 512
HELD = 12


def split_of(slots, tall):
    half = slots // CORES
    piece = half // SUBS
    lone = round(piece * LONE) if tall == 2 and piece >= 8 else 0
    return half, piece, lone, piece - lone


def reduce_kernel(grid, slots, widths, left_at, right_at, vec, *refs):
    wide, tall, deep = grid
    count = sum(len(w) for w in widths)
    arrays = refs[:count]
    (out, vec_out, turned, right, held, acc, stage, land_c, land_y, land_x, land_z, fin, vbuf, vland,
     s_left, s_right, s_c, r_c, s_y, r_y, s_x, r_x, s_z, r_z, s_f, r_f, s_m, r_m, s_v, r_v, free) = refs[count:]
    n = wide * deep
    x, y, z, c = place(grid)
    half, size, lone, bulk = split_of(slots, tall)
    me = z * wide + x
    seq = y * CORES + c
    mate = y * CORES + (1 - c)
    bulk_at = y * lone
    lone_at = y * bulk
    other_at = (1 - y) * bulk
    bits = lambda length: [1 << b for b in range(length.bit_length() - 1)]
    partners = [(me, mate)]
    partners += [(me, (y ^ b) * CORES + c) for b in bits(tall)]
    partners += [(z * wide + (x ^ b), seq) for b in bits(wide)]
    partners += [((z ^ b) * wide + x, seq) for b in bits(deep)]
    rounds = len(partners)

    chunks, k, at = [], 0, 0
    for width in widths[0]:
        for q in range(0, width, CHUNK):
            chunks.append((k, q, at + q))
        k, at = k + 1, at + width

    def chunk_copy(i):
        k, q, _ = chunks[i]
        return pltpu.make_async_copy(arrays[k].at[:, pl.ds(q, CHUNK)], held.at[i % HELD], s_left.at[i % HELD])

    ahead = min(HELD, len(chunks))
    for i in range(ahead):
        chunk_copy(i).start()
    copies, at = [], 0
    for width in widths[1]:
        def one(q, _, k=k, at=at):
            cols = pl.ds(pl.multiple_of(q * BS, BS), BS)
            pltpu.make_async_copy(arrays[k].at[:, cols], right.at[at + q], s_right.at[k - len(widths[0])]).start()
            return 0

        lax.fori_loop(0, width // BS, one, 0)
        part = right.at[pl.ds(at, width // BS)]
        copies.append(pltpu.make_async_copy(part, part, s_right.at[k - len(widths[0])]))
        k, at = k + 1, at + width // BS

    barrier = pltpu.get_barrier_semaphore()
    awaited = jnp.int32(0)
    for step_by, at, length in ((wide, z, deep), (1, x, wide)):
        for step in (1, -1):
            ok = (at + step >= 0) & (at + step < length)

            @pl.when(ok)
            def _(there=me + step * step_by):
                pl.semaphore_signal(barrier, inc=1, device_id=(there, seq), device_id_type=MESH)

            awaited = awaited + ok.astype(jnp.int32)
    for device in partners:
        pl.semaphore_signal(barrier, inc=1, device_id=device, device_id_type=MESH)
    pl.semaphore_wait(barrier, awaited + rounds)

    def remote(source, target, send_sem, recv_sem, device):
        return pltpu.make_async_remote_copy(
            src_ref=source, dst_ref=target, send_sem=send_sem, recv_sem=recv_sem,
            device_id=device, device_id_type=MESH,
        )

    def landed(target, recv_sem):
        remote(target, target, s_left.at[0], recv_sem, (me, seq)).wait_recv()

    def vec_copy(t):
        return remote(vbuf.at[t], vland.at[t], s_v.at[t], r_v.at[t], partners[t])

    vbuf[0] = vec[...]
    vec_copy(0).start()
    for i in range(len(chunks)):
        chunk_copy(i).wait()
        for q in range(0, CHUNK, BS):
            turned[(chunks[i][2] + q) // BS] = held[i % HELD, :, q : q + BS].T
        if i + HELD < len(chunks):
            chunk_copy(i + HELD).start()
    for copy in copies:
        copy.wait()

    group = wide * SUBS
    total = n * SUBS

    def item_of(k):
        xs = far_first(x, wide, k % wide)
        zs = far_first(z, deep, k // group)
        sub = (k // wide) % SUBS
        return xs, zs, sub, (zs * wide + xs) * SUBS + sub

    def swap(k):
        return remote(stage.at[k % STAGED], land_c.at[k % RING], s_c.at[k % STAGED], r_c.at[k % RING], (me, mate))

    def cross(item):
        return remote(acc.at[item, pl.ds(other_at, lone)], land_y.at[item], s_y.at[item], r_y.at[item], (me, (tall - 1 - y) * CORES + c))

    def grads(k, core, ref, first):
        xs, zs, sub, item = item_of(k)
        base = (zs * wide + xs) * slots + core * half + sub * size

        def one(i, _):
            ref[first, i] = dot(turned[left_at[base + i]], right[right_at[base + i]]).astype(ref.dtype)
            return 0

        lax.fori_loop(0, size, one, 0, unroll=min(4, size))

    def add(item, at, length, ref, first):
        def one(i, _):
            acc[item, at + i] = acc[item, at + i] + ref[first + (i,)]
            return 0

        lax.fori_loop(0, length, one, 0, unroll=min(3, length))

    def step_x(k, begin_it):
        xs, zs, sub, item = item_of(k)
        for below, step in ((True, 1), (False, -1)):
            to = entry(x + step, wide, below, xs)
            sent = remote(acc.at[item, pl.ds(bulk_at, bulk)], land_x.at[to, zs * SUBS + sub], s_x.at[item],
                          r_x.at[to, zs * SUBS + sub], (me + step, seq))

            @pl.when((xs - x) * step > 0)
            def _():
                if begin_it:
                    sent.start()
                else:
                    sent.wait_send()

    def take_x(k):
        xs, zs, sub, item = item_of(k)
        for below, step in ((True, 1), (False, -1)):
            comes = ((xs - x) * step >= 0) & (x - step >= 0) & (x - step < wide)
            at = entry(x, wide, below, xs)

            @pl.when(comes)
            def _():
                landed(land_x.at[at, zs * SUBS + sub], r_x.at[at, zs * SUBS + sub])
                add(item, bulk_at, bulk, land_x, (at, zs * SUBS + sub))

    def step_z(k, begin_it):
        xs, zs, sub, item = item_of(k)
        for below, step in ((True, 1), (False, -1)):
            to = entry(z + step, deep, below, zs)
            sent = remote(acc.at[item, pl.ds(bulk_at, bulk)], land_z.at[to, sub], s_z.at[zs * SUBS + sub], r_z.at[to, sub],
                          (me + step * wide, seq))

            @pl.when((zs - z) * step > 0)
            def _():
                if begin_it:
                    sent.start()
                else:
                    sent.wait_send()

    def take_z(k):
        xs, zs, sub, item = item_of(k)
        for below, step in ((True, 1), (False, -1)):
            comes = ((zs - z) * step >= 0) & (z - step >= 0) & (z - step < deep)
            at = entry(z, deep, below, zs)

            @pl.when(comes)
            def _():
                landed(land_z.at[at, sub], r_z.at[at, sub])
                add(item, bulk_at, bulk, land_z, (at, sub))

    planes = bits(tall)

    def swap_plane(t, sub):
        mine = pl.ds(bulk_at, bulk)
        return remote(acc.at[me * SUBS + sub, mine], fin.at[t, sub, mine], s_f.at[t, sub], r_f.at[t, sub], (me, (y ^ planes[t]) * CORES + c))

    def take_plane(t, sub):
        item = me * SUBS + sub
        theirs = pl.ds((1 - y) * lone if lone else 0, bulk)
        landed(fin.at[t, sub, theirs], r_f.at[t, sub])
        swap_plane(t, sub).wait_send()
        add(item, lone, size - 2 * lone, fin.at[t, sub, pl.ds(lone, size - 2 * lone)], ())
        if lone:
            cross(item).wait_send()
            acc[item, pl.ds(other_at, lone)] = fin[t, sub, pl.ds(other_at, lone)]

    def swap_core(sub):
        return remote(acc.at[me * SUBS + sub], out.at[pl.ds(c * half + sub * size, size)], s_m.at[sub], r_m.at[sub], (me, mate))

    late_z = LATE_Z + PER_HOP * jnp.minimum(z, deep - 1 - z)

    def turn_of(k, _):
        @pl.when(k < total)
        def _():
            @pl.when(k >= STAGED)
            def _():
                swap(k - STAGED).wait_send()

            grads(k, 1 - c, stage, k % STAGED)

            @pl.when(k >= RING)
            def _():
                pl.semaphore_wait(free, 1)

            swap(k).start()
            grads(k, c, acc, item_of(k)[3])

        for t in range(1, rounds + 1):
            @pl.when(k == t)
            def _(t=t):
                landed(vland.at[t - 1], r_v.at[t - 1])
                vbuf[t] = vbuf[t - 1] + vland[t - 1]
                if t < rounds:
                    vec_copy(t).start()
                else:
                    vec_out[...] = vbuf[t]

        b = k - LATE_ADD

        @pl.when((b >= 0) & (b < total))
        def _():
            item = item_of(b)[3]
            landed(land_c.at[b % RING], r_c.at[b % RING])
            add(item, 0, size, land_c, (b % RING,))

            @pl.when(b < total - RING)
            def _():
                pl.semaphore_signal(free, inc=1, device_id=(me, mate), device_id_type=MESH)

            if lone:
                cross(item).start()

        b = k - LATE_X

        @pl.when((b >= 0) & (b < total))
        def _():
            item = item_of(b)[3]
            if lone:
                landed(land_y.at[item], r_y.at[item])
                add(item, lone_at, lone, land_y, (item,))
            if wide > 2:
                @pl.when(item_of(b)[0] != x)
                def _():
                    take_x(b)
            step_x(b, True)

        b = k - late_z

        @pl.when((b >= 0) & (b < total) & (b % wide == wide - 1))
        def _():
            take_x(b)
            take_z(b)
            step_z(b, True)
            if planes:
                @pl.when(item_of(b)[1] == z)
                def _():
                    swap_plane(0, item_of(b)[2]).start()

        return 0

    lax.fori_loop(0, total + LATE_Z + PER_HOP * ((deep - 1) // 2), turn_of, 0)

    def finish(k, _):
        if lone:
            item = item_of(k)[3]

            @pl.when(item // SUBS != me)
            def _():
                cross(item).wait_send()

        step_x(k, False)

        @pl.when(k % wide == wide - 1)
        def _():
            step_z(k, False)

        return 0

    for t in range(len(planes)):
        for sub in range(SUBS):
            if t:
                swap_plane(t, sub).start()
        for sub in range(SUBS):
            take_plane(t, sub)
            if t == len(planes) - 1:
                swap_core(sub).start()
                out[pl.ds(c * half + sub * size, size)] = acc[me * SUBS + sub]
    lax.fori_loop(0, total, finish, 0)
    for k in range(max(total - STAGED, 0), total):
        swap(k).wait_send()
    for t in range(rounds):
        vec_copy(t).wait_send()
    for sub in range(SUBS):
        swap_core(sub).wait_send()
        landed(out.at[pl.ds((1 - c) * half + sub * size, size)], r_m.at[sub])


def reduce_blocks(grid, slots, left_at, right_at, lefts, rights, vec):
    wide, tall, deep = grid
    n = wide * deep
    half, size, lone, bulk = split_of(slots, tall)
    tile = (BS, BS)
    low = lefts[0].dtype
    tokens = lefts[0].shape[0]
    widths = [[a.shape[1] for a in lefts], [a.shape[1] for a in rights]]
    sem = pltpu.SemaphoreType.DMA
    rounds = sum(length.bit_length() - 1 for length in (CORES, wide, tall, deep))
    planes = max(tall.bit_length() - 1, 1)
    items = n * SUBS
    buf = lambda *lead: pltpu.VMEM(lead + tile, low)
    smem, vmem, hbm = (pl.BlockSpec(memory_space=m) for m in (pltpu.SMEM, pltpu.VMEM, pl.ANY))
    return pl.pallas_call(
        functools.partial(reduce_kernel, grid, slots, widths),
        out_shape=(jax.ShapeDtypeStruct((slots,) + tile, low), jax.ShapeDtypeStruct(vec.shape, vec.dtype)),
        in_specs=[smem, smem, vmem] + [hbm] * (len(lefts) + len(rights)),
        out_specs=(vmem, vmem),
        scratch_shapes=[
            pltpu.VMEM((sum(widths[0]) // BS, BS, tokens), low), pltpu.VMEM((sum(widths[1]) // BS, tokens, BS), low), pltpu.VMEM((HELD, tokens, CHUNK), low),
            buf(items, size), buf(STAGED, size), buf(RING, size), buf(items, max(lone, 1)), buf(entries(wide), deep * SUBS, bulk),
            buf(entries(deep), SUBS, bulk), buf(planes, SUBS, size),
            pltpu.VMEM((rounds + 1,) + vec.shape, vec.dtype), pltpu.VMEM((rounds,) + vec.shape, vec.dtype),
            sem((HELD,)), sem((len(rights),)), sem((STAGED,)), sem((RING,)), sem((items,)), sem((items,)), sem((items,)),
            sem((entries(wide), deep * SUBS)), sem((deep * SUBS,)), sem((entries(deep), SUBS)),
            sem((planes, SUBS)), sem((planes, SUBS)), sem((SUBS,)), sem((SUBS,)), sem((rounds,)), sem((rounds,)),
            pltpu.SemaphoreType.REGULAR,
        ],
        compiler_params=pltpu.CompilerParams(collective_id=1, has_side_effects=True, vmem_limit_bytes=63 << 20),
        name="reduce_blocks",
    )(left_at, right_at, vec, *lefts, *rights)


BLOCK = 256
HALO = 8


def lane_index(shape):
    return lax.broadcasted_iota(jnp.int32, shape, len(shape) - 1)


def conv_tile(extended, taps, marks, count):
    total = jnp.broadcast_to(taps[KERNEL : KERNEL + 1, :], (count, extended.shape[1]))
    for tap in range(KERNEL):
        total = total + taps[tap : tap + 1, :] * near_rows(extended, tap, count) * marks[:, tap : tap + 1]
    return total


def near_rows(extended, tap, count):
    back = REACH - tap
    moved = pltpu.roll(extended, back, 0) if back else extended
    return moved[HALO : HALO + count, :]


def softplus(v):
    return jnp.maximum(v, 0.0) + jnp.log(1.0 + jnp.exp(-jnp.abs(v)))


def chunk_decays(raw, params):
    delta = softplus(raw + params[0:1, :])
    decay = -delta * jnp.exp(params[1:2, :])
    block = raw.shape[0] if raw.shape[0] < BLOCK else BLOCK
    rows = lax.broadcasted_iota(jnp.int32, (block, block), 0)
    lower = (rows >= lane_index((block, block))).astype(F32)
    sums = [dot(lower, decay[i : i + block, :], HIGHEST) for i in range(0, raw.shape[0], block)]
    return delta, decay, jnp.concatenate(sums, axis=0)


def end_weights(delta, sums, marks):
    last = sums[-1:, :]
    return jnp.exp(last - sums) * delta * marks[:, 5:6], jnp.exp(last) * marks[-1:, 4:5]


def spread_matrix():
    rows = lax.broadcasted_iota(jnp.int32, (LANES, INNER), 0)
    return (rows == lane_index((LANES, INNER)) // HEAD).astype(F32)


def mix_first_kernel(proj_x, proj_bc, halo, taps, params, raw, marks, xbc, decays, decays_t, state, factor):
    tokens = raw.shape[0]
    mark = marks[...]
    for ref, at in ((proj_x, 0), (proj_bc, INNER)):
        step = 256
        for q in range(0, ref.shape[1], step):
            cols = slice(at + q, at + q + step)
            own = ref[:, q : q + step].astype(F32)
            extended = jnp.concatenate([halo[:, cols].astype(F32), own], axis=0)
            value = conv_tile(extended, taps[:, cols], mark, tokens)
            xbc[:, cols] = (value * sigmoid(value)).astype(BF16)
    delta, decay, sums = chunk_decays(raw[...], params[...])
    decays[0] = delta
    decays[1] = sums
    for i in range(tokens // BLOCK):
        decays_t[i] = sums[i * BLOCK : (i + 1) * BLOCK].T
    spread = spread_matrix()
    total = jnp.zeros((NSTATE, INNER), F32)
    product = jnp.ones((1, LANES), F32)
    for i in range(0, tokens, BLOCK):
        rows = slice(i, i + BLOCK)
        weight, own = end_weights(delta[rows], sums[rows], mark[rows])
        weighted = (xbc[rows, :INNER].astype(F32) * dot(weight.astype(BF16), spread.astype(BF16))).astype(BF16)
        keep = dot(jnp.broadcast_to(own, (8, LANES)), spread, HIGHEST)[0:1]
        total = keep * total + dot_tn(xbc[rows, INNER : INNER + NSTATE], weighted)
        product = product * own
    state[...] = total.astype(BF16)
    factor[...] = jnp.broadcast_to(product, factor.shape)


def mix_first(proj, halo, taps, params, raw, marks):
    tokens = raw.shape[0]
    vmem = pl.BlockSpec(memory_space=pltpu.VMEM)
    return pl.pallas_call(
        mix_first_kernel,
        out_shape=(
            jax.ShapeDtypeStruct((tokens, CHANNELS), BF16),
            jax.ShapeDtypeStruct((2, tokens, LANES), F32),
            jax.ShapeDtypeStruct((tokens // BLOCK, LANES, BLOCK), F32),
            jax.ShapeDtypeStruct((NSTATE, INNER), BF16),
            jax.ShapeDtypeStruct((8, LANES), F32),
        ),
        grid=(1,),
        in_specs=[
            pl.BlockSpec((tokens, INNER), lambda i: (0, 1)),
            pl.BlockSpec((tokens, 2 * NSTATE), lambda i: (0, 2 * INNER // (2 * NSTATE))),
            vmem, vmem, vmem, vmem, vmem,
        ],
        out_specs=(vmem,) * 5,
        compiler_params=kernel_params(),
        name="mix_first",
    )(proj, proj, halo, taps, params, raw, marks)


def attend(left, right, mark_rows, mark_cols):
    return jnp.where(mark_rows & mark_cols, dot_nt(left, right), 0.0)


def halves(tile):
    low = lane_index(tile.shape) < HEAD
    zero = jnp.zeros_like(tile)
    return jnp.where(low, tile, zero), jnp.where(low, zero, tile)


def pair_column(values, a):
    return values[:, a * HEAD : a * HEAD + 1]


def mix_second_kernel(x, b, c, z, decays, decays_t, marks, labels, incoming, skip, gain, y, normed, states,
                      wide_sums, wide_delta, wide_end, keep, near, b_t, state, gated, squares):
    j = pl.program_id(0)
    tokens = x.shape[0]
    blocks = tokens // BLOCK
    cols = pl.ds(pl.multiple_of(j * LANES, LANES), LANES)

    @pl.when(j == 0)
    def _():
        spread = spread_matrix()
        rows = lax.broadcasted_iota(jnp.int32, (BLOCK, BLOCK), 0)
        ordered = rows >= lane_index((BLOCK, BLOCK))
        for i in range(blocks):
            at = slice(i * BLOCK, (i + 1) * BLOCK)
            mark = marks[at]
            same = mark[:, 6:7] == labels[0:1, at]
            near[i] = jnp.where(ordered & same, dot_nt(c[at], b[at]), 0.0)
            b_t[i] = b[at].T
            weight, own = end_weights(decays[0, at], decays[1, at], mark)
            wide_end[at] = dot(weight.astype(BF16), spread.astype(BF16)).astype(BF16)
            wide_sums[at] = dot(decays[1, at], spread, HIGHEST)
            wide_delta[at] = dot(decays[0, at].astype(BF16), spread.astype(BF16)).astype(BF16)
            keep[i] = dot(jnp.broadcast_to(own, (8, LANES)), spread, HIGHEST)
        squares[...] = jnp.zeros_like(squares)

    state[...] = incoming[...].astype(F32)
    for i in range(blocks):
        at = slice(i * BLOCK, (i + 1) * BLOCK)
        states[i] = state[...]
        tile = x[at].astype(F32)
        scaled = (tile * wide_delta[at, cols].astype(F32)).astype(BF16)
        sums = wide_sums[at, cols]
        total = jnp.zeros((BLOCK, LANES), F32)
        for a, part in enumerate(halves(scaled)):
            row = decays_t[i, pl.ds(2 * j + a, 1), :]
            weight = near[i] * jnp.exp(jnp.minimum(pair_column(sums, a) - row, 0.0))
            total = total + dot(weight.astype(BF16), part)
        carried = dot(c[at], state[...].astype(BF16))
        total = total + carried * jnp.exp(sums) * marks[at, 4:5] + skip[0:1, cols] * tile
        y[at] = total
        gate = z[at].astype(F32)
        gate = total * gate * sigmoid(gate)
        gated[at, cols] = gate
        squares[at] += gate * gate
        weighted = (tile * wide_end[at, cols].astype(F32)).astype(BF16)
        state[...] = keep[i, 0:1, cols] * state[...] + dot(b_t[i], weighted)
    states[blocks] = state[...]

    @pl.when(j == PAIRS - 1)
    def _():
        for i in range(blocks):
            at = slice(i * BLOCK, (i + 1) * BLOCK)
            scale = lax.rsqrt(jnp.sum(squares[at], axis=1, keepdims=True) / INNER + EPS)
            normed[at] = (gated[at] * scale * gain[0:1, :]).astype(BF16)


def mix_second(xbc, proj, decays, decays_t, marks, labels, incoming, skip, gain):
    tokens = xbc.shape[0]
    blocks = tokens // BLOCK
    tile = pl.BlockSpec((tokens, LANES), lambda j: (0, j))
    return pl.pallas_call(
        mix_second_kernel,
        out_shape=(
            jax.ShapeDtypeStruct((tokens, INNER), F32),
            jax.ShapeDtypeStruct((tokens, INNER), BF16),
            jax.ShapeDtypeStruct((blocks + 1, NSTATE, INNER), F32),
        ),
        grid=(PAIRS,),
        in_specs=[
            tile,
            pl.BlockSpec((tokens, NSTATE), lambda j: (0, INNER // NSTATE)),
            pl.BlockSpec((tokens, NSTATE), lambda j: (0, INNER // NSTATE + 1)),
            tile,
            whole(decays.shape), whole(decays_t.shape), whole(marks.shape), whole(labels.shape),
            pl.BlockSpec((NSTATE, LANES), lambda j: (0, j)),
            whole(skip.shape), whole(gain.shape),
        ],
        out_specs=(tile, whole((tokens, INNER)), pl.BlockSpec((blocks + 1, NSTATE, LANES), lambda j: (0, 0, j))),
        scratch_shapes=[
            pltpu.VMEM((tokens, INNER), F32), pltpu.VMEM((tokens, INNER), BF16), pltpu.VMEM((tokens, INNER), BF16),
            pltpu.VMEM((blocks, 8, INNER), F32), pltpu.VMEM((blocks, BLOCK, BLOCK), F32),
            pltpu.VMEM((blocks, NSTATE, BLOCK), BF16), pltpu.VMEM((NSTATE, LANES), F32),
            pltpu.VMEM((tokens, INNER), F32), pltpu.VMEM((tokens, LANES), F32),
        ],
        compiler_params=kernel_params(),
        name="mix_second",
    )(xbc, xbc, xbc, proj, decays, decays_t, marks, labels, incoming, skip, gain)


def gate_back_kernel(grad, y, z, gain, c, decays, marks, g_y, g_z, g_gain, g_state):
    step = pl.program_id(0)
    value, gate = y[...], z[...].astype(F32)
    opened = sigmoid(gate)
    swish = gate * opened
    gated = value * swish
    scale = lax.rsqrt(jnp.mean(gated * gated, axis=1, keepdims=True) + EPS)
    unit = gated * scale
    given = grad[...].astype(F32)
    scaled = given * gain[0:1, :]
    g_gated = scale * (scaled - unit * jnp.mean(scaled * unit, axis=1, keepdims=True))
    fresh = g_gated * swish
    g_y[...] = fresh.astype(BF16)
    g_z[...] = (g_gated * value * (opened + swish * (1.0 - opened))).astype(BF16)
    spread = spread_matrix()
    sums = decays[1]
    mark = marks[...]
    entry_weight = jnp.exp(sums) * mark[:, 4:5]
    own = jnp.exp(sums[-1:, :]) * mark[-1:, 4:5]
    keep = dot(jnp.broadcast_to(own, (8, LANES)), spread, HIGHEST)[0:1]
    weighted = (fresh * dot(entry_weight.astype(BF16), spread.astype(BF16))).astype(BF16)
    local = dot_tn(c[...], weighted)
    gains = jnp.sum(given * unit, axis=0, keepdims=True)

    @pl.when(step == 0)
    def _():
        g_state[...] = local
        g_gain[...] = gains

    @pl.when(step > 0)
    def _():
        g_state[...] = keep * g_state[...] + local
        g_gain[...] += gains


def gate_back(grad, y, proj, gain, xbc, decays, marks):
    tokens = y.shape[0]
    blocks = tokens // BLOCK
    rows = lambda width, col: pl.BlockSpec((BLOCK, width), lambda i: (blocks - 1 - i, col))
    return pl.pallas_call(
        gate_back_kernel,
        out_shape=(
            jax.ShapeDtypeStruct((tokens, INNER), BF16),
            jax.ShapeDtypeStruct((tokens, INNER), BF16),
            jax.ShapeDtypeStruct((1, INNER), F32),
            jax.ShapeDtypeStruct((NSTATE, INNER), F32),
        ),
        grid=(blocks,),
        in_specs=[
            rows(INNER, 0), rows(INNER, 0), rows(INNER, 0), whole(gain.shape), rows(NSTATE, INNER // NSTATE + 1),
            pl.BlockSpec((2, BLOCK, LANES), lambda i: (0, blocks - 1 - i, 0)), rows(LANES, 0),
        ],
        out_specs=(rows(INNER, 0), rows(INNER, 0), whole((1, INNER)), whole((NSTATE, INNER))),
        compiler_params=kernel_params(),
        name="gate_back",
    )(grad, y, proj, gain, xbc, decays, marks)


def conv_back(grad, extended, taps, marks, count):
    acc = conv_tile(extended, taps, marks, count)
    opened = sigmoid(acc)
    g_acc = grad * (opened + acc * opened * (1.0 - opened))
    width = g_acc.shape[1]
    weights, result = [], jnp.zeros((HALO + count, width), F32)
    for tap in range(KERNEL):
        marked = g_acc * marks[:, tap : tap + 1]
        weights.append(jnp.sum(marked * near_rows(extended, tap, count), axis=0, keepdims=True))
        spread = jnp.concatenate([jnp.zeros((HALO, width), F32), marked * taps[tap : tap + 1, :]], axis=0)
        back = REACH - tap
        result = result + (pltpu.roll(spread, HALO + count - back, 0) if back else spread)
    weights.append(jnp.sum(g_acc, axis=0, keepdims=True))
    weights.append(jnp.zeros((8 - KERNEL - 1, width), F32))
    return result, jnp.concatenate(weights, axis=0)


def mix_back_kernel(x, b, c, proj_x, proj_bc, halo, taps, y, g_y, decays, decays_t, raw, params, marks, labels, states, leaving, skip,
                    g_conv, g_rim, g_taps, g_raw, g_params,
                    wide_sums, wide_delta, wide_end, wide_skip, keep, near, c_t, state, g_near, g_b, g_c, g_cum, g_delta, g_skip, ends):
    j = pl.program_id(0)
    tokens = x.shape[0]
    blocks = tokens // BLOCK
    cols = pl.ds(pl.multiple_of(j * LANES, LANES), LANES)
    lane = lane_index((LANES, LANES))
    gather = ((lax.broadcasted_iota(jnp.int32, (LANES, LANES), 0) // HEAD + 2 * j) == lane).astype(BF16)

    def collect(values):
        high = values.astype(BF16)
        return dot(high, gather) + dot((values - high.astype(F32)).astype(BF16), gather)

    @pl.when(j == 0)
    def _():
        spread = spread_matrix()
        rows = lax.broadcasted_iota(jnp.int32, (BLOCK, BLOCK), 0)
        ordered = rows <= lane_index((BLOCK, BLOCK))
        for i in range(blocks):
            at = slice(i * BLOCK, (i + 1) * BLOCK)
            mark = marks[at]
            same = mark[:, 6:7] == labels[0:1, at]
            near[i] = jnp.where(ordered & same, dot_nt(b[at], c[at]), 0.0)
            c_t[i] = c[at].T
            weight, own = end_weights(decays[0, at], decays[1, at], mark)
            end_only = jnp.exp(decays[1, at][-1:, :] - decays[1, at]) * mark[:, 5:6]
            wide_end[at] = dot(end_only.astype(BF16), spread.astype(BF16)).astype(BF16)
            wide_sums[at] = dot(decays[1, at], spread, HIGHEST)
            wide_delta[at] = dot(decays[0, at].astype(BF16), spread.astype(BF16)).astype(BF16)
            keep[i] = dot(jnp.broadcast_to(own, (8, LANES)), spread, HIGHEST)
        for ref in (g_near, g_b, g_c, g_cum, g_delta, g_skip, ends):
            ref[...] = jnp.zeros_like(ref)

    state[...] = leaving[...].astype(F32)
    g_x = []
    for i in range(blocks - 1, -1, -1):
        at = slice(i * BLOCK, (i + 1) * BLOCK)
        tile = x[at].astype(F32)
        step = wide_delta[at, cols].astype(F32)
        scaled = tile * step
        low_scaled = scaled.astype(BF16)
        sums = wide_sums[at, cols]
        end = wide_end[at, cols].astype(F32)
        given = g_y[at]
        low_state = state[...].astype(BF16)
        ends[i] += collect(jnp.broadcast_to(jnp.sum(states[i + 1] * state[...], axis=0, keepdims=True), (8, LANES)))
        total = end * dot(b[at], low_state)
        for a, (part, grad) in enumerate(zip(halves(low_scaled), halves(given))):
            row = decays_t[i, pl.ds(2 * j + a, 1), :]
            decay = jnp.exp(jnp.minimum(row - pair_column(sums, a), 0.0))
            total = total + dot((near[i] * decay).astype(BF16), grad)
            g_near[i] += decay * dot_nt(part, given)
        given = given.astype(F32)
        entry = jnp.exp(sums) * marks[at, 4:5]
        reached = (given * entry).astype(BF16)
        g_b[at] += dot_nt((scaled * end).astype(BF16), low_state)
        g_c[at] += dot_nt(reached, states[i].astype(BF16))
        own_skip = skip[0:1, cols]
        g_cum[at] += collect(given * (y[at] - own_skip * tile) - scaled * total)
        g_delta[at] += collect(total * tile)
        g_skip[...] += collect(jnp.broadcast_to(jnp.sum(given * tile, axis=0, keepdims=True), (8, LANES)))
        g_x.append(step * total + own_skip * given)
        state[...] = keep[i, 0:1, cols] * state[...] + dot(c_t[i], reached)

    mark = marks[...]
    own = proj_x[...].astype(F32)
    extended = jnp.concatenate([halo[:, cols].astype(F32), own], axis=0)
    result, weights = conv_back(jnp.concatenate(g_x[::-1], axis=0), extended, taps[:, cols], mark, tokens)
    g_rim[:HALO, cols] = result[:HALO]
    g_rim[HALO:, cols] = result[tokens:]
    g_conv[:, cols] = result[HALO:].astype(BF16)
    g_taps[:, cols] = weights

    @pl.when(j == PAIRS - 1)
    def _():
        for i in range(blocks):
            at = slice(i * BLOCK, (i + 1) * BLOCK)
            rows = lax.broadcasted_iota(jnp.int32, (BLOCK, BLOCK), 0)
            seen = (rows <= lane_index((BLOCK, BLOCK))) & (marks[at, 6:7] == labels[0:1, at])
            grad = jnp.where(seen, g_near[i], 0.0)
            g_b[at] += dot(grad.astype(BF16), c[at])
            g_c[at] += dot(grad.T.astype(BF16), b[at])
        for k, ref in enumerate((g_b, g_c)):
            at = slice(INNER + k * NSTATE, INNER + (k + 1) * NSTATE)
            own = proj_bc[:, k * NSTATE : (k + 1) * NSTATE].astype(F32)
            extended = jnp.concatenate([halo[:, at].astype(F32), own], axis=0)
            result, weights = conv_back(ref[...], extended, taps[:, at], mark, tokens)
            g_rim[:HALO, at] = result[:HALO]
            g_rim[HALO:, at] = result[tokens:]
            g_conv[:, at] = result[HALO:].astype(BF16)
            g_taps[:, at] = weights
        rate = -jnp.exp(params[1:2, :])
        bias_sum = jnp.zeros((1, LANES), F32)
        rate_sum = jnp.zeros((1, LANES), F32)
        rows = lax.broadcasted_iota(jnp.int32, (BLOCK, BLOCK), 0)
        upper = (rows <= lane_index((BLOCK, BLOCK))).astype(F32)
        for i in range(blocks):
            at = slice(i * BLOCK, (i + 1) * BLOCK)
            g_decay = dot(upper, g_cum[at], HIGHEST) + ends[i, 0:1, :]
            delta = decays[0, at]
            full = g_delta[at] + g_decay * rate
            full = full * sigmoid(raw[at] + params[0:1, :])
            g_raw[at] = full.astype(BF16)
            bias_sum = bias_sum + jnp.sum(full, axis=0, keepdims=True)
            rate_sum = rate_sum + jnp.sum(g_decay * delta * rate, axis=0, keepdims=True)
        g_params[...] = jnp.concatenate([bias_sum, rate_sum, g_skip[0:1, :], jnp.zeros((5, LANES), F32)], axis=0)


def mix_back(xbc, proj, halo, taps, y, g_y, decays, decays_t, raw, params, marks, labels, states, leaving, skip):
    tokens = xbc.shape[0]
    blocks = tokens // BLOCK
    tile = pl.BlockSpec((tokens, LANES), lambda j: (0, j))
    acc = lambda *shape: pltpu.VMEM(shape, F32)
    return pl.pallas_call(
        mix_back_kernel,
        out_shape=(
            jax.ShapeDtypeStruct((tokens, CHANNELS), BF16),
            jax.ShapeDtypeStruct((2 * HALO, CHANNELS), F32),
            jax.ShapeDtypeStruct((8, CHANNELS), F32),
            jax.ShapeDtypeStruct((tokens, LANES), BF16),
            jax.ShapeDtypeStruct((8, LANES), F32),
        ),
        grid=(PAIRS,),
        in_specs=[
            tile,
            pl.BlockSpec((tokens, NSTATE), lambda j: (0, INNER // NSTATE)),
            pl.BlockSpec((tokens, NSTATE), lambda j: (0, INNER // NSTATE + 1)),
            pl.BlockSpec((tokens, LANES), lambda j: (0, PAIRS + j)),
            pl.BlockSpec((tokens, 2 * NSTATE), lambda j: (0, 2 * INNER // (2 * NSTATE))),
            whole(halo.shape), whole(taps.shape), tile, tile,
            whole(decays.shape), whole(decays_t.shape), whole(raw.shape), whole(params.shape), whole(marks.shape), whole(labels.shape),
            pl.BlockSpec((blocks + 1, NSTATE, LANES), lambda j: (0, 0, j)),
            pl.BlockSpec((NSTATE, LANES), lambda j: (0, j)),
            whole(skip.shape),
        ],
        out_specs=(
            whole((tokens, CHANNELS)), whole((2 * HALO, CHANNELS)), whole((8, CHANNELS)), whole((tokens, LANES)), whole((8, LANES)),
        ),
        scratch_shapes=[
            acc(tokens, INNER), pltpu.VMEM((tokens, INNER), BF16), pltpu.VMEM((tokens, INNER), BF16), acc(8, LANES),
            acc(blocks, 8, INNER), acc(blocks, BLOCK, BLOCK), pltpu.VMEM((blocks, NSTATE, BLOCK), BF16), acc(NSTATE, LANES),
            acc(blocks, BLOCK, BLOCK), acc(tokens, NSTATE), acc(tokens, NSTATE), acc(tokens, LANES), acc(tokens, LANES),
            acc(8, LANES), acc(blocks, 8, LANES),
        ],
        compiler_params=kernel_params(),
        name="mix_back",
    )(xbc, xbc, xbc, proj, proj, halo, taps, y, g_y, decays, decays_t, raw, params, marks, labels, states, leaving, skip)


QBLOCK = 256
GROUPS = HEADS // KV_HEADS
QPAIRS = QDIM // LANES
SCALE = 1.0 / math.sqrt(HEAD)


def swap_halves(values):
    half = HEAD // 2
    front = lane_index(values.shape) % HEAD < half
    width = values.shape[-1]
    return jnp.where(front, pltpu.roll(values, width - half, 1), pltpu.roll(values, half, 1))


def turn(values, cosine, sine):
    return values * cosine + swap_halves(values) * sine


def both_sides(tile, both):
    low = lane_index(tile.shape) < HEAD
    zero = jnp.zeros_like(tile)
    moved = pltpu.roll(tile.astype(F32), HEAD, 1).astype(tile.dtype)
    both[0, 0] = jnp.where(low, tile, zero)
    both[0, 1] = jnp.where(low, zero, moved)
    both[1, 0] = jnp.where(low, moved, zero)
    both[1, 1] = jnp.where(low, zero, tile)


def attend_kernel(q, kv, key_labels, marks, context, stats, keys, values):
    block, pair = pl.program_id(0), pl.program_id(1)
    window = DOC_MOST + QBLOCK
    start = pl.multiple_of(block * QBLOCK, QBLOCK)

    @pl.when((block == 0) & (pair == 0))
    def _():
        both_sides(kv[:, :KDIM], keys)
        both_sides(kv[:, KDIM:], values)

    group = pair // (GROUPS // 2)
    rows = lax.broadcasted_iota(jnp.int32, (QBLOCK, window), 0)
    cols = lane_index((QBLOCK, window))
    seen = (cols <= rows + DOC_MOST) & (marks[:, 6:7] == key_labels[0, 0:1, :])
    total = jnp.zeros((QBLOCK, LANES), F32)
    found = jnp.zeros((QBLOCK, LANES), F32)
    for a in range(2):
        scores = dot_nt(q[...], keys[group, a, pl.ds(start, window), :]) * SCALE
        scores = jnp.where(seen, scores, NEG_BIG)
        most = jnp.max(scores, axis=1, keepdims=True)
        probs = jnp.exp(scores - most)
        mass = jnp.sum(probs, axis=1, keepdims=True)
        probs = probs * (1.0 / mass)
        total = total + dot(probs.astype(BF16), values[group, a, pl.ds(start, window), :])
        found = jnp.where(lane_index(found.shape) == a, most + jnp.log(mass), found)
    context[...] = total.astype(BF16)
    stats[0] = found.T[0:8, :]


def attend(q, kv, key_labels, marks):
    tokens = q.shape[0]
    blocks = tokens // QBLOCK
    tile = pl.BlockSpec((QBLOCK, LANES), lambda i, p: (i, p))
    return pl.pallas_call(
        attend_kernel,
        out_shape=(jax.ShapeDtypeStruct((tokens, QDIM), BF16), jax.ShapeDtypeStruct((QPAIRS, 8, tokens), F32)),
        grid=(blocks, QPAIRS),
        in_specs=[
            tile, whole(kv.shape), pl.BlockSpec((1,) + key_labels.shape[1:], lambda i, p: (i, 0, 0)),
            pl.BlockSpec((QBLOCK, LANES), lambda i, p: (i, 0)),
        ],
        out_specs=(tile, pl.BlockSpec((1, 8, QBLOCK), lambda i, p: (p, 0, i))),
        scratch_shapes=[pltpu.VMEM((2, 2) + (kv.shape[0], LANES), BF16)] * 2,
        compiler_params=kernel_params(),
        name="attend",
    )(q, kv, key_labels, marks)


def attend_back_kernel(q, kv, given, key_marks, query_labels, stats, cosine, sine, g_q, g_kv, keys, values, g_key, g_value):
    block, pair = pl.program_id(0), pl.program_id(1)
    window = DOC_MOST + QBLOCK
    start = pl.multiple_of(block * QBLOCK, QBLOCK)

    @pl.when((block == 0) & (pair == 0))
    def _():
        both_sides(kv[:, :KDIM], keys)
        both_sides(kv[:, KDIM:], values)
        g_key[...] = jnp.zeros_like(g_key)
        g_value[...] = jnp.zeros_like(g_value)

    group = pair // (GROUPS // 2)
    rows = lax.broadcasted_iota(jnp.int32, (window, QBLOCK), 0)
    cols = lane_index((window, QBLOCK))
    seen = (rows <= cols + DOC_MOST) & (key_marks[0, :, 0:1] == query_labels[0:1, :])
    at = pl.ds(start, window)
    query, grad = q[...], given[...]
    total = jnp.zeros((QBLOCK, LANES), F32)
    for a, (query_part, grad_part) in enumerate(zip(halves(query), halves(grad))):
        key = keys[group, a, at, :]
        scores = jnp.where(seen, dot_nt(key, query) * SCALE, NEG_BIG)
        probs = jnp.exp(scores - stats[0, a : a + 1, :])
        g_probs = dot_nt(values[group, a, at, :], grad)
        mean = jnp.sum(probs * g_probs, axis=0, keepdims=True)
        g_scores = (probs * (g_probs - mean)).astype(BF16)
        g_key[group, at] += dot(g_scores, query_part) * SCALE
        g_value[group, at] += dot(probs.astype(BF16), grad_part)
        total = total + dot_tn(g_scores, key)
    g_q[...] = turn(total * SCALE, cosine[...], -sine[...]).astype(BF16)

    @pl.when((block == pl.num_programs(0) - 1) & (pair == QPAIRS - 1))
    def _():
        for k, ref in enumerate((g_key, g_value)):
            first = ref[0] + pltpu.roll(ref[0], HEAD, 1)
            second = ref[1] + pltpu.roll(ref[1], HEAD, 1)
            g_kv[:, k * KDIM : (k + 1) * KDIM] = jnp.where(lane_index(first.shape) < HEAD, first, second).astype(BF16)


def attend_back(q, kv, given, key_marks, query_labels, stats, cosine, sine):
    tokens = q.shape[0]
    blocks = tokens // QBLOCK
    tile = pl.BlockSpec((QBLOCK, LANES), lambda i, p: (i, p))
    row = pl.BlockSpec((QBLOCK, LANES), lambda i, p: (i, 0))
    return pl.pallas_call(
        attend_back_kernel,
        out_shape=(jax.ShapeDtypeStruct((tokens, QDIM), BF16), jax.ShapeDtypeStruct(kv.shape, BF16)),
        grid=(blocks, QPAIRS),
        in_specs=[
            tile, whole(kv.shape), pl.BlockSpec((QBLOCK, LANES), lambda i, p: (i, PAIRS + p)),
            pl.BlockSpec((1,) + key_marks.shape[1:], lambda i, p: (i, 0, 0)),
            pl.BlockSpec((8, QBLOCK), lambda i, p: (0, i)),
            pl.BlockSpec((1, 8, QBLOCK), lambda i, p: (p, 0, i)), row, row,
        ],
        out_specs=(tile, whole(kv.shape)),
        scratch_shapes=[pltpu.VMEM((2, 2) + (kv.shape[0], LANES), BF16)] * 2 + [pltpu.VMEM((2, kv.shape[0], LANES), F32)] * 2,
        compiler_params=kernel_params(),
        name="attend_back",
    )(q, kv, given, key_marks, query_labels, stats, cosine, sine)


def turn_back_kernel(g_kv, cosine, sine, out):
    out[:, :KDIM] = turn(g_kv[:, :KDIM], cosine[...], -sine[...]).astype(BF16)
    out[:, KDIM:] = g_kv[:, KDIM:].astype(BF16)


def turn_back(g_kv, cosine, sine):
    return pl.pallas_call(
        turn_back_kernel, out_shape=jax.ShapeDtypeStruct(g_kv.shape, BF16), compiler_params=kernel_params(), name="turn_back",
    )(g_kv, cosine, sine)


FF_TILE = 1024


def feed_kernel(rows, scanned, context, given, gain, w_out, w_gate, w_up, w_down,
                normed, mixed, g_gate, g_up, result, g_hidden, low, g_gain, g_out, hidden, total, g_mid):
    j = pl.program_id(0)

    @pl.when(j == 0)
    def _():
        values = rows[...].astype(F32) + (dot(scanned[...], w_out[:INNER, :]) + dot(context[...], w_out[INNER:, :]))
        hidden[...] = values
        normed[...] = (values * rms_scale(values) * gain[0:1, :]).astype(BF16)

    gate = dot(normed[...], w_gate[...])
    upper = dot(normed[...], w_up[...])
    grad = dot_nt(given[...], w_down[...])
    opened = sigmoid(gate)
    swish = gate * opened
    product = (swish * upper).astype(BF16)
    left = (grad * upper * (opened + swish * (1.0 - opened))).astype(BF16)
    right = (grad * swish).astype(BF16)
    mixed[...] = product
    g_gate[...] = left
    g_up[...] = right
    forward = dot(product, w_down[...])
    backward = dot_nt(left, w_gate[...]) + dot_nt(right, w_up[...])

    @pl.when(j == 0)
    def _():
        total[...] = forward
        g_mid[...] = backward

    @pl.when(j > 0)
    def _():
        total[...] += forward
        g_mid[...] += backward

    @pl.when(j == pl.num_programs(0) - 1)
    def _():
        values = hidden[...]
        result[...] = (values + total[...]).astype(BF16)
        scale = rms_scale(values)
        unit = values * scale
        back = g_mid[...]
        scaled = back * gain[0:1, :]
        fresh = given[...].astype(F32) + scale * (scaled - unit * jnp.mean(scaled * unit, axis=1, keepdims=True))
        g_hidden[...] = fresh
        low[...] = fresh.astype(BF16)
        g_gain[...] = jnp.sum(back * unit, axis=0, keepdims=True)
        for at in range(0, g_out.shape[1], FF_TILE):
            g_out[:, at : at + FF_TILE] = dot_nt(low[...], w_out[at : at + FF_TILE, :]).astype(BF16)


def feed(inputs, scanned, context, given, gain, w_out, w_ff, w_down):
    tokens = inputs.shape[0]
    tiles = FF // FF_TILE
    rows = whole((tokens, D))
    once = lambda a: pl.BlockSpec(a.shape, lambda j: (0, 0), pipeline_mode=pl.Buffered(1))
    tile = pl.BlockSpec((tokens, FF_TILE), lambda j: (0, j))
    return pl.pallas_call(
        feed_kernel,
        out_shape=(
            jax.ShapeDtypeStruct((tokens, D), BF16),
            jax.ShapeDtypeStruct((tokens, FF), BF16), jax.ShapeDtypeStruct((tokens, FF), BF16), jax.ShapeDtypeStruct((tokens, FF), BF16),
            jax.ShapeDtypeStruct((tokens, D), BF16), jax.ShapeDtypeStruct((tokens, D), F32), jax.ShapeDtypeStruct((tokens, D), BF16),
            jax.ShapeDtypeStruct((1, D), F32), jax.ShapeDtypeStruct((tokens, INNER + QDIM), BF16),
        ),
        grid=(tiles,),
        in_specs=[
            once(inputs), once(scanned), once(context), once(given), once(gain), once(w_out),
            pl.BlockSpec((D, FF_TILE), lambda j: (0, j)), pl.BlockSpec((D, FF_TILE), lambda j: (0, tiles + j)),
            pl.BlockSpec((FF_TILE, D), lambda j: (j, 0)),
        ],
        out_specs=(rows, tile, tile, tile, rows, rows, rows, whole((1, D)), whole((tokens, INNER + QDIM))),
        scratch_shapes=[pltpu.VMEM((tokens, D), F32)] * 3,
        compiler_params=kernel_params(),
        name="feed",
    )(inputs, scanned, context, given, gain, w_out, w_ff, w_ff, w_down)


STEP_BLOCKS = 32
DEPTH = 4


def project_kernel(table, blocks, rows, gain, w_dt, cosine, sine, w_in, w_out, w_ff, w_down, proj, q_out, kv_out, normed, raw, halo,
                   held, wide, tall, s_first, s_put, s_in, s_out):
    across = held.shape[1] // BS
    down = held.shape[0] // BS

    def first(r):
        def one(i, _):
            cols = pl.ds(pl.multiple_of(i * BS, BS), BS)
            pltpu.make_async_copy(blocks.at[table[r * across + i]], held.at[pl.ds(r * BS, BS), cols], s_first.at[r]).start()
            return 0

        lax.fori_loop(0, across, one, 0)

    outs = []
    for ref in (w_out, w_ff, w_down):
        count, cols = ref.shape
        per_row = cols // BS
        deep = STEP_BLOCKS // per_row
        for r in range(count // (BS * deep)):
            outs.append((ref, r * BS * deep, deep, per_row))

    def target(step):
        ref, at, deep, per_row = outs[step]
        slot = step % DEPTH
        return (wide.at[slot] if deep == 1 else tall.at[slot]), ref.at[pl.ds(at, BS * deep)], per_row

    def fetch(step):
        buffer, _, per_row = target(step)

        def one(i, _):
            block_rows = pl.ds(pl.multiple_of(i // per_row * BS, BS), BS)
            cols = pl.ds(pl.multiple_of(i % per_row * BS, BS), BS)
            source = blocks.at[table[down * across + step * STEP_BLOCKS + i]]
            pltpu.make_async_copy(source, buffer.at[block_rows, cols], s_in.at[step % DEPTH]).start()
            return 0

        lax.fori_loop(0, STEP_BLOCKS, one, 0)

    def put(step):
        buffer, place_to, _ = target(step)
        return pltpu.make_async_copy(buffer, place_to, s_out.at[step % DEPTH])

    steps = len(outs)

    def advance(step):
        buffer, place_to, _ = target(step)
        pltpu.make_async_copy(place_to, buffer, s_in.at[step % DEPTH]).wait()
        put(step).start()
        ahead = step + DEPTH - 1
        if ahead < steps:
            if step >= 1:
                put(step - 1).wait()
            fetch(ahead)

    for r in range(down):
        first(r)
    for step in range(min(DEPTH - 1, steps)):
        fetch(step)
    values = rows[...].astype(F32)
    low = (values * rms_scale(values) * gain[0:1, :]).astype(BF16)
    normed[...] = low
    raw[...] = dot(low, w_dt[...])
    for r in range(down):
        part = held.at[pl.ds(r * BS, BS)]
        pltpu.make_async_copy(part, part, s_first.at[r]).wait()
    whole_put = pltpu.make_async_copy(held, w_in, s_put.at[0])
    whole_put.start()
    cos, sin = cosine[...], sine[...]
    tokens = rows.shape[0]
    plain = proj.shape[1]
    cuts = [(at, min(512, plain - at)) for at in range(0, plain, 512)] + [(plain, QDIM), (plain + QDIM, 2 * KDIM)]
    done = 0
    for k, (at, width) in enumerate(cuts):
        value = dot(normed[...], held[:, at : at + width])
        if at < plain:
            proj[:, at : at + width] = value.astype(BF16)
        elif at == plain:
            for p in range(QPAIRS):
                lanes = slice(p * LANES, (p + 1) * LANES)
                q_out[:, lanes] = turn(value[:, lanes], cos, sin).astype(BF16)
        else:
            kv_out[:, :KDIM] = turn(value[:, :KDIM], cos, sin).astype(BF16)
            kv_out[:, KDIM:] = value[:, KDIM:].astype(BF16)
        goal = steps * (k + 1) // len(cuts)
        for step in range(done, goal):
            advance(step)
        done = goal
    halo[...] = proj[tokens - halo.shape[0] :, INNER:]
    for step in range(max(steps - DEPTH, 0), steps):
        put(step).wait()
    whole_put.wait()


def slots_in_order(block_of_slot, order):
    match = jnp.array(order, jnp.int32)[:, None] == block_of_slot[None, :]
    return jnp.sum(jnp.where(match, jnp.arange(block_of_slot.shape[0], dtype=jnp.int32)[None, :], 0), axis=1)


def values_of(block_of_slot, values):
    match = block_of_slot[:, None] == jnp.arange(len(values), dtype=jnp.int32)[None, :]
    return jnp.sum(jnp.where(match, jnp.array(values, jnp.int32)[None, :], 0), axis=1)


def grad_tables():
    lefts, rights = [], []
    left_base = right_base = 0
    for members, beside in ((WIDE_IN, True), (TALL_OUT, False), (WIDE_FF, True), (TALL_FF, False)):
        for m in members:
            rows, cols = SHAPES[m]
            for r in range(0, rows, BS):
                for q in range(0, cols, BS):
                    lefts.append((left_base + r) // BS)
                    rights.append((right_base + q) // BS)
            if beside:
                right_base += cols
            else:
                left_base += rows
        if beside:
            left_base += rows
        else:
            right_base += cols
    return lefts, rights


def project(blocks, table, rows, gain, w_dt, cosine, sine):
    tokens = rows.shape[0]
    total = sum(SHAPES[m][1] for m in WIDE_IN)
    plain = total - QDIM - 2 * KDIM
    shapes = [(D, total), (sum(SHAPES[m][0] for m in TALL_OUT), D), (D, 2 * FF), (FF, D)]
    results = [(tokens, plain), (tokens, QDIM), (tokens, 2 * KDIM), (tokens, D), (tokens, LANES), (HALO, CHANNELS)]
    kinds = [BF16, BF16, BF16, BF16, F32, BF16]
    hbm = pl.BlockSpec(memory_space=pl.ANY)
    vmem = pl.BlockSpec(memory_space=pltpu.VMEM)
    return pl.pallas_call(
        project_kernel,
        out_shape=tuple(jax.ShapeDtypeStruct(shape, BF16) for shape in shapes)
        + tuple(jax.ShapeDtypeStruct(shape, kind) for shape, kind in zip(results, kinds)),
        grid_spec=pltpu.PrefetchScalarGridSpec(
            num_scalar_prefetch=1, grid=(1,), in_specs=[hbm] + [vmem] * 5, out_specs=(hbm,) * 4 + (vmem,) * 6,
            scratch_shapes=[
                pltpu.VMEM((D, total), BF16),
                pltpu.VMEM((DEPTH, BS, STEP_BLOCKS * BS), BF16),
                pltpu.VMEM((DEPTH, STEP_BLOCKS // (D // BS) * BS, D), BF16),
                pltpu.SemaphoreType.DMA((D // BS,)), pltpu.SemaphoreType.DMA((1,)),
                pltpu.SemaphoreType.DMA((DEPTH,)), pltpu.SemaphoreType.DMA((DEPTH,)),
            ],
        ),
        compiler_params=kernel_params(),
        name="project",
    )(table, blocks, rows, gain, w_dt, cosine, sine)


SHAMPOO = 24


def shampoo_kernel(norm, total, master, left, right, left_root, right_root, grad, new_left, new_right, new_master, low):
    scale = 0.5 * norm * norm / BS
    for i in range(0, total.shape[0], 2):
        pair = (i, i + 1)
        rows = jnp.concatenate([total[k] for k in pair], axis=0)
        cols = jnp.concatenate([total[k] for k in pair], axis=1)
        outer = dot_nt(rows, rows) * scale
        inner = dot_tn(cols, cols) * scale
        moved = dot(rows, jnp.concatenate([right_root[k] for k in pair], axis=1).astype(BF16))
        moved = jnp.concatenate([moved[:BS, :BS], moved[BS:, BS:]], axis=1).astype(BF16)
        moved = dot(jnp.concatenate([left_root[k] for k in pair], axis=0).astype(BF16), moved) * (LR_MATRIX * norm)
        for k, at in zip(pair, (slice(0, BS), slice(BS, 2 * BS))):
            grad[k] = total[k].astype(F32) * norm
            new_left[k] = 0.5 * left[k] + outer[at, at]
            new_right[k] = 0.5 * right[k] + inner[at, at]
            fresh = master[k] - moved[at, at]
            new_master[k] = fresh
            low[k] = fresh.astype(BF16)


def shampoo(norm, total, master, left, right, left_root, right_root):
    slots = total.shape[0]
    each = math.gcd(slots, SHAMPOO)
    spec = pl.BlockSpec((each, BS, BS), lambda i: (i, 0, 0))
    full = jax.ShapeDtypeStruct(master.shape, F32)
    return pl.pallas_call(
        functools.partial(shampoo_kernel, norm),
        out_shape=(full, full, full, full, jax.ShapeDtypeStruct(master.shape, BF16)),
        grid=(slots // each,),
        in_specs=[spec] * 6,
        out_specs=(spec,) * 5,
        compiler_params=kernel_params(),
        name="shampoo",
    )(total, master, left, right, left_root, right_root)


def ungroup(values, micro):
    seq = lax.axis_size("seq")
    each = seq // micro
    here = lax.axis_index("seq")
    order = here // each
    stacked = jnp.stack(values)
    cut = stacked.reshape((len(values), micro, -1) + stacked.shape[2:])
    pieces = []
    for t in range(micro):
        pairs = [(((j + t) % micro) * each + j // micro, j) for j in range(seq)]
        pieces.append(lax.ppermute(lax.dynamic_index_in_dim(cut, (order - t) % micro, 1, False), "seq", pairs))
    results = []
    for m in range(micro):
        chosen = pieces[0]
        for t in range(1, micro):
            chosen = jnp.where((m - here) % micro == t, pieces[t], chosen)
        results.append(chosen)
    return [jnp.stack([chosen[k] for chosen in results]) for k in range(len(values))]


def along(value, steps, micro):
    seq = lax.axis_size("seq")
    each = seq // micro
    pairs = [(s, s + steps) for s in range(seq) if 0 <= s % each + steps < each]
    return lax.ppermute(value, "seq", pairs)


def pad_rows(*rows):
    width = rows[0].shape[-1]
    return jnp.concatenate([r.reshape(-1, width) for r in rows] + [jnp.zeros((8 - sum(r.size // width for r in rows), width), F32)], axis=0)


def shards(grid, tokens, cotangent, doc_ids, master_blocks, block_of_slot, left_stats, right_stats, left_roots, right_roots,
           vector_params, first_moment, second_moment, adam_step):
    micro, piece = tokens.shape[:2]
    seq = lax.axis_size("seq")
    each = seq // micro
    count = micro * piece
    here = lax.axis_index("seq")
    rank = here % each
    start = rank * count
    slots = master_blocks.shape[0]

    orders = all_orders()
    table = slots_in_order(block_of_slot, sum(orders, []))
    left_at, right_at = (values_of(block_of_slot, values) for values in grad_tables())
    gathered, rows, given, labels_all = gather_blocks(grid, master_blocks, tokens, cotangent, doc_ids)
    rows, given = rows.reshape(count, D), given.reshape(count, D)
    gain_in, gain_mid, gain_mix, conv_weight, conv_bias, dt_bias, a_log, skip, w_dt = unpack_vectors(vector_params)
    w_dt = jnp.pad(w_dt.reshape(D, HEADS_SSM), ((0, 0), (0, LANES - HEADS_SSM))).astype(BF16)
    taps = pad_rows(conv_weight.reshape(KERNEL, CHANNELS), conv_bias)
    lane_pad = lambda v: jnp.pad(v, (0, LANES - HEADS_SSM))
    params = pad_rows(lane_pad(dt_bias), lane_pad(a_log))
    wide_skip = jnp.repeat(skip, HEAD)[None]
    wide_gain = gain_mix[None]

    row = lax.dynamic_index_in_dim(labels_all, here // each, 1, False).reshape(-1)
    before = jnp.concatenate([jnp.full((DOC_MOST,), -1, jnp.int32), row])
    window = lax.dynamic_slice_in_dim(before, start, DOC_MOST + count)
    labels = window[DOC_MOST:]
    blocks = count // BLOCK
    columns = [(window[DOC_MOST - REACH + tap : DOC_MOST - REACH + tap + count] == labels).astype(F32) for tap in range(KERNEL)]
    by_block = labels.reshape(blocks, BLOCK)
    entries_at = window[DOC_MOST - 1 : DOC_MOST - 1 + count].reshape(blocks, BLOCK)[:, :1]
    columns.append((by_block == entries_at).astype(F32).reshape(-1))
    columns.append((by_block == by_block[:, -1:]).astype(F32).reshape(-1))
    columns.append(labels.astype(F32))
    marks = jnp.pad(jnp.stack(columns, axis=1), ((0, 0), (0, LANES - len(columns))))
    label_rows = jnp.broadcast_to(labels.astype(F32)[None], (8, count))
    far = jnp.stack([window[i : i + DOC_MOST + QBLOCK] for i in range(0, count, QBLOCK)]).astype(F32)
    key_labels = jnp.broadcast_to(far[:, None, :], (far.shape[0], 8, far.shape[1]))
    key_marks = jnp.broadcast_to(far[:, :, None], far.shape + (8,))
    first = jnp.sum((row[None, :] < labels[:, None]).astype(jnp.int32), axis=1)
    positions = (start + jnp.arange(count) - first).astype(F32)
    half = HEAD // 2
    frequency = jnp.exp(jnp.arange(half, dtype=F32) * (-2.0 * math.log(THETA) / HEAD))
    angles = positions[:, None] * jnp.tile(frequency, LANES // half)[None, :]
    cosine = jnp.cos(angles)
    sine = jnp.sin(angles) * jnp.where(jnp.arange(LANES) % HEAD < half, -1.0, 1.0).astype(F32)[None, :]

    inputs = rows.astype(F32)
    w_in, w_out, w_ff, w_down, proj, q, kv, normed_in, raw, halo = project(
        gathered.reshape(-1, BS, BS), table, rows, gain_in[None], w_dt, cosine, sine
    )
    halo = along(halo, 1, micro)
    xbc, decays, decays_t, state, factor = mix_first(proj, halo, taps, params, raw, marks)
    past = min(each - 1, -(-DOC_MOST // count))
    earlier = [along(kv, back, micro) for back in range(past, 0, -1)]
    if past * count < DOC_MOST:
        earlier.insert(0, jnp.zeros((DOC_MOST - past * count, kv.shape[1]), BF16))
    reach = jnp.concatenate(earlier + [kv], axis=0)[-(DOC_MOST + count) :]
    wide = lambda f: jnp.repeat(f[0, :HEADS_SSM], HEAD)[None]
    incoming = along(state, each - 1, micro).astype(F32) if each > 1 else jnp.zeros(state.shape, F32)
    for back in range(each - 2, 0, -1):
        incoming = along(state, back, micro).astype(F32) + wide(along(factor, back, micro)) * incoming
    y, normed_ssm, states = mix_second(xbc, proj, decays, decays_t, marks, label_rows, incoming, wide_skip, wide_gain)
    context, stats = attend(q, reach, key_labels, marks)
    def norm_back(grad, values, gain):
        scale = rms_scale(values)
        unit = values * scale
        scaled = grad * gain
        return scale * (scaled - unit * jnp.mean(scaled * unit, axis=1, keepdims=True)), jnp.sum(grad * unit, axis=0)

    normed_mid, mixed, g_gate, g_up, result, g_hidden, hidden_low, g_gain_mid, g_out = feed(
        rows, normed_ssm, context, given, gain_mid[None], w_out, w_ff, w_down
    )
    (layer_out,) = ungroup([result], micro)
    g_y, g_z, g_gain_mix, g_state = gate_back(g_out, y, proj, wide_gain, xbc, decays, marks)
    low_state = g_state.astype(BF16)
    leaving = along(low_state, 1 - each, micro).astype(F32) if each > 1 else jnp.zeros(state.shape, F32)
    for ahead in range(each - 2, 0, -1):
        leaving = along(low_state, -ahead, micro).astype(F32) + wide(along(factor, -ahead, micro)) * leaving
    g_q, g_reach = attend_back(q, reach, g_out, key_marks, label_rows, stats, cosine, sine)
    g_conv, g_rim, g_taps, g_raw, g_params = mix_back(
        xbc, proj, halo, taps, y, g_y, decays, decays_t, raw, params, marks, label_rows, states, leaving, wide_skip
    )
    g_kv = g_reach[-count:].astype(F32)
    for back in range(1, past + 1):
        low = max(0, DOC_MOST - back * count)
        part = g_reach[low : DOC_MOST - (back - 1) * count]
        moved = along(part, -back, micro).astype(F32)
        g_kv = g_kv + jnp.pad(moved, ((count - part.shape[0], 0), (0, 0)))
    g_kv = turn_back(g_kv, cosine, sine)
    rim = along(g_rim[:HALO], -1, micro)
    g_conv = lax.dynamic_update_slice(g_conv, (g_rim[HALO:] + rim).astype(BF16), (count - HALO, 0))
    g_in = jnp.concatenate([g_z, g_conv, g_q, g_kv], axis=1)
    g_values, g_gain_in = norm_back(dot_nt(g_in, w_in) + dot_nt(g_raw, w_dt), inputs, gain_in)
    (grad_tokens,) = ungroup([(g_values + g_hidden).astype(BF16)], micro)
    grad_tokens = grad_tokens.astype(F32)
    g_w_dt = dot_tn(normed_in, g_raw)

    parts = [g_gain_in, g_gain_mid[0], g_gain_mix[0], g_taps[:KERNEL].reshape(-1), g_taps[KERNEL]]
    parts += [g_params[i, :HEADS_SSM] for i in range(3)] + [g_w_dt[:, :HEADS_SSM].reshape(-1)]
    width = vector_params.shape[0]
    height = -(-width // (8 * LANES)) * 8
    vector = jnp.concatenate(parts + [jnp.zeros((height * LANES - width,), F32)]).reshape(height, LANES)
    total, vector = reduce_blocks(grid, slots, left_at, right_at, [normed_in, normed_ssm, context, normed_mid, mixed],
                                  [g_z, g_conv, g_q, g_kv, hidden_low, g_gate, g_up, given], vector)
    norm = 1.0 / math.sqrt(count * seq * lax.axis_size("dp"))
    updates = shampoo(norm, total, master_blocks, left_stats, right_stats, left_roots, right_roots)
    g_vector = vector.reshape(-1)[:width] * norm
    step = adam_step[0].astype(F32)
    new_first = BETA_ONE * first_moment + (1.0 - BETA_ONE) * g_vector
    new_second = BETA_TWO * second_moment + (1.0 - BETA_TWO) * g_vector * g_vector
    first_hat = new_first / (1.0 - jnp.power(BETA_ONE, step))
    second_hat = new_second / (1.0 - jnp.power(BETA_TWO, step))
    new_vector = vector_params - LR_VECTOR * first_hat / (jnp.sqrt(second_hat) + ADAM_EPS)
    return (layer_out, grad_tokens) + tuple(updates) + (g_vector, new_vector, new_first, new_second)


def solution(mesh):
    line, block, copied = P("dp", "seq", None), P("dp", None, None), P()
    return jax.shard_map(
        functools.partial(shards, grid_of(mesh)),
        mesh=mesh,
        in_specs=(line, line, P("dp", "seq"), block, copied, block, block, block, block, copied, copied, copied, copied),
        out_specs=(line, line) + (block,) * 5 + (copied,) * 4,
        check_vma=False,
    )
```
